32 devices in a mesh: seq: 8 (over z, x), batch: 4 (over y, core).
Axes of the slice: x: 2, y: 2, z: 4, core: 2. Of those that a mesh axis runs over, the one named last changes fastest.
Arguments:
- tokens: bfloat16 [8, 1024, 768], P('batch', 'seq'), may hold values from -6 to 6
- cotangent: bfloat16 [8, 1024, 768], P('batch', 'seq'), may hold values from -6 to 6
- lengths: int32 [8], P('batch'), may hold values from 128 to 1024, as said below
- mixer_gain: bfloat16 [768], P(('seq', 'batch')), may hold values from 0.5 to 1.5
- mixer_inputs: bfloat16 [768, 2304], P(('seq', 'batch')), may hold values from -0.21875 to 0.21875
- shift_taps: bfloat16 [768, 4], P(('seq', 'batch')), may hold values from -3 to 3
- decay_rate: bfloat16 [768, 64], P(('seq', 'batch')), may hold values from 9.765625e-05 to 0.5
- state_in: bfloat16 [768, 64], P(('seq', 'batch')), may hold values from -3 to 3
- state_out: bfloat16 [768, 64], P(('seq', 'batch')), may hold values from -0.75 to 0.75
- state_skip: bfloat16 [768], P(('seq', 'batch')), may hold values from -4 to 4
- mixer_output: bfloat16 [768, 768], P(('seq', 'batch')), may hold values from -0.21875 to 0.21875
- first_gain: bfloat16 [768], P(('seq', 'batch')), may hold values from 0.5 to 1.5
- first_up: bfloat16 [768, 3072], P(('seq', 'batch')), may hold values from -0.21875 to 0.21875
- first_down: bfloat16 [3072, 768], P(('seq', 'batch')), may hold values from -0.109375 to 0.109375
- attend_gain: bfloat16 [768], P(('seq', 'batch')), may hold values from 0.5 to 1.5
- attend_inputs: bfloat16 [768, 2304], P(('seq', 'batch')), may hold values from -0.21875 to 0.21875
- attend_output: bfloat16 [768, 768], P(('seq', 'batch')), may hold values from -1.75 to 1.75
- second_gain: bfloat16 [768], P(('seq', 'batch')), may hold values from 0.5 to 1.5
- second_up: bfloat16 [768, 3072], P(('seq', 'batch')), may hold values from -0.21875 to 0.21875
- second_down: bfloat16 [3072, 768], P(('seq', 'batch')), may hold values from -0.109375 to 0.109375
Outputs:
- mixed: bfloat16 [8, 1024, 768], P('batch', 'seq')
- tokens_gradient: bfloat16 [8, 1024, 768], P('batch', 'seq')
- mixer_gain_gradient: float32 [768], P(('seq', 'batch'))
- mixer_inputs_gradient: float32 [768, 2304], P(('seq', 'batch'))
- shift_taps_gradient: float32 [768, 4], P(('seq', 'batch'))
- decay_rate_gradient: float32 [768, 64], P(('seq', 'batch'))
- state_in_gradient: float32 [768, 64], P(('seq', 'batch'))
- state_out_gradient: float32 [768, 64], P(('seq', 'batch'))
- state_skip_gradient: float32 [768], P(('seq', 'batch'))
- mixer_output_gradient: float32 [768, 768], P(('seq', 'batch'))
- first_gain_gradient: float32 [768], P(('seq', 'batch'))
- first_up_gradient: float32 [768, 3072], P(('seq', 'batch'))
- first_down_gradient: float32 [3072, 768], P(('seq', 'batch'))
- attend_gain_gradient: float32 [768], P(('seq', 'batch'))
- attend_inputs_gradient: float32 [768, 2304], P(('seq', 'batch'))
- attend_output_gradient: float32 [768, 768], P(('seq', 'batch'))
- second_gain_gradient: float32 [768], P(('seq', 'batch'))
- second_up_gradient: float32 [768, 3072], P(('seq', 'batch'))
- second_down_gradient: float32 [3072, 768], P(('seq', 'batch'))
The draws below stay inside these ranges and needn't reach their ends.
Inputs may be any that keep to these rules, and one draw needn't show every extreme that they name: `lengths`: both ends are reached in every draw.
All inputs are finite; a program needn't handle non-finite values.
Results may differ from the reference program's by a relative error of at most 0.03.
Values may be sent and summed in bfloat16 or wider, within the bound.
A program may use at most 640 MiB of HBM per device.

```python
import math
import jax
import jax.numpy as jnp
from jax import lax

D = 768
FF = 3072
HEADS = 12
HEAD_DIM = 64
STATE = 64
SHIFT = 4
SEQ_LEN = 1024
BATCH_SEQS = 8


def draw_lengths(key, part):
    first_key, second_key = jax.random.split(jax.random.fold_in(key, 11))
    drawn = jax.random.randint(first_key, (BATCH_SEQS,), SEQ_LEN // 8, SEQ_LEN + 1)
    order = jax.random.permutation(second_key, BATCH_SEQS)
    drawn = drawn.at[order[0]].set(SEQ_LEN)
    drawn = drawn.at[order[1]].set(SEQ_LEN // 8)
    return drawn.astype(jnp.int32)


def rate_table(key, bend):
    stratum_key, jitter_key = jax.random.split(jax.random.fold_in(key, 23))
    channel_keys = jax.random.split(stratum_key, D)
    strata = jax.vmap(lambda channel_key: jax.random.permutation(channel_key, STATE))(channel_keys)
    jitter = jax.random.uniform(jitter_key, (D, STATE), jnp.float32)
    position = (strata.astype(jnp.float32) + jitter) / STATE
    position = position ** bend
    low_end = math.log(1.05 / (10.0 * SEQ_LEN))
    high_end = math.log(0.49)
    return jnp.exp(low_end + (high_end - low_end) * position)


def draw_decay_rate(key, part):
    rates = rate_table(key, 1.0)
    return rates.astype(jnp.bfloat16)


def draw_state_in(key, part):
    factor_key = jax.random.fold_in(key, 37)
    rates = rate_table(key, 1.0)
    factor = jnp.clip(jax.random.normal(factor_key, (D, STATE), jnp.float32), -3.0, 3.0)
    return (factor * jnp.sqrt(2.0 * rates)).astype(jnp.bfloat16)


def block_scale(stream_key, shape, shards, smallest, largest):
    level = 1.0
    for dim, parts in shards:
        steps = jax.random.uniform(jax.random.fold_in(jax.random.fold_in(stream_key, 6), dim), (parts,), jnp.float32, smallest / len(shards), largest / len(shards))
        level = level * jnp.repeat(jnp.exp(steps), shape[dim] // parts).reshape((-1,) + (1,) * (len(shape) - 1 - dim))
    return level


def noise(key, dims, width, limit, cuts=(), kind=jnp.bfloat16):
    factor_of = block_scale(key, dims, cuts, -0.22, 0.18) if cuts else 1.0
    entries = jax.random.normal(key, dims, jnp.float32) * width * factor_of
    return jnp.minimum(jnp.maximum(entries, -limit), limit).astype(kind)


def setup_inputs(seed: int = 0) -> dict:
    seeds = jax.random.split(jax.random.key(seed), 21)
    tokens = noise(seeds[0], (BATCH_SEQS, SEQ_LEN, D), 1.0, 6.0, ((0, 4), (1, 8)))
    cotangent = noise(seeds[1], (BATCH_SEQS, SEQ_LEN, D), 1.0, 6.0, ((0, 4), (1, 8)))
    lengths = draw_lengths(jax.random.fold_in(seeds[20], 71), 0)
    mixer_gain = jnp.clip(1.0 + 0.1 * jax.random.normal(seeds[3], (D,), jnp.float32), 0.5, 1.5).astype(jnp.bfloat16)
    mixer_inputs = noise(seeds[4], (D, 3 * D), D ** -0.5, 0.21875, ((0, 32),))
    shift_taps = noise(seeds[5], (D, SHIFT), SHIFT ** -0.5, 3.0, ((0, 32),))
    decay_rate = draw_decay_rate(jax.random.fold_in(seeds[20], 71), 0)
    state_in = draw_state_in(jax.random.fold_in(seeds[20], 71), 0)
    state_out = noise(seeds[8], (D, STATE), STATE ** -0.5, 0.75, ((0, 32),))
    state_skip = noise(seeds[9], (D,), 0.3, 4.0, ((0, 32),))
    mixer_output = noise(seeds[10], (D, D), D ** -0.5, 0.21875, ((0, 32),))
    first_gain = jnp.clip(1.0 + 0.1 * jax.random.normal(seeds[11], (D,), jnp.float32), 0.5, 1.5).astype(jnp.bfloat16)
    first_up = noise(seeds[12], (D, FF), D ** -0.5, 0.21875, ((0, 32),))
    first_down = noise(seeds[13], (FF, D), FF ** -0.5, 0.109375, ((0, 32),))
    attend_gain = jnp.clip(1.0 + 0.1 * jax.random.normal(seeds[14], (D,), jnp.float32), 0.5, 1.5).astype(jnp.bfloat16)
    attend_inputs = noise(seeds[15], (D, 3 * D), D ** -0.5, 0.21875, ((0, 32),))
    attend_output = noise(seeds[16], (D, D), (D // 64) ** -0.5, 1.75, ((0, 32),))
    second_gain = jnp.clip(1.0 + 0.1 * jax.random.normal(seeds[17], (D,), jnp.float32), 0.5, 1.5).astype(jnp.bfloat16)
    second_up = noise(seeds[18], (D, FF), D ** -0.5, 0.21875, ((0, 32),))
    second_down = noise(seeds[19], (FF, D), FF ** -0.5, 0.109375, ((0, 32),))
    return dict(tokens=tokens, cotangent=cotangent, lengths=lengths, mixer_gain=mixer_gain, mixer_inputs=mixer_inputs, shift_taps=shift_taps, decay_rate=decay_rate, state_in=state_in, state_out=state_out, state_skip=state_skip, mixer_output=mixer_output, first_gain=first_gain, first_up=first_up, first_down=first_down, attend_gain=attend_gain, attend_inputs=attend_inputs, attend_output=attend_output, second_gain=second_gain, second_up=second_up, second_down=second_down)


highest = lax.Precision.HIGHEST
eps = 1e-05
masked_score = -1e+30

@jax.custom_vjp
def low(v):
    return lax.optimization_barrier(v.astype(jnp.bfloat16)).astype(jnp.float32)

@jax.custom_vjp
def low_back(v):
    return v

def low_keep(v):
    return (low(v), None)

def low_pass(kept, grad):
    return (grad,)

def back_keep(v):
    return (v, None)

def back_low(kept, grad):
    return (low(grad),)
low.defvjp(low_keep, low_pass)
low_back.defvjp(back_keep, back_low)

def layer_norm(value, gain):
    centred = value - lax.optimization_barrier(jnp.mean(value, axis=-1, keepdims=True))
    spread = lax.optimization_barrier(jnp.mean(centred * centred, axis=-1, keepdims=True))
    return centred * lax.rsqrt(spread + eps) * gain

def project(value, weight):
    return low_back(jnp.dot(low(value), weight, precision=highest))

def feed_forward(resid, gain, up_weight, down_weight):
    hidden = project(layer_norm(resid, gain), up_weight)
    return resid + project(jax.nn.gelu(hidden, approximate=True), down_weight)

def state_kernel(decay_rate, state_in, state_out):
    block_len = math.gcd(SEQ_LEN, 512)
    joined = state_in * state_out

    def one_block(first_row):
        steps = (first_row + jnp.arange(block_len, dtype=jnp.int32)).astype(jnp.float32)
        powers = jnp.exp(-decay_rate[:, :, None] * steps[None, None, :])
        return jnp.einsum('cn,cnt->tc', joined, powers, precision=highest)
    starts = jnp.arange(SEQ_LEN // block_len, dtype=jnp.int32) * block_len
    return lax.map(jax.checkpoint(one_block), starts).reshape(SEQ_LEN, D)

def h3_mixer(resid, mixer_gain, mixer_inputs, shift_taps, state_skip, mixer_output, kernel):
    projected = project(layer_norm(resid, mixer_gain), mixer_inputs)
    query_part, keys_part, value_part = jnp.split(projected, 3, axis=1)
    padded = jnp.pad(keys_part, ((SHIFT - 1, 0), (0, 0)))
    shifted = padded[SHIFT - 1:SHIFT - 1 + SEQ_LEN] * shift_taps[:, 0]
    for tap_index in range(1, SHIFT):
        shifted = shifted + padded[SHIFT - 1 - tap_index:SHIFT - 1 - tap_index + SEQ_LEN] * shift_taps[:, tap_index]
    inner = shifted * value_part
    length_fft = 2 * SEQ_LEN
    spectrum = jnp.fft.rfft(inner, n=length_fft, axis=0) * jnp.fft.rfft(kernel, n=length_fft, axis=0)
    state_y = jnp.fft.irfft(spectrum, n=length_fft, axis=0)[:SEQ_LEN] + state_skip * inner
    return resid + project(query_part * state_y, mixer_output)

def attend_mixer(resid, attend_gain, attend_inputs, attend_output):
    projected = low(project(layer_norm(resid, attend_gain), attend_inputs))
    query_part, keys_part, value_part = [one_part.reshape(SEQ_LEN, HEADS, HEAD_DIM) for one_part in jnp.split(projected, 3, axis=1)]
    block_len = math.gcd(SEQ_LEN, 512)
    places = jnp.arange(SEQ_LEN, dtype=jnp.int32)

    def one_block(first_row):
        query_rows = lax.dynamic_slice_in_dim(query_part, first_row, block_len, 0)
        scores = low_back(jnp.einsum('qhe,khe->hqk', query_rows, keys_part, precision=highest) * HEAD_DIM ** (-0.5))
        causal_mask = places[None, :] <= (first_row + jnp.arange(block_len, dtype=jnp.int32))[:, None]
        scores = jnp.where(causal_mask[None], scores, masked_score)
        shifted = jnp.exp(scores - lax.optimization_barrier(jnp.max(scores, axis=-1, keepdims=True)))
        weights_soft = shifted / lax.optimization_barrier(jnp.sum(shifted, axis=-1, keepdims=True))
        return jnp.einsum('hqk,khe->qhe', low(weights_soft), value_part, precision=highest)
    starts = jnp.arange(SEQ_LEN // block_len, dtype=jnp.int32) * block_len
    attended = lax.map(jax.checkpoint(one_block), starts).reshape(SEQ_LEN, D)
    return resid + project(low_back(attended), attend_output)

def forward(inputs, valid, mixer_gain, mixer_inputs, shift_taps, decay_rate, state_in, state_out, state_skip, mixer_output, first_gain, first_up, first_down, attend_gain, attend_inputs, attend_output, second_gain, second_up, second_down):
    kernel = state_kernel(decay_rate, state_in, state_out)

    def one_sequence(operand):
        sequence, mask_row = operand
        resid_a = h3_mixer(sequence, mixer_gain, mixer_inputs, shift_taps, state_skip, mixer_output, kernel)
        resid_b = feed_forward(resid_a, first_gain, first_up, first_down)
        resid_c = attend_mixer(resid_b, attend_gain, attend_inputs, attend_output)
        final = feed_forward(resid_c, second_gain, second_up, second_down)
        return final * mask_row[:, None]
    return lax.map(jax.checkpoint(one_sequence), (inputs, valid))

def reference(tokens, cotangent, lengths, mixer_gain, mixer_inputs, shift_taps, decay_rate, state_in, state_out, state_skip, mixer_output, first_gain, first_up, first_down, attend_gain, attend_inputs, attend_output, second_gain, second_up, second_down):
    weight_args = (mixer_gain, mixer_inputs, shift_taps, decay_rate, state_in, state_out, state_skip, mixer_output, first_gain, first_up, first_down, attend_gain, attend_inputs, attend_output, second_gain, second_up, second_down)
    floats = tuple((weight_arg.astype(jnp.float32) for weight_arg in weight_args))
    valid = (jnp.arange(SEQ_LEN, dtype=jnp.int32)[None, :] < lengths[:, None]).astype(jnp.float32)

    def wrapped(inputs, *weights):
        return forward(inputs, valid, *weights)
    mixed, pullback = jax.vjp(wrapped, tokens.astype(jnp.float32), *floats)
    grads = pullback(cotangent.astype(jnp.float32))
    return (mixed.astype(jnp.bfloat16), grads[0].astype(jnp.bfloat16), grads[1], grads[2], grads[3], grads[4], grads[5], grads[6], grads[7], grads[8], grads[9], grads[10], grads[11], grads[12], grads[13], grads[14], grads[15], grads[16], grads[17])
```

```python
import functools

import jax
import jax.numpy as jnp
from jax import lax
from jax.experimental import pallas as pl
from jax.experimental.pallas import tpu as pltpu
from jax.sharding import PartitionSpec as P

HEADS = 12
HEAD_DIM = 64

eps = 1e-05
masked_score = -1e30
lanes = 128
sublanes = 8
everyone = ("seq", "batch")
f32 = jnp.float32
bf16 = jnp.bfloat16


def rows_of(ref, seq, block):
    return ref[seq, pl.ds(pl.multiple_of(block * sublanes, sublanes), sublanes), :]


def spread(rows, index, count):
    return jnp.broadcast_to(rows[index : index + 1], (count, lanes))


def encode_kernel(reverse, input_ref, decay_ref, end_ref):
    seq_count, step_count, _ = input_ref.shape
    state_count = decay_ref.shape[0]
    blocks = step_count // sublanes
    power = jnp.exp(-decay_ref[...])

    def one_block(step, states):
        block = blocks - 1 - step if reverse else step
        rows = [rows_of(input_ref, seq, block) for seq in range(seq_count)]
        order = range(sublanes - 1, -1, -1) if reverse else range(sublanes)
        states = list(states)
        for index in order:
            for seq in range(seq_count):
                states[seq] = states[seq] * power + spread(rows[seq], index, state_count)
        return tuple(states)

    start = tuple(jnp.zeros((state_count, lanes), f32) for _ in range(seq_count))
    ends = lax.fori_loop(0, blocks, one_block, start)
    for seq in range(seq_count):
        end_ref[seq] = ends[seq]


def output_kernel(input_ref, query_ref, carried_ref, decay_ref, weight_ref, skip_ref, out_ref, gated_ref):
    seq_count, step_count, _ = input_ref.shape
    state_count = decay_ref.shape[0]
    power = jnp.exp(-decay_ref[...])
    weight = weight_ref[...]
    skip = skip_ref[...]

    def one_block(block, states):
        states = list(states)
        rows = [rows_of(input_ref, seq, block) for seq in range(seq_count)]
        found = [[] for _ in range(seq_count)]
        for index in range(sublanes):
            for seq in range(seq_count):
                states[seq] = states[seq] * power + spread(rows[seq], index, state_count)
                found[seq].append(jnp.sum(states[seq] * weight, axis=0, keepdims=True))
        place = pl.ds(pl.multiple_of(block * sublanes, sublanes), sublanes)
        for seq in range(seq_count):
            result = jnp.concatenate(found[seq], axis=0) + skip * rows[seq]
            out_ref[seq, place, :] = result
            gated_ref[seq, place, :] = result * rows_of(query_ref, seq, block)
        return tuple(states)

    start = tuple(carried_ref[seq].astype(f32) for seq in range(seq_count))
    lax.fori_loop(0, step_count // sublanes, one_block, start)


def back_kernel(
    input_ref,
    grad_ref,
    carried_ref,
    later_ref,
    decay_ref,
    weight_ref,
    skip_ref,
    input_grad_ref,
    weight_grad_ref,
    power_grad_ref,
    skip_grad_ref,
    held,
):
    seq_count, step_count, _ = input_ref.shape
    state_count = decay_ref.shape[0]
    blocks = step_count // sublanes
    power = jnp.exp(-decay_ref[...])
    weight = weight_ref[...]
    skip = skip_ref[...]
    seqs = range(seq_count)

    def forward_block(block, state):
        states, total, skip_total = list(state[0]), state[1], state[2]
        rows = [rows_of(input_ref, seq, block) for seq in seqs]
        grads = [rows_of(grad_ref, seq, block) for seq in seqs]
        for index in range(sublanes):
            for seq in seqs:
                held[block * sublanes + index, seq] = states[seq]
                states[seq] = states[seq] * power + spread(rows[seq], index, state_count)
                total = total + states[seq] * spread(grads[seq], index, state_count)
        for seq in seqs:
            skip_total = skip_total + rows[seq] * grads[seq]
        return (tuple(states), total, skip_total)

    zeros = jnp.zeros((state_count, lanes), f32)
    _, total, skip_total = lax.fori_loop(
        0,
        blocks,
        forward_block,
        (
            tuple(carried_ref[seq].astype(f32) for seq in seqs),
            zeros,
            jnp.zeros((sublanes, lanes), f32),
        ),
    )
    weight_grad_ref[...] = total
    skip_grad_ref[...] = jnp.sum(skip_total, axis=0, keepdims=True)

    def back_block(step, state):
        states, total = list(state[0]), state[1]
        block = blocks - 1 - step
        grads = [rows_of(grad_ref, seq, block) for seq in seqs]
        found = [[None] * sublanes for _ in seqs]
        for index in range(sublanes - 1, -1, -1):
            for seq in seqs:
                states[seq] = states[seq] * power + spread(grads[seq], index, state_count)
                found[seq][index] = jnp.sum(states[seq] * weight, axis=0, keepdims=True)
                total = total + states[seq] * held[block * sublanes + index, seq]
        place = pl.ds(pl.multiple_of(block * sublanes, sublanes), sublanes)
        for seq in seqs:
            input_grad_ref[seq, place, :] = jnp.concatenate(found[seq], axis=0) + skip * grads[seq]
        return (tuple(states), total)

    _, total = lax.fori_loop(
        0, blocks, back_block, (tuple(later_ref[seq].astype(f32) for seq in seqs), zeros)
    )
    power_grad_ref[...] = total * weight


def per_lane_tile(kernel, args, outs, scratch=(), flops=0):
    def spec(shape):
        lead = len(shape) - 1
        return pl.BlockSpec(tuple(shape[:-1]) + (lanes,), lambda tile: (0,) * lead + (tile,))

    bytes_moved = sum(a.size * a.dtype.itemsize for a in args)
    return pl.pallas_call(
        kernel,
        grid=(args[0].shape[-1] // lanes,),
        in_specs=[spec(a.shape) for a in args],
        out_specs=[spec(o.shape) for o in outs],
        out_shape=list(outs),
        scratch_shapes=list(scratch),
        cost_estimate=pl.CostEstimate(flops=flops, bytes_accessed=bytes_moved, transcendentals=0),
        compiler_params=pltpu.CompilerParams(vmem_limit_bytes=48 * 1024 * 1024),
    )(*args)


def shaped(*dims, dtype=f32):
    return jax.ShapeDtypeStruct(dims, dtype)


def encode(value, decay, reverse):
    seq_count, _, width = value.shape
    (ends,) = per_lane_tile(
        functools.partial(encode_kernel, reverse),
        (value, decay),
        (shaped(seq_count, decay.shape[0], width),),
    )
    return ends


def passed_along(block, axis, distance):
    devices = range(lax.axis_size(axis))
    route = [(i - distance, i) for i in devices if i - distance in devices]
    return lax.ppermute(block, axis, route)


def carried_in(ends, block_power, direction):
    count = lax.axis_size("seq")
    carried = passed_along(ends.astype(bf16), "seq", direction).astype(f32)
    distance = 1
    while distance < count - 1:
        arrived = passed_along(carried.astype(bf16), "seq", direction * distance).astype(f32)
        carried = carried + jnp.power(block_power, distance)[None] * arrived
        distance *= 2
    return carried


def split_heads(ref, scratch, heads, parts, first=0):
    for part in range(parts):
        for head in range(heads):
            start = (part * heads + head) * HEAD_DIM + first
            scratch[part * heads + head] = ref[:, start : start + HEAD_DIM]


def score_block(query, keys, first, scale):
    scores = (
        lax.dot_general(query, keys, (((1,), (1,)), ((), ())), preferred_element_type=f32) * scale
    )
    rows = lax.broadcasted_iota(jnp.int32, scores.shape, 0) + first
    columns = lax.broadcasted_iota(jnp.int32, scores.shape, 1)
    return jnp.where(columns <= rows, scores, masked_score)


def attend_kernel(heads, block, scale, qkv_ref, low_ref, full_ref, stat_ref, parts, outs):
    length = qkv_ref.shape[0]
    split_heads(qkv_ref, parts, heads, 3)

    @pl.loop(0, heads)
    def _(head):
        for first in range(0, length, block):
            extent = first + block
            query = parts[head, first:extent, :]
            scores = score_block(query, parts[heads + head, :extent, :], first, scale)
            top = jnp.max(scores, axis=1, keepdims=True)
            soft = jnp.exp(scores - top)
            whole = jnp.sum(soft, axis=1, keepdims=True)
            soft = soft * (1.0 / whole)
            outs[head, first:extent, :] = jnp.dot(
                soft.astype(bf16), parts[2 * heads + head, :extent, :], preferred_element_type=f32
            )
            stat_ref[head, first:extent, :] = jnp.broadcast_to(top + jnp.log(whole), (block, lanes))

    for head in range(heads):
        place = slice(head * HEAD_DIM, (head + 1) * HEAD_DIM)
        full_ref[:, place] = outs[head]
        low_ref[:, place] = outs[head].astype(bf16)


def attend_back_kernel(
    heads, block, scale, qkv_ref, dout_ref, full_ref, stat_ref, grad_ref, parts, douts, fulls, grads
):
    length = qkv_ref.shape[0]
    split_heads(qkv_ref, parts, heads, 3)
    split_heads(dout_ref, douts, heads, 1)
    split_heads(full_ref, fulls, heads, 1)
    grads[...] = jnp.zeros_like(grads)

    @pl.loop(0, heads)
    def _(head):
        for first in range(0, length, block):
            extent = first + block
            query = parts[head, first:extent, :]
            keys = parts[heads + head, :extent, :]
            value = parts[2 * heads + head, :extent, :]
            dout = douts[head, first:extent, :]
            delta = jnp.sum(dout.astype(f32) * fulls[head, first:extent, :], axis=1, keepdims=True)
            scores = score_block(query, keys, first, scale)
            soft = jnp.exp(scores - stat_ref[head, first:extent, :1])
            across = (((1,), (1,)), ((), ()))
            along = (((0,), (0,)), ((), ()))
            dprob = lax.dot_general(dout, value, across, preferred_element_type=f32)
            dscore = (soft * (dprob - delta) * scale).astype(bf16)
            grads[head, first:extent, :] = jnp.dot(dscore, keys, preferred_element_type=f32)
            grads[heads + head, :extent, :] += lax.dot_general(
                dscore, query, along, preferred_element_type=f32
            )
            grads[2 * heads + head, :extent, :] += lax.dot_general(
                soft.astype(bf16), dout, along, preferred_element_type=f32
            )

    grad_ref[...] = jnp.zeros_like(grad_ref)
    for part in range(3 * heads):
        grad_ref[:, part * HEAD_DIM : (part + 1) * HEAD_DIM] = grads[part].astype(bf16)


def attend_params():
    return pltpu.CompilerParams(vmem_limit_bytes=56 * 1024 * 1024)


def attend_whole(qkv, heads, block):
    length = qkv.shape[0]
    width = heads * HEAD_DIM
    return pl.pallas_call(
        functools.partial(attend_kernel, heads, block, HEAD_DIM ** (-0.5)),
        out_shape=[
            shaped(length, width, dtype=bf16),
            shaped(length, width),
            shaped(heads, length, lanes),
        ],
        scratch_shapes=[
            pltpu.VMEM((3 * heads, length, HEAD_DIM), bf16),
            pltpu.VMEM((heads, length, HEAD_DIM), f32),
        ],
        compiler_params=attend_params(),
    )(qkv)


def attend_whole_back(qkv, dout, full, stat, heads, block):
    length = qkv.shape[0]
    return pl.pallas_call(
        functools.partial(attend_back_kernel, heads, block, HEAD_DIM ** (-0.5)),
        out_shape=shaped(*qkv.shape, dtype=bf16),
        scratch_shapes=[
            pltpu.VMEM((3 * heads, length, HEAD_DIM), bf16),
            pltpu.VMEM((heads, length, HEAD_DIM), bf16),
            pltpu.VMEM((heads, length, HEAD_DIM), f32),
            pltpu.VMEM((3 * heads, length, HEAD_DIM), f32),
        ],
        compiler_params=attend_params(),
    )(qkv, dout, full, stat)


def split_blocks(array, block_len):
    shaped_blocks = array.reshape(
        (array.shape[0], array.shape[1] // block_len, block_len) + array.shape[2:]
    )
    return jnp.moveaxis(shaped_blocks, 1, 0)


def general_attention(proj_low, seq_count, block_len, places, any_live, longest):
    model_width = HEADS * HEAD_DIM
    scale = HEAD_DIM ** (-0.5)
    offsets = jnp.arange(block_len, dtype=jnp.int32)
    head_shape = (seq_count, block_len, HEADS, HEAD_DIM)
    query_low = proj_low[:, :model_width].reshape(head_shape)
    keys_low = proj_low[:, model_width : 2 * model_width].reshape(head_shape)
    value_low = proj_low[:, 2 * model_width :].reshape(head_shape)

    def block_scores(queries, keys_block, query_places, key_places):
        scores = (
            jnp.einsum("sqhe,skhe->sqhk", queries, keys_block, preferred_element_type=jnp.float32)
            * scale
        )
        causal_mask = key_places[None, :] <= query_places[:, None]
        return jnp.where(causal_mask[None, :, None, :], scores, masked_score)

    def key_needed(key_first):
        return (key_first <= places[-1]) & ((key_first == places[0]) | any_live)

    stat_shape = (seq_count, block_len, HEADS)
    start_state = (
        jnp.full(stat_shape, masked_score, jnp.float32),
        jnp.zeros(stat_shape, jnp.float32),
        jnp.zeros(head_shape, jnp.float32),
    )
    shard_piece = (
        lax.all_gather(keys_low, "seq", axis=1, tiled=True),
        lax.all_gather(value_low, "seq", axis=1, tiled=True),
    )
    keys_blocks = split_blocks(shard_piece[0], block_len)
    value_blocks = split_blocks(shard_piece[1], block_len)
    firsts = jnp.arange(keys_blocks.shape[0], dtype=jnp.int32) * block_len

    def attend_one_step(state_now, operand):
        keys_block, value_block, key_first = operand

        def attend_work(state_in_block):
            running_max, running_sum, running_out = state_in_block
            scores = block_scores(query_low, keys_block, places, key_first + offsets)
            new_max = jnp.maximum(running_max, jnp.max(scores, axis=-1))
            fade = jnp.exp(running_max - new_max)
            shifted = jnp.exp(scores - new_max[..., None])
            new_sum = running_sum * fade + jnp.sum(shifted, axis=-1)
            new_out = running_out * fade[..., None] + jnp.einsum(
                "sqhk,skhe->sqhe",
                shifted.astype(jnp.bfloat16),
                value_block,
                preferred_element_type=jnp.float32,
            )
            return (new_max, new_sum, new_out)

        return (
            lax.cond(
                key_needed(key_first), attend_work, lambda state_in_block: state_in_block, state_now
            ),
            None,
        )

    result, _ = lax.scan(attend_one_step, start_state, (keys_blocks, value_blocks, firsts))
    running_max, running_sum, running_out = result
    attended = running_out / running_sum[..., None]
    logsum = running_max + jnp.log(running_sum)
    def backward(dout_low):
        delta = jnp.sum(dout_low.astype(jnp.float32) * attended, axis=-1)
        shard_piece = (
            lax.all_gather(keys_low, "seq", axis=1, tiled=True),
            lax.all_gather(value_low, "seq", axis=1, tiled=True),
        )
        keys_blocks = split_blocks(shard_piece[0], block_len)
        value_blocks = split_blocks(shard_piece[1], block_len)
        firsts = jnp.arange(keys_blocks.shape[0], dtype=jnp.int32) * block_len

        def query_one_step(query_grad, operand):
            keys_block, value_block, key_first = operand

            def query_work(grad_now):
                scores = block_scores(query_low, keys_block, places, key_first + offsets)
                soft = jnp.exp(scores - logsum[..., None])
                dprob = jnp.einsum(
                    "sqhe,skhe->sqhk", dout_low, value_block, preferred_element_type=jnp.float32
                )
                dscore = (soft * (dprob - delta[..., None])).astype(jnp.bfloat16)
                return (
                    grad_now
                    + jnp.einsum(
                        "sqhk,skhe->sqhe", dscore, keys_block, preferred_element_type=jnp.float32
                    )
                    * scale
                )

            return (
                lax.cond(key_needed(key_first), query_work, lambda grad_now: grad_now, query_grad),
                None,
            )

        result, _ = lax.scan(
            query_one_step, jnp.zeros(head_shape, jnp.float32), (keys_blocks, value_blocks, firsts)
        )
        query_grad = result
        sent = (query_low.astype(jnp.float32), dout_low.astype(jnp.float32), logsum, delta)
        shard_piece = (
            lax.all_gather(sent[0].astype(jnp.bfloat16), "seq", axis=1, tiled=True).astype(jnp.float32),
            lax.all_gather(sent[1].astype(jnp.bfloat16), "seq", axis=1, tiled=True).astype(jnp.float32),
            lax.all_gather(sent[2].astype(jnp.bfloat16), "seq", axis=1, tiled=True).astype(jnp.float32),
            lax.all_gather(sent[3].astype(jnp.bfloat16), "seq", axis=1, tiled=True).astype(jnp.float32),
        )
        query_blocks = split_blocks(shard_piece[0], block_len)
        dout_blocks = split_blocks(shard_piece[1], block_len)
        logsum_blocks = split_blocks(shard_piece[2], block_len)
        delta_blocks = split_blocks(shard_piece[3], block_len)
        firsts = jnp.arange(query_blocks.shape[0], dtype=jnp.int32) * block_len

        def key_one_step(grads_now, operand):
            query_block, dout_block, logsum_block, delta_block, query_first = operand

            def key_work(grads_in):
                keys_grad, value_grad = grads_in
                query_cast = query_block.astype(jnp.bfloat16)
                dout_cast = dout_block.astype(jnp.bfloat16)
                scores = block_scores(query_cast, keys_low, query_first + offsets, places)
                soft = jnp.exp(scores - logsum_block[..., None])
                value_grad = value_grad + jnp.einsum(
                    "sqhk,sqhe->skhe",
                    soft.astype(jnp.bfloat16),
                    dout_cast,
                    preferred_element_type=jnp.float32,
                )
                dprob = jnp.einsum(
                    "sqhe,skhe->sqhk", dout_cast, value_low, preferred_element_type=jnp.float32
                )
                dscore = (soft * (dprob - delta_block[..., None])).astype(jnp.bfloat16)
                keys_grad = (
                    keys_grad
                    + jnp.einsum(
                        "sqhk,sqhe->skhe", dscore, query_cast, preferred_element_type=jnp.float32
                    )
                    * scale
                )
                return (keys_grad, value_grad)

            needed = (query_first + block_len - 1 >= places[0]) & (
                (query_first == places[0]) | (query_first < longest)
            )
            return (lax.cond(needed, key_work, lambda grads_in: grads_in, grads_now), None)

        result, _ = lax.scan(
            key_one_step,
            (jnp.zeros(head_shape, jnp.float32), jnp.zeros(head_shape, jnp.float32)),
            (query_blocks, dout_blocks, logsum_blocks, delta_blocks, firsts),
        )
        keys_grad, value_grad = result
        return (query_grad, keys_grad, value_grad)

    return attended, backward


def layer_norm(value, gain):
    centred = value - jnp.mean(value, axis=-1, keepdims=True)
    spread_of = jnp.mean(centred * centred, axis=-1, keepdims=True)
    return centred * lax.rsqrt(spread_of + eps) * gain


def gelu_tanh(value):
    return jax.nn.gelu(value, approximate=True)


def dense(left, weight):
    return jnp.dot(left, weight, preferred_element_type=f32)


def dense_back(left, weight, upstream):
    into_left = lax.dot_general(
        upstream, weight, (((1,), (1,)), ((), ())), preferred_element_type=f32
    )
    into_weight = lax.dot_general(
        left, upstream, (((0,), (0,)), ((), ())), preferred_element_type=f32
    ).astype(bf16)
    return (into_left, into_weight)


def shift_mix(extended, taps, value_part):
    step_count = value_part.shape[1]
    reach = taps.shape[1]
    shifted = extended[:, reach - 1 : reach - 1 + step_count] * taps[:, 0]
    for tap_index in range(1, reach):
        shifted = (
            shifted
            + extended[:, reach - 1 - tap_index : reach - 1 - tap_index + step_count]
            * taps[:, tap_index]
        )
    return shifted * value_part


def feed_forward(resid, gain, up_weight, down_weight):
    normed, norm_back = jax.vjp(layer_norm, resid, gain)
    normed_low = normed.astype(bf16)
    hidden = dense(normed_low, up_weight)
    active, active_back = jax.vjp(gelu_tanh, hidden)
    active_low = active.astype(bf16)
    return (
        resid + dense(active_low, down_weight),
        (norm_back, normed_low, active_back, active_low),
    )


def feed_back(stored, up_weight, down_weight, upstream):
    norm_back, normed_low, active_back, active_low = stored
    into_active, down_grad = dense_back(active_low, down_weight, upstream.astype(bf16))
    (into_hidden,) = active_back(into_active)
    into_normed, up_grad = dense_back(normed_low, up_weight, into_hidden.astype(bf16))
    into_resid, gain_grad = norm_back(into_normed)
    return (upstream + into_resid, gain_grad, up_grad, down_grad)


def fold_rows(weight, share):
    rows, width = weight.shape
    fold = rows // share
    return weight.reshape(fold, share, width).transpose(1, 0, 2).reshape(share, fold * width)


def unfold_rows(folded, fold, share):
    rows, width = folded.shape
    width //= fold
    parts = folded.reshape(rows // share, share, fold, width).transpose(0, 2, 1, 3)
    return parts.reshape(rows * fold, width)


def fold_all(weight, share, rows):
    tall, width = weight.shape
    fold = tall // rows
    parts = weight.reshape(rows // share, fold, share, width).transpose(0, 2, 1, 3)
    return parts.reshape(rows, fold * width)


def group_columns(weight, groups, padded):
    rows, columns = weight.shape
    part = columns // 3 // groups
    grouped = weight.reshape(rows, 3, groups, part).transpose(0, 2, 1, 3).reshape(rows, groups, 3 * part)
    return jnp.pad(grouped, ((0, 0), (0, 0), (0, padded - 3 * part))).reshape(rows, groups * padded)


def ungroup_columns(grouped, groups, padded, columns):
    rows = grouped.shape[0]
    part = columns // 3 // groups
    parts = grouped.reshape(rows, groups, padded)[:, :, : 3 * part].reshape(rows, groups, 3, part)
    return parts.transpose(0, 2, 1, 3).reshape(rows, columns)


def cut(array, widths):
    pieces, start = [], 0
    for width in widths:
        pieces.append(array[:, start : start + width])
        start += width
    return pieces


def gathered(parts):
    whole = lax.all_gather(jnp.concatenate(parts, axis=1), everyone, axis=0, tiled=True)
    return cut(whole, [p.shape[1] for p in parts])


def scattered(parts):
    mine = lax.psum_scatter(
        jnp.concatenate(parts, axis=1), everyone, scatter_dimension=0, tiled=True
    )
    return cut(mine, [p.shape[1] for p in parts])


def body(
    tokens,
    cotangent,
    lengths,
    mixer_gain,
    mixer_inputs,
    shift_taps,
    decay_rate,
    state_in,
    state_out,
    state_skip,
    mixer_output,
    first_gain,
    first_up,
    first_down,
    attend_gain,
    attend_inputs,
    attend_output,
    second_gain,
    second_up,
    second_down,
):
    seq_count, block_len, model_width = tokens.shape
    row_count = seq_count * block_len
    seq_devices = lax.axis_size("seq")
    share = mixer_inputs.shape[0]
    states, reach = decay_rate.shape[1], shift_taps.shape[1]
    fold = first_down.shape[0] // share
    deals = seq_count * HEADS
    dealt = deals % seq_devices == 0 and HEADS % (deals // seq_devices) == 0
    heads = deals // seq_devices if dealt else HEADS
    groups = HEADS // heads
    group_width = heads * HEAD_DIM
    padded = -(-3 * group_width // lanes) * lanes if dealt else 3 * group_width

    columns = [decay_rate, state_in, state_out, shift_taps]
    columns += [g[:, None] for g in (mixer_gain, first_gain, attend_gain, second_gain, state_skip)]
    small = jnp.concatenate(columns, axis=1)
    small_count = small.shape[1]
    small_width = -(-small_count // lanes) * lanes
    small = jnp.pad(small, ((0, 0), (0, small_width - small_count)))
    w_mixer_in, w_small = gathered([mixer_inputs, small])
    attend_cols = attend_inputs.shape[1]
    w_mixer_out, w_up1, w_down1, w_attend_in, w_attend_out, w_up2, w_down2 = gathered(
        [
            mixer_output,
            first_up,
            fold_rows(first_down, share),
            group_columns(attend_inputs, groups, padded),
            attend_output,
            second_up,
            fold_rows(second_down, share),
        ]
    )
    w_down1 = unfold_rows(w_down1, fold, share)
    w_down2 = unfold_rows(w_down2, fold, share)

    rows = w_small.T.astype(f32)
    decay, table_in, table_out = rows[:states], rows[states : 2 * states], rows[2 * states : 3 * states]
    taps_rows = rows[3 * states : 3 * states + reach]
    gain_mixer, gain_first, gain_attend, gain_second, skip = (
        rows[3 * states + reach + i] for i in range(5)
    )
    taps = taps_rows.T
    weight = table_in * table_out

    rank_seq = lax.axis_index("seq")
    offsets = jnp.arange(block_len, dtype=jnp.int32)
    places = rank_seq * block_len + offsets
    valid = (places[None, :] < lengths[:, None]).astype(f32)
    longest = jnp.max(lengths)
    any_live = places[0] < longest

    start_resid = tokens.reshape(row_count, model_width).astype(f32)
    normed_mixer, back_mixer = jax.vjp(layer_norm, start_resid, gain_mixer)
    normed_low_mixer = normed_mixer.astype(bf16)
    projected = dense(normed_low_mixer, w_mixer_in).reshape(seq_count, block_len, 3 * model_width)
    query_mixer = projected[:, :, :model_width]
    keys_mixer = projected[:, :, model_width : 2 * model_width]
    value_mixer = projected[:, :, 2 * model_width :]
    rim_rows = passed_along(keys_mixer[:, block_len - reach + 1 :], "seq", 1)
    extended = jnp.concatenate([rim_rows, keys_mixer], axis=1)
    inner, shift_back = jax.vjp(shift_mix, extended, taps, value_mixer)
    block_power = jnp.exp(-decay * block_len)
    ends = encode(inner, decay, False)
    carried = carried_in(ends, block_power, 1)
    wide = shaped(seq_count, block_len, model_width)
    state_y, gated = per_lane_tile(
        output_kernel,
        (inner, query_mixer, carried, decay, weight, skip[None]),
        (wide, wide),
    )
    gated_low = gated.astype(bf16).reshape(row_count, model_width)
    resid_mixer = start_resid + dense(gated_low, w_mixer_out)
    resid_first, stored_first = feed_forward(resid_mixer, gain_first, w_up1, w_down1)

    normed_attend, back_attend = jax.vjp(layer_norm, resid_first, gain_attend)
    normed_low_attend = normed_attend.astype(bf16)
    proj_low = dense(normed_low_attend, w_attend_in).astype(bf16)
    if dealt:
        length = seq_devices * block_len
        block = min(256, length)

        def deal(array, width):
            parts = array.reshape(seq_count, block_len, groups, width).transpose(0, 2, 1, 3)
            parts = parts.reshape(seq_count * groups, block_len, width)
            dealt_parts = lax.all_to_all(parts, "seq", split_axis=0, concat_axis=0, tiled=True)
            return dealt_parts.reshape(length, width)

        def collect(array, width):
            parts = array.reshape(seq_devices, block_len, width)
            back = lax.all_to_all(parts, "seq", split_axis=0, concat_axis=0, tiled=True)
            back = back.reshape(seq_count, groups, block_len, width).transpose(0, 2, 1, 3)
            return back.reshape(row_count, groups * width)

        qkv = deal(proj_low, padded)
        attended_part, attended_full, stat = attend_whole(qkv, heads, block)
        attended_low = collect(attended_part, group_width)
    else:
        attended, attended_back = general_attention(
            proj_low, seq_count, block_len, places, any_live, longest
        )
        attended_low = attended.reshape(row_count, model_width).astype(bf16)
    resid_attend = resid_first + dense(attended_low, w_attend_out)
    final, stored_second = feed_forward(resid_attend, gain_second, w_up2, w_down2)
    mixed = (final.reshape(seq_count, block_len, model_width) * valid[..., None]).astype(bf16)

    upstream = (cotangent.astype(f32) * valid[..., None]).reshape(row_count, model_width)
    upstream, second_gain_grad, second_up_grad, second_down_grad = feed_back(
        stored_second, w_up2, w_down2, upstream
    )
    into_attended, attend_output_grad = dense_back(
        attended_low, w_attend_out, upstream.astype(bf16)
    )
    second_up_out, second_down_out, attend_output_out = scattered(
        [second_up_grad, fold_all(second_down_grad, share, model_width), attend_output_grad]
    )
    dout_low = into_attended.astype(bf16)
    if dealt:
        dout = deal(dout_low, group_width)
        proj_grad = collect(
            attend_whole_back(qkv, dout, attended_full, stat, heads, block), padded
        )
    else:
        parts = attended_back(dout_low.reshape(seq_count, block_len, HEADS, HEAD_DIM))
        proj_grad = jnp.concatenate(
            [p.reshape(row_count, model_width) for p in parts], axis=1
        ).astype(bf16)
    into_normed, attend_inputs_grad = dense_back(normed_low_attend, w_attend_in, proj_grad)
    into_resid, attend_gain_grad = back_attend(into_normed)
    upstream = upstream + into_resid
    upstream, first_gain_grad, first_up_grad, first_down_grad = feed_back(
        stored_first, w_up1, w_down1, upstream
    )
    into_gated, mixer_output_grad = dense_back(gated_low, w_mixer_out, upstream.astype(bf16))
    into_gated = into_gated.reshape(seq_count, block_len, model_width)
    query_mixer_grad = into_gated * state_y
    state_grad = into_gated * query_mixer
    later = carried_in(encode(state_grad, decay, True), block_power, -1)
    table = shaped(states, model_width)
    inner_grad, weight_grad, power_grad, skip_grad = per_lane_tile(
        back_kernel,
        (inner, state_grad, carried, later, decay, weight, skip[None]),
        (wide, table, table, shaped(1, model_width)),
        scratch=[pltpu.VMEM((block_len, seq_count, states, lanes), f32)],
    )
    extended_grad, taps_grad, value_mixer_grad = shift_back(inner_grad)
    spill = passed_along(extended_grad[:, : reach - 1], "seq", -1)
    keys_mixer_grad = extended_grad[:, reach - 1 :] + jnp.pad(
        spill, ((0, 0), (block_len - reach + 1, 0), (0, 0))
    )
    proj_grad_mixer = (
        jnp.concatenate([query_mixer_grad, keys_mixer_grad, value_mixer_grad], axis=2)
        .astype(bf16)
        .reshape(row_count, 3 * model_width)
    )
    into_normed_mixer, mixer_inputs_grad = dense_back(normed_low_mixer, w_mixer_in, proj_grad_mixer)
    into_start, mixer_gain_grad = back_mixer(into_normed_mixer)
    tokens_gradient = (upstream + into_start).reshape(seq_count, block_len, model_width).astype(bf16)

    small_rows = jnp.concatenate(
        [-jnp.exp(-decay) * power_grad, weight_grad * table_out, weight_grad * table_in, taps_grad.T]
        + [
            g[None]
            for g in (mixer_gain_grad, first_gain_grad, attend_gain_grad, second_gain_grad, skip_grad[0])
        ],
        axis=0,
    )
    small_grad = jnp.pad(small_rows, ((0, small_width - small_count), (0, 0))).T.astype(bf16)
    attend_inputs_out, first_up_out, first_down_out, mixer_output_out, mixer_inputs_out, small_out = scattered(
        [
            attend_inputs_grad,
            first_up_grad,
            fold_all(first_down_grad, share, model_width),
            mixer_output_grad,
            mixer_inputs_grad,
            small_grad,
        ]
    )
    small_out = small_out.astype(f32)
    gains_at = 3 * states + reach

    def unfolded(folded):
        return folded.reshape(share, fold, model_width).transpose(1, 0, 2).reshape(share * fold, model_width)

    return (
        mixed,
        tokens_gradient,
        small_out[:, gains_at],
        mixer_inputs_out.astype(f32),
        small_out[:, 3 * states : gains_at],
        small_out[:, :states],
        small_out[:, states : 2 * states],
        small_out[:, 2 * states : 3 * states],
        small_out[:, gains_at + 4],
        mixer_output_out.astype(f32),
        small_out[:, gains_at + 1],
        first_up_out.astype(f32),
        unfolded(first_down_out).astype(f32),
        small_out[:, gains_at + 2],
        ungroup_columns(attend_inputs_out, groups, padded, attend_cols).astype(f32),
        attend_output_out.astype(f32),
        small_out[:, gains_at + 3],
        second_up_out.astype(f32),
        unfolded(second_down_out).astype(f32),
    )


def solution(mesh):
    return jax.shard_map(
        body,
        mesh=mesh,
        in_specs=(
            P("batch", "seq", None),
            P("batch", "seq", None),
            P("batch"),
            P(("seq", "batch")),
            P(("seq", "batch"), None),
            P(("seq", "batch"), None),
            P(("seq", "batch"), None),
            P(("seq", "batch"), None),
            P(("seq", "batch"), None),
            P(("seq", "batch")),
            P(("seq", "batch"), None),
            P(("seq", "batch")),
            P(("seq", "batch"), None),
            P(("seq", "batch"), None),
            P(("seq", "batch")),
            P(("seq", "batch"), None),
            P(("seq", "batch"), None),
            P(("seq", "batch")),
            P(("seq", "batch"), None),
            P(("seq", "batch"), None),
        ),
        out_specs=(
            P("batch", "seq", None),
            P("batch", "seq", None),
            P(("seq", "batch")),
            P(("seq", "batch"), None),
            P(("seq", "batch"), None),
            P(("seq", "batch"), None),
            P(("seq", "batch"), None),
            P(("seq", "batch"), None),
            P(("seq", "batch")),
            P(("seq", "batch"), None),
            P(("seq", "batch")),
            P(("seq", "batch"), None),
            P(("seq", "batch"), None),
            P(("seq", "batch")),
            P(("seq", "batch"), None),
            P(("seq", "batch"), None),
            P(("seq", "batch")),
            P(("seq", "batch"), None),
            P(("seq", "batch"), None),
        ),
        check_vma=False,
    )
```

```python
import functools

import jax
import jax.numpy as jnp
from jax import lax
from jax.experimental import pallas as pl
from jax.experimental.pallas import tpu as pltpu
from jax.sharding import PartitionSpec as P

HEADS = 12
HEAD_DIM = 64

eps = 1e-05
masked_score = -1e30
lanes = 128
sublanes = 8
everyone = ("seq", "batch")
f32 = jnp.float32
bf16 = jnp.bfloat16


def rows_of(ref, seq, block):
    return ref[seq, pl.ds(pl.multiple_of(block * sublanes, sublanes), sublanes), :]


def spread(rows, index, count):
    return jnp.broadcast_to(rows[index : index + 1], (count, lanes))


def encode_kernel(reverse, input_ref, decay_ref, end_ref):
    seq_count, step_count, _ = input_ref.shape
    state_count = decay_ref.shape[0]
    blocks = step_count // sublanes
    power = jnp.exp(-decay_ref[...])

    def one_block(step, states):
        block = blocks - 1 - step if reverse else step
        rows = [rows_of(input_ref, seq, block) for seq in range(seq_count)]
        order = range(sublanes - 1, -1, -1) if reverse else range(sublanes)
        states = list(states)
        for index in order:
            for seq in range(seq_count):
                states[seq] = states[seq] * power + spread(rows[seq], index, state_count)
        return tuple(states)

    start = tuple(jnp.zeros((state_count, lanes), f32) for _ in range(seq_count))
    ends = lax.fori_loop(0, blocks, one_block, start)
    for seq in range(seq_count):
        end_ref[seq] = ends[seq]


def output_kernel(input_ref, query_ref, carried_ref, decay_ref, weight_ref, skip_ref, out_ref, gated_ref):
    seq_count, step_count, _ = input_ref.shape
    state_count = decay_ref.shape[0]
    power = jnp.exp(-decay_ref[...])
    weight = weight_ref[...]
    skip = skip_ref[...]

    def one_block(block, states):
        states = list(states)
        rows = [rows_of(input_ref, seq, block) for seq in range(seq_count)]
        found = [[] for _ in range(seq_count)]
        for index in range(sublanes):
            for seq in range(seq_count):
                states[seq] = states[seq] * power + spread(rows[seq], index, state_count)
                found[seq].append(jnp.sum(states[seq] * weight, axis=0, keepdims=True))
        place = pl.ds(pl.multiple_of(block * sublanes, sublanes), sublanes)
        for seq in range(seq_count):
            result = jnp.concatenate(found[seq], axis=0) + skip * rows[seq]
            out_ref[seq, place, :] = result
            gated_ref[seq, place, :] = result * rows_of(query_ref, seq, block)
        return tuple(states)

    start = tuple(carried_ref[seq].astype(f32) for seq in range(seq_count))
    lax.fori_loop(0, step_count // sublanes, one_block, start)


def back_kernel(
    input_ref,
    grad_ref,
    carried_ref,
    later_ref,
    decay_ref,
    weight_ref,
    skip_ref,
    input_grad_ref,
    weight_grad_ref,
    power_grad_ref,
    skip_grad_ref,
    held,
):
    seq_count, step_count, _ = input_ref.shape
    state_count = decay_ref.shape[0]
    blocks = step_count // sublanes
    power = jnp.exp(-decay_ref[...])
    weight = weight_ref[...]
    skip = skip_ref[...]
    seqs = range(seq_count)

    def forward_block(block, state):
        states, total, skip_total = list(state[0]), state[1], state[2]
        rows = [rows_of(input_ref, seq, block) for seq in seqs]
        grads = [rows_of(grad_ref, seq, block) for seq in seqs]
        for index in range(sublanes):
            for seq in seqs:
                held[block * sublanes + index, seq] = states[seq]
                states[seq] = states[seq] * power + spread(rows[seq], index, state_count)
                total = total + states[seq] * spread(grads[seq], index, state_count)
        for seq in seqs:
            skip_total = skip_total + rows[seq] * grads[seq]
        return (tuple(states), total, skip_total)

    zeros = jnp.zeros((state_count, lanes), f32)
    _, total, skip_total = lax.fori_loop(
        0,
        blocks,
        forward_block,
        (
            tuple(carried_ref[seq].astype(f32) for seq in seqs),
            zeros,
            jnp.zeros((sublanes, lanes), f32),
        ),
    )
    weight_grad_ref[...] = total
    skip_grad_ref[...] = jnp.sum(skip_total, axis=0, keepdims=True)

    def back_block(step, state):
        states, total = list(state[0]), state[1]
        block = blocks - 1 - step
        grads = [rows_of(grad_ref, seq, block) for seq in seqs]
        found = [[None] * sublanes for _ in seqs]
        for index in range(sublanes - 1, -1, -1):
            for seq in seqs:
                states[seq] = states[seq] * power + spread(grads[seq], index, state_count)
                found[seq][index] = jnp.sum(states[seq] * weight, axis=0, keepdims=True)
                total = total + states[seq] * held[block * sublanes + index, seq]
        place = pl.ds(pl.multiple_of(block * sublanes, sublanes), sublanes)
        for seq in seqs:
            input_grad_ref[seq, place, :] = jnp.concatenate(found[seq], axis=0) + skip * grads[seq]
        return (tuple(states), total)

    _, total = lax.fori_loop(
        0, blocks, back_block, (tuple(later_ref[seq].astype(f32) for seq in seqs), zeros)
    )
    power_grad_ref[...] = total * weight


def per_lane_tile(kernel, args, outs, scratch=(), flops=0):
    def spec(shape):
        lead = len(shape) - 1
        return pl.BlockSpec(tuple(shape[:-1]) + (lanes,), lambda tile: (0,) * lead + (tile,))

    bytes_moved = sum(a.size * a.dtype.itemsize for a in args)
    return pl.pallas_call(
        kernel,
        grid=(args[0].shape[-1] // lanes,),
        in_specs=[spec(a.shape) for a in args],
        out_specs=[spec(o.shape) for o in outs],
        out_shape=list(outs),
        scratch_shapes=list(scratch),
        cost_estimate=pl.CostEstimate(flops=flops, bytes_accessed=bytes_moved, transcendentals=0),
        compiler_params=pltpu.CompilerParams(vmem_limit_bytes=48 * 1024 * 1024),
    )(*args)


def shaped(*dims, dtype=f32):
    return jax.ShapeDtypeStruct(dims, dtype)


def encode(value, decay, reverse):
    seq_count, _, width = value.shape
    (ends,) = per_lane_tile(
        functools.partial(encode_kernel, reverse),
        (value, decay),
        (shaped(seq_count, decay.shape[0], width),),
    )
    return ends


def passed_along(block, axis, distance):
    devices = range(lax.axis_size(axis))
    route = [(i - distance, i) for i in devices if i - distance in devices]
    return lax.ppermute(block, axis, route)


def carried_in(ends, decay, block_len, reverse):
    seq_count, state_count, width = ends.shape
    count = lax.axis_size("seq")
    part = state_count // count

    def exchanged(parts):
        return lax.all_to_all(parts.astype(bf16), "seq", split_axis=0, concat_axis=0, tiled=True)

    parts = ends.reshape(seq_count, count, part, width).transpose(1, 0, 2, 3)
    arrived = exchanged(parts.reshape(count, seq_count * part, width)).astype(f32)
    rates = lax.dynamic_slice_in_dim(decay, lax.axis_index("seq") * part, part, 0)
    power = jnp.tile(jnp.exp(-rates * block_len), (seq_count, 1))
    state, joined = jnp.zeros_like(arrived[0]), [None] * count
    for block in reversed(range(count)) if reverse else range(count):
        joined[block] = state
        state = power * state + arrived[block]
    back = exchanged(jnp.stack(joined))
    back = back.reshape(count, seq_count, part, width).transpose(1, 0, 2, 3)
    return back.reshape(seq_count, state_count, width)


MESH = pl.DeviceIdType.MESH
box = (4, 2, 2, 2)


def here():
    seq, batch = lax.axis_index("seq"), lax.axis_index("batch")
    return lax.div(seq, 2), lax.rem(seq, 2), lax.div(batch, 2), lax.rem(batch, 2)


def device(z, x, y, core):
    return (2 * z + x, 2 * y + core)


def line_peer(z, step):
    return lax.rem(z + step, box[0])


def greet():
    z, x, y, core = here()
    barrier = pltpu.get_barrier_semaphore()
    peers = [device(line_peer(z, step), x, y, core) for step in range(1, box[0])]
    peers += [device(z, 1 - x, y, core), device(z, x, 1 - y, core), device(z, x, y, 1 - core)]
    for peer in peers:
        pl.semaphore_signal(barrier, inc=1, device_id=peer, device_id_type=MESH)
    pl.semaphore_wait(barrier, len(peers))


def staggered(count, stages, gap):
    for turn in range(count + gap * (stages - 1)):
        for stage in reversed(range(stages)):
            chunk = turn - gap * stage
            if 0 <= chunk < count:
                yield stage, chunk


def gather_kernel(plan, gap, *refs):
    count = 1 + max(item[0] for item in plan)
    ins, outs = refs[:count], refs[count : 2 * count]
    send, receive, local = refs[2 * count :]
    z, x, y, core = here()
    greet()
    started = {}

    def push(chunk, slot, source, target, peer):
        copy = pltpu.make_async_remote_copy(
            src_ref=source,
            dst_ref=target,
            send_sem=send.at[chunk, slot],
            recv_sem=receive.at[chunk, slot],
            device_id=peer,
            device_id_type=MESH,
        )
        copy.start()
        started[chunk, slot] = copy

    own = []
    for chunk, (index, first, width, x_first) in enumerate(plan):
        columns = pl.ds(first, width)
        source = ins[index].at[:, columns]
        target = outs[index].at[z, x, y, core, :, columns]
        for step in range(1, box[0]):
            push(chunk, step - 1, source, target, device(line_peer(z, step), x, y, core))
        keep = pltpu.make_async_copy(source, target, local.at[chunk])
        keep.start()
        own.append(keep)

    for stage, chunk in staggered(len(plan), 3, gap):
        index, first, width, x_first = plan[chunk]
        columns = pl.ds(first, width)
        out = outs[index]
        if stage == 0:
            for step in range(1, box[0]):
                started[chunk, step - 1].wait_recv()
            own[chunk].wait()
            part = out.at[:, x, y, core, :, columns]
            peer = device(z, 1 - x, y, core) if x_first else device(z, x, 1 - y, core)
            push(chunk, 3, part, part, peer)
        elif stage == 1:
            started[chunk, 3].wait_recv()
            if x_first:
                part, peer = out.at[:, :, y, core, :, columns], device(z, x, 1 - y, core)
            else:
                part, peer = out.at[:, x, :, core, :, columns], device(z, 1 - x, y, core)
            push(chunk, 4, part, part, peer)
        else:
            started[chunk, 4].wait_recv()
            part = out.at[:, :, :, core, :, columns]
            push(chunk, 5, part, part, device(z, x, y, 1 - core))
    for chunk in range(len(plan)):
        started[chunk, 5].wait_recv()
        for slot in range(6):
            started[chunk, slot].wait_send()


def gather_blocks(blocks, plan, gap=2, collective=0):
    outs = [jax.ShapeDtypeStruct(box + b.shape, b.dtype) for b in blocks]
    sent = sum(b.size * b.dtype.itemsize for b in blocks)
    whole = pl.pallas_call(
        functools.partial(gather_kernel, plan, gap),
        out_shape=outs,
        in_specs=[pl.BlockSpec(memory_space=pltpu.VMEM)] * len(blocks),
        out_specs=[pl.BlockSpec(memory_space=pl.ANY)] * len(blocks),
        scratch_shapes=[
            pltpu.SemaphoreType.DMA((len(plan), 6)),
            pltpu.SemaphoreType.DMA((len(plan), 6)),
            pltpu.SemaphoreType.DMA((len(plan),)),
        ],
        cost_estimate=pl.CostEstimate(flops=0, bytes_accessed=64 * sent, transcendentals=0),
        compiler_params=pltpu.CompilerParams(collective_id=collective, has_side_effects=True),
    )(*blocks)
    return [w.reshape((32 * w.shape[4], w.shape[5])) for w in whole]


def add_into(total, other):
    return (total.astype(f32) + other.astype(f32)).astype(bf16)


def scatter_kernel(plan, gap, *refs):
    count = 1 + max(item[0] for item in plan)
    ins, outs = refs[:count], refs[count : 2 * count]
    buffers = refs[2 * count : -3]
    send, receive, local = refs[-3:]
    z, x, y, core = here()
    greet()
    started = {}

    def push(chunk, slot, source, target, peer):
        copy = pltpu.make_async_remote_copy(
            src_ref=source,
            dst_ref=target,
            send_sem=send.at[chunk, slot],
            recv_sem=receive.at[chunk, slot],
            device_id=peer,
            device_id_type=MESH,
        )
        copy.start()
        started[chunk, slot] = copy

    loads = []
    for chunk, (index, first, width, _) in enumerate(plan):
        columns = pl.ds(first, width)
        held, from_core = buffers[5 * chunk : 5 * chunk + 2]
        grad = ins[index]
        push(chunk, 0, grad.at[:, :, :, 1 - core, :, columns], from_core, device(z, x, y, 1 - core))
        load = pltpu.make_async_copy(grad.at[:, :, :, core, :, columns], held, local.at[chunk])
        load.start()
        loads.append(load)

    for stage, chunk in staggered(len(plan), 4, gap):
        index, first, width, x_first = plan[chunk]
        held, from_core, from_one, from_two, from_line = buffers[5 * chunk : 5 * chunk + 5]
        to_x, to_y = device(z, 1 - x, y, core), device(z, x, 1 - y, core)
        if stage == 0:
            started[chunk, 0].wait_recv()
            loads[chunk].wait()

            @pl.loop(0, box[0])
            def _(row):
                for i in range(2):
                    for j in range(2):
                        held[row, i, j] = add_into(held[row, i, j], from_core[row, i, j])

            if x_first:
                push(chunk, 1, held.at[:, :, 1 - y], from_one, to_y)
            else:
                push(chunk, 1, held.at[:, 1 - x], from_one, to_x)
        elif stage == 1:
            started[chunk, 1].wait_recv()

            @pl.loop(0, box[0])
            def _(row):
                for i in range(2):
                    if x_first:
                        held[row, i, y] = add_into(held[row, i, y], from_one[row, i])
                    else:
                        held[row, x, i] = add_into(held[row, x, i], from_one[row, i])

            if x_first:
                push(chunk, 2, held.at[:, 1 - x, y], from_two, to_x)
            else:
                push(chunk, 2, held.at[:, x, 1 - y], from_two, to_y)
        elif stage == 2:
            started[chunk, 2].wait_recv()

            @pl.loop(0, box[0])
            def _(row):
                held[row, x, y] = add_into(held[row, x, y], from_two[row])

            for step in range(1, box[0]):
                peer = line_peer(z, step)
                push(chunk, 2 + step, held.at[peer, x, y], from_line.at[step - 1], device(peer, x, y, core))
        else:
            total = held[z, x, y].astype(f32)
            for step in range(1, box[0]):
                started[chunk, 2 + step].wait_recv()
                total = total + from_line[step - 1].astype(f32)
            outs[index][:, pl.ds(first, width)] = total
    for chunk in range(len(plan)):
        for slot in range(6):
            started[chunk, slot].wait_send()


def scatter_blocks(grads, plan, gap=2, collective=1):
    views = [g.reshape(box + (g.shape[0] // 32, g.shape[1])) for g in grads]
    scratch = []
    for index, _, width, _ in plan:
        tile = (views[index].shape[4], width)
        for lead in ((4, 2, 2), (4, 2, 2), (4, 2), (4,), (3,)):
            scratch.append(pltpu.VMEM(lead + tile, bf16))
    sent = sum(v.size * v.dtype.itemsize for v in views)
    return pl.pallas_call(
        functools.partial(scatter_kernel, plan, gap),
        out_shape=[jax.ShapeDtypeStruct(v.shape[4:], f32) for v in views],
        in_specs=[pl.BlockSpec(memory_space=pl.ANY)] * len(views),
        out_specs=[pl.BlockSpec(memory_space=pltpu.VMEM)] * len(views),
        scratch_shapes=scratch
        + [
            pltpu.SemaphoreType.DMA((len(plan), 6)),
            pltpu.SemaphoreType.DMA((len(plan), 6)),
            pltpu.SemaphoreType.DMA((len(plan),)),
        ],
        cost_estimate=pl.CostEstimate(flops=0, bytes_accessed=4 * sent, transcendentals=0),
        compiler_params=pltpu.CompilerParams(
            collective_id=collective, has_side_effects=True, vmem_limit_bytes=60 * 1024 * 1024
        ),
    )(*views)


def chunked(widths, pieces):
    plan = []
    for index, (width, number) in enumerate(zip(widths, pieces)):
        tiles = width // lanes
        edges = [tiles * i // number for i in range(number + 1)]
        for i in range(number):
            plan.append((index, edges[i] * lanes, (edges[i + 1] - edges[i]) * lanes, len(plan) % 2 == 0))
    return plan


def split_heads(ref, scratch, heads, parts, first=0):
    for part in range(parts):
        for head in range(heads):
            start = (part * heads + head) * HEAD_DIM + first
            scratch[part * heads + head] = ref[:, start : start + HEAD_DIM]


def score_block(query, keys, first, scale):
    scores = (
        lax.dot_general(query, keys, (((1,), (1,)), ((), ())), preferred_element_type=f32) * scale
    )
    rows = lax.broadcasted_iota(jnp.int32, scores.shape, 0) + first
    columns = lax.broadcasted_iota(jnp.int32, scores.shape, 1)
    return jnp.where(columns <= rows, scores, masked_score)


def attend_kernel(heads, block, scale, qkv_ref, low_ref, full_ref, stat_ref, parts, outs):
    length = qkv_ref.shape[0]
    split_heads(qkv_ref, parts, heads, 3)

    @pl.loop(0, heads)
    def _(head):
        for first in range(0, length, block):
            extent = first + block
            query = parts[head, first:extent, :]
            scores = score_block(query, parts[heads + head, :extent, :], first, scale)
            top = jnp.max(scores, axis=1, keepdims=True)
            soft = jnp.exp(scores - top)
            whole = jnp.sum(soft, axis=1, keepdims=True)
            soft = soft * (1.0 / whole)
            outs[head, first:extent, :] = jnp.dot(
                soft.astype(bf16), parts[2 * heads + head, :extent, :], preferred_element_type=f32
            )
            stat_ref[head, first:extent, :] = jnp.broadcast_to(top + jnp.log(whole), (block, lanes))

    for head in range(heads):
        place = slice(head * HEAD_DIM, (head + 1) * HEAD_DIM)
        full_ref[:, place] = outs[head]
        low_ref[:, place] = outs[head].astype(bf16)


def attend_back_kernel(
    heads, block, scale, qkv_ref, dout_ref, full_ref, stat_ref, grad_ref, parts, douts, fulls, grads
):
    length = qkv_ref.shape[0]
    split_heads(qkv_ref, parts, heads, 3)
    split_heads(dout_ref, douts, heads, 1)
    split_heads(full_ref, fulls, heads, 1)
    grads[...] = jnp.zeros_like(grads)

    @pl.loop(0, heads)
    def _(head):
        for first in range(0, length, block):
            extent = first + block
            query = parts[head, first:extent, :]
            keys = parts[heads + head, :extent, :]
            value = parts[2 * heads + head, :extent, :]
            dout = douts[head, first:extent, :]
            delta = jnp.sum(dout.astype(f32) * fulls[head, first:extent, :], axis=1, keepdims=True)
            scores = score_block(query, keys, first, scale)
            soft = jnp.exp(scores - stat_ref[head, first:extent, :1])
            across = (((1,), (1,)), ((), ()))
            along = (((0,), (0,)), ((), ()))
            dprob = lax.dot_general(dout, value, across, preferred_element_type=f32)
            dscore = (soft * (dprob - delta) * scale).astype(bf16)
            grads[head, first:extent, :] = jnp.dot(dscore, keys, preferred_element_type=f32)
            grads[heads + head, :extent, :] += lax.dot_general(
                dscore, query, along, preferred_element_type=f32
            )
            grads[2 * heads + head, :extent, :] += lax.dot_general(
                soft.astype(bf16), dout, along, preferred_element_type=f32
            )

    grad_ref[...] = jnp.zeros_like(grad_ref)
    for part in range(3 * heads):
        grad_ref[:, part * HEAD_DIM : (part + 1) * HEAD_DIM] = grads[part].astype(bf16)


def attend_params():
    return pltpu.CompilerParams(vmem_limit_bytes=56 * 1024 * 1024)


def attend_whole(qkv, heads, block):
    length = qkv.shape[0]
    width = heads * HEAD_DIM
    return pl.pallas_call(
        functools.partial(attend_kernel, heads, block, HEAD_DIM ** (-0.5)),
        out_shape=[
            shaped(length, width, dtype=bf16),
            shaped(length, width),
            shaped(heads, length, lanes),
        ],
        scratch_shapes=[
            pltpu.VMEM((3 * heads, length, HEAD_DIM), bf16),
            pltpu.VMEM((heads, length, HEAD_DIM), f32),
        ],
        compiler_params=attend_params(),
    )(qkv)


def attend_whole_back(qkv, dout, full, stat, heads, block):
    length = qkv.shape[0]
    return pl.pallas_call(
        functools.partial(attend_back_kernel, heads, block, HEAD_DIM ** (-0.5)),
        out_shape=shaped(*qkv.shape, dtype=bf16),
        scratch_shapes=[
            pltpu.VMEM((3 * heads, length, HEAD_DIM), bf16),
            pltpu.VMEM((heads, length, HEAD_DIM), bf16),
            pltpu.VMEM((heads, length, HEAD_DIM), f32),
            pltpu.VMEM((3 * heads, length, HEAD_DIM), f32),
        ],
        compiler_params=attend_params(),
    )(qkv, dout, full, stat)


def split_blocks(array, block_len):
    shaped_blocks = array.reshape(
        (array.shape[0], array.shape[1] // block_len, block_len) + array.shape[2:]
    )
    return jnp.moveaxis(shaped_blocks, 1, 0)


def general_attention(proj_low, seq_count, block_len, places, any_live, longest):
    model_width = HEADS * HEAD_DIM
    scale = HEAD_DIM ** (-0.5)
    offsets = jnp.arange(block_len, dtype=jnp.int32)
    head_shape = (seq_count, block_len, HEADS, HEAD_DIM)
    query_low = proj_low[:, :model_width].reshape(head_shape)
    keys_low = proj_low[:, model_width : 2 * model_width].reshape(head_shape)
    value_low = proj_low[:, 2 * model_width :].reshape(head_shape)

    def block_scores(queries, keys_block, query_places, key_places):
        scores = (
            jnp.einsum("sqhe,skhe->sqhk", queries, keys_block, preferred_element_type=jnp.float32)
            * scale
        )
        causal_mask = key_places[None, :] <= query_places[:, None]
        return jnp.where(causal_mask[None, :, None, :], scores, masked_score)

    def key_needed(key_first):
        return (key_first <= places[-1]) & ((key_first == places[0]) | any_live)

    stat_shape = (seq_count, block_len, HEADS)
    start_state = (
        jnp.full(stat_shape, masked_score, jnp.float32),
        jnp.zeros(stat_shape, jnp.float32),
        jnp.zeros(head_shape, jnp.float32),
    )
    shard_piece = (
        lax.all_gather(keys_low, "seq", axis=1, tiled=True),
        lax.all_gather(value_low, "seq", axis=1, tiled=True),
    )
    keys_blocks = split_blocks(shard_piece[0], block_len)
    value_blocks = split_blocks(shard_piece[1], block_len)
    firsts = jnp.arange(keys_blocks.shape[0], dtype=jnp.int32) * block_len

    def attend_one_step(state_now, operand):
        keys_block, value_block, key_first = operand

        def attend_work(state_in_block):
            running_max, running_sum, running_out = state_in_block
            scores = block_scores(query_low, keys_block, places, key_first + offsets)
            new_max = jnp.maximum(running_max, jnp.max(scores, axis=-1))
            fade = jnp.exp(running_max - new_max)
            shifted = jnp.exp(scores - new_max[..., None])
            new_sum = running_sum * fade + jnp.sum(shifted, axis=-1)
            new_out = running_out * fade[..., None] + jnp.einsum(
                "sqhk,skhe->sqhe",
                shifted.astype(jnp.bfloat16),
                value_block,
                preferred_element_type=jnp.float32,
            )
            return (new_max, new_sum, new_out)

        return (
            lax.cond(
                key_needed(key_first), attend_work, lambda state_in_block: state_in_block, state_now
            ),
            None,
        )

    result, _ = lax.scan(attend_one_step, start_state, (keys_blocks, value_blocks, firsts))
    running_max, running_sum, running_out = result
    attended = running_out / running_sum[..., None]
    logsum = running_max + jnp.log(running_sum)
    def backward(dout_low):
        delta = jnp.sum(dout_low.astype(jnp.float32) * attended, axis=-1)
        shard_piece = (
            lax.all_gather(keys_low, "seq", axis=1, tiled=True),
            lax.all_gather(value_low, "seq", axis=1, tiled=True),
        )
        keys_blocks = split_blocks(shard_piece[0], block_len)
        value_blocks = split_blocks(shard_piece[1], block_len)
        firsts = jnp.arange(keys_blocks.shape[0], dtype=jnp.int32) * block_len

        def query_one_step(query_grad, operand):
            keys_block, value_block, key_first = operand

            def query_work(grad_now):
                scores = block_scores(query_low, keys_block, places, key_first + offsets)
                soft = jnp.exp(scores - logsum[..., None])
                dprob = jnp.einsum(
                    "sqhe,skhe->sqhk", dout_low, value_block, preferred_element_type=jnp.float32
                )
                dscore = (soft * (dprob - delta[..., None])).astype(jnp.bfloat16)
                return (
                    grad_now
                    + jnp.einsum(
                        "sqhk,skhe->sqhe", dscore, keys_block, preferred_element_type=jnp.float32
                    )
                    * scale
                )

            return (
                lax.cond(key_needed(key_first), query_work, lambda grad_now: grad_now, query_grad),
                None,
            )

        result, _ = lax.scan(
            query_one_step, jnp.zeros(head_shape, jnp.float32), (keys_blocks, value_blocks, firsts)
        )
        query_grad = result
        sent = (query_low.astype(jnp.float32), dout_low.astype(jnp.float32), logsum, delta)
        shard_piece = (
            lax.all_gather(sent[0].astype(jnp.bfloat16), "seq", axis=1, tiled=True).astype(jnp.float32),
            lax.all_gather(sent[1].astype(jnp.bfloat16), "seq", axis=1, tiled=True).astype(jnp.float32),
            lax.all_gather(sent[2].astype(jnp.bfloat16), "seq", axis=1, tiled=True).astype(jnp.float32),
            lax.all_gather(sent[3].astype(jnp.bfloat16), "seq", axis=1, tiled=True).astype(jnp.float32),
        )
        query_blocks = split_blocks(shard_piece[0], block_len)
        dout_blocks = split_blocks(shard_piece[1], block_len)
        logsum_blocks = split_blocks(shard_piece[2], block_len)
        delta_blocks = split_blocks(shard_piece[3], block_len)
        firsts = jnp.arange(query_blocks.shape[0], dtype=jnp.int32) * block_len

        def key_one_step(grads_now, operand):
            query_block, dout_block, logsum_block, delta_block, query_first = operand

            def key_work(grads_in):
                keys_grad, value_grad = grads_in
                query_cast = query_block.astype(jnp.bfloat16)
                dout_cast = dout_block.astype(jnp.bfloat16)
                scores = block_scores(query_cast, keys_low, query_first + offsets, places)
                soft = jnp.exp(scores - logsum_block[..., None])
                value_grad = value_grad + jnp.einsum(
                    "sqhk,sqhe->skhe",
                    soft.astype(jnp.bfloat16),
                    dout_cast,
                    preferred_element_type=jnp.float32,
                )
                dprob = jnp.einsum(
                    "sqhe,skhe->sqhk", dout_cast, value_low, preferred_element_type=jnp.float32
                )
                dscore = (soft * (dprob - delta_block[..., None])).astype(jnp.bfloat16)
                keys_grad = (
                    keys_grad
                    + jnp.einsum(
                        "sqhk,sqhe->skhe", dscore, query_cast, preferred_element_type=jnp.float32
                    )
                    * scale
                )
                return (keys_grad, value_grad)

            needed = (query_first + block_len - 1 >= places[0]) & (
                (query_first == places[0]) | (query_first < longest)
            )
            return (lax.cond(needed, key_work, lambda grads_in: grads_in, grads_now), None)

        result, _ = lax.scan(
            key_one_step,
            (jnp.zeros(head_shape, jnp.float32), jnp.zeros(head_shape, jnp.float32)),
            (query_blocks, dout_blocks, logsum_blocks, delta_blocks, firsts),
        )
        keys_grad, value_grad = result
        return (query_grad, keys_grad, value_grad)

    return attended, backward


def layer_norm(value, gain):
    centred = value - jnp.mean(value, axis=-1, keepdims=True)
    spread_of = jnp.mean(centred * centred, axis=-1, keepdims=True)
    return centred * lax.rsqrt(spread_of + eps) * gain


def gelu_tanh(value):
    return jax.nn.gelu(value, approximate=True)


def dense(left, weight):
    return jnp.dot(left, weight, preferred_element_type=f32)


def dense_back(left, weight, upstream):
    into_left = lax.dot_general(
        upstream, weight, (((1,), (1,)), ((), ())), preferred_element_type=f32
    )
    into_weight = lax.dot_general(
        left, upstream, (((0,), (0,)), ((), ())), preferred_element_type=f32
    ).astype(bf16)
    return (into_left, into_weight)


def shift_mix(extended, taps, value_part):
    step_count = value_part.shape[1]
    reach = taps.shape[1]
    shifted = extended[:, reach - 1 : reach - 1 + step_count] * taps[:, 0]
    for tap_index in range(1, reach):
        shifted = (
            shifted
            + extended[:, reach - 1 - tap_index : reach - 1 - tap_index + step_count]
            * taps[:, tap_index]
        )
    return shifted * value_part


def feed_forward(resid, gain, up_weight, down_weight):
    normed, norm_back = jax.vjp(layer_norm, resid, gain)
    normed_low = normed.astype(bf16)
    hidden = dense(normed_low, up_weight)
    active, active_back = jax.vjp(gelu_tanh, hidden)
    active_low = active.astype(bf16)
    return (
        resid + dense(active_low, down_weight),
        (norm_back, normed_low, active_back, active_low),
    )


def feed_back(stored, up_weight, down_weight, upstream):
    norm_back, normed_low, active_back, active_low = stored
    into_active, down_grad = dense_back(active_low, down_weight, upstream.astype(bf16))
    (into_hidden,) = active_back(into_active)
    into_normed, up_grad = dense_back(normed_low, up_weight, into_hidden.astype(bf16))
    into_resid, gain_grad = norm_back(into_normed)
    return (upstream + into_resid, gain_grad, up_grad, down_grad)


def fold_rows(weight, share):
    rows, width = weight.shape
    fold = rows // share
    return weight.reshape(fold, share, width).transpose(1, 0, 2).reshape(share, fold * width)


def unfold_rows(folded, fold, share):
    rows, width = folded.shape
    width //= fold
    parts = folded.reshape(rows // share, share, fold, width).transpose(0, 2, 1, 3)
    return parts.reshape(rows * fold, width)


def fold_all(weight, share, rows):
    tall, width = weight.shape
    fold = tall // rows
    parts = weight.reshape(rows // share, fold, share, width).transpose(0, 2, 1, 3)
    return parts.reshape(rows, fold * width)


def group_columns(weight, groups, padded):
    rows, columns = weight.shape
    part = columns // 3 // groups
    grouped = weight.reshape(rows, 3, groups, part).transpose(0, 2, 1, 3).reshape(rows, groups, 3 * part)
    return jnp.pad(grouped, ((0, 0), (0, 0), (0, padded - 3 * part))).reshape(rows, groups * padded)


def ungroup_columns(grouped, groups, padded, columns):
    rows = grouped.shape[0]
    part = columns // 3 // groups
    parts = grouped.reshape(rows, groups, padded)[:, :, : 3 * part].reshape(rows, groups, 3, part)
    return parts.transpose(0, 2, 1, 3).reshape(rows, columns)


def cut(array, widths):
    pieces, start = [], 0
    for width in widths:
        pieces.append(array[:, start : start + width])
        start += width
    return pieces


def gathered(parts):
    whole = lax.all_gather(jnp.concatenate(parts, axis=1), everyone, axis=0, tiled=True)
    return cut(whole, [p.shape[1] for p in parts])


def scattered(parts):
    mine = lax.psum_scatter(
        jnp.concatenate(parts, axis=1), everyone, scatter_dimension=0, tiled=True
    )
    return cut(mine, [p.shape[1] for p in parts])


def body(
    tokens,
    cotangent,
    lengths,
    mixer_gain,
    mixer_inputs,
    shift_taps,
    decay_rate,
    state_in,
    state_out,
    state_skip,
    mixer_output,
    first_gain,
    first_up,
    first_down,
    attend_gain,
    attend_inputs,
    attend_output,
    second_gain,
    second_up,
    second_down,
):
    seq_count, block_len, model_width = tokens.shape
    row_count = seq_count * block_len
    seq_devices = lax.axis_size("seq")
    share = mixer_inputs.shape[0]
    states, reach = decay_rate.shape[1], shift_taps.shape[1]
    fold = first_down.shape[0] // share
    deals = seq_count * HEADS
    dealt = deals % seq_devices == 0 and HEADS % (deals // seq_devices) == 0
    heads = deals // seq_devices if dealt else HEADS
    groups = HEADS // heads
    group_width = heads * HEAD_DIM
    padded = -(-3 * group_width // lanes) * lanes if dealt else 3 * group_width

    columns = [decay_rate, state_in, state_out, shift_taps]
    columns += [g[:, None] for g in (mixer_gain, first_gain, attend_gain, second_gain, state_skip)]
    small = jnp.concatenate(columns, axis=1)
    small_count = small.shape[1]
    small_width = -(-small_count // lanes) * lanes
    small = jnp.pad(small, ((0, 0), (0, small_width - small_count)))
    attend_cols = attend_inputs.shape[1]
    grouped = group_columns(attend_inputs, groups, padded)
    by_kernel = seq_devices == 8 and lax.axis_size("batch") == 4
    packed = [mixer_output, first_up, grouped, attend_output, second_up]
    if by_kernel:
        joint = jnp.concatenate([mixer_inputs, small], axis=1)
        w_mixer_out, w_up1, w_attend_in, w_attend_out, w_up2 = gathered(packed)
        widths = (joint.shape[1], model_width, model_width)
        w_joint, w_down1, w_down2 = gather_blocks(
            (joint, first_down, second_down), chunked(widths, (4, 6, 6)), gap=4
        )
        w_mixer_in, w_small = cut(w_joint, [mixer_inputs.shape[1], small_width])
    else:
        w_mixer_in, w_small = gathered([mixer_inputs, small])
        packed += [fold_rows(first_down, share), fold_rows(second_down, share)]
        w_mixer_out, w_up1, w_attend_in, w_attend_out, w_up2, w_down1, w_down2 = gathered(packed)
        w_down1 = unfold_rows(w_down1, fold, share)
        w_down2 = unfold_rows(w_down2, fold, share)

    rows = w_small.T.astype(f32)
    decay, table_in, table_out = rows[:states], rows[states : 2 * states], rows[2 * states : 3 * states]
    taps_rows = rows[3 * states : 3 * states + reach]
    gain_mixer, gain_first, gain_attend, gain_second, skip = (
        rows[3 * states + reach + i] for i in range(5)
    )
    taps = taps_rows.T
    weight = table_in * table_out

    rank_seq = lax.axis_index("seq")
    offsets = jnp.arange(block_len, dtype=jnp.int32)
    places = rank_seq * block_len + offsets
    valid = (places[None, :] < lengths[:, None]).astype(f32)
    longest = jnp.max(lengths)
    any_live = places[0] < longest

    start_resid = tokens.reshape(row_count, model_width).astype(f32)
    normed_mixer, back_mixer = jax.vjp(layer_norm, start_resid, gain_mixer)
    normed_low_mixer = normed_mixer.astype(bf16)
    projected = dense(normed_low_mixer, w_mixer_in).reshape(seq_count, block_len, 3 * model_width)
    query_mixer = projected[:, :, :model_width]
    keys_mixer = projected[:, :, model_width : 2 * model_width]
    value_mixer = projected[:, :, 2 * model_width :]
    rim_rows = passed_along(keys_mixer[:, block_len - reach + 1 :], "seq", 1)
    extended = jnp.concatenate([rim_rows, keys_mixer], axis=1)
    inner, shift_back = jax.vjp(shift_mix, extended, taps, value_mixer)
    carried = carried_in(encode(inner, decay, False), decay, block_len, False)
    wide = shaped(seq_count, block_len, model_width)
    state_y, gated = per_lane_tile(
        output_kernel,
        (inner, query_mixer, carried, decay, weight, skip[None]),
        (wide, wide),
    )
    gated_low = gated.astype(bf16).reshape(row_count, model_width)
    resid_mixer = start_resid + dense(gated_low, w_mixer_out)
    resid_first, stored_first = feed_forward(resid_mixer, gain_first, w_up1, w_down1)

    normed_attend, back_attend = jax.vjp(layer_norm, resid_first, gain_attend)
    normed_low_attend = normed_attend.astype(bf16)
    proj_low = dense(normed_low_attend, w_attend_in).astype(bf16)
    if dealt:
        length = seq_devices * block_len
        block = min(256, length)

        def deal(array, width):
            parts = array.reshape(seq_count, block_len, groups, width).transpose(0, 2, 1, 3)
            parts = parts.reshape(seq_count * groups, block_len, width)
            dealt_parts = lax.all_to_all(parts, "seq", split_axis=0, concat_axis=0, tiled=True)
            return dealt_parts.reshape(length, width)

        def collect(array, width):
            parts = array.reshape(seq_devices, block_len, width)
            back = lax.all_to_all(parts, "seq", split_axis=0, concat_axis=0, tiled=True)
            back = back.reshape(seq_count, groups, block_len, width).transpose(0, 2, 1, 3)
            return back.reshape(row_count, groups * width)

        qkv = deal(proj_low, padded)
        attended_part, attended_full, stat = attend_whole(qkv, heads, block)
        attended_low = collect(attended_part, group_width)
    else:
        attended, attended_back = general_attention(
            proj_low, seq_count, block_len, places, any_live, longest
        )
        attended_low = attended.reshape(row_count, model_width).astype(bf16)
    resid_attend = resid_first + dense(attended_low, w_attend_out)
    final, stored_second = feed_forward(resid_attend, gain_second, w_up2, w_down2)
    mixed = (final.reshape(seq_count, block_len, model_width) * valid[..., None]).astype(bf16)

    upstream = (cotangent.astype(f32) * valid[..., None]).reshape(row_count, model_width)
    upstream, second_gain_grad, second_up_grad, second_down_grad = feed_back(
        stored_second, w_up2, w_down2, upstream
    )
    into_attended, attend_output_grad = dense_back(
        attended_low, w_attend_out, upstream.astype(bf16)
    )
    second_up_out, second_down_out, attend_output_out = scattered(
        [second_up_grad, fold_all(second_down_grad, share, model_width), attend_output_grad]
    )
    dout_low = into_attended.astype(bf16)
    if dealt:
        dout = deal(dout_low, group_width)
        proj_grad = collect(
            attend_whole_back(qkv, dout, attended_full, stat, heads, block), padded
        )
    else:
        parts = attended_back(dout_low.reshape(seq_count, block_len, HEADS, HEAD_DIM))
        proj_grad = jnp.concatenate(
            [p.reshape(row_count, model_width) for p in parts], axis=1
        ).astype(bf16)
    into_normed, attend_inputs_grad = dense_back(normed_low_attend, w_attend_in, proj_grad)
    into_resid, attend_gain_grad = back_attend(into_normed)
    upstream = upstream + into_resid
    upstream, first_gain_grad, first_up_grad, first_down_grad = feed_back(
        stored_first, w_up1, w_down1, upstream
    )
    into_gated, mixer_output_grad = dense_back(gated_low, w_mixer_out, upstream.astype(bf16))
    into_gated = into_gated.reshape(seq_count, block_len, model_width)
    query_mixer_grad = into_gated * state_y
    state_grad = into_gated * query_mixer
    later = carried_in(encode(state_grad, decay, True), decay, block_len, True)
    table = shaped(states, model_width)
    inner_grad, weight_grad, power_grad, skip_grad = per_lane_tile(
        back_kernel,
        (inner, state_grad, carried, later, decay, weight, skip[None]),
        (wide, table, table, shaped(1, model_width)),
        scratch=[pltpu.VMEM((block_len, seq_count, states, lanes), f32)],
    )
    extended_grad, taps_grad, value_mixer_grad = shift_back(inner_grad)
    spill = passed_along(extended_grad[:, : reach - 1], "seq", -1)
    keys_mixer_grad = extended_grad[:, reach - 1 :] + jnp.pad(
        spill, ((0, 0), (block_len - reach + 1, 0), (0, 0))
    )
    proj_grad_mixer = (
        jnp.concatenate([query_mixer_grad, keys_mixer_grad, value_mixer_grad], axis=2)
        .astype(bf16)
        .reshape(row_count, 3 * model_width)
    )
    into_normed_mixer, mixer_inputs_grad = dense_back(normed_low_mixer, w_mixer_in, proj_grad_mixer)
    into_start, mixer_gain_grad = back_mixer(into_normed_mixer)
    tokens_gradient = (upstream + into_start).reshape(seq_count, block_len, model_width).astype(bf16)

    small_rows = jnp.concatenate(
        [-jnp.exp(-decay) * power_grad, weight_grad * table_out, weight_grad * table_in, taps_grad.T]
        + [
            g[None]
            for g in (mixer_gain_grad, first_gain_grad, attend_gain_grad, second_gain_grad, skip_grad[0])
        ],
        axis=0,
    )
    small_grad = jnp.pad(small_rows, ((0, small_width - small_count), (0, 0))).T.astype(bf16)
    def unfolded(folded):
        return folded.reshape(share, fold, model_width).transpose(1, 0, 2).reshape(share * fold, model_width)

    last = [attend_inputs_grad, first_up_grad, mixer_output_grad, mixer_inputs_grad, small_grad]
    if by_kernel:
        last.append(first_down_grad)
        plan = chunked([g.shape[1] for g in last], (4, 4, 2, 4, 2, 4))
        *last, first_down_out = scatter_blocks(last, plan, gap=4)
    else:
        *last, folded = scattered(last + [fold_all(first_down_grad, share, model_width)])
        first_down_out = unfolded(folded)
    attend_inputs_out, first_up_out, mixer_output_out, mixer_inputs_out, small_out = last
    small_out = small_out.astype(f32)
    gains_at = 3 * states + reach
    return (
        mixed,
        tokens_gradient,
        small_out[:, gains_at],
        mixer_inputs_out.astype(f32),
        small_out[:, 3 * states : gains_at],
        small_out[:, :states],
        small_out[:, states : 2 * states],
        small_out[:, 2 * states : 3 * states],
        small_out[:, gains_at + 4],
        mixer_output_out.astype(f32),
        small_out[:, gains_at + 1],
        first_up_out.astype(f32),
        first_down_out.astype(f32),
        small_out[:, gains_at + 2],
        ungroup_columns(attend_inputs_out, groups, padded, attend_cols).astype(f32),
        attend_output_out.astype(f32),
        small_out[:, gains_at + 3],
        second_up_out.astype(f32),
        unfolded(second_down_out).astype(f32),
    )


def solution(mesh):
    return jax.shard_map(
        body,
        mesh=mesh,
        in_specs=(
            P("batch", "seq", None),
            P("batch", "seq", None),
            P("batch"),
            P(("seq", "batch")),
            P(("seq", "batch"), None),
            P(("seq", "batch"), None),
            P(("seq", "batch"), None),
            P(("seq", "batch"), None),
            P(("seq", "batch"), None),
            P(("seq", "batch")),
            P(("seq", "batch"), None),
            P(("seq", "batch")),
            P(("seq", "batch"), None),
            P(("seq", "batch"), None),
            P(("seq", "batch")),
            P(("seq", "batch"), None),
            P(("seq", "batch"), None),
            P(("seq", "batch")),
            P(("seq", "batch"), None),
            P(("seq", "batch"), None),
        ),
        out_specs=(
            P("batch", "seq", None),
            P("batch", "seq", None),
            P(("seq", "batch")),
            P(("seq", "batch"), None),
            P(("seq", "batch"), None),
            P(("seq", "batch"), None),
            P(("seq", "batch"), None),
            P(("seq", "batch"), None),
            P(("seq", "batch")),
            P(("seq", "batch"), None),
            P(("seq", "batch")),
            P(("seq", "batch"), None),
            P(("seq", "batch"), None),
            P(("seq", "batch")),
            P(("seq", "batch"), None),
            P(("seq", "batch"), None),
            P(("seq", "batch")),
            P(("seq", "batch"), None),
            P(("seq", "batch"), None),
        ),
        check_vma=False,
    )
```

```python
import functools

import jax
import jax.numpy as jnp
from jax import lax
from jax.experimental import pallas as pl
from jax.experimental.pallas import tpu as pltpu
from jax.sharding import PartitionSpec as P

HEADS = 12
HEAD_DIM = 64

eps = 1e-05
masked_score = -1e30
lanes = 128
sublanes = 8
everyone = ("seq", "batch")
f32 = jnp.float32
bf16 = jnp.bfloat16


def rows_of(ref, seq, block):
    return ref[seq, pl.ds(pl.multiple_of(block * sublanes, sublanes), sublanes), :]


def spread(rows, index, count):
    return jnp.broadcast_to(rows[index : index + 1], (count, lanes))


def encode_kernel(reverse, input_ref, decay_ref, end_ref):
    seq_count, step_count, _ = input_ref.shape
    state_count = decay_ref.shape[0]
    blocks = step_count // sublanes
    power = jnp.exp(-decay_ref[...])

    def one_block(step, states):
        block = blocks - 1 - step if reverse else step
        rows = [rows_of(input_ref, seq, block) for seq in range(seq_count)]
        order = range(sublanes - 1, -1, -1) if reverse else range(sublanes)
        states = list(states)
        for index in order:
            for seq in range(seq_count):
                states[seq] = states[seq] * power + spread(rows[seq], index, state_count)
        return tuple(states)

    start = tuple(jnp.zeros((state_count, lanes), f32) for _ in range(seq_count))
    ends = lax.fori_loop(0, blocks, one_block, start)
    for seq in range(seq_count):
        end_ref[seq] = ends[seq]


def output_kernel(input_ref, query_ref, carried_ref, decay_ref, weight_ref, skip_ref, out_ref, gated_ref):
    seq_count, step_count, _ = input_ref.shape
    state_count = decay_ref.shape[0]
    power = jnp.exp(-decay_ref[...])
    weight = weight_ref[...]
    skip = skip_ref[...]

    def one_block(block, states):
        states = list(states)
        rows = [rows_of(input_ref, seq, block) for seq in range(seq_count)]
        found = [[] for _ in range(seq_count)]
        for index in range(sublanes):
            for seq in range(seq_count):
                states[seq] = states[seq] * power + spread(rows[seq], index, state_count)
                found[seq].append(jnp.sum(states[seq] * weight, axis=0, keepdims=True))
        place = pl.ds(pl.multiple_of(block * sublanes, sublanes), sublanes)
        for seq in range(seq_count):
            result = jnp.concatenate(found[seq], axis=0) + skip * rows[seq]
            out_ref[seq, place, :] = result
            gated_ref[seq, place, :] = result * rows_of(query_ref, seq, block)
        return tuple(states)

    start = tuple(carried_ref[seq].astype(f32) for seq in range(seq_count))
    lax.fori_loop(0, step_count // sublanes, one_block, start)


def back_kernel(
    input_ref,
    grad_ref,
    carried_ref,
    later_ref,
    decay_ref,
    weight_ref,
    skip_ref,
    input_grad_ref,
    weight_grad_ref,
    power_grad_ref,
    skip_grad_ref,
    held,
):
    seq_count, step_count, _ = input_ref.shape
    state_count = decay_ref.shape[0]
    blocks = step_count // sublanes
    power = jnp.exp(-decay_ref[...])
    weight = weight_ref[...]
    skip = skip_ref[...]
    seqs = range(seq_count)

    def forward_block(block, state):
        states, total, skip_total = list(state[0]), state[1], state[2]
        rows = [rows_of(input_ref, seq, block) for seq in seqs]
        grads = [rows_of(grad_ref, seq, block) for seq in seqs]
        for index in range(sublanes):
            for seq in seqs:
                held[block * sublanes + index, seq] = states[seq]
                states[seq] = states[seq] * power + spread(rows[seq], index, state_count)
                total = total + states[seq] * spread(grads[seq], index, state_count)
        for seq in seqs:
            skip_total = skip_total + rows[seq] * grads[seq]
        return (tuple(states), total, skip_total)

    zeros = jnp.zeros((state_count, lanes), f32)
    _, total, skip_total = lax.fori_loop(
        0,
        blocks,
        forward_block,
        (
            tuple(carried_ref[seq].astype(f32) for seq in seqs),
            zeros,
            jnp.zeros((sublanes, lanes), f32),
        ),
    )
    weight_grad_ref[...] = total
    skip_grad_ref[...] = jnp.sum(skip_total, axis=0, keepdims=True)

    def back_block(step, state):
        states, total = list(state[0]), state[1]
        block = blocks - 1 - step
        grads = [rows_of(grad_ref, seq, block) for seq in seqs]
        found = [[None] * sublanes for _ in seqs]
        for index in range(sublanes - 1, -1, -1):
            for seq in seqs:
                states[seq] = states[seq] * power + spread(grads[seq], index, state_count)
                found[seq][index] = jnp.sum(states[seq] * weight, axis=0, keepdims=True)
                total = total + states[seq] * held[block * sublanes + index, seq]
        place = pl.ds(pl.multiple_of(block * sublanes, sublanes), sublanes)
        for seq in seqs:
            input_grad_ref[seq, place, :] = jnp.concatenate(found[seq], axis=0) + skip * grads[seq]
        return (tuple(states), total)

    _, total = lax.fori_loop(
        0, blocks, back_block, (tuple(later_ref[seq].astype(f32) for seq in seqs), zeros)
    )
    power_grad_ref[...] = total * weight


def per_lane_tile(kernel, args, outs, scratch=(), flops=0):
    def spec(shape):
        lead = len(shape) - 1
        return pl.BlockSpec(tuple(shape[:-1]) + (lanes,), lambda tile: (0,) * lead + (tile,))

    bytes_moved = sum(a.size * a.dtype.itemsize for a in args)
    return pl.pallas_call(
        kernel,
        grid=(args[0].shape[-1] // lanes,),
        in_specs=[spec(a.shape) for a in args],
        out_specs=[spec(o.shape) for o in outs],
        out_shape=list(outs),
        scratch_shapes=list(scratch),
        cost_estimate=pl.CostEstimate(flops=flops, bytes_accessed=bytes_moved, transcendentals=0),
        compiler_params=pltpu.CompilerParams(vmem_limit_bytes=48 * 1024 * 1024),
    )(*args)


def shaped(*dims, dtype=f32):
    return jax.ShapeDtypeStruct(dims, dtype)


def encode(value, decay, reverse):
    seq_count, _, width = value.shape
    (ends,) = per_lane_tile(
        functools.partial(encode_kernel, reverse),
        (value, decay),
        (shaped(seq_count, decay.shape[0], width),),
    )
    return ends


def passed_along(block, axis, distance):
    devices = range(lax.axis_size(axis))
    route = [(i - distance, i) for i in devices if i - distance in devices]
    return lax.ppermute(block, axis, route)


def carried_in(ends, decay, block_len, reverse):
    seq_count, state_count, width = ends.shape
    count = lax.axis_size("seq")
    part = state_count // count

    def exchanged(parts):
        return lax.all_to_all(parts.astype(bf16), "seq", split_axis=0, concat_axis=0, tiled=True)

    parts = ends.reshape(seq_count, count, part, width).transpose(1, 0, 2, 3)
    arrived = exchanged(parts.reshape(count, seq_count * part, width)).astype(f32)
    rates = lax.dynamic_slice_in_dim(decay, lax.axis_index("seq") * part, part, 0)
    power = jnp.tile(jnp.exp(-rates * block_len), (seq_count, 1))
    state, joined = jnp.zeros_like(arrived[0]), [None] * count
    for block in reversed(range(count)) if reverse else range(count):
        joined[block] = state
        state = power * state + arrived[block]
    back = exchanged(jnp.stack(joined))
    back = back.reshape(count, seq_count, part, width).transpose(1, 0, 2, 3)
    return back.reshape(seq_count, state_count, width)


MESH = pl.DeviceIdType.MESH
box = (4, 2, 2, 2)


def here():
    seq, batch = lax.axis_index("seq"), lax.axis_index("batch")
    return lax.div(seq, 2), lax.rem(seq, 2), lax.div(batch, 2), lax.rem(batch, 2)


def device(z, x, y, core):
    return (2 * z + x, 2 * y + core)


def line_peer(z, step):
    return lax.rem(z + step, box[0])


def greet():
    z, x, y, core = here()
    barrier = pltpu.get_barrier_semaphore()
    peers = [device(line_peer(z, step), x, y, core) for step in range(1, box[0])]
    peers += [device(z, 1 - x, y, core), device(z, x, 1 - y, core), device(z, x, y, 1 - core)]
    for peer in peers:
        pl.semaphore_signal(barrier, inc=1, device_id=peer, device_id_type=MESH)
    pl.semaphore_wait(barrier, len(peers))


def staggered(count, stages, gap):
    for turn in range(count + gap * (stages - 1)):
        for stage in reversed(range(stages)):
            chunk = turn - gap * stage
            if 0 <= chunk < count:
                yield stage, chunk


def gather_kernel(plan, gap, *refs):
    count = 1 + max(item[0] for item in plan)
    ins, outs = refs[:count], refs[count : 2 * count]
    send, receive, local = refs[2 * count :]
    z, x, y, core = here()
    greet()
    started = {}

    def push(chunk, slot, source, target, peer):
        copy = pltpu.make_async_remote_copy(
            src_ref=source,
            dst_ref=target,
            send_sem=send.at[chunk, slot],
            recv_sem=receive.at[chunk, slot],
            device_id=peer,
            device_id_type=MESH,
        )
        copy.start()
        started[chunk, slot] = copy

    own = []
    for chunk, (index, first, width, x_first) in enumerate(plan):
        columns = pl.ds(first, width)
        source = ins[index].at[:, columns]
        target = outs[index].at[z, x, y, core, :, columns]
        for step in range(1, box[0]):
            push(chunk, step - 1, source, target, device(line_peer(z, step), x, y, core))
        keep = pltpu.make_async_copy(source, target, local.at[chunk])
        keep.start()
        own.append(keep)

    for stage, chunk in staggered(len(plan), 3, gap):
        index, first, width, x_first = plan[chunk]
        columns = pl.ds(first, width)
        out = outs[index]
        if stage == 0:
            for step in range(1, box[0]):
                started[chunk, step - 1].wait_recv()
            own[chunk].wait()
            part = out.at[:, x, y, core, :, columns]
            peer = device(z, 1 - x, y, core) if x_first else device(z, x, 1 - y, core)
            push(chunk, 3, part, part, peer)
        elif stage == 1:
            started[chunk, 3].wait_recv()
            if x_first:
                part, peer = out.at[:, :, y, core, :, columns], device(z, x, 1 - y, core)
            else:
                part, peer = out.at[:, x, :, core, :, columns], device(z, 1 - x, y, core)
            push(chunk, 4, part, part, peer)
        else:
            started[chunk, 4].wait_recv()
            part = out.at[:, :, :, core, :, columns]
            push(chunk, 5, part, part, device(z, x, y, 1 - core))
    for chunk in range(len(plan)):
        started[chunk, 5].wait_recv()
        for slot in range(6):
            started[chunk, slot].wait_send()


def gather_blocks(blocks, plan, gap=2, collective=0):
    outs = [jax.ShapeDtypeStruct(box + b.shape, b.dtype) for b in blocks]
    sent = sum(b.size * b.dtype.itemsize for b in blocks)
    whole = pl.pallas_call(
        functools.partial(gather_kernel, plan, gap),
        out_shape=outs,
        in_specs=[pl.BlockSpec(memory_space=pltpu.VMEM)] * len(blocks),
        out_specs=[pl.BlockSpec(memory_space=pl.ANY)] * len(blocks),
        scratch_shapes=[
            pltpu.SemaphoreType.DMA((len(plan), 6)),
            pltpu.SemaphoreType.DMA((len(plan), 6)),
            pltpu.SemaphoreType.DMA((len(plan),)),
        ],
        cost_estimate=pl.CostEstimate(flops=0, bytes_accessed=64 * sent, transcendentals=0),
        compiler_params=pltpu.CompilerParams(collective_id=collective, has_side_effects=True),
    )(*blocks)
    return [w.reshape((32 * w.shape[4], w.shape[5])) for w in whole]


def add_into(total, other):
    return (total.astype(f32) + other.astype(f32)).astype(bf16)


def scatter_kernel(plan, gap, finish, counts, *refs):
    count, out_count = counts
    ins, results = refs[:count], refs[count : count + out_count]
    outs, buffers = refs[count + out_count : 2 * count + out_count], refs[2 * count + out_count : -3]
    send, receive, local = refs[-3:]
    z, x, y, core = here()
    greet()
    started = {}

    def push(chunk, slot, source, target, peer):
        copy = pltpu.make_async_remote_copy(
            src_ref=source,
            dst_ref=target,
            send_sem=send.at[chunk, slot],
            recv_sem=receive.at[chunk, slot],
            device_id=peer,
            device_id_type=MESH,
        )
        copy.start()
        started[chunk, slot] = copy

    loads = []
    for chunk, (index, first, width, _) in enumerate(plan):
        columns = pl.ds(first, width)
        held, from_core = buffers[5 * chunk : 5 * chunk + 2]
        grad = ins[index]
        push(chunk, 0, grad.at[:, :, :, 1 - core, :, columns], from_core, device(z, x, y, 1 - core))
        load = pltpu.make_async_copy(grad.at[:, :, :, core, :, columns], held, local.at[chunk])
        load.start()
        loads.append(load)

    for stage, chunk in staggered(len(plan), 4, gap):
        index, first, width, x_first = plan[chunk]
        held, from_core, from_one, from_two, from_line = buffers[5 * chunk : 5 * chunk + 5]
        to_x, to_y = device(z, 1 - x, y, core), device(z, x, 1 - y, core)
        if stage == 0:
            started[chunk, 0].wait_recv()
            loads[chunk].wait()

            @pl.loop(0, box[0])
            def _(row):
                for i in range(2):
                    for j in range(2):
                        held[row, i, j] = add_into(held[row, i, j], from_core[row, i, j])

            if x_first:
                push(chunk, 1, held.at[:, :, 1 - y], from_one, to_y)
            else:
                push(chunk, 1, held.at[:, 1 - x], from_one, to_x)
        elif stage == 1:
            started[chunk, 1].wait_recv()

            @pl.loop(0, box[0])
            def _(row):
                for i in range(2):
                    if x_first:
                        held[row, i, y] = add_into(held[row, i, y], from_one[row, i])
                    else:
                        held[row, x, i] = add_into(held[row, x, i], from_one[row, i])

            if x_first:
                push(chunk, 2, held.at[:, 1 - x, y], from_two, to_x)
            else:
                push(chunk, 2, held.at[:, x, 1 - y], from_two, to_y)
        elif stage == 2:
            started[chunk, 2].wait_recv()

            @pl.loop(0, box[0])
            def _(row):
                held[row, x, y] = add_into(held[row, x, y], from_two[row])

            for step in range(1, box[0]):
                peer = line_peer(z, step)
                push(chunk, 2 + step, held.at[peer, x, y], from_line.at[step - 1], device(peer, x, y, core))
        else:
            total = held[z, x, y].astype(f32)
            for step in range(1, box[0]):
                started[chunk, 2 + step].wait_recv()
                total = total + from_line[step - 1].astype(f32)
            outs[index][:, pl.ds(first, width)] = total
            if not any(item[0] == index for item in plan[chunk + 1 :]):
                finish(index, outs[index], results)
    for chunk in range(len(plan)):
        for slot in range(6):
            started[chunk, slot].wait_send()


def scatter_blocks(grads, plan, finish, results, gap=2, collective=1):
    views = [g.reshape(box + (g.shape[0] // 32, g.shape[1])) for g in grads]
    scratch = [pltpu.VMEM(v.shape[4:], f32) for v in views]
    for index, _, width, _ in plan:
        tile = (views[index].shape[4], width)
        for lead in ((4, 2, 2), (4, 2, 2), (4, 2), (4,), (3,)):
            scratch.append(pltpu.VMEM(lead + tile, bf16))
    sent = sum(v.size * v.dtype.itemsize for v in views)
    return pl.pallas_call(
        functools.partial(scatter_kernel, plan, gap, finish, (len(views), len(results))),
        out_shape=list(results),
        in_specs=[pl.BlockSpec(memory_space=pl.ANY)] * len(views),
        out_specs=[pl.BlockSpec(memory_space=pltpu.VMEM)] * len(results),
        scratch_shapes=scratch
        + [
            pltpu.SemaphoreType.DMA((len(plan), 6)),
            pltpu.SemaphoreType.DMA((len(plan), 6)),
            pltpu.SemaphoreType.DMA((len(plan),)),
        ],
        cost_estimate=pl.CostEstimate(flops=0, bytes_accessed=4 * sent, transcendentals=0),
        compiler_params=pltpu.CompilerParams(
            collective_id=collective, has_side_effects=True, vmem_limit_bytes=60 * 1024 * 1024
        ),
    )(*views)


def chunked(widths, pieces):
    plan = []
    for index, (width, number) in enumerate(zip(widths, pieces)):
        tiles = width // lanes
        edges = [tiles * i // number for i in range(number + 1)]
        for i in range(number):
            plan.append((index, edges[i] * lanes, (edges[i + 1] - edges[i]) * lanes, len(plan) % 2 == 0))
    return plan


def split_heads(ref, scratch, heads, parts, first=0):
    for part in range(parts):
        for head in range(heads):
            start = (part * heads + head) * HEAD_DIM + first
            scratch[part * heads + head] = ref[:, start : start + HEAD_DIM]


def score_block(query, keys, first, scale):
    scores = (
        lax.dot_general(query, keys, (((1,), (1,)), ((), ())), preferred_element_type=f32) * scale
    )
    rows = lax.broadcasted_iota(jnp.int32, scores.shape, 0) + first
    columns = lax.broadcasted_iota(jnp.int32, scores.shape, 1)
    return jnp.where(columns <= rows, scores, masked_score)


def attend_kernel(heads, block, scale, qkv_ref, low_ref, full_ref, stat_ref, parts, outs):
    length = qkv_ref.shape[0]
    split_heads(qkv_ref, parts, heads, 3)

    @pl.loop(0, heads)
    def _(head):
        for first in range(0, length, block):
            extent = first + block
            query = parts[head, first:extent, :]
            scores = score_block(query, parts[heads + head, :extent, :], first, scale)
            top = jnp.max(scores, axis=1, keepdims=True)
            soft = jnp.exp(scores - top)
            whole = jnp.sum(soft, axis=1, keepdims=True)
            soft = soft * (1.0 / whole)
            outs[head, first:extent, :] = jnp.dot(
                soft.astype(bf16), parts[2 * heads + head, :extent, :], preferred_element_type=f32
            )
            stat_ref[head, first:extent, :] = jnp.broadcast_to(top + jnp.log(whole), (block, lanes))

    if low_ref.shape[1] > heads * HEAD_DIM:
        low_ref[:, heads * HEAD_DIM :] = jnp.zeros((length, low_ref.shape[1] - heads * HEAD_DIM), bf16)
    for head in range(heads):
        place = slice(head * HEAD_DIM, (head + 1) * HEAD_DIM)
        full_ref[:, place] = outs[head]
        low_ref[:, place] = outs[head].astype(bf16)


def attend_back_kernel(
    heads, block, scale, qkv_ref, dout_ref, full_ref, stat_ref, grad_ref, parts, douts, fulls, grads
):
    length = qkv_ref.shape[0]
    split_heads(qkv_ref, parts, heads, 3)
    split_heads(dout_ref, douts, heads, 1)
    split_heads(full_ref, fulls, heads, 1)
    grads[...] = jnp.zeros_like(grads)

    @pl.loop(0, heads)
    def _(head):
        for first in range(0, length, block):
            extent = first + block
            query = parts[head, first:extent, :]
            keys = parts[heads + head, :extent, :]
            value = parts[2 * heads + head, :extent, :]
            dout = douts[head, first:extent, :]
            delta = jnp.sum(dout.astype(f32) * fulls[head, first:extent, :], axis=1, keepdims=True)
            scores = score_block(query, keys, first, scale)
            soft = jnp.exp(scores - stat_ref[head, first:extent, :1])
            across = (((1,), (1,)), ((), ()))
            along = (((0,), (0,)), ((), ()))
            dprob = lax.dot_general(dout, value, across, preferred_element_type=f32)
            dscore = (soft * (dprob - delta) * scale).astype(bf16)
            grads[head, first:extent, :] = jnp.dot(dscore, keys, preferred_element_type=f32)
            grads[heads + head, :extent, :] += lax.dot_general(
                dscore, query, along, preferred_element_type=f32
            )
            grads[2 * heads + head, :extent, :] += lax.dot_general(
                soft.astype(bf16), dout, along, preferred_element_type=f32
            )

    grad_ref[...] = jnp.zeros_like(grad_ref)
    for part in range(3 * heads):
        grad_ref[:, part * HEAD_DIM : (part + 1) * HEAD_DIM] = grads[part].astype(bf16)


def attend_params():
    return pltpu.CompilerParams(vmem_limit_bytes=56 * 1024 * 1024)


def attend_whole(qkv, heads, block):
    length = qkv.shape[0]
    width = heads * HEAD_DIM
    return pl.pallas_call(
        functools.partial(attend_kernel, heads, block, HEAD_DIM ** (-0.5)),
        out_shape=[
            shaped(length, -(-width // lanes) * lanes, dtype=bf16),
            shaped(length, width),
            shaped(heads, length, lanes),
        ],
        scratch_shapes=[
            pltpu.VMEM((3 * heads, length, HEAD_DIM), bf16),
            pltpu.VMEM((heads, length, HEAD_DIM), f32),
        ],
        compiler_params=attend_params(),
    )(qkv)


def attend_whole_back(qkv, dout, full, stat, heads, block):
    length = qkv.shape[0]
    return pl.pallas_call(
        functools.partial(attend_back_kernel, heads, block, HEAD_DIM ** (-0.5)),
        out_shape=shaped(*qkv.shape, dtype=bf16),
        scratch_shapes=[
            pltpu.VMEM((3 * heads, length, HEAD_DIM), bf16),
            pltpu.VMEM((heads, length, HEAD_DIM), bf16),
            pltpu.VMEM((heads, length, HEAD_DIM), f32),
            pltpu.VMEM((3 * heads, length, HEAD_DIM), f32),
        ],
        compiler_params=attend_params(),
    )(qkv, dout, full, stat)


def split_blocks(array, block_len):
    shaped_blocks = array.reshape(
        (array.shape[0], array.shape[1] // block_len, block_len) + array.shape[2:]
    )
    return jnp.moveaxis(shaped_blocks, 1, 0)


def general_attention(proj_low, seq_count, block_len, places, any_live, longest):
    model_width = HEADS * HEAD_DIM
    scale = HEAD_DIM ** (-0.5)
    offsets = jnp.arange(block_len, dtype=jnp.int32)
    head_shape = (seq_count, block_len, HEADS, HEAD_DIM)
    query_low = proj_low[:, :model_width].reshape(head_shape)
    keys_low = proj_low[:, model_width : 2 * model_width].reshape(head_shape)
    value_low = proj_low[:, 2 * model_width :].reshape(head_shape)

    def block_scores(queries, keys_block, query_places, key_places):
        scores = (
            jnp.einsum("sqhe,skhe->sqhk", queries, keys_block, preferred_element_type=jnp.float32)
            * scale
        )
        causal_mask = key_places[None, :] <= query_places[:, None]
        return jnp.where(causal_mask[None, :, None, :], scores, masked_score)

    def key_needed(key_first):
        return (key_first <= places[-1]) & ((key_first == places[0]) | any_live)

    stat_shape = (seq_count, block_len, HEADS)
    start_state = (
        jnp.full(stat_shape, masked_score, jnp.float32),
        jnp.zeros(stat_shape, jnp.float32),
        jnp.zeros(head_shape, jnp.float32),
    )
    shard_piece = (
        lax.all_gather(keys_low, "seq", axis=1, tiled=True),
        lax.all_gather(value_low, "seq", axis=1, tiled=True),
    )
    keys_blocks = split_blocks(shard_piece[0], block_len)
    value_blocks = split_blocks(shard_piece[1], block_len)
    firsts = jnp.arange(keys_blocks.shape[0], dtype=jnp.int32) * block_len

    def attend_one_step(state_now, operand):
        keys_block, value_block, key_first = operand

        def attend_work(state_in_block):
            running_max, running_sum, running_out = state_in_block
            scores = block_scores(query_low, keys_block, places, key_first + offsets)
            new_max = jnp.maximum(running_max, jnp.max(scores, axis=-1))
            fade = jnp.exp(running_max - new_max)
            shifted = jnp.exp(scores - new_max[..., None])
            new_sum = running_sum * fade + jnp.sum(shifted, axis=-1)
            new_out = running_out * fade[..., None] + jnp.einsum(
                "sqhk,skhe->sqhe",
                shifted.astype(jnp.bfloat16),
                value_block,
                preferred_element_type=jnp.float32,
            )
            return (new_max, new_sum, new_out)

        return (
            lax.cond(
                key_needed(key_first), attend_work, lambda state_in_block: state_in_block, state_now
            ),
            None,
        )

    result, _ = lax.scan(attend_one_step, start_state, (keys_blocks, value_blocks, firsts))
    running_max, running_sum, running_out = result
    attended = running_out / running_sum[..., None]
    logsum = running_max + jnp.log(running_sum)
    def backward(dout_low):
        delta = jnp.sum(dout_low.astype(jnp.float32) * attended, axis=-1)
        shard_piece = (
            lax.all_gather(keys_low, "seq", axis=1, tiled=True),
            lax.all_gather(value_low, "seq", axis=1, tiled=True),
        )
        keys_blocks = split_blocks(shard_piece[0], block_len)
        value_blocks = split_blocks(shard_piece[1], block_len)
        firsts = jnp.arange(keys_blocks.shape[0], dtype=jnp.int32) * block_len

        def query_one_step(query_grad, operand):
            keys_block, value_block, key_first = operand

            def query_work(grad_now):
                scores = block_scores(query_low, keys_block, places, key_first + offsets)
                soft = jnp.exp(scores - logsum[..., None])
                dprob = jnp.einsum(
                    "sqhe,skhe->sqhk", dout_low, value_block, preferred_element_type=jnp.float32
                )
                dscore = (soft * (dprob - delta[..., None])).astype(jnp.bfloat16)
                return (
                    grad_now
                    + jnp.einsum(
                        "sqhk,skhe->sqhe", dscore, keys_block, preferred_element_type=jnp.float32
                    )
                    * scale
                )

            return (
                lax.cond(key_needed(key_first), query_work, lambda grad_now: grad_now, query_grad),
                None,
            )

        result, _ = lax.scan(
            query_one_step, jnp.zeros(head_shape, jnp.float32), (keys_blocks, value_blocks, firsts)
        )
        query_grad = result
        sent = (query_low.astype(jnp.float32), dout_low.astype(jnp.float32), logsum, delta)
        shard_piece = (
            lax.all_gather(sent[0].astype(jnp.bfloat16), "seq", axis=1, tiled=True).astype(jnp.float32),
            lax.all_gather(sent[1].astype(jnp.bfloat16), "seq", axis=1, tiled=True).astype(jnp.float32),
            lax.all_gather(sent[2].astype(jnp.bfloat16), "seq", axis=1, tiled=True).astype(jnp.float32),
            lax.all_gather(sent[3].astype(jnp.bfloat16), "seq", axis=1, tiled=True).astype(jnp.float32),
        )
        query_blocks = split_blocks(shard_piece[0], block_len)
        dout_blocks = split_blocks(shard_piece[1], block_len)
        logsum_blocks = split_blocks(shard_piece[2], block_len)
        delta_blocks = split_blocks(shard_piece[3], block_len)
        firsts = jnp.arange(query_blocks.shape[0], dtype=jnp.int32) * block_len

        def key_one_step(grads_now, operand):
            query_block, dout_block, logsum_block, delta_block, query_first = operand

            def key_work(grads_in):
                keys_grad, value_grad = grads_in
                query_cast = query_block.astype(jnp.bfloat16)
                dout_cast = dout_block.astype(jnp.bfloat16)
                scores = block_scores(query_cast, keys_low, query_first + offsets, places)
                soft = jnp.exp(scores - logsum_block[..., None])
                value_grad = value_grad + jnp.einsum(
                    "sqhk,sqhe->skhe",
                    soft.astype(jnp.bfloat16),
                    dout_cast,
                    preferred_element_type=jnp.float32,
                )
                dprob = jnp.einsum(
                    "sqhe,skhe->sqhk", dout_cast, value_low, preferred_element_type=jnp.float32
                )
                dscore = (soft * (dprob - delta_block[..., None])).astype(jnp.bfloat16)
                keys_grad = (
                    keys_grad
                    + jnp.einsum(
                        "sqhk,sqhe->skhe", dscore, query_cast, preferred_element_type=jnp.float32
                    )
                    * scale
                )
                return (keys_grad, value_grad)

            needed = (query_first + block_len - 1 >= places[0]) & (
                (query_first == places[0]) | (query_first < longest)
            )
            return (lax.cond(needed, key_work, lambda grads_in: grads_in, grads_now), None)

        result, _ = lax.scan(
            key_one_step,
            (jnp.zeros(head_shape, jnp.float32), jnp.zeros(head_shape, jnp.float32)),
            (query_blocks, dout_blocks, logsum_blocks, delta_blocks, firsts),
        )
        keys_grad, value_grad = result
        return (query_grad, keys_grad, value_grad)

    return attended, backward


def layer_norm(value, gain):
    centred = value - jnp.mean(value, axis=-1, keepdims=True)
    spread_of = jnp.mean(centred * centred, axis=-1, keepdims=True)
    return centred * lax.rsqrt(spread_of + eps) * gain


def gelu_tanh(value):
    return jax.nn.gelu(value, approximate=True)


def dense(left, weight):
    return jnp.dot(left, weight, preferred_element_type=f32)


def dense_back(left, weight, upstream):
    into_left = lax.dot_general(
        upstream, weight, (((1,), (1,)), ((), ())), preferred_element_type=f32
    )
    into_weight = lax.dot_general(
        left, upstream, (((0,), (0,)), ((), ())), preferred_element_type=f32
    ).astype(bf16)
    return (into_left, into_weight)


def shift_mix(extended, taps, value_part):
    step_count = value_part.shape[1]
    reach = taps.shape[1]
    shifted = extended[:, reach - 1 : reach - 1 + step_count] * taps[:, 0]
    for tap_index in range(1, reach):
        shifted = (
            shifted
            + extended[:, reach - 1 - tap_index : reach - 1 - tap_index + step_count]
            * taps[:, tap_index]
        )
    return shifted * value_part


def feed_forward(resid, gain, up_weight, down_weight):
    normed, norm_back = jax.vjp(layer_norm, resid, gain)
    normed_low = normed.astype(bf16)
    hidden = dense(normed_low, up_weight)
    active, active_back = jax.vjp(gelu_tanh, hidden)
    active_low = active.astype(bf16)
    return (
        resid + dense(active_low, down_weight),
        (norm_back, normed_low, active_back, active_low),
    )


def feed_back(stored, up_weight, down_weight, upstream):
    norm_back, normed_low, active_back, active_low = stored
    into_active, down_grad = dense_back(active_low, down_weight, upstream.astype(bf16))
    (into_hidden,) = active_back(into_active)
    into_normed, up_grad = dense_back(normed_low, up_weight, into_hidden.astype(bf16))
    into_resid, gain_grad = norm_back(into_normed)
    return (upstream + into_resid, gain_grad, up_grad, down_grad)


def fold_rows(weight, share):
    rows, width = weight.shape
    fold = rows // share
    return weight.reshape(fold, share, width).transpose(1, 0, 2).reshape(share, fold * width)


def unfold_rows(folded, fold, share):
    rows, width = folded.shape
    width //= fold
    parts = folded.reshape(rows // share, share, fold, width).transpose(0, 2, 1, 3)
    return parts.reshape(rows * fold, width)


def fold_all(weight, share, rows):
    tall, width = weight.shape
    fold = tall // rows
    parts = weight.reshape(rows // share, fold, share, width).transpose(0, 2, 1, 3)
    return parts.reshape(rows, fold * width)


def group_columns(weight, groups, padded):
    rows, columns = weight.shape
    part = columns // 3 // groups
    grouped = weight.reshape(rows, 3, groups, part).transpose(0, 2, 1, 3).reshape(rows, groups, 3 * part)
    return jnp.pad(grouped, ((0, 0), (0, 0), (0, padded - 3 * part))).reshape(rows, groups * padded)


def pad_groups(weight, groups, padded):
    rows, columns = weight.shape
    part = rows // groups
    grouped = weight.reshape(groups, part, columns)
    return jnp.pad(grouped, ((0, 0), (0, padded - part), (0, 0))).reshape(groups * padded, columns)


def ungroup_columns(grouped, groups, padded, columns):
    rows = grouped.shape[0]
    part = columns // 3 // groups
    parts = grouped.reshape(rows, groups, padded)[:, :, : 3 * part].reshape(rows, groups, 3, part)
    return parts.transpose(0, 2, 1, 3).reshape(rows, columns)


def cut(array, widths):
    pieces, start = [], 0
    for width in widths:
        pieces.append(array[:, start : start + width])
        start += width
    return pieces


def cut_last(array, count):
    width = array.shape[-1] // count
    return [array[..., i * width : (i + 1) * width] for i in range(count)]


def gathered(parts):
    whole = lax.all_gather(jnp.concatenate(parts, axis=1), everyone, axis=0, tiled=True)
    return cut(whole, [p.shape[1] for p in parts])


def scattered(parts):
    mine = lax.psum_scatter(
        jnp.concatenate(parts, axis=1), everyone, scatter_dimension=0, tiled=True
    )
    return cut(mine, [p.shape[1] for p in parts])


def body(
    tokens,
    cotangent,
    lengths,
    mixer_gain,
    mixer_inputs,
    shift_taps,
    decay_rate,
    state_in,
    state_out,
    state_skip,
    mixer_output,
    first_gain,
    first_up,
    first_down,
    attend_gain,
    attend_inputs,
    attend_output,
    second_gain,
    second_up,
    second_down,
):
    seq_count, block_len, model_width = tokens.shape
    row_count = seq_count * block_len
    seq_devices = lax.axis_size("seq")
    share = mixer_inputs.shape[0]
    states, reach = decay_rate.shape[1], shift_taps.shape[1]
    fold = first_down.shape[0] // share
    deals = seq_count * HEADS
    dealt = deals % seq_devices == 0 and HEADS % (deals // seq_devices) == 0
    heads = deals // seq_devices if dealt else HEADS
    groups = HEADS // heads
    group_width = heads * HEAD_DIM
    padded = -(-3 * group_width // lanes) * lanes if dealt else 3 * group_width
    out_width = -(-group_width // lanes) * lanes if dealt else group_width

    columns = [decay_rate, state_in, state_out, shift_taps]
    columns += [g[:, None] for g in (mixer_gain, first_gain, attend_gain, second_gain, state_skip)]
    small = jnp.concatenate(columns, axis=1)
    small_count = small.shape[1]
    small_width = -(-small_count // lanes) * lanes
    small = jnp.pad(small, ((0, 0), (0, small_width - small_count)))
    attend_cols = attend_inputs.shape[1]
    grouped = group_columns(attend_inputs, groups, padded)
    by_kernel = seq_devices == 8 and lax.axis_size("batch") == 4
    packed = [mixer_output, first_up, grouped, attend_output, second_up]
    if by_kernel:
        joint = jnp.concatenate([mixer_inputs, small], axis=1)
        w_mixer_out, w_up1, w_attend_in, w_attend_out, w_up2 = gathered(packed)
        widths = (joint.shape[1], model_width)
        w_joint, w_down1 = gather_blocks((joint, first_down), chunked(widths, (4, 6)), gap=3)
        w_mixer_in, w_small = cut(w_joint, [mixer_inputs.shape[1], small_width])
        second_down, w_small = lax.optimization_barrier((second_down, w_small))
        w_down2 = lax.all_gather(second_down, everyone, axis=0, tiled=True)
    else:
        w_mixer_in, w_small = gathered([mixer_inputs, small])
        packed += [fold_rows(first_down, share), fold_rows(second_down, share)]
        w_mixer_out, w_up1, w_attend_in, w_attend_out, w_up2, w_down1, w_down2 = gathered(packed)
        w_down1 = unfold_rows(w_down1, fold, share)
        w_down2 = unfold_rows(w_down2, fold, share)

    rows = w_small.T.astype(f32)
    decay, table_in, table_out = rows[:states], rows[states : 2 * states], rows[2 * states : 3 * states]
    taps_rows = rows[3 * states : 3 * states + reach]
    gain_mixer, gain_first, gain_attend, gain_second, skip = (
        rows[3 * states + reach + i] for i in range(5)
    )
    taps = taps_rows.T
    weight = table_in * table_out

    rank_seq = lax.axis_index("seq")
    offsets = jnp.arange(block_len, dtype=jnp.int32)
    places = rank_seq * block_len + offsets
    valid = (places[None, :] < lengths[:, None]).astype(f32)
    longest = jnp.max(lengths)
    any_live = places[0] < longest

    start_resid = tokens.reshape(row_count, model_width).astype(f32)
    normed_mixer, back_mixer = jax.vjp(layer_norm, start_resid, gain_mixer)
    normed_low_mixer = normed_mixer.astype(bf16)
    projected = dense(normed_low_mixer, w_mixer_in).reshape(seq_count, block_len, 3 * model_width)
    query_mixer = projected[:, :, :model_width]
    keys_mixer = projected[:, :, model_width : 2 * model_width]
    value_mixer = projected[:, :, 2 * model_width :]
    rim_rows = passed_along(keys_mixer[:, block_len - reach + 1 :], "seq", 1)
    extended = jnp.concatenate([rim_rows, keys_mixer], axis=1)
    inner, shift_back = jax.vjp(shift_mix, extended, taps, value_mixer)
    carried = carried_in(encode(inner, decay, False), decay, block_len, False)
    wide = shaped(seq_count, block_len, model_width)
    state_y, gated = per_lane_tile(
        output_kernel,
        (inner, query_mixer, carried, decay, weight, skip[None]),
        (wide, wide),
    )
    gated_low = gated.astype(bf16).reshape(row_count, model_width)
    resid_mixer = start_resid + dense(gated_low, w_mixer_out)
    resid_first, stored_first = feed_forward(resid_mixer, gain_first, w_up1, w_down1)

    normed_attend, back_attend = jax.vjp(layer_norm, resid_first, gain_attend)
    normed_low_attend = normed_attend.astype(bf16)
    proj_low = dense(normed_low_attend, w_attend_in).astype(bf16)
    if dealt:
        length = seq_devices * block_len
        block = min(256, length)

        def deal(array, width):
            array = array.reshape(seq_count, block_len, groups * width)
            parts = jnp.stack(cut_last(array, groups), axis=1)
            parts = parts.reshape(seq_count * groups, block_len, width)
            dealt_parts = lax.all_to_all(parts, "seq", split_axis=0, concat_axis=0, tiled=True)
            return dealt_parts.reshape(length, width)

        def collect(array, width):
            parts = array.reshape(seq_devices, block_len, width)
            back = lax.all_to_all(parts, "seq", split_axis=0, concat_axis=0, tiled=True)
            back = back.reshape(seq_count, groups, block_len, width)
            back = jnp.concatenate([back[:, group] for group in range(groups)], axis=-1)
            return back.reshape(row_count, groups * width)

        qkv = deal(proj_low, padded)
        attended_part, attended_full, stat = attend_whole(qkv, heads, block)
        attended_low = collect(attended_part, out_width)
        w_attend_out = pad_groups(w_attend_out, groups, out_width)
    else:
        attended, attended_back = general_attention(
            proj_low, seq_count, block_len, places, any_live, longest
        )
        attended_low = attended.reshape(row_count, model_width).astype(bf16)
    resid_attend = resid_first + dense(attended_low, w_attend_out)
    final, stored_second = feed_forward(resid_attend, gain_second, w_up2, w_down2)
    mixed = (final.reshape(seq_count, block_len, model_width) * valid[..., None]).astype(bf16)

    upstream = (cotangent.astype(f32) * valid[..., None]).reshape(row_count, model_width)
    upstream, second_gain_grad, second_up_grad, second_down_grad = feed_back(
        stored_second, w_up2, w_down2, upstream
    )
    into_attended, attend_output_grad = dense_back(
        attended_low, w_attend_out, upstream.astype(bf16)
    )
    if dealt:
        attend_output_grad = attend_output_grad.reshape(groups, out_width, model_width)
        attend_output_grad = attend_output_grad[:, :group_width].reshape(model_width, model_width)
    early = [second_up_grad, fold_all(second_down_grad, share, model_width), attend_output_grad]
    early_widths = [g.shape[1] for g in early]
    early = jnp.concatenate(early, axis=1)
    dout_low = into_attended.astype(bf16)
    if dealt:
        dout, early = lax.optimization_barrier((deal(dout_low, out_width), early))
        proj_grad = collect(
            attend_whole_back(qkv, dout, attended_full, stat, heads, block), padded
        )
    else:
        parts = attended_back(dout_low.reshape(seq_count, block_len, HEADS, HEAD_DIM))
        proj_grad = jnp.concatenate(
            [p.reshape(row_count, model_width) for p in parts], axis=1
        ).astype(bf16)
    early = lax.psum_scatter(early, everyone, scatter_dimension=0, tiled=True)
    second_up_out, second_down_out, attend_output_out = cut(early, early_widths)
    into_normed, attend_inputs_grad = dense_back(normed_low_attend, w_attend_in, proj_grad)
    into_resid, attend_gain_grad = back_attend(into_normed)
    upstream = upstream + into_resid
    upstream, first_gain_grad, first_up_grad, first_down_grad = feed_back(
        stored_first, w_up1, w_down1, upstream
    )
    into_gated, mixer_output_grad = dense_back(gated_low, w_mixer_out, upstream.astype(bf16))
    into_gated = into_gated.reshape(seq_count, block_len, model_width)
    query_mixer_grad = into_gated * state_y
    state_grad = into_gated * query_mixer
    later = carried_in(encode(state_grad, decay, True), decay, block_len, True)
    table = shaped(states, model_width)
    inner_grad, weight_grad, power_grad, skip_grad = per_lane_tile(
        back_kernel,
        (inner, state_grad, carried, later, decay, weight, skip[None]),
        (wide, table, table, shaped(1, model_width)),
        scratch=[pltpu.VMEM((block_len, seq_count, states, lanes), f32)],
    )
    extended_grad, taps_grad, value_mixer_grad = shift_back(inner_grad)
    spill = passed_along(extended_grad[:, : reach - 1], "seq", -1)
    keys_mixer_grad = extended_grad[:, reach - 1 :] + jnp.pad(
        spill, ((0, 0), (block_len - reach + 1, 0), (0, 0))
    )
    proj_grad_mixer = (
        jnp.concatenate([query_mixer_grad, keys_mixer_grad, value_mixer_grad], axis=2)
        .astype(bf16)
        .reshape(row_count, 3 * model_width)
    )
    into_normed_mixer, mixer_inputs_grad = dense_back(normed_low_mixer, w_mixer_in, proj_grad_mixer)
    into_start, mixer_gain_grad = back_mixer(into_normed_mixer)
    tokens_gradient = (upstream + into_start).reshape(seq_count, block_len, model_width).astype(bf16)

    small_rows = jnp.concatenate(
        [-jnp.exp(-decay) * power_grad, weight_grad * table_out, weight_grad * table_in, taps_grad.T]
        + [
            g[None]
            for g in (mixer_gain_grad, first_gain_grad, attend_gain_grad, second_gain_grad, skip_grad[0])
        ],
        axis=0,
    )
    small_grad = jnp.pad(small_rows, ((0, small_width - small_count), (0, 0))).T.astype(bf16)
    def unfolded(folded):
        return folded.reshape(share, fold, model_width).transpose(1, 0, 2).reshape(share * fold, model_width)

    gains_at = 3 * states + reach
    table_edges = [0, states, 2 * states, 3 * states, gains_at, small_width]

    def tables_of(block):
        return [block[:, a:b] for a, b in zip(table_edges, table_edges[1:])]

    last = [attend_inputs_grad, first_up_grad, mixer_output_grad, mixer_inputs_grad, small_grad]
    if by_kernel:
        last.append(first_down_grad)
        plan = chunked([g.shape[1] for g in last], (4, 4, 2, 4, 2, 4))
        part = attend_cols // 3 // groups

        def finish(index, block, results):
            if index == 0:
                for group in range(groups):
                    for kind in range(3):
                        start = (kind * groups + group) * part
                        source = group * padded + kind * part
                        results[0][:, start : start + part] = block[:, source : source + part]
            elif index == 4:
                for place, table in enumerate(tables_of(block)):
                    results[5 + place][...] = table
            else:
                results[{1: 1, 2: 2, 3: 3, 5: 4}[index]][...] = block[...]

        widths = [attend_cols] + [g.shape[1] for g in last[1:4]]
        results = [shaped(share, w) for w in widths] + [shaped(share * fold, model_width)]
        results += [shaped(share, b - a) for a, b in zip(table_edges, table_edges[1:])]
        attend_inputs_out, first_up_out, mixer_output_out, mixer_inputs_out, first_down_out, *tables = (
            scatter_blocks(last, plan, finish, results, gap=4)
        )
    else:
        *last, folded = scattered(last + [fold_all(first_down_grad, share, model_width)])
        first_down_out = unfolded(folded).astype(f32)
        grouped, first_up_out, mixer_output_out, mixer_inputs_out, small_out = (
            g.astype(f32) for g in last
        )
        attend_inputs_out = ungroup_columns(grouped, groups, padded, attend_cols)
        tables = tables_of(small_out)
    decay_out, in_out, out_out, taps_out, vectors = tables

    return (
        mixed,
        tokens_gradient,
        vectors[:, 0],
        mixer_inputs_out,
        taps_out,
        decay_out,
        in_out,
        out_out,
        vectors[:, 4],
        mixer_output_out,
        vectors[:, 1],
        first_up_out,
        first_down_out,
        vectors[:, 2],
        attend_inputs_out,
        attend_output_out.astype(f32),
        vectors[:, 3],
        second_up_out.astype(f32),
        unfolded(second_down_out).astype(f32),
    )


def solution(mesh):
    return jax.shard_map(
        body,
        mesh=mesh,
        in_specs=(
            P("batch", "seq", None),
            P("batch", "seq", None),
            P("batch"),
            P(("seq", "batch")),
            P(("seq", "batch"), None),
            P(("seq", "batch"), None),
            P(("seq", "batch"), None),
            P(("seq", "batch"), None),
            P(("seq", "batch"), None),
            P(("seq", "batch")),
            P(("seq", "batch"), None),
            P(("seq", "batch")),
            P(("seq", "batch"), None),
            P(("seq", "batch"), None),
            P(("seq", "batch")),
            P(("seq", "batch"), None),
            P(("seq", "batch"), None),
            P(("seq", "batch")),
            P(("seq", "batch"), None),
            P(("seq", "batch"), None),
        ),
        out_specs=(
            P("batch", "seq", None),
            P("batch", "seq", None),
            P(("seq", "batch")),
            P(("seq", "batch"), None),
            P(("seq", "batch"), None),
            P(("seq", "batch"), None),
            P(("seq", "batch"), None),
            P(("seq", "batch"), None),
            P(("seq", "batch")),
            P(("seq", "batch"), None),
            P(("seq", "batch")),
            P(("seq", "batch"), None),
            P(("seq", "batch"), None),
            P(("seq", "batch")),
            P(("seq", "batch"), None),
            P(("seq", "batch"), None),
            P(("seq", "batch")),
            P(("seq", "batch"), None),
            P(("seq", "batch"), None),
        ),
        check_vma=False,
    )
```

```python
import functools

import jax
import jax.numpy as jnp
from jax import lax
from jax.experimental import pallas as pl
from jax.experimental.pallas import tpu as pltpu
from jax.sharding import PartitionSpec as P

HEADS = 12
HEAD_DIM = 64

eps = 1e-05
masked_score = -1e30
lanes = 128
sublanes = 8
everyone = ("seq", "batch")
f32 = jnp.float32
bf16 = jnp.bfloat16


def rows_of(ref, seq, block):
    return ref[seq, pl.ds(pl.multiple_of(block * sublanes, sublanes), sublanes), :]


def spread(rows, index, count):
    return jnp.broadcast_to(rows[index : index + 1], (count, lanes))


def encode_kernel(reverse, input_ref, decay_ref, end_ref):
    seq_count, step_count, _ = input_ref.shape
    state_count = decay_ref.shape[0]
    blocks = step_count // sublanes
    power = jnp.exp(-decay_ref[...])

    def one_block(step, states):
        block = blocks - 1 - step if reverse else step
        rows = [rows_of(input_ref, seq, block) for seq in range(seq_count)]
        order = range(sublanes - 1, -1, -1) if reverse else range(sublanes)
        states = list(states)
        for index in order:
            for seq in range(seq_count):
                states[seq] = states[seq] * power + spread(rows[seq], index, state_count)
        return tuple(states)

    start = tuple(jnp.zeros((state_count, lanes), f32) for _ in range(seq_count))
    ends = lax.fori_loop(0, blocks, one_block, start)
    for seq in range(seq_count):
        end_ref[seq] = ends[seq]


def output_kernel(input_ref, query_ref, carried_ref, decay_ref, weight_ref, skip_ref, out_ref, gated_ref):
    seq_count, step_count, _ = input_ref.shape
    state_count = decay_ref.shape[0]
    power = jnp.exp(-decay_ref[...])
    weight = weight_ref[...]
    skip = skip_ref[...]

    def one_block(block, states):
        states = list(states)
        rows = [rows_of(input_ref, seq, block) for seq in range(seq_count)]
        found = [[] for _ in range(seq_count)]
        for index in range(sublanes):
            for seq in range(seq_count):
                states[seq] = states[seq] * power + spread(rows[seq], index, state_count)
                found[seq].append(jnp.sum(states[seq] * weight, axis=0, keepdims=True))
        place = pl.ds(pl.multiple_of(block * sublanes, sublanes), sublanes)
        for seq in range(seq_count):
            result = jnp.concatenate(found[seq], axis=0) + skip * rows[seq]
            out_ref[seq, place, :] = result
            gated_ref[seq, place, :] = result * rows_of(query_ref, seq, block)
        return tuple(states)

    start = tuple(carried_ref[seq].astype(f32) for seq in range(seq_count))
    lax.fori_loop(0, step_count // sublanes, one_block, start)


def back_kernel(
    input_ref,
    grad_ref,
    carried_ref,
    later_ref,
    decay_ref,
    weight_ref,
    skip_ref,
    input_grad_ref,
    weight_grad_ref,
    power_grad_ref,
    skip_grad_ref,
    held,
):
    seq_count, step_count, _ = input_ref.shape
    state_count = decay_ref.shape[0]
    blocks = step_count // sublanes
    power = jnp.exp(-decay_ref[...])
    weight = weight_ref[...]
    skip = skip_ref[...]
    seqs = range(seq_count)

    def forward_block(block, state):
        states, total, skip_total = list(state[0]), state[1], state[2]
        rows = [rows_of(input_ref, seq, block) for seq in seqs]
        grads = [rows_of(grad_ref, seq, block) for seq in seqs]
        for index in range(sublanes):
            for seq in seqs:
                held[block * sublanes + index, seq] = states[seq]
                states[seq] = states[seq] * power + spread(rows[seq], index, state_count)
                total = total + states[seq] * spread(grads[seq], index, state_count)
        for seq in seqs:
            skip_total = skip_total + rows[seq] * grads[seq]
        return (tuple(states), total, skip_total)

    zeros = jnp.zeros((state_count, lanes), f32)
    _, total, skip_total = lax.fori_loop(
        0,
        blocks,
        forward_block,
        (
            tuple(carried_ref[seq].astype(f32) for seq in seqs),
            zeros,
            jnp.zeros((sublanes, lanes), f32),
        ),
    )
    weight_grad_ref[...] = total
    skip_grad_ref[...] = jnp.sum(skip_total, axis=0, keepdims=True)

    def back_block(step, state):
        states, total = list(state[0]), state[1]
        block = blocks - 1 - step
        grads = [rows_of(grad_ref, seq, block) for seq in seqs]
        found = [[None] * sublanes for _ in seqs]
        for index in range(sublanes - 1, -1, -1):
            for seq in seqs:
                states[seq] = states[seq] * power + spread(grads[seq], index, state_count)
                found[seq][index] = jnp.sum(states[seq] * weight, axis=0, keepdims=True)
                total = total + states[seq] * held[block * sublanes + index, seq]
        place = pl.ds(pl.multiple_of(block * sublanes, sublanes), sublanes)
        for seq in seqs:
            input_grad_ref[seq, place, :] = jnp.concatenate(found[seq], axis=0) + skip * grads[seq]
        return (tuple(states), total)

    _, total = lax.fori_loop(
        0, blocks, back_block, (tuple(later_ref[seq].astype(f32) for seq in seqs), zeros)
    )
    power_grad_ref[...] = total * weight


def per_lane_tile(kernel, args, outs, scratch=(), flops=0):
    def spec(shape):
        lead = len(shape) - 1
        return pl.BlockSpec(tuple(shape[:-1]) + (lanes,), lambda tile: (0,) * lead + (tile,))

    bytes_moved = sum(a.size * a.dtype.itemsize for a in args)
    return pl.pallas_call(
        kernel,
        grid=(args[0].shape[-1] // lanes,),
        in_specs=[spec(a.shape) for a in args],
        out_specs=[spec(o.shape) for o in outs],
        out_shape=list(outs),
        scratch_shapes=list(scratch),
        cost_estimate=pl.CostEstimate(flops=flops, bytes_accessed=bytes_moved, transcendentals=0),
        compiler_params=pltpu.CompilerParams(vmem_limit_bytes=48 * 1024 * 1024),
    )(*args)


def shaped(*dims, dtype=f32):
    return jax.ShapeDtypeStruct(dims, dtype)


def encode(value, decay, reverse):
    seq_count, _, width = value.shape
    (ends,) = per_lane_tile(
        functools.partial(encode_kernel, reverse),
        (value, decay),
        (shaped(seq_count, decay.shape[0], width),),
    )
    return ends


def passed_along(block, axis, distance):
    devices = range(lax.axis_size(axis))
    route = [(i - distance, i) for i in devices if i - distance in devices]
    return lax.ppermute(block, axis, route)


def carried_in(ends, decay, block_len, reverse):
    seq_count, state_count, width = ends.shape
    count = lax.axis_size("seq")
    part = state_count // count

    def exchanged(parts):
        return lax.all_to_all(parts.astype(bf16), "seq", split_axis=0, concat_axis=0, tiled=True)

    parts = ends.reshape(seq_count, count, part, width).transpose(1, 0, 2, 3)
    arrived = exchanged(parts.reshape(count, seq_count * part, width)).astype(f32)
    rates = lax.dynamic_slice_in_dim(decay, lax.axis_index("seq") * part, part, 0)
    power = jnp.tile(jnp.exp(-rates * block_len), (seq_count, 1))
    state, joined = jnp.zeros_like(arrived[0]), [None] * count
    for block in reversed(range(count)) if reverse else range(count):
        joined[block] = state
        state = power * state + arrived[block]
    back = exchanged(jnp.stack(joined))
    back = back.reshape(count, seq_count, part, width).transpose(1, 0, 2, 3)
    return back.reshape(seq_count, state_count, width)


MESH = pl.DeviceIdType.MESH
box = (4, 2, 2, 2)


def here():
    seq, batch = lax.axis_index("seq"), lax.axis_index("batch")
    return lax.div(seq, 2), lax.rem(seq, 2), lax.div(batch, 2), lax.rem(batch, 2)


def device(z, x, y, core):
    return (2 * z + x, 2 * y + core)


def line_peer(z, step):
    return lax.rem(z + step, box[0])


def greet():
    z, x, y, core = here()
    barrier = pltpu.get_barrier_semaphore()
    peers = [device(line_peer(z, step), x, y, core) for step in range(1, box[0])]
    peers += [device(z, 1 - x, y, core), device(z, x, 1 - y, core), device(z, x, y, 1 - core)]
    for peer in peers:
        pl.semaphore_signal(barrier, inc=1, device_id=peer, device_id_type=MESH)
    pl.semaphore_wait(barrier, len(peers))


def staggered(count, stages, gap):
    for turn in range(count + gap * (stages - 1)):
        for stage in reversed(range(stages)):
            chunk = turn - gap * stage
            if 0 <= chunk < count:
                yield stage, chunk


def gather_kernel(plan, gap, *refs):
    count = 1 + max(item[0] for item in plan)
    ins, outs = refs[:count], refs[count : 2 * count]
    send, receive, local = refs[2 * count :]
    z, x, y, core = here()
    greet()
    started = {}

    def push(chunk, slot, source, target, peer):
        copy = pltpu.make_async_remote_copy(
            src_ref=source,
            dst_ref=target,
            send_sem=send.at[chunk, slot],
            recv_sem=receive.at[chunk, slot],
            device_id=peer,
            device_id_type=MESH,
        )
        copy.start()
        started[chunk, slot] = copy

    own = []
    for chunk, (index, first, width, x_first) in enumerate(plan):
        columns = pl.ds(first, width)
        source = ins[index].at[:, columns]
        target = outs[index].at[z, x, y, core, :, columns]
        for step in range(1, box[0]):
            push(chunk, step - 1, source, target, device(line_peer(z, step), x, y, core))
        keep = pltpu.make_async_copy(source, target, local.at[chunk])
        keep.start()
        own.append(keep)

    for stage, chunk in staggered(len(plan), 3, gap):
        index, first, width, x_first = plan[chunk]
        columns = pl.ds(first, width)
        out = outs[index]
        if stage == 0:
            for step in range(1, box[0]):
                started[chunk, step - 1].wait_recv()
            own[chunk].wait()
            part = out.at[:, x, y, core, :, columns]
            peer = device(z, 1 - x, y, core) if x_first else device(z, x, 1 - y, core)
            push(chunk, 3, part, part, peer)
        elif stage == 1:
            started[chunk, 3].wait_recv()
            if x_first:
                part, peer = out.at[:, :, y, core, :, columns], device(z, x, 1 - y, core)
            else:
                part, peer = out.at[:, x, :, core, :, columns], device(z, 1 - x, y, core)
            push(chunk, 4, part, part, peer)
        else:
            started[chunk, 4].wait_recv()
            part = out.at[:, :, :, core, :, columns]
            push(chunk, 5, part, part, device(z, x, y, 1 - core))
    for chunk in range(len(plan)):
        started[chunk, 5].wait_recv()
        for slot in range(6):
            started[chunk, slot].wait_send()


def gather_blocks(blocks, plan, gap=2, collective=0):
    outs = [jax.ShapeDtypeStruct(box + b.shape, b.dtype) for b in blocks]
    sent = sum(b.size * b.dtype.itemsize for b in blocks)
    whole = pl.pallas_call(
        functools.partial(gather_kernel, plan, gap),
        out_shape=outs,
        in_specs=[pl.BlockSpec(memory_space=pltpu.VMEM)] * len(blocks),
        out_specs=[pl.BlockSpec(memory_space=pl.ANY)] * len(blocks),
        scratch_shapes=[
            pltpu.SemaphoreType.DMA((len(plan), 6)),
            pltpu.SemaphoreType.DMA((len(plan), 6)),
            pltpu.SemaphoreType.DMA((len(plan),)),
        ],
        cost_estimate=pl.CostEstimate(flops=0, bytes_accessed=64 * sent, transcendentals=0),
        compiler_params=pltpu.CompilerParams(collective_id=collective, has_side_effects=True),
    )(*blocks)
    return [w.reshape((32 * w.shape[4], w.shape[5])) for w in whole]


def add_into(total, other):
    return (total.astype(f32) + other.astype(f32)).astype(bf16)


def scatter_kernel(plan, gap, finish, counts, *refs):
    count, out_count = counts
    ins, results = refs[:count], refs[count : count + out_count]
    outs, buffers = refs[count + out_count : 2 * count + out_count], refs[2 * count + out_count : -3]
    send, receive, local = refs[-3:]
    z, x, y, core = here()
    greet()
    started = {}

    def push(chunk, slot, source, target, peer):
        copy = pltpu.make_async_remote_copy(
            src_ref=source,
            dst_ref=target,
            send_sem=send.at[chunk, slot],
            recv_sem=receive.at[chunk, slot],
            device_id=peer,
            device_id_type=MESH,
        )
        copy.start()
        started[chunk, slot] = copy

    loads = []
    for chunk, (index, first, width, _) in enumerate(plan):
        columns = pl.ds(first, width)
        held, from_core = buffers[5 * chunk : 5 * chunk + 2]
        grad = ins[index]
        push(chunk, 0, grad.at[:, :, :, 1 - core, :, columns], from_core, device(z, x, y, 1 - core))
        load = pltpu.make_async_copy(grad.at[:, :, :, core, :, columns], held, local.at[chunk])
        load.start()
        loads.append(load)

    for stage, chunk in staggered(len(plan), 4, gap):
        index, first, width, x_first = plan[chunk]
        held, from_core, from_one, from_two, from_line = buffers[5 * chunk : 5 * chunk + 5]
        to_x, to_y = device(z, 1 - x, y, core), device(z, x, 1 - y, core)
        if stage == 0:
            started[chunk, 0].wait_recv()
            loads[chunk].wait()

            @pl.loop(0, box[0])
            def _(row):
                for i in range(2):
                    for j in range(2):
                        held[row, i, j] = add_into(held[row, i, j], from_core[row, i, j])

            if x_first:
                push(chunk, 1, held.at[:, :, 1 - y], from_one, to_y)
            else:
                push(chunk, 1, held.at[:, 1 - x], from_one, to_x)
        elif stage == 1:
            started[chunk, 1].wait_recv()

            @pl.loop(0, box[0])
            def _(row):
                for i in range(2):
                    if x_first:
                        held[row, i, y] = add_into(held[row, i, y], from_one[row, i])
                    else:
                        held[row, x, i] = add_into(held[row, x, i], from_one[row, i])

            if x_first:
                push(chunk, 2, held.at[:, 1 - x, y], from_two, to_x)
            else:
                push(chunk, 2, held.at[:, x, 1 - y], from_two, to_y)
        elif stage == 2:
            started[chunk, 2].wait_recv()

            @pl.loop(0, box[0])
            def _(row):
                held[row, x, y] = add_into(held[row, x, y], from_two[row])

            for step in range(1, box[0]):
                peer = line_peer(z, step)
                push(chunk, 2 + step, held.at[peer, x, y], from_line.at[step - 1], device(peer, x, y, core))
        else:
            total = held[z, x, y].astype(f32)
            for step in range(1, box[0]):
                started[chunk, 2 + step].wait_recv()
                total = total + from_line[step - 1].astype(f32)
            outs[index][:, pl.ds(first, width)] = total
            if not any(item[0] == index for item in plan[chunk + 1 :]):
                finish(index, outs[index], results)
    for chunk in range(len(plan)):
        for slot in range(6):
            started[chunk, slot].wait_send()


def scatter_blocks(grads, plan, finish, results, gap=2, collective=1):
    views = [g.reshape(box + (g.shape[0] // 32, g.shape[1])) for g in grads]
    scratch = [pltpu.VMEM(v.shape[4:], f32) for v in views]
    for index, _, width, _ in plan:
        tile = (views[index].shape[4], width)
        for lead in ((4, 2, 2), (4, 2, 2), (4, 2), (4,), (3,)):
            scratch.append(pltpu.VMEM(lead + tile, bf16))
    sent = sum(v.size * v.dtype.itemsize for v in views)
    return pl.pallas_call(
        functools.partial(scatter_kernel, plan, gap, finish, (len(views), len(results))),
        out_shape=list(results),
        in_specs=[pl.BlockSpec(memory_space=pl.ANY)] * len(views),
        out_specs=[pl.BlockSpec(memory_space=pltpu.VMEM)] * len(results),
        scratch_shapes=scratch
        + [
            pltpu.SemaphoreType.DMA((len(plan), 6)),
            pltpu.SemaphoreType.DMA((len(plan), 6)),
            pltpu.SemaphoreType.DMA((len(plan),)),
        ],
        cost_estimate=pl.CostEstimate(flops=0, bytes_accessed=4 * sent, transcendentals=0),
        compiler_params=pltpu.CompilerParams(
            collective_id=collective, has_side_effects=True, vmem_limit_bytes=60 * 1024 * 1024
        ),
    )(*views)


def chunked(widths, pieces):
    plan = []
    for index, (width, number) in enumerate(zip(widths, pieces)):
        tiles = width // lanes
        edges = [tiles * i // number for i in range(number + 1)]
        for i in range(number):
            plan.append((index, edges[i] * lanes, (edges[i + 1] - edges[i]) * lanes, len(plan) % 2 == 0))
    return plan


hidden_block = 768
gelu_scale = 0.7978845608
gelu_cubic = 0.044715


def feed_kernel(resid_ref, gain_ref, up_ref, down_ref, out_ref, normed_ref, hidden_ref, active_ref):
    @pl.when(pl.program_id(0) == 0)
    def _():
        resid = resid_ref[...]
        normed_ref[...] = layer_norm(resid, gain_ref[...]).astype(bf16)
        out_ref[...] = resid

    hidden = jnp.dot(normed_ref[...], up_ref[...], preferred_element_type=f32)
    hidden_ref[...] = hidden
    bend = jnp.tanh(gelu_scale * (hidden + gelu_cubic * hidden * hidden * hidden))
    active = (0.5 * hidden * (1.0 + bend)).astype(bf16)
    active_ref[...] = active
    out_ref[...] += jnp.dot(active, down_ref[...], preferred_element_type=f32)


def feed_forward_blocks(resid, gain, up_packed, up_at, down):
    rows, width = resid.shape
    inner = down.shape[0]
    first = up_at // hidden_block
    whole = pl.BlockSpec((rows, width), lambda j: (0, 0))
    part = pl.BlockSpec((rows, hidden_block), lambda j: (0, j))
    out, normed, hidden, active = pl.pallas_call(
        feed_kernel,
        grid=(inner // hidden_block,),
        in_specs=[
            whole,
            pl.BlockSpec((1, width), lambda j: (0, 0)),
            pl.BlockSpec((width, hidden_block), lambda j: (0, first + j)),
            pl.BlockSpec((hidden_block, width), lambda j: (j, 0)),
        ],
        out_specs=[whole, whole, part, part],
        out_shape=[
            shaped(rows, width),
            shaped(rows, width, dtype=bf16),
            shaped(rows, inner),
            shaped(rows, inner, dtype=bf16),
        ],
        cost_estimate=pl.CostEstimate(
            flops=4 * rows * width * inner, bytes_accessed=10 * width * inner, transcendentals=rows * inner
        ),
        compiler_params=pltpu.CompilerParams(vmem_limit_bytes=40 * 1024 * 1024),
    )(resid, gain[None], up_packed, down)
    return out, (resid, gain, normed, hidden, active)


def feed_back_kernel(
    packed,
    upstream_ref,
    resid_ref,
    gain_ref,
    normed_ref,
    hidden_ref,
    active_ref,
    up_ref,
    down_ref,
    out_ref,
    gain_grad_ref,
    *rest,
):
    step = pl.program_id(0)
    last = pl.num_programs(0) - 1
    across = (((1,), (1,)), ((), ()))
    along = (((0,), (0,)), ((), ()))
    upstream_low = upstream_ref[...].astype(bf16)
    into_active = lax.dot_general(upstream_low, down_ref[...], across, preferred_element_type=f32)
    hidden = hidden_ref[...]
    square = hidden * hidden
    bend = jnp.tanh(gelu_scale * hidden * (1.0 + gelu_cubic * square))
    slope = 0.5 * (1.0 + bend) + 0.5 * hidden * (1.0 - bend * bend) * (
        gelu_scale * (1.0 + 3.0 * gelu_cubic * square)
    )
    into_hidden = (into_active * slope).astype(bf16)
    part = lax.dot_general(into_hidden, up_ref[...], across, preferred_element_type=f32)

    @pl.when(step == 0)
    def _():
        out_ref[...] = part

    @pl.when(step > 0)
    def _():
        out_ref[...] += part

    up_grad = lax.dot_general(normed_ref[...], into_hidden, along, preferred_element_type=f32)
    down_grad = lax.dot_general(active_ref[...], upstream_low, along, preferred_element_type=f32)
    if packed:
        grads_ref, up_held, down_held, sems = rest
        share, fold = packed
        width = up_grad.shape[0]
        inner = hidden_block * grads_ref.shape[1] // (2 * hidden_block)
        tall = hidden_block // fold
        slot = lax.rem(step, 2)

        def copies(at, slot):
            columns = pl.ds(pl.multiple_of(at * hidden_block, hidden_block), hidden_block)
            rows = pl.ds(pl.multiple_of(at * tall, tall), tall)
            return (
                pltpu.make_async_copy(up_held.at[slot], grads_ref.at[:, columns], sems.at[0, slot]),
                pltpu.make_async_copy(down_held.at[slot], grads_ref.at[rows, inner:], sems.at[1, slot]),
            )

        @pl.when(step >= 2)
        def _():
            for copy in copies(step - 2, slot):
                copy.wait()

        up_held[slot] = up_grad.astype(bf16)
        for place in range(fold):
            starts = range(place * share, hidden_block, fold * share)
            piece = jnp.concatenate([down_grad[a : a + share] for a in starts], axis=0)
            down_held[slot, :, place * width : (place + 1) * width] = piece.astype(bf16)
        for copy in copies(step, slot):
            copy.start()

        @pl.when(step == last)
        def _():
            for copy in copies(step - 1, 1 - slot) + copies(step, slot):
                copy.wait()
    else:
        up_grad_ref, down_grad_ref = rest
        up_grad_ref[...] = up_grad.astype(bf16)
        down_grad_ref[...] = down_grad.astype(bf16)

    @pl.when(step == last)
    def _():
        into_normed = out_ref[...]
        resid = resid_ref[...]
        centred = resid - jnp.mean(resid, axis=-1, keepdims=True)
        inverse = lax.rsqrt(jnp.mean(centred * centred, axis=-1, keepdims=True) + eps)
        unit = centred * inverse
        gain_grad_ref[...] = jnp.sum(into_normed * unit, axis=0, keepdims=True)
        scaled = into_normed * gain_ref[...]
        along_unit = jnp.mean(scaled * unit, axis=-1, keepdims=True)
        into_resid = inverse * (scaled - jnp.mean(scaled, axis=-1, keepdims=True) - unit * along_unit)
        out_ref[...] = upstream_ref[...] + into_resid


def feed_back_blocks(stored, up_packed, up_at, down, upstream, packed=()):
    resid, gain, normed, hidden, active = stored
    rows, width = resid.shape
    inner = down.shape[0]
    first = up_at // hidden_block
    whole = pl.BlockSpec((rows, width), lambda j: (0, 0))
    part = pl.BlockSpec((rows, hidden_block), lambda j: (0, j))
    line = pl.BlockSpec((1, width), lambda j: (0, 0))
    up_spec = pl.BlockSpec((width, hidden_block), lambda j: (0, j))
    down_spec = pl.BlockSpec((hidden_block, width), lambda j: (j, 0))
    scratch = []
    if packed:
        grad_specs = [pl.BlockSpec(memory_space=pl.ANY)]
        grad_shapes = [shaped(width, 2 * inner, dtype=bf16)]
        scratch = [
            pltpu.VMEM((2, width, hidden_block), bf16),
            pltpu.VMEM((2, hidden_block // packed[1], inner), bf16),
            pltpu.SemaphoreType.DMA((2, 2)),
        ]
    else:
        grad_specs = [up_spec, down_spec]
        grad_shapes = [shaped(width, inner, dtype=bf16), shaped(inner, width, dtype=bf16)]
    out, gain_grad, *grads = pl.pallas_call(
        functools.partial(feed_back_kernel, packed),
        grid=(inner // hidden_block,),
        in_specs=[
            whole,
            whole,
            line,
            whole,
            part,
            part,
            pl.BlockSpec((width, hidden_block), lambda j: (0, first + j)),
            down_spec,
        ],
        out_specs=[whole, line] + grad_specs,
        out_shape=[shaped(rows, width), shaped(1, width)] + grad_shapes,
        scratch_shapes=scratch,
        cost_estimate=pl.CostEstimate(
            flops=8 * rows * width * inner, bytes_accessed=16 * width * inner, transcendentals=rows * inner
        ),
        compiler_params=pltpu.CompilerParams(vmem_limit_bytes=48 * 1024 * 1024),
    )(upstream, resid, gain[None], normed, hidden, active, up_packed, down)
    return (out, gain_grad[0], *grads)


def split_heads(ref, scratch, heads, parts, first=0):
    for part in range(parts):
        for head in range(heads):
            start = (part * heads + head) * HEAD_DIM + first
            scratch[part * heads + head] = ref[:, start : start + HEAD_DIM]


def score_block(query, keys, first, scale):
    scores = (
        lax.dot_general(query, keys, (((1,), (1,)), ((), ())), preferred_element_type=f32) * scale
    )
    rows = lax.broadcasted_iota(jnp.int32, scores.shape, 0) + first
    columns = lax.broadcasted_iota(jnp.int32, scores.shape, 1)
    return jnp.where(columns <= rows, scores, masked_score)


def attend_kernel(heads, block, scale, qkv_ref, low_ref, full_ref, stat_ref, parts, outs):
    length = qkv_ref.shape[0]
    split_heads(qkv_ref, parts, heads, 3)

    @pl.loop(0, heads)
    def _(head):
        for first in range(0, length, block):
            extent = first + block
            query = parts[head, first:extent, :]
            scores = score_block(query, parts[heads + head, :extent, :], first, scale)
            top = jnp.max(scores, axis=1, keepdims=True)
            soft = jnp.exp(scores - top)
            whole = jnp.sum(soft, axis=1, keepdims=True)
            soft = soft * (1.0 / whole)
            outs[head, first:extent, :] = jnp.dot(
                soft.astype(bf16), parts[2 * heads + head, :extent, :], preferred_element_type=f32
            )
            stat_ref[head, first:extent, :] = jnp.broadcast_to(top + jnp.log(whole), (block, lanes))

    if low_ref.shape[1] > heads * HEAD_DIM:
        low_ref[:, heads * HEAD_DIM :] = jnp.zeros((length, low_ref.shape[1] - heads * HEAD_DIM), bf16)
    for head in range(heads):
        place = slice(head * HEAD_DIM, (head + 1) * HEAD_DIM)
        full_ref[:, place] = outs[head]
        low_ref[:, place] = outs[head].astype(bf16)


def attend_back_kernel(
    heads, block, scale, qkv_ref, dout_ref, full_ref, stat_ref, grad_ref, parts, douts, fulls, grads
):
    length = qkv_ref.shape[0]
    split_heads(qkv_ref, parts, heads, 3)
    split_heads(dout_ref, douts, heads, 1)
    split_heads(full_ref, fulls, heads, 1)
    grads[...] = jnp.zeros_like(grads)

    @pl.loop(0, heads)
    def _(head):
        for first in range(0, length, block):
            extent = first + block
            query = parts[head, first:extent, :]
            keys = parts[heads + head, :extent, :]
            value = parts[2 * heads + head, :extent, :]
            dout = douts[head, first:extent, :]
            delta = jnp.sum(dout.astype(f32) * fulls[head, first:extent, :], axis=1, keepdims=True)
            scores = score_block(query, keys, first, scale)
            soft = jnp.exp(scores - stat_ref[head, first:extent, :1])
            across = (((1,), (1,)), ((), ()))
            along = (((0,), (0,)), ((), ()))
            dprob = lax.dot_general(dout, value, across, preferred_element_type=f32)
            dscore = (soft * (dprob - delta) * scale).astype(bf16)
            grads[head, first:extent, :] = jnp.dot(dscore, keys, preferred_element_type=f32)
            grads[heads + head, :extent, :] += lax.dot_general(
                dscore, query, along, preferred_element_type=f32
            )
            grads[2 * heads + head, :extent, :] += lax.dot_general(
                soft.astype(bf16), dout, along, preferred_element_type=f32
            )

    grad_ref[...] = jnp.zeros_like(grad_ref)
    for part in range(3 * heads):
        grad_ref[:, part * HEAD_DIM : (part + 1) * HEAD_DIM] = grads[part].astype(bf16)


def attend_params():
    return pltpu.CompilerParams(vmem_limit_bytes=56 * 1024 * 1024)


def attend_whole(qkv, heads, block):
    length = qkv.shape[0]
    width = heads * HEAD_DIM
    return pl.pallas_call(
        functools.partial(attend_kernel, heads, block, HEAD_DIM ** (-0.5)),
        out_shape=[
            shaped(length, -(-width // lanes) * lanes, dtype=bf16),
            shaped(length, width),
            shaped(heads, length, lanes),
        ],
        scratch_shapes=[
            pltpu.VMEM((3 * heads, length, HEAD_DIM), bf16),
            pltpu.VMEM((heads, length, HEAD_DIM), f32),
        ],
        compiler_params=attend_params(),
    )(qkv)


def attend_whole_back(qkv, dout, full, stat, heads, block):
    length = qkv.shape[0]
    return pl.pallas_call(
        functools.partial(attend_back_kernel, heads, block, HEAD_DIM ** (-0.5)),
        out_shape=shaped(*qkv.shape, dtype=bf16),
        scratch_shapes=[
            pltpu.VMEM((3 * heads, length, HEAD_DIM), bf16),
            pltpu.VMEM((heads, length, HEAD_DIM), bf16),
            pltpu.VMEM((heads, length, HEAD_DIM), f32),
            pltpu.VMEM((3 * heads, length, HEAD_DIM), f32),
        ],
        compiler_params=attend_params(),
    )(qkv, dout, full, stat)


def split_blocks(array, block_len):
    shaped_blocks = array.reshape(
        (array.shape[0], array.shape[1] // block_len, block_len) + array.shape[2:]
    )
    return jnp.moveaxis(shaped_blocks, 1, 0)


def general_attention(proj_low, seq_count, block_len, places, any_live, longest):
    model_width = HEADS * HEAD_DIM
    scale = HEAD_DIM ** (-0.5)
    offsets = jnp.arange(block_len, dtype=jnp.int32)
    head_shape = (seq_count, block_len, HEADS, HEAD_DIM)
    query_low = proj_low[:, :model_width].reshape(head_shape)
    keys_low = proj_low[:, model_width : 2 * model_width].reshape(head_shape)
    value_low = proj_low[:, 2 * model_width :].reshape(head_shape)

    def block_scores(queries, keys_block, query_places, key_places):
        scores = (
            jnp.einsum("sqhe,skhe->sqhk", queries, keys_block, preferred_element_type=jnp.float32)
            * scale
        )
        causal_mask = key_places[None, :] <= query_places[:, None]
        return jnp.where(causal_mask[None, :, None, :], scores, masked_score)

    def key_needed(key_first):
        return (key_first <= places[-1]) & ((key_first == places[0]) | any_live)

    stat_shape = (seq_count, block_len, HEADS)
    start_state = (
        jnp.full(stat_shape, masked_score, jnp.float32),
        jnp.zeros(stat_shape, jnp.float32),
        jnp.zeros(head_shape, jnp.float32),
    )
    shard_piece = (
        lax.all_gather(keys_low, "seq", axis=1, tiled=True),
        lax.all_gather(value_low, "seq", axis=1, tiled=True),
    )
    keys_blocks = split_blocks(shard_piece[0], block_len)
    value_blocks = split_blocks(shard_piece[1], block_len)
    firsts = jnp.arange(keys_blocks.shape[0], dtype=jnp.int32) * block_len

    def attend_one_step(state_now, operand):
        keys_block, value_block, key_first = operand

        def attend_work(state_in_block):
            running_max, running_sum, running_out = state_in_block
            scores = block_scores(query_low, keys_block, places, key_first + offsets)
            new_max = jnp.maximum(running_max, jnp.max(scores, axis=-1))
            fade = jnp.exp(running_max - new_max)
            shifted = jnp.exp(scores - new_max[..., None])
            new_sum = running_sum * fade + jnp.sum(shifted, axis=-1)
            new_out = running_out * fade[..., None] + jnp.einsum(
                "sqhk,skhe->sqhe",
                shifted.astype(jnp.bfloat16),
                value_block,
                preferred_element_type=jnp.float32,
            )
            return (new_max, new_sum, new_out)

        return (
            lax.cond(
                key_needed(key_first), attend_work, lambda state_in_block: state_in_block, state_now
            ),
            None,
        )

    result, _ = lax.scan(attend_one_step, start_state, (keys_blocks, value_blocks, firsts))
    running_max, running_sum, running_out = result
    attended = running_out / running_sum[..., None]
    logsum = running_max + jnp.log(running_sum)
    def backward(dout_low):
        delta = jnp.sum(dout_low.astype(jnp.float32) * attended, axis=-1)
        shard_piece = (
            lax.all_gather(keys_low, "seq", axis=1, tiled=True),
            lax.all_gather(value_low, "seq", axis=1, tiled=True),
        )
        keys_blocks = split_blocks(shard_piece[0], block_len)
        value_blocks = split_blocks(shard_piece[1], block_len)
        firsts = jnp.arange(keys_blocks.shape[0], dtype=jnp.int32) * block_len

        def query_one_step(query_grad, operand):
            keys_block, value_block, key_first = operand

            def query_work(grad_now):
                scores = block_scores(query_low, keys_block, places, key_first + offsets)
                soft = jnp.exp(scores - logsum[..., None])
                dprob = jnp.einsum(
                    "sqhe,skhe->sqhk", dout_low, value_block, preferred_element_type=jnp.float32
                )
                dscore = (soft * (dprob - delta[..., None])).astype(jnp.bfloat16)
                return (
                    grad_now
                    + jnp.einsum(
                        "sqhk,skhe->sqhe", dscore, keys_block, preferred_element_type=jnp.float32
                    )
                    * scale
                )

            return (
                lax.cond(key_needed(key_first), query_work, lambda grad_now: grad_now, query_grad),
                None,
            )

        result, _ = lax.scan(
            query_one_step, jnp.zeros(head_shape, jnp.float32), (keys_blocks, value_blocks, firsts)
        )
        query_grad = result
        sent = (query_low.astype(jnp.float32), dout_low.astype(jnp.float32), logsum, delta)
        shard_piece = (
            lax.all_gather(sent[0].astype(jnp.bfloat16), "seq", axis=1, tiled=True).astype(jnp.float32),
            lax.all_gather(sent[1].astype(jnp.bfloat16), "seq", axis=1, tiled=True).astype(jnp.float32),
            lax.all_gather(sent[2].astype(jnp.bfloat16), "seq", axis=1, tiled=True).astype(jnp.float32),
            lax.all_gather(sent[3].astype(jnp.bfloat16), "seq", axis=1, tiled=True).astype(jnp.float32),
        )
        query_blocks = split_blocks(shard_piece[0], block_len)
        dout_blocks = split_blocks(shard_piece[1], block_len)
        logsum_blocks = split_blocks(shard_piece[2], block_len)
        delta_blocks = split_blocks(shard_piece[3], block_len)
        firsts = jnp.arange(query_blocks.shape[0], dtype=jnp.int32) * block_len

        def key_one_step(grads_now, operand):
            query_block, dout_block, logsum_block, delta_block, query_first = operand

            def key_work(grads_in):
                keys_grad, value_grad = grads_in
                query_cast = query_block.astype(jnp.bfloat16)
                dout_cast = dout_block.astype(jnp.bfloat16)
                scores = block_scores(query_cast, keys_low, query_first + offsets, places)
                soft = jnp.exp(scores - logsum_block[..., None])
                value_grad = value_grad + jnp.einsum(
                    "sqhk,sqhe->skhe",
                    soft.astype(jnp.bfloat16),
                    dout_cast,
                    preferred_element_type=jnp.float32,
                )
                dprob = jnp.einsum(
                    "sqhe,skhe->sqhk", dout_cast, value_low, preferred_element_type=jnp.float32
                )
                dscore = (soft * (dprob - delta_block[..., None])).astype(jnp.bfloat16)
                keys_grad = (
                    keys_grad
                    + jnp.einsum(
                        "sqhk,sqhe->skhe", dscore, query_cast, preferred_element_type=jnp.float32
                    )
                    * scale
                )
                return (keys_grad, value_grad)

            needed = (query_first + block_len - 1 >= places[0]) & (
                (query_first == places[0]) | (query_first < longest)
            )
            return (lax.cond(needed, key_work, lambda grads_in: grads_in, grads_now), None)

        result, _ = lax.scan(
            key_one_step,
            (jnp.zeros(head_shape, jnp.float32), jnp.zeros(head_shape, jnp.float32)),
            (query_blocks, dout_blocks, logsum_blocks, delta_blocks, firsts),
        )
        keys_grad, value_grad = result
        return (query_grad, keys_grad, value_grad)

    return attended, backward


def layer_norm(value, gain):
    centred = value - jnp.mean(value, axis=-1, keepdims=True)
    spread_of = jnp.mean(centred * centred, axis=-1, keepdims=True)
    return centred * lax.rsqrt(spread_of + eps) * gain


def gelu_tanh(value):
    return jax.nn.gelu(value, approximate=True)


def dense(left, weight):
    return jnp.dot(left, weight, preferred_element_type=f32)


def dense_back(left, weight, upstream):
    into_left = lax.dot_general(
        upstream, weight, (((1,), (1,)), ((), ())), preferred_element_type=f32
    )
    into_weight = lax.dot_general(
        left, upstream, (((0,), (0,)), ((), ())), preferred_element_type=f32
    ).astype(bf16)
    return (into_left, into_weight)


def shift_mix(extended, taps, value_part):
    step_count = value_part.shape[1]
    reach = taps.shape[1]
    shifted = extended[:, reach - 1 : reach - 1 + step_count] * taps[:, 0]
    for tap_index in range(1, reach):
        shifted = (
            shifted
            + extended[:, reach - 1 - tap_index : reach - 1 - tap_index + step_count]
            * taps[:, tap_index]
        )
    return shifted * value_part


def feed_forward(resid, gain, up_weight, down_weight):
    normed, norm_back = jax.vjp(layer_norm, resid, gain)
    normed_low = normed.astype(bf16)
    hidden = dense(normed_low, up_weight)
    active, active_back = jax.vjp(gelu_tanh, hidden)
    active_low = active.astype(bf16)
    return (
        resid + dense(active_low, down_weight),
        (norm_back, normed_low, active_back, active_low),
    )


def feed_back(stored, up_weight, down_weight, upstream):
    norm_back, normed_low, active_back, active_low = stored
    into_active, down_grad = dense_back(active_low, down_weight, upstream.astype(bf16))
    (into_hidden,) = active_back(into_active)
    into_normed, up_grad = dense_back(normed_low, up_weight, into_hidden.astype(bf16))
    into_resid, gain_grad = norm_back(into_normed)
    return (upstream + into_resid, gain_grad, up_grad, down_grad)


def fold_rows(weight, share):
    rows, width = weight.shape
    fold = rows // share
    return weight.reshape(fold, share, width).transpose(1, 0, 2).reshape(share, fold * width)


def unfold_rows(folded, fold, share):
    rows, width = folded.shape
    width //= fold
    parts = folded.reshape(rows // share, share, fold, width).transpose(0, 2, 1, 3)
    return parts.reshape(rows * fold, width)


def fold_all(weight, share, rows):
    tall, width = weight.shape
    fold = tall // rows
    parts = weight.reshape(rows // share, fold, share, width).transpose(0, 2, 1, 3)
    return parts.reshape(rows, fold * width)


def group_columns(weight, groups, padded):
    rows, columns = weight.shape
    part = columns // 3 // groups
    grouped = weight.reshape(rows, 3, groups, part).transpose(0, 2, 1, 3).reshape(rows, groups, 3 * part)
    return jnp.pad(grouped, ((0, 0), (0, 0), (0, padded - 3 * part))).reshape(rows, groups * padded)


def pad_groups(weight, groups, padded):
    rows, columns = weight.shape
    part = rows // groups
    grouped = weight.reshape(groups, part, columns)
    return jnp.pad(grouped, ((0, 0), (0, padded - part), (0, 0))).reshape(groups * padded, columns)


def ungroup_columns(grouped, groups, padded, columns):
    rows = grouped.shape[0]
    part = columns // 3 // groups
    parts = grouped.reshape(rows, groups, padded)[:, :, : 3 * part].reshape(rows, groups, 3, part)
    return parts.transpose(0, 2, 1, 3).reshape(rows, columns)


def cut(array, widths):
    pieces, start = [], 0
    for width in widths:
        pieces.append(array[:, start : start + width])
        start += width
    return pieces


def cut_last(array, count):
    width = array.shape[-1] // count
    return [array[..., i * width : (i + 1) * width] for i in range(count)]


def gathered(parts):
    whole = lax.all_gather(jnp.concatenate(parts, axis=1), everyone, axis=0, tiled=True)
    return cut(whole, [p.shape[1] for p in parts])


def scattered(parts):
    mine = lax.psum_scatter(
        jnp.concatenate(parts, axis=1), everyone, scatter_dimension=0, tiled=True
    )
    return cut(mine, [p.shape[1] for p in parts])


def body(
    tokens,
    cotangent,
    lengths,
    mixer_gain,
    mixer_inputs,
    shift_taps,
    decay_rate,
    state_in,
    state_out,
    state_skip,
    mixer_output,
    first_gain,
    first_up,
    first_down,
    attend_gain,
    attend_inputs,
    attend_output,
    second_gain,
    second_up,
    second_down,
):
    seq_count, block_len, model_width = tokens.shape
    row_count = seq_count * block_len
    seq_devices = lax.axis_size("seq")
    share = mixer_inputs.shape[0]
    states, reach = decay_rate.shape[1], shift_taps.shape[1]
    fold = first_down.shape[0] // share
    deals = seq_count * HEADS
    dealt = deals % seq_devices == 0 and HEADS % (deals // seq_devices) == 0
    heads = deals // seq_devices if dealt else HEADS
    groups = HEADS // heads
    group_width = heads * HEAD_DIM
    padded = -(-3 * group_width // lanes) * lanes if dealt else 3 * group_width
    out_width = -(-group_width // lanes) * lanes if dealt else group_width

    columns = [decay_rate, state_in, state_out, shift_taps]
    columns += [g[:, None] for g in (mixer_gain, first_gain, attend_gain, second_gain, state_skip)]
    small = jnp.concatenate(columns, axis=1)
    small_count = small.shape[1]
    small_width = -(-small_count // lanes) * lanes
    small = jnp.pad(small, ((0, 0), (0, small_width - small_count)))
    attend_cols = attend_inputs.shape[1]
    grouped = group_columns(attend_inputs, groups, padded)
    by_kernel = seq_devices == 8 and lax.axis_size("batch") == 4
    packed = [mixer_output, attend_output, first_up, second_up, grouped]
    up1_at = 2 * model_width
    up2_at = up1_at + first_up.shape[1]
    if by_kernel:
        joint = jnp.concatenate([mixer_inputs, small], axis=1)
        w_packed = lax.all_gather(jnp.concatenate(packed, axis=1), everyone, axis=0, tiled=True)
        w_mixer_out, w_attend_out, _, _, w_attend_in = cut(w_packed, [p.shape[1] for p in packed])
        widths = (joint.shape[1], model_width)
        w_joint, w_down1 = gather_blocks((joint, first_down), chunked(widths, (4, 6)), gap=3)
        w_mixer_in, w_small = cut(w_joint, [mixer_inputs.shape[1], small_width])
        second_down, w_small = lax.optimization_barrier((second_down, w_small))
        w_down2 = lax.all_gather(second_down, everyone, axis=0, tiled=True)
    else:
        w_mixer_in, w_small = gathered([mixer_inputs, small])
        packed += [fold_rows(first_down, share), fold_rows(second_down, share)]
        w_mixer_out, w_attend_out, w_up1, w_up2, w_attend_in, w_down1, w_down2 = gathered(packed)
        w_down1 = unfold_rows(w_down1, fold, share)
        w_down2 = unfold_rows(w_down2, fold, share)

    rows = w_small.T.astype(f32)
    decay, table_in, table_out = rows[:states], rows[states : 2 * states], rows[2 * states : 3 * states]
    taps_rows = rows[3 * states : 3 * states + reach]
    gain_mixer, gain_first, gain_attend, gain_second, skip = (
        rows[3 * states + reach + i] for i in range(5)
    )
    taps = taps_rows.T
    weight = table_in * table_out

    rank_seq = lax.axis_index("seq")
    offsets = jnp.arange(block_len, dtype=jnp.int32)
    places = rank_seq * block_len + offsets
    valid = (places[None, :] < lengths[:, None]).astype(f32)
    longest = jnp.max(lengths)
    any_live = places[0] < longest

    start_resid = tokens.reshape(row_count, model_width).astype(f32)
    normed_mixer, back_mixer = jax.vjp(layer_norm, start_resid, gain_mixer)
    normed_low_mixer = normed_mixer.astype(bf16)
    projected = dense(normed_low_mixer, w_mixer_in).reshape(seq_count, block_len, 3 * model_width)
    query_mixer = projected[:, :, :model_width]
    keys_mixer = projected[:, :, model_width : 2 * model_width]
    value_mixer = projected[:, :, 2 * model_width :]
    rim_rows = passed_along(keys_mixer[:, block_len - reach + 1 :], "seq", 1)
    extended = jnp.concatenate([rim_rows, keys_mixer], axis=1)
    inner, shift_back = jax.vjp(shift_mix, extended, taps, value_mixer)
    carried = carried_in(encode(inner, decay, False), decay, block_len, False)
    wide = shaped(seq_count, block_len, model_width)
    state_y, gated = per_lane_tile(
        output_kernel,
        (inner, query_mixer, carried, decay, weight, skip[None]),
        (wide, wide),
    )
    gated_low = gated.astype(bf16).reshape(row_count, model_width)
    resid_mixer = start_resid + dense(gated_low, w_mixer_out)
    if by_kernel:
        resid_first, stored_first = feed_forward_blocks(
            resid_mixer, gain_first, w_packed, up1_at, w_down1
        )
    else:
        resid_first, stored_first = feed_forward(resid_mixer, gain_first, w_up1, w_down1)

    normed_attend, back_attend = jax.vjp(layer_norm, resid_first, gain_attend)
    normed_low_attend = normed_attend.astype(bf16)
    proj_low = dense(normed_low_attend, w_attend_in).astype(bf16)
    if dealt:
        length = seq_devices * block_len
        block = min(256, length)

        def deal(array, width):
            array = array.reshape(seq_count, block_len, groups * width)
            parts = jnp.stack(cut_last(array, groups), axis=1)
            parts = parts.reshape(seq_count * groups, block_len, width)
            dealt_parts = lax.all_to_all(parts, "seq", split_axis=0, concat_axis=0, tiled=True)
            return dealt_parts.reshape(length, width)

        def collect(array, width):
            parts = array.reshape(seq_devices, block_len, width)
            back = lax.all_to_all(parts, "seq", split_axis=0, concat_axis=0, tiled=True)
            back = back.reshape(seq_count, groups, block_len, width)
            back = jnp.concatenate([back[:, group] for group in range(groups)], axis=-1)
            return back.reshape(row_count, groups * width)

        qkv = deal(proj_low, padded)
        attended_part, attended_full, stat = attend_whole(qkv, heads, block)
        attended_low = collect(attended_part, out_width)
        w_attend_out = pad_groups(w_attend_out, groups, out_width)
    else:
        attended, attended_back = general_attention(
            proj_low, seq_count, block_len, places, any_live, longest
        )
        attended_low = attended.reshape(row_count, model_width).astype(bf16)
    resid_attend = resid_first + dense(attended_low, w_attend_out)
    if by_kernel:
        final, stored_second = feed_forward_blocks(
            resid_attend, gain_second, w_packed, up2_at, w_down2
        )
    else:
        final, stored_second = feed_forward(resid_attend, gain_second, w_up2, w_down2)
    mixed = (final.reshape(seq_count, block_len, model_width) * valid[..., None]).astype(bf16)

    upstream = (cotangent.astype(f32) * valid[..., None]).reshape(row_count, model_width)
    if by_kernel:
        upstream, second_gain_grad, early = feed_back_blocks(
            stored_second, w_packed, up2_at, w_down2, upstream, packed=(share, fold)
        )
    else:
        upstream, second_gain_grad, second_up_grad, second_down_grad = feed_back(
            stored_second, w_up2, w_down2, upstream
        )
        early = [second_up_grad, fold_all(second_down_grad, share, model_width)]
        early = jnp.concatenate(early, axis=1)
    into_attended, attend_output_grad = dense_back(
        attended_low, w_attend_out, upstream.astype(bf16)
    )
    if dealt:
        attend_output_grad = attend_output_grad.reshape(groups, out_width, model_width)
        attend_output_grad = attend_output_grad[:, :group_width].reshape(model_width, model_width)
    dout_low = into_attended.astype(bf16)
    if dealt:
        dout = deal(dout_low, out_width)
        proj_grad = collect(
            attend_whole_back(qkv, dout, attended_full, stat, heads, block), padded
        )
    else:
        parts = attended_back(dout_low.reshape(seq_count, block_len, HEADS, HEAD_DIM))
        proj_grad = jnp.concatenate(
            [p.reshape(row_count, model_width) for p in parts], axis=1
        ).astype(bf16)
    early = lax.psum_scatter(early, everyone, scatter_dimension=0, tiled=True)
    second_up_out, second_down_out = cut(early, [second_up.shape[1], fold * model_width])
    into_normed, attend_inputs_grad = dense_back(normed_low_attend, w_attend_in, proj_grad)
    into_resid, attend_gain_grad = back_attend(into_normed)
    upstream = upstream + into_resid
    if by_kernel:
        upstream, first_gain_grad, first_up_grad, first_down_grad = feed_back_blocks(
            stored_first, w_packed, up1_at, w_down1, upstream
        )
    else:
        upstream, first_gain_grad, first_up_grad, first_down_grad = feed_back(
            stored_first, w_up1, w_down1, upstream
        )
    into_gated, mixer_output_grad = dense_back(gated_low, w_mixer_out, upstream.astype(bf16))
    into_gated = into_gated.reshape(seq_count, block_len, model_width)
    query_mixer_grad = into_gated * state_y
    state_grad = into_gated * query_mixer
    later = carried_in(encode(state_grad, decay, True), decay, block_len, True)
    table = shaped(states, model_width)
    inner_grad, weight_grad, power_grad, skip_grad = per_lane_tile(
        back_kernel,
        (inner, state_grad, carried, later, decay, weight, skip[None]),
        (wide, table, table, shaped(1, model_width)),
        scratch=[pltpu.VMEM((block_len, seq_count, states, lanes), f32)],
    )
    extended_grad, taps_grad, value_mixer_grad = shift_back(inner_grad)
    spill = passed_along(extended_grad[:, : reach - 1], "seq", -1)
    keys_mixer_grad = extended_grad[:, reach - 1 :] + jnp.pad(
        spill, ((0, 0), (block_len - reach + 1, 0), (0, 0))
    )
    proj_grad_mixer = (
        jnp.concatenate([query_mixer_grad, keys_mixer_grad, value_mixer_grad], axis=2)
        .astype(bf16)
        .reshape(row_count, 3 * model_width)
    )
    into_normed_mixer, mixer_inputs_grad = dense_back(normed_low_mixer, w_mixer_in, proj_grad_mixer)
    into_start, mixer_gain_grad = back_mixer(into_normed_mixer)
    tokens_gradient = (upstream + into_start).reshape(seq_count, block_len, model_width).astype(bf16)

    small_rows = jnp.concatenate(
        [-jnp.exp(-decay) * power_grad, weight_grad * table_out, weight_grad * table_in, taps_grad.T]
        + [
            g[None]
            for g in (mixer_gain_grad, first_gain_grad, attend_gain_grad, second_gain_grad, skip_grad[0])
        ],
        axis=0,
    )
    small_grad = jnp.pad(small_rows, ((0, small_width - small_count), (0, 0))).T.astype(bf16)
    def unfolded(folded):
        return folded.reshape(share, fold, model_width).transpose(1, 0, 2).reshape(share * fold, model_width)

    gains_at = 3 * states + reach
    table_edges = [0, states, 2 * states, 3 * states, gains_at, small_width]

    def tables_of(block):
        return [block[:, a:b] for a, b in zip(table_edges, table_edges[1:])]

    last = [attend_inputs_grad, first_up_grad, mixer_output_grad, mixer_inputs_grad, small_grad]
    if by_kernel:
        last += [first_down_grad, attend_output_grad]
        plan = chunked([g.shape[1] for g in last], (6, 6, 2, 6, 2, 4, 2))
        part = attend_cols // 3 // groups

        def finish(index, block, results):
            if index == 0:
                for group in range(groups):
                    for kind in range(3):
                        start = (kind * groups + group) * part
                        source = group * padded + kind * part
                        results[0][:, start : start + part] = block[:, source : source + part]
            elif index == 4:
                for place, table in enumerate(tables_of(block)):
                    results[5 + place][...] = table
            else:
                results[{1: 1, 2: 2, 3: 3, 5: 4, 6: 10}[index]][...] = block[...]

        widths = [attend_cols] + [g.shape[1] for g in last[1:4]]
        results = [shaped(share, w) for w in widths] + [shaped(share * fold, model_width)]
        results += [shaped(share, b - a) for a, b in zip(table_edges, table_edges[1:])]
        results.append(shaped(share, model_width))
        attend_inputs_out, first_up_out, mixer_output_out, mixer_inputs_out, first_down_out, *tables = (
            scatter_blocks(last, plan, finish, results, gap=4)
        )
        *tables, attend_output_out = tables
    else:
        last += [fold_all(first_down_grad, share, model_width), attend_output_grad]
        *last, folded, attend_output_out = scattered(last)
        first_down_out = unfolded(folded).astype(f32)
        grouped, first_up_out, mixer_output_out, mixer_inputs_out, small_out = (
            g.astype(f32) for g in last
        )
        attend_inputs_out = ungroup_columns(grouped, groups, padded, attend_cols)
        tables = tables_of(small_out)
    decay_out, in_out, out_out, taps_out, vectors = tables

    return (
        mixed,
        tokens_gradient,
        vectors[:, 0],
        mixer_inputs_out,
        taps_out,
        decay_out,
        in_out,
        out_out,
        vectors[:, 4],
        mixer_output_out,
        vectors[:, 1],
        first_up_out,
        first_down_out,
        vectors[:, 2],
        attend_inputs_out,
        attend_output_out.astype(f32),
        vectors[:, 3],
        second_up_out.astype(f32),
        unfolded(second_down_out).astype(f32),
    )


def solution(mesh):
    return jax.shard_map(
        body,
        mesh=mesh,
        in_specs=(
            P("batch", "seq", None),
            P("batch", "seq", None),
            P("batch"),
            P(("seq", "batch")),
            P(("seq", "batch"), None),
            P(("seq", "batch"), None),
            P(("seq", "batch"), None),
            P(("seq", "batch"), None),
            P(("seq", "batch"), None),
            P(("seq", "batch")),
            P(("seq", "batch"), None),
            P(("seq", "batch")),
            P(("seq", "batch"), None),
            P(("seq", "batch"), None),
            P(("seq", "batch")),
            P(("seq", "batch"), None),
            P(("seq", "batch"), None),
            P(("seq", "batch")),
            P(("seq", "batch"), None),
            P(("seq", "batch"), None),
        ),
        out_specs=(
            P("batch", "seq", None),
            P("batch", "seq", None),
            P(("seq", "batch")),
            P(("seq", "batch"), None),
            P(("seq", "batch"), None),
            P(("seq", "batch"), None),
            P(("seq", "batch"), None),
            P(("seq", "batch"), None),
            P(("seq", "batch")),
            P(("seq", "batch"), None),
            P(("seq", "batch")),
            P(("seq", "batch"), None),
            P(("seq", "batch"), None),
            P(("seq", "batch")),
            P(("seq", "batch"), None),
            P(("seq", "batch"), None),
            P(("seq", "batch")),
            P(("seq", "batch"), None),
            P(("seq", "batch"), None),
        ),
        check_vma=False,
    )
```

```python
import functools

import jax
import jax.numpy as jnp
from jax import lax
from jax.experimental import pallas as pl
from jax.experimental.pallas import tpu as pltpu
from jax.sharding import PartitionSpec as P

HEADS = 12
HEAD_DIM = 64

eps = 1e-05
masked_score = -1e30
lanes = 128
sublanes = 8
everyone = ("seq", "batch")
f32 = jnp.float32
bf16 = jnp.bfloat16


def rows_of(ref, seq, block):
    return ref[seq, pl.ds(pl.multiple_of(block * sublanes, sublanes), sublanes), :]


def spread(rows, index, count):
    return jnp.broadcast_to(rows[index : index + 1], (count, lanes))


def encode_kernel(reverse, input_ref, decay_ref, end_ref):
    seq_count, step_count, _ = input_ref.shape
    state_count = decay_ref.shape[0]
    blocks = step_count // sublanes
    power = jnp.exp(-decay_ref[...])

    def one_block(step, states):
        block = blocks - 1 - step if reverse else step
        rows = [rows_of(input_ref, seq, block) for seq in range(seq_count)]
        order = range(sublanes - 1, -1, -1) if reverse else range(sublanes)
        states = list(states)
        for index in order:
            for seq in range(seq_count):
                states[seq] = states[seq] * power + spread(rows[seq], index, state_count)
        return tuple(states)

    start = tuple(jnp.zeros((state_count, lanes), f32) for _ in range(seq_count))
    ends = lax.fori_loop(0, blocks, one_block, start)
    for seq in range(seq_count):
        end_ref[seq] = ends[seq]


def output_kernel(input_ref, query_ref, carried_ref, decay_ref, weight_ref, skip_ref, out_ref, gated_ref):
    seq_count, step_count, _ = input_ref.shape
    state_count = decay_ref.shape[0]
    power = jnp.exp(-decay_ref[...])
    weight = weight_ref[...]
    skip = skip_ref[...]

    def one_block(block, states):
        states = list(states)
        rows = [rows_of(input_ref, seq, block) for seq in range(seq_count)]
        found = [[] for _ in range(seq_count)]
        for index in range(sublanes):
            for seq in range(seq_count):
                states[seq] = states[seq] * power + spread(rows[seq], index, state_count)
                found[seq].append(jnp.sum(states[seq] * weight, axis=0, keepdims=True))
        place = pl.ds(pl.multiple_of(block * sublanes, sublanes), sublanes)
        for seq in range(seq_count):
            result = jnp.concatenate(found[seq], axis=0) + skip * rows[seq]
            out_ref[seq, place, :] = result
            gated_ref[seq, place, :] = result * rows_of(query_ref, seq, block)
        return tuple(states)

    start = tuple(carried_ref[seq].astype(f32) for seq in range(seq_count))
    lax.fori_loop(0, step_count // sublanes, one_block, start)


def back_kernel(
    input_ref,
    grad_ref,
    carried_ref,
    later_ref,
    decay_ref,
    weight_ref,
    skip_ref,
    input_grad_ref,
    weight_grad_ref,
    power_grad_ref,
    skip_grad_ref,
    held,
):
    seq_count, step_count, _ = input_ref.shape
    state_count = decay_ref.shape[0]
    blocks = step_count // sublanes
    power = jnp.exp(-decay_ref[...])
    weight = weight_ref[...]
    skip = skip_ref[...]
    seqs = range(seq_count)

    def forward_block(block, state):
        states, total, skip_total = list(state[0]), state[1], state[2]
        rows = [rows_of(input_ref, seq, block) for seq in seqs]
        grads = [rows_of(grad_ref, seq, block) for seq in seqs]
        for index in range(sublanes):
            for seq in seqs:
                held[block * sublanes + index, seq] = states[seq]
                states[seq] = states[seq] * power + spread(rows[seq], index, state_count)
                total = total + states[seq] * spread(grads[seq], index, state_count)
        for seq in seqs:
            skip_total = skip_total + rows[seq] * grads[seq]
        return (tuple(states), total, skip_total)

    zeros = jnp.zeros((state_count, lanes), f32)
    _, total, skip_total = lax.fori_loop(
        0,
        blocks,
        forward_block,
        (
            tuple(carried_ref[seq].astype(f32) for seq in seqs),
            zeros,
            jnp.zeros((sublanes, lanes), f32),
        ),
    )
    weight_grad_ref[...] = total
    skip_grad_ref[...] = jnp.sum(skip_total, axis=0, keepdims=True)

    def back_block(step, state):
        states, total = list(state[0]), state[1]
        block = blocks - 1 - step
        grads = [rows_of(grad_ref, seq, block) for seq in seqs]
        found = [[None] * sublanes for _ in seqs]
        for index in range(sublanes - 1, -1, -1):
            for seq in seqs:
                states[seq] = states[seq] * power + spread(grads[seq], index, state_count)
                found[seq][index] = jnp.sum(states[seq] * weight, axis=0, keepdims=True)
                total = total + states[seq] * held[block * sublanes + index, seq]
        place = pl.ds(pl.multiple_of(block * sublanes, sublanes), sublanes)
        for seq in seqs:
            input_grad_ref[seq, place, :] = jnp.concatenate(found[seq], axis=0) + skip * grads[seq]
        return (tuple(states), total)

    _, total = lax.fori_loop(
        0, blocks, back_block, (tuple(later_ref[seq].astype(f32) for seq in seqs), zeros)
    )
    power_grad_ref[...] = total * weight


def per_lane_tile(kernel, args, outs, scratch=(), flops=0):
    def spec(shape):
        lead = len(shape) - 1
        return pl.BlockSpec(tuple(shape[:-1]) + (lanes,), lambda tile: (0,) * lead + (tile,))

    bytes_moved = sum(a.size * a.dtype.itemsize for a in args)
    return pl.pallas_call(
        kernel,
        grid=(args[0].shape[-1] // lanes,),
        in_specs=[spec(a.shape) for a in args],
        out_specs=[spec(o.shape) for o in outs],
        out_shape=list(outs),
        scratch_shapes=list(scratch),
        cost_estimate=pl.CostEstimate(flops=flops, bytes_accessed=bytes_moved, transcendentals=0),
        compiler_params=pltpu.CompilerParams(vmem_limit_bytes=48 * 1024 * 1024),
    )(*args)


def shaped(*dims, dtype=f32):
    return jax.ShapeDtypeStruct(dims, dtype)


def encode(value, decay, reverse):
    seq_count, _, width = value.shape
    (ends,) = per_lane_tile(
        functools.partial(encode_kernel, reverse),
        (value, decay),
        (shaped(seq_count, decay.shape[0], width),),
    )
    return ends


def passed_along(block, axis, distance):
    devices = range(lax.axis_size(axis))
    route = [(i - distance, i) for i in devices if i - distance in devices]
    return lax.ppermute(block, axis, route)


def carried_in(ends, decay, block_len, reverse):
    seq_count, state_count, width = ends.shape
    count = lax.axis_size("seq")
    part = state_count // count

    def exchanged(parts):
        return lax.all_to_all(parts.astype(bf16), "seq", split_axis=0, concat_axis=0, tiled=True)

    parts = ends.reshape(seq_count, count, part, width).transpose(1, 0, 2, 3)
    arrived = exchanged(parts.reshape(count, seq_count * part, width)).astype(f32)
    rates = lax.dynamic_slice_in_dim(decay, lax.axis_index("seq") * part, part, 0)
    power = jnp.tile(jnp.exp(-rates * block_len), (seq_count, 1))
    state, joined = jnp.zeros_like(arrived[0]), [None] * count
    for block in reversed(range(count)) if reverse else range(count):
        joined[block] = state
        state = power * state + arrived[block]
    back = exchanged(jnp.stack(joined))
    back = back.reshape(count, seq_count, part, width).transpose(1, 0, 2, 3)
    return back.reshape(seq_count, state_count, width)


MESH = pl.DeviceIdType.MESH
box = (4, 2, 2, 2)


def here():
    seq, batch = lax.axis_index("seq"), lax.axis_index("batch")
    return lax.div(seq, 2), lax.rem(seq, 2), lax.div(batch, 2), lax.rem(batch, 2)


def device(z, x, y, core):
    return (2 * z + x, 2 * y + core)


def line_peer(z, step):
    return lax.rem(z + step, box[0])


def greet():
    z, x, y, core = here()
    barrier = pltpu.get_barrier_semaphore()
    peers = [device(line_peer(z, step), x, y, core) for step in range(1, box[0])]
    peers += [device(z, 1 - x, y, core), device(z, x, 1 - y, core), device(z, x, y, 1 - core)]
    for peer in peers:
        pl.semaphore_signal(barrier, inc=1, device_id=peer, device_id_type=MESH)
    pl.semaphore_wait(barrier, len(peers))


def staggered(count, stages, gap):
    for turn in range(count + gap * (stages - 1)):
        for stage in reversed(range(stages)):
            chunk = turn - gap * stage
            if 0 <= chunk < count:
                yield stage, chunk


def gather_kernel(plan, gap, *refs):
    count = 1 + max(item[0] for item in plan)
    ins, outs = refs[:count], refs[count : 2 * count]
    send, receive, local = refs[2 * count :]
    z, x, y, core = here()
    greet()
    started = {}

    def push(chunk, slot, source, target, peer):
        copy = pltpu.make_async_remote_copy(
            src_ref=source,
            dst_ref=target,
            send_sem=send.at[chunk, slot],
            recv_sem=receive.at[chunk, slot],
            device_id=peer,
            device_id_type=MESH,
        )
        copy.start()
        started[chunk, slot] = copy

    own = []
    for chunk, (index, first, width, _) in enumerate(plan):
        columns = pl.ds(first, width)
        source = ins[index].at[:, columns]
        target = outs[index].at[z, x, y, core, :, columns]
        for step in range(1, box[0]):
            push(chunk, step - 1, source, target, device(line_peer(z, step), x, y, core))
        keep = pltpu.make_async_copy(source, target, local.at[chunk])
        keep.start()
        own.append(keep)

    for stage, chunk in staggered(len(plan), 3, gap):
        index, first, width, order = plan[chunk]
        x_first = order[1] == "x"
        columns = pl.ds(first, width)
        out = outs[index]
        if stage == 0:
            for step in range(1, box[0]):
                started[chunk, step - 1].wait_recv()
            own[chunk].wait()
            part = out.at[:, x, y, core, :, columns]
            peer = device(z, 1 - x, y, core) if x_first else device(z, x, 1 - y, core)
            push(chunk, 3, part, part, peer)
        elif stage == 1:
            started[chunk, 3].wait_recv()
            if x_first:
                part, peer = out.at[:, :, y, core, :, columns], device(z, x, 1 - y, core)
            else:
                part, peer = out.at[:, x, :, core, :, columns], device(z, 1 - x, y, core)
            push(chunk, 4, part, part, peer)
        else:
            started[chunk, 4].wait_recv()
            part = out.at[:, :, :, core, :, columns]
            push(chunk, 5, part, part, device(z, x, y, 1 - core))
    for chunk in range(len(plan)):
        started[chunk, 5].wait_recv()
        for slot in range(6):
            started[chunk, slot].wait_send()


def gather_blocks(blocks, plan, gap=2, collective=0):
    outs = [jax.ShapeDtypeStruct(box + b.shape, b.dtype) for b in blocks]
    sent = sum(b.size * b.dtype.itemsize for b in blocks)
    whole = pl.pallas_call(
        functools.partial(gather_kernel, plan, gap),
        out_shape=outs,
        in_specs=[pl.BlockSpec(memory_space=pltpu.VMEM)] * len(blocks),
        out_specs=[pl.BlockSpec(memory_space=pl.ANY)] * len(blocks),
        scratch_shapes=[
            pltpu.SemaphoreType.DMA((len(plan), 6)),
            pltpu.SemaphoreType.DMA((len(plan), 6)),
            pltpu.SemaphoreType.DMA((len(plan),)),
        ],
        cost_estimate=pl.CostEstimate(flops=0, bytes_accessed=64 * sent, transcendentals=0),
        compiler_params=pltpu.CompilerParams(collective_id=collective, has_side_effects=True),
    )(*blocks)
    return [w.reshape((32 * w.shape[4], w.shape[5])) for w in whole]


def add_into(total, other):
    return (total.astype(f32) + other.astype(f32)).astype(bf16)


def scatter_kernel(plan, gap, finish, counts, *refs):
    count, out_count = counts
    ins, results = refs[:count], refs[count : count + out_count]
    outs, buffers = refs[count + out_count : 2 * count + out_count], refs[2 * count + out_count : -3]
    send, receive, local = refs[-3:]
    z, x, y, core = here()
    greet()
    started = {}

    def push(chunk, slot, source, target, peer):
        copy = pltpu.make_async_remote_copy(
            src_ref=source,
            dst_ref=target,
            send_sem=send.at[chunk, slot],
            recv_sem=receive.at[chunk, slot],
            device_id=peer,
            device_id_type=MESH,
        )
        copy.start()
        started[chunk, slot] = copy

    loads = []
    for chunk, (index, first, width, _) in enumerate(plan):
        columns = pl.ds(first, width)
        held, from_core = buffers[5 * chunk : 5 * chunk + 2]
        grad = ins[index]
        push(chunk, 0, grad.at[:, :, :, 1 - core, :, columns], from_core, device(z, x, y, 1 - core))
        load = pltpu.make_async_copy(grad.at[:, :, :, core, :, columns], held, local.at[chunk])
        load.start()
        loads.append(load)

    for stage, chunk in staggered(len(plan), 4, gap):
        index, first, width, order = plan[chunk]
        x_first, line_last = order[0] == "y", order[-1] == "z"
        held, from_core, from_one, from_two, from_line = buffers[5 * chunk : 5 * chunk + 5]
        to_x, to_y = device(z, 1 - x, y, core), device(z, x, 1 - y, core)
        if stage == 0:
            started[chunk, 0].wait_recv()
            loads[chunk].wait()

            @pl.loop(0, box[0])
            def _(row):
                for i in range(2):
                    for j in range(2):
                        held[row, i, j] = add_into(held[row, i, j], from_core[row, i, j])

            if x_first:
                push(chunk, 1, held.at[:, :, 1 - y], from_one, to_y)
            else:
                push(chunk, 1, held.at[:, 1 - x], from_one, to_x)
        elif stage == 1:
            started[chunk, 1].wait_recv()

            @pl.loop(0, box[0])
            def _(row):
                for i in range(2):
                    if x_first:
                        held[row, i, y] = add_into(held[row, i, y], from_one[row, i])
                    else:
                        held[row, x, i] = add_into(held[row, x, i], from_one[row, i])

            if not line_last:
                for step in range(1, box[0]):
                    peer = line_peer(z, step)
                    rest = held.at[peer, :, y] if x_first else held.at[peer, x]
                    push(chunk, 2 + step, rest, from_line.at[step - 1], device(peer, x, y, core))
            elif x_first:
                push(chunk, 2, held.at[:, 1 - x, y], from_two, to_x)
            else:
                push(chunk, 2, held.at[:, x, 1 - y], from_two, to_y)
        elif stage == 2 and not line_last:
            for step in range(1, box[0]):
                started[chunk, 2 + step].wait_recv()
            for i in range(2):
                at = (z, i, y) if x_first else (z, x, i)
                total = held[at].astype(f32)
                for step in range(1, box[0]):
                    total = total + from_line[step - 1, i].astype(f32)
                held[at] = total.astype(bf16)
            if x_first:
                push(chunk, 2, held.at[z, 1 - x, y], from_two, to_x)
            else:
                push(chunk, 2, held.at[z, x, 1 - y], from_two, to_y)
        elif stage == 2:
            started[chunk, 2].wait_recv()

            @pl.loop(0, box[0])
            def _(row):
                held[row, x, y] = add_into(held[row, x, y], from_two[row])

            for step in range(1, box[0]):
                peer = line_peer(z, step)
                push(chunk, 2 + step, held.at[peer, x, y], from_line.at[step - 1], device(peer, x, y, core))
        else:
            total = held[z, x, y].astype(f32)
            if line_last:
                for step in range(1, box[0]):
                    started[chunk, 2 + step].wait_recv()
                    total = total + from_line[step - 1].astype(f32)
            else:
                started[chunk, 2].wait_recv()
                total = total + from_two[...].astype(f32)
            outs[index][:, pl.ds(first, width)] = total
            if not any(item[0] == index for item in plan[chunk + 1 :]):
                finish(index, outs[index], results)
    for chunk in range(len(plan)):
        for slot in range(6):
            started[chunk, slot].wait_send()


def scatter_blocks(grads, plan, finish, results, gap=2, collective=1):
    views = [g.reshape(box + (g.shape[0] // 32, g.shape[1])) for g in grads]
    scratch = [pltpu.VMEM(v.shape[4:], f32) for v in views]
    for index, _, width, order in plan:
        tile = (views[index].shape[4], width)
        ends_of = ((4,), (3,)) if order[-1] == "z" else ((), (3, 2))
        for lead in ((4, 2, 2), (4, 2, 2), (4, 2)) + ends_of:
            scratch.append(pltpu.VMEM(lead + tile, bf16))
    sent = sum(v.size * v.dtype.itemsize for v in views)
    return pl.pallas_call(
        functools.partial(scatter_kernel, plan, gap, finish, (len(views), len(results))),
        out_shape=list(results),
        in_specs=[pl.BlockSpec(memory_space=pl.ANY)] * len(views),
        out_specs=[pl.BlockSpec(memory_space=pltpu.VMEM)] * len(results),
        scratch_shapes=scratch
        + [
            pltpu.SemaphoreType.DMA((len(plan), 6)),
            pltpu.SemaphoreType.DMA((len(plan), 6)),
            pltpu.SemaphoreType.DMA((len(plan),)),
        ],
        cost_estimate=pl.CostEstimate(flops=0, bytes_accessed=4 * sent, transcendentals=0),
        compiler_params=pltpu.CompilerParams(
            collective_id=collective, has_side_effects=True, vmem_limit_bytes=60 * 1024 * 1024
        ),
    )(*views)


def chunked(widths, pieces, orders):
    plan = []
    for index, (width, number) in enumerate(zip(widths, pieces)):
        tiles = width // lanes
        edges = [tiles * i // number for i in range(number + 1)]
        for i in range(number):
            plan.append((index, edges[i] * lanes, (edges[i + 1] - edges[i]) * lanes, orders[len(plan) % len(orders)]))
    return plan


def carry_kernel(
    reverse, input_ref, decay_ref, carried_ref, ends, outgoing, arrived, joined, final, send, receive
):
    seq_count, step_count, width = input_ref.shape
    count = lax.axis_size("seq")
    part = decay_ref.shape[0] // count
    me, batch = lax.axis_index("seq"), lax.axis_index("batch")
    others = range(1, count)
    barrier = pltpu.get_barrier_semaphore()
    for step in others:
        peer = (lax.rem(me + step, count), batch)
        pl.semaphore_signal(barrier, inc=1, device_id=peer, device_id_type=MESH)

    for tile in range(width // lanes):
        columns = slice(tile * lanes, (tile + 1) * lanes)
        encode_kernel(reverse, input_ref.at[:, :, columns], decay_ref.at[:, columns], ends)
        for group in range(count):
            rows = slice(group * part, (group + 1) * part)
            mine = jnp.concatenate([ends[seq, rows] for seq in range(seq_count)], axis=0)
            outgoing[group, :, columns] = mine.astype(bf16)
    pl.semaphore_wait(barrier, count - 1)

    def exchange(phase, source, target):
        copies = []
        for step in others:
            peer = lax.rem(me + step, count)
            copy = pltpu.make_async_remote_copy(
                src_ref=source.at[peer],
                dst_ref=target.at[me],
                send_sem=send.at[phase, step - 1],
                recv_sem=receive.at[phase, step - 1],
                device_id=(peer, batch),
                device_id_type=MESH,
            )
            copy.start()
            copies.append(copy)
        target[me] = source[me]
        for copy in copies:
            copy.wait()

    exchange(0, outgoing, arrived)
    rates = decay_ref[pl.ds(pl.multiple_of(me * part, part), part), :]
    power = jnp.exp(-rates * step_count)
    power = jnp.concatenate([power] * seq_count, axis=0)
    state = jnp.zeros(power.shape, f32)
    for block in reversed(range(count)) if reverse else range(count):
        joined[block] = state.astype(bf16)
        state = power * state + arrived[block].astype(f32)
    exchange(1, joined, final)
    for group in range(count):
        rows = slice(group * part, (group + 1) * part)
        found = final[group].astype(f32)
        for seq in range(seq_count):
            carried_ref[seq, rows] = found[seq * part : (seq + 1) * part]


def carried_by_kernel(value, decay, reverse, collective):
    seq_count, _, width = value.shape
    state_count = decay.shape[0]
    count = lax.axis_size("seq")
    parts = pltpu.VMEM((count, seq_count * state_count // count, width), bf16)
    return pl.pallas_call(
        functools.partial(carry_kernel, reverse),
        out_shape=shaped(seq_count, state_count, width),
        in_specs=[pl.BlockSpec(memory_space=pltpu.VMEM)] * 2,
        out_specs=pl.BlockSpec(memory_space=pltpu.VMEM),
        scratch_shapes=[pltpu.VMEM((seq_count, state_count, lanes), f32)]
        + [parts] * 4
        + [pltpu.SemaphoreType.DMA((2, count - 1)), pltpu.SemaphoreType.DMA((2, count - 1))],
        cost_estimate=pl.CostEstimate(flops=0, bytes_accessed=32 * value.size, transcendentals=0),
        compiler_params=pltpu.CompilerParams(collective_id=collective, has_side_effects=True),
    )(value, decay)


hidden_block = 768
gelu_scale = 0.7978845608
gelu_cubic = 0.044715


def feed_kernel(resid_ref, gain_ref, up_ref, down_ref, out_ref, normed_ref, hidden_ref, active_ref):
    @pl.when(pl.program_id(0) == 0)
    def _():
        resid = resid_ref[...]
        normed_ref[...] = layer_norm(resid, gain_ref[...]).astype(bf16)
        out_ref[...] = resid

    hidden = jnp.dot(normed_ref[...], up_ref[...], preferred_element_type=f32)
    hidden_ref[...] = hidden
    bend = jnp.tanh(gelu_scale * (hidden + gelu_cubic * hidden * hidden * hidden))
    active = (0.5 * hidden * (1.0 + bend)).astype(bf16)
    active_ref[...] = active
    out_ref[...] += jnp.dot(active, down_ref[...], preferred_element_type=f32)


def feed_forward_blocks(resid, gain, up_packed, up_at, down):
    rows, width = resid.shape
    inner = down.shape[0]
    first = up_at // hidden_block
    whole = pl.BlockSpec((rows, width), lambda j: (0, 0))
    part = pl.BlockSpec((rows, hidden_block), lambda j: (0, j))
    out, normed, hidden, active = pl.pallas_call(
        feed_kernel,
        grid=(inner // hidden_block,),
        in_specs=[
            whole,
            pl.BlockSpec((1, width), lambda j: (0, 0)),
            pl.BlockSpec((width, hidden_block), lambda j: (0, first + j)),
            pl.BlockSpec((hidden_block, width), lambda j: (j, 0)),
        ],
        out_specs=[whole, whole, part, part],
        out_shape=[
            shaped(rows, width),
            shaped(rows, width, dtype=bf16),
            shaped(rows, inner),
            shaped(rows, inner, dtype=bf16),
        ],
        cost_estimate=pl.CostEstimate(
            flops=4 * rows * width * inner, bytes_accessed=10 * width * inner, transcendentals=rows * inner
        ),
        compiler_params=pltpu.CompilerParams(vmem_limit_bytes=40 * 1024 * 1024),
    )(resid, gain[None], up_packed, down)
    return out, (resid, gain, normed, hidden, active)


def feed_back_kernel(
    packed,
    upstream_ref,
    resid_ref,
    gain_ref,
    normed_ref,
    hidden_ref,
    active_ref,
    up_ref,
    down_ref,
    out_ref,
    gain_grad_ref,
    *rest,
):
    step = pl.program_id(0)
    last = pl.num_programs(0) - 1
    across = (((1,), (1,)), ((), ()))
    along = (((0,), (0,)), ((), ()))
    upstream_low = upstream_ref[...].astype(bf16)
    into_active = lax.dot_general(upstream_low, down_ref[...], across, preferred_element_type=f32)
    hidden = hidden_ref[...]
    square = hidden * hidden
    bend = jnp.tanh(gelu_scale * hidden * (1.0 + gelu_cubic * square))
    slope = 0.5 * (1.0 + bend) + 0.5 * hidden * (1.0 - bend * bend) * (
        gelu_scale * (1.0 + 3.0 * gelu_cubic * square)
    )
    into_hidden = (into_active * slope).astype(bf16)
    part = lax.dot_general(into_hidden, up_ref[...], across, preferred_element_type=f32)

    @pl.when(step == 0)
    def _():
        out_ref[...] = part

    @pl.when(step > 0)
    def _():
        out_ref[...] += part

    up_grad = lax.dot_general(normed_ref[...], into_hidden, along, preferred_element_type=f32)
    down_grad = lax.dot_general(active_ref[...], upstream_low, along, preferred_element_type=f32)
    if packed:
        grads_ref, up_held, down_held, sems = rest
        share, fold = packed
        width = up_grad.shape[0]
        inner = hidden_block * grads_ref.shape[1] // (2 * hidden_block)
        tall = hidden_block // fold
        slot = lax.rem(step, 2)

        def copies(at, slot):
            columns = pl.ds(pl.multiple_of(at * hidden_block, hidden_block), hidden_block)
            rows = pl.ds(pl.multiple_of(at * tall, tall), tall)
            return (
                pltpu.make_async_copy(up_held.at[slot], grads_ref.at[:, columns], sems.at[0, slot]),
                pltpu.make_async_copy(down_held.at[slot], grads_ref.at[rows, inner:], sems.at[1, slot]),
            )

        @pl.when(step >= 2)
        def _():
            for copy in copies(step - 2, slot):
                copy.wait()

        up_held[slot] = up_grad.astype(bf16)
        for place in range(fold):
            starts = range(place * share, hidden_block, fold * share)
            piece = jnp.concatenate([down_grad[a : a + share] for a in starts], axis=0)
            down_held[slot, :, place * width : (place + 1) * width] = piece.astype(bf16)
        for copy in copies(step, slot):
            copy.start()

        @pl.when(step == last)
        def _():
            for copy in copies(step - 1, 1 - slot) + copies(step, slot):
                copy.wait()
    else:
        up_grad_ref, down_grad_ref = rest
        up_grad_ref[...] = up_grad.astype(bf16)
        down_grad_ref[...] = down_grad.astype(bf16)

    @pl.when(step == last)
    def _():
        into_normed = out_ref[...]
        resid = resid_ref[...]
        centred = resid - jnp.mean(resid, axis=-1, keepdims=True)
        inverse = lax.rsqrt(jnp.mean(centred * centred, axis=-1, keepdims=True) + eps)
        unit = centred * inverse
        gain_grad_ref[...] = jnp.sum(into_normed * unit, axis=0, keepdims=True)
        scaled = into_normed * gain_ref[...]
        along_unit = jnp.mean(scaled * unit, axis=-1, keepdims=True)
        into_resid = inverse * (scaled - jnp.mean(scaled, axis=-1, keepdims=True) - unit * along_unit)
        out_ref[...] = upstream_ref[...] + into_resid


def feed_back_blocks(stored, up_packed, up_at, down, upstream, packed=()):
    resid, gain, normed, hidden, active = stored
    rows, width = resid.shape
    inner = down.shape[0]
    first = up_at // hidden_block
    whole = pl.BlockSpec((rows, width), lambda j: (0, 0))
    part = pl.BlockSpec((rows, hidden_block), lambda j: (0, j))
    line = pl.BlockSpec((1, width), lambda j: (0, 0))
    up_spec = pl.BlockSpec((width, hidden_block), lambda j: (0, j))
    down_spec = pl.BlockSpec((hidden_block, width), lambda j: (j, 0))
    scratch = []
    if packed:
        grad_specs = [pl.BlockSpec(memory_space=pl.ANY)]
        grad_shapes = [shaped(width, 2 * inner, dtype=bf16)]
        scratch = [
            pltpu.VMEM((2, width, hidden_block), bf16),
            pltpu.VMEM((2, hidden_block // packed[1], inner), bf16),
            pltpu.SemaphoreType.DMA((2, 2)),
        ]
    else:
        grad_specs = [up_spec, down_spec]
        grad_shapes = [shaped(width, inner, dtype=bf16), shaped(inner, width, dtype=bf16)]
    out, gain_grad, *grads = pl.pallas_call(
        functools.partial(feed_back_kernel, packed),
        grid=(inner // hidden_block,),
        in_specs=[
            whole,
            whole,
            line,
            whole,
            part,
            part,
            pl.BlockSpec((width, hidden_block), lambda j: (0, first + j)),
            down_spec,
        ],
        out_specs=[whole, line] + grad_specs,
        out_shape=[shaped(rows, width), shaped(1, width)] + grad_shapes,
        scratch_shapes=scratch,
        cost_estimate=pl.CostEstimate(
            flops=8 * rows * width * inner, bytes_accessed=16 * width * inner, transcendentals=rows * inner
        ),
        compiler_params=pltpu.CompilerParams(vmem_limit_bytes=48 * 1024 * 1024),
    )(upstream, resid, gain[None], normed, hidden, active, up_packed, down)
    return (out, gain_grad[0], *grads)


def split_heads(ref, scratch, heads, parts, first=0):
    for part in range(parts):
        for head in range(heads):
            start = (part * heads + head) * HEAD_DIM + first
            scratch[part * heads + head] = ref[:, start : start + HEAD_DIM]


def score_block(query, keys, first, scale):
    scores = (
        lax.dot_general(query, keys, (((1,), (1,)), ((), ())), preferred_element_type=f32) * scale
    )
    rows = lax.broadcasted_iota(jnp.int32, scores.shape, 0) + first
    columns = lax.broadcasted_iota(jnp.int32, scores.shape, 1)
    return jnp.where(columns <= rows, scores, masked_score)


def attend_kernel(heads, block, scale, qkv_ref, low_ref, full_ref, stat_ref, parts, outs):
    length = qkv_ref.shape[0]
    split_heads(qkv_ref, parts, heads, 3)

    @pl.loop(0, heads)
    def _(head):
        for first in range(0, length, block):
            extent = first + block
            query = parts[head, first:extent, :]
            scores = score_block(query, parts[heads + head, :extent, :], first, scale)
            top = jnp.max(scores, axis=1, keepdims=True)
            soft = jnp.exp(scores - top)
            whole = jnp.sum(soft, axis=1, keepdims=True)
            soft = soft * (1.0 / whole)
            outs[head, first:extent, :] = jnp.dot(
                soft.astype(bf16), parts[2 * heads + head, :extent, :], preferred_element_type=f32
            )
            stat_ref[head, first:extent, :] = jnp.broadcast_to(top + jnp.log(whole), (block, lanes))

    if low_ref.shape[1] > heads * HEAD_DIM:
        low_ref[:, heads * HEAD_DIM :] = jnp.zeros((length, low_ref.shape[1] - heads * HEAD_DIM), bf16)
    for head in range(heads):
        place = slice(head * HEAD_DIM, (head + 1) * HEAD_DIM)
        full_ref[:, place] = outs[head]
        low_ref[:, place] = outs[head].astype(bf16)


def attend_back_kernel(
    heads, block, scale, qkv_ref, dout_ref, full_ref, stat_ref, grad_ref, parts, douts, fulls, grads
):
    length = qkv_ref.shape[0]
    split_heads(qkv_ref, parts, heads, 3)
    split_heads(dout_ref, douts, heads, 1)
    split_heads(full_ref, fulls, heads, 1)
    grads[...] = jnp.zeros_like(grads)

    @pl.loop(0, heads)
    def _(head):
        for first in range(0, length, block):
            extent = first + block
            query = parts[head, first:extent, :]
            keys = parts[heads + head, :extent, :]
            value = parts[2 * heads + head, :extent, :]
            dout = douts[head, first:extent, :]
            delta = jnp.sum(dout.astype(f32) * fulls[head, first:extent, :], axis=1, keepdims=True)
            scores = score_block(query, keys, first, scale)
            soft = jnp.exp(scores - stat_ref[head, first:extent, :1])
            across = (((1,), (1,)), ((), ()))
            along = (((0,), (0,)), ((), ()))
            dprob = lax.dot_general(dout, value, across, preferred_element_type=f32)
            dscore = (soft * (dprob - delta) * scale).astype(bf16)
            grads[head, first:extent, :] = jnp.dot(dscore, keys, preferred_element_type=f32)
            grads[heads + head, :extent, :] += lax.dot_general(
                dscore, query, along, preferred_element_type=f32
            )
            grads[2 * heads + head, :extent, :] += lax.dot_general(
                soft.astype(bf16), dout, along, preferred_element_type=f32
            )

    grad_ref[...] = jnp.zeros_like(grad_ref)
    for part in range(3 * heads):
        grad_ref[:, part * HEAD_DIM : (part + 1) * HEAD_DIM] = grads[part].astype(bf16)


def attend_params():
    return pltpu.CompilerParams(vmem_limit_bytes=56 * 1024 * 1024)


def attend_whole(qkv, heads, block):
    length = qkv.shape[0]
    width = heads * HEAD_DIM
    return pl.pallas_call(
        functools.partial(attend_kernel, heads, block, HEAD_DIM ** (-0.5)),
        out_shape=[
            shaped(length, -(-width // lanes) * lanes, dtype=bf16),
            shaped(length, width),
            shaped(heads, length, lanes),
        ],
        scratch_shapes=[
            pltpu.VMEM((3 * heads, length, HEAD_DIM), bf16),
            pltpu.VMEM((heads, length, HEAD_DIM), f32),
        ],
        compiler_params=attend_params(),
    )(qkv)


def attend_whole_back(qkv, dout, full, stat, heads, block):
    length = qkv.shape[0]
    return pl.pallas_call(
        functools.partial(attend_back_kernel, heads, block, HEAD_DIM ** (-0.5)),
        out_shape=shaped(*qkv.shape, dtype=bf16),
        scratch_shapes=[
            pltpu.VMEM((3 * heads, length, HEAD_DIM), bf16),
            pltpu.VMEM((heads, length, HEAD_DIM), bf16),
            pltpu.VMEM((heads, length, HEAD_DIM), f32),
            pltpu.VMEM((3 * heads, length, HEAD_DIM), f32),
        ],
        compiler_params=attend_params(),
    )(qkv, dout, full, stat)


def split_blocks(array, block_len):
    shaped_blocks = array.reshape(
        (array.shape[0], array.shape[1] // block_len, block_len) + array.shape[2:]
    )
    return jnp.moveaxis(shaped_blocks, 1, 0)


def general_attention(proj_low, seq_count, block_len, places, any_live, longest):
    model_width = HEADS * HEAD_DIM
    scale = HEAD_DIM ** (-0.5)
    offsets = jnp.arange(block_len, dtype=jnp.int32)
    head_shape = (seq_count, block_len, HEADS, HEAD_DIM)
    query_low = proj_low[:, :model_width].reshape(head_shape)
    keys_low = proj_low[:, model_width : 2 * model_width].reshape(head_shape)
    value_low = proj_low[:, 2 * model_width :].reshape(head_shape)

    def block_scores(queries, keys_block, query_places, key_places):
        scores = (
            jnp.einsum("sqhe,skhe->sqhk", queries, keys_block, preferred_element_type=jnp.float32)
            * scale
        )
        causal_mask = key_places[None, :] <= query_places[:, None]
        return jnp.where(causal_mask[None, :, None, :], scores, masked_score)

    def key_needed(key_first):
        return (key_first <= places[-1]) & ((key_first == places[0]) | any_live)

    stat_shape = (seq_count, block_len, HEADS)
    start_state = (
        jnp.full(stat_shape, masked_score, jnp.float32),
        jnp.zeros(stat_shape, jnp.float32),
        jnp.zeros(head_shape, jnp.float32),
    )
    shard_piece = (
        lax.all_gather(keys_low, "seq", axis=1, tiled=True),
        lax.all_gather(value_low, "seq", axis=1, tiled=True),
    )
    keys_blocks = split_blocks(shard_piece[0], block_len)
    value_blocks = split_blocks(shard_piece[1], block_len)
    firsts = jnp.arange(keys_blocks.shape[0], dtype=jnp.int32) * block_len

    def attend_one_step(state_now, operand):
        keys_block, value_block, key_first = operand

        def attend_work(state_in_block):
            running_max, running_sum, running_out = state_in_block
            scores = block_scores(query_low, keys_block, places, key_first + offsets)
            new_max = jnp.maximum(running_max, jnp.max(scores, axis=-1))
            fade = jnp.exp(running_max - new_max)
            shifted = jnp.exp(scores - new_max[..., None])
            new_sum = running_sum * fade + jnp.sum(shifted, axis=-1)
            new_out = running_out * fade[..., None] + jnp.einsum(
                "sqhk,skhe->sqhe",
                shifted.astype(jnp.bfloat16),
                value_block,
                preferred_element_type=jnp.float32,
            )
            return (new_max, new_sum, new_out)

        return (
            lax.cond(
                key_needed(key_first), attend_work, lambda state_in_block: state_in_block, state_now
            ),
            None,
        )

    result, _ = lax.scan(attend_one_step, start_state, (keys_blocks, value_blocks, firsts))
    running_max, running_sum, running_out = result
    attended = running_out / running_sum[..., None]
    logsum = running_max + jnp.log(running_sum)
    def backward(dout_low):
        delta = jnp.sum(dout_low.astype(jnp.float32) * attended, axis=-1)
        shard_piece = (
            lax.all_gather(keys_low, "seq", axis=1, tiled=True),
            lax.all_gather(value_low, "seq", axis=1, tiled=True),
        )
        keys_blocks = split_blocks(shard_piece[0], block_len)
        value_blocks = split_blocks(shard_piece[1], block_len)
        firsts = jnp.arange(keys_blocks.shape[0], dtype=jnp.int32) * block_len

        def query_one_step(query_grad, operand):
            keys_block, value_block, key_first = operand

            def query_work(grad_now):
                scores = block_scores(query_low, keys_block, places, key_first + offsets)
                soft = jnp.exp(scores - logsum[..., None])
                dprob = jnp.einsum(
                    "sqhe,skhe->sqhk", dout_low, value_block, preferred_element_type=jnp.float32
                )
                dscore = (soft * (dprob - delta[..., None])).astype(jnp.bfloat16)
                return (
                    grad_now
                    + jnp.einsum(
                        "sqhk,skhe->sqhe", dscore, keys_block, preferred_element_type=jnp.float32
                    )
                    * scale
                )

            return (
                lax.cond(key_needed(key_first), query_work, lambda grad_now: grad_now, query_grad),
                None,
            )

        result, _ = lax.scan(
            query_one_step, jnp.zeros(head_shape, jnp.float32), (keys_blocks, value_blocks, firsts)
        )
        query_grad = result
        sent = (query_low.astype(jnp.float32), dout_low.astype(jnp.float32), logsum, delta)
        shard_piece = (
            lax.all_gather(sent[0].astype(jnp.bfloat16), "seq", axis=1, tiled=True).astype(jnp.float32),
            lax.all_gather(sent[1].astype(jnp.bfloat16), "seq", axis=1, tiled=True).astype(jnp.float32),
            lax.all_gather(sent[2].astype(jnp.bfloat16), "seq", axis=1, tiled=True).astype(jnp.float32),
            lax.all_gather(sent[3].astype(jnp.bfloat16), "seq", axis=1, tiled=True).astype(jnp.float32),
        )
        query_blocks = split_blocks(shard_piece[0], block_len)
        dout_blocks = split_blocks(shard_piece[1], block_len)
        logsum_blocks = split_blocks(shard_piece[2], block_len)
        delta_blocks = split_blocks(shard_piece[3], block_len)
        firsts = jnp.arange(query_blocks.shape[0], dtype=jnp.int32) * block_len

        def key_one_step(grads_now, operand):
            query_block, dout_block, logsum_block, delta_block, query_first = operand

            def key_work(grads_in):
                keys_grad, value_grad = grads_in
                query_cast = query_block.astype(jnp.bfloat16)
                dout_cast = dout_block.astype(jnp.bfloat16)
                scores = block_scores(query_cast, keys_low, query_first + offsets, places)
                soft = jnp.exp(scores - logsum_block[..., None])
                value_grad = value_grad + jnp.einsum(
                    "sqhk,sqhe->skhe",
                    soft.astype(jnp.bfloat16),
                    dout_cast,
                    preferred_element_type=jnp.float32,
                )
                dprob = jnp.einsum(
                    "sqhe,skhe->sqhk", dout_cast, value_low, preferred_element_type=jnp.float32
                )
                dscore = (soft * (dprob - delta_block[..., None])).astype(jnp.bfloat16)
                keys_grad = (
                    keys_grad
                    + jnp.einsum(
                        "sqhk,sqhe->skhe", dscore, query_cast, preferred_element_type=jnp.float32
                    )
                    * scale
                )
                return (keys_grad, value_grad)

            needed = (query_first + block_len - 1 >= places[0]) & (
                (query_first == places[0]) | (query_first < longest)
            )
            return (lax.cond(needed, key_work, lambda grads_in: grads_in, grads_now), None)

        result, _ = lax.scan(
            key_one_step,
            (jnp.zeros(head_shape, jnp.float32), jnp.zeros(head_shape, jnp.float32)),
            (query_blocks, dout_blocks, logsum_blocks, delta_blocks, firsts),
        )
        keys_grad, value_grad = result
        return (query_grad, keys_grad, value_grad)

    return attended, backward


def layer_norm(value, gain):
    centred = value - jnp.mean(value, axis=-1, keepdims=True)
    spread_of = jnp.mean(centred * centred, axis=-1, keepdims=True)
    return centred * lax.rsqrt(spread_of + eps) * gain


def gelu_tanh(value):
    return jax.nn.gelu(value, approximate=True)


def dense(left, weight):
    return jnp.dot(left, weight, preferred_element_type=f32)


def dense_back(left, weight, upstream):
    into_left = lax.dot_general(
        upstream, weight, (((1,), (1,)), ((), ())), preferred_element_type=f32
    )
    into_weight = lax.dot_general(
        left, upstream, (((0,), (0,)), ((), ())), preferred_element_type=f32
    ).astype(bf16)
    return (into_left, into_weight)


def shift_mix(extended, taps, value_part):
    step_count = value_part.shape[1]
    reach = taps.shape[1]
    shifted = extended[:, reach - 1 : reach - 1 + step_count] * taps[:, 0]
    for tap_index in range(1, reach):
        shifted = (
            shifted
            + extended[:, reach - 1 - tap_index : reach - 1 - tap_index + step_count]
            * taps[:, tap_index]
        )
    return shifted * value_part


def feed_forward(resid, gain, up_weight, down_weight):
    normed, norm_back = jax.vjp(layer_norm, resid, gain)
    normed_low = normed.astype(bf16)
    hidden = dense(normed_low, up_weight)
    active, active_back = jax.vjp(gelu_tanh, hidden)
    active_low = active.astype(bf16)
    return (
        resid + dense(active_low, down_weight),
        (norm_back, normed_low, active_back, active_low),
    )


def feed_back(stored, up_weight, down_weight, upstream):
    norm_back, normed_low, active_back, active_low = stored
    into_active, down_grad = dense_back(active_low, down_weight, upstream.astype(bf16))
    (into_hidden,) = active_back(into_active)
    into_normed, up_grad = dense_back(normed_low, up_weight, into_hidden.astype(bf16))
    into_resid, gain_grad = norm_back(into_normed)
    return (upstream + into_resid, gain_grad, up_grad, down_grad)


def fold_rows(weight, share):
    rows, width = weight.shape
    fold = rows // share
    return weight.reshape(fold, share, width).transpose(1, 0, 2).reshape(share, fold * width)


def unfold_rows(folded, fold, share):
    rows, width = folded.shape
    width //= fold
    parts = folded.reshape(rows // share, share, fold, width).transpose(0, 2, 1, 3)
    return parts.reshape(rows * fold, width)


def fold_all(weight, share, rows):
    tall, width = weight.shape
    fold = tall // rows
    parts = weight.reshape(rows // share, fold, share, width).transpose(0, 2, 1, 3)
    return parts.reshape(rows, fold * width)


def group_columns(weight, groups, padded):
    rows, columns = weight.shape
    part = columns // 3 // groups
    grouped = weight.reshape(rows, 3, groups, part).transpose(0, 2, 1, 3).reshape(rows, groups, 3 * part)
    return jnp.pad(grouped, ((0, 0), (0, 0), (0, padded - 3 * part))).reshape(rows, groups * padded)


def pad_groups(weight, groups, padded):
    rows, columns = weight.shape
    part = rows // groups
    grouped = weight.reshape(groups, part, columns)
    return jnp.pad(grouped, ((0, 0), (0, padded - part), (0, 0))).reshape(groups * padded, columns)


def ungroup_columns(grouped, groups, padded, columns):
    rows = grouped.shape[0]
    part = columns // 3 // groups
    parts = grouped.reshape(rows, groups, padded)[:, :, : 3 * part].reshape(rows, groups, 3, part)
    return parts.transpose(0, 2, 1, 3).reshape(rows, columns)


def cut(array, widths):
    pieces, start = [], 0
    for width in widths:
        pieces.append(array[:, start : start + width])
        start += width
    return pieces


def cut_last(array, count):
    width = array.shape[-1] // count
    return [array[..., i * width : (i + 1) * width] for i in range(count)]


def gathered(parts):
    whole = lax.all_gather(jnp.concatenate(parts, axis=1), everyone, axis=0, tiled=True)
    return cut(whole, [p.shape[1] for p in parts])


def scattered(parts):
    mine = lax.psum_scatter(
        jnp.concatenate(parts, axis=1), everyone, scatter_dimension=0, tiled=True
    )
    return cut(mine, [p.shape[1] for p in parts])


def body(
    tokens,
    cotangent,
    lengths,
    mixer_gain,
    mixer_inputs,
    shift_taps,
    decay_rate,
    state_in,
    state_out,
    state_skip,
    mixer_output,
    first_gain,
    first_up,
    first_down,
    attend_gain,
    attend_inputs,
    attend_output,
    second_gain,
    second_up,
    second_down,
):
    seq_count, block_len, model_width = tokens.shape
    row_count = seq_count * block_len
    seq_devices = lax.axis_size("seq")
    share = mixer_inputs.shape[0]
    states, reach = decay_rate.shape[1], shift_taps.shape[1]
    fold = first_down.shape[0] // share
    deals = seq_count * HEADS
    dealt = deals % seq_devices == 0 and HEADS % (deals // seq_devices) == 0
    heads = deals // seq_devices if dealt else HEADS
    groups = HEADS // heads
    group_width = heads * HEAD_DIM
    padded = -(-3 * group_width // lanes) * lanes if dealt else 3 * group_width
    out_width = -(-group_width // lanes) * lanes if dealt else group_width

    columns = [decay_rate, state_in, state_out, shift_taps]
    columns += [g[:, None] for g in (mixer_gain, first_gain, attend_gain, second_gain, state_skip)]
    small = jnp.concatenate(columns, axis=1)
    small_count = small.shape[1]
    small_width = -(-small_count // lanes) * lanes
    small = jnp.pad(small, ((0, 0), (0, small_width - small_count)))
    attend_cols = attend_inputs.shape[1]
    grouped = group_columns(attend_inputs, groups, padded)
    by_kernel = seq_devices == 8 and lax.axis_size("batch") == 4
    packed = [mixer_output, attend_output, first_up, second_up, grouped]
    up1_at = 2 * model_width
    up2_at = up1_at + first_up.shape[1]
    if by_kernel:
        joint = jnp.concatenate([mixer_inputs, small], axis=1)
        w_packed = lax.all_gather(jnp.concatenate(packed, axis=1), everyone, axis=0, tiled=True)
        w_mixer_out, w_attend_out, _, _, w_attend_in = cut(w_packed, [p.shape[1] for p in packed])
        widths = (joint.shape[1], model_width)
        w_joint, w_down1 = gather_blocks((joint, first_down), chunked(widths, (4, 6), ("zxy", "zyx")), gap=3)
        w_mixer_in, w_small = cut(w_joint, [mixer_inputs.shape[1], small_width])
        second_down, w_small = lax.optimization_barrier((second_down, w_small))
        w_down2 = lax.all_gather(second_down, everyone, axis=0, tiled=True)
    else:
        w_mixer_in, w_small = gathered([mixer_inputs, small])
        packed += [fold_rows(first_down, share), fold_rows(second_down, share)]
        w_mixer_out, w_attend_out, w_up1, w_up2, w_attend_in, w_down1, w_down2 = gathered(packed)
        w_down1 = unfold_rows(w_down1, fold, share)
        w_down2 = unfold_rows(w_down2, fold, share)

    rows = w_small.T.astype(f32)
    decay, table_in, table_out = rows[:states], rows[states : 2 * states], rows[2 * states : 3 * states]
    taps_rows = rows[3 * states : 3 * states + reach]
    gain_mixer, gain_first, gain_attend, gain_second, skip = (
        rows[3 * states + reach + i] for i in range(5)
    )
    taps = taps_rows.T
    weight = table_in * table_out

    rank_seq = lax.axis_index("seq")
    offsets = jnp.arange(block_len, dtype=jnp.int32)
    places = rank_seq * block_len + offsets
    valid = (places[None, :] < lengths[:, None]).astype(f32)
    longest = jnp.max(lengths)
    any_live = places[0] < longest

    start_resid = tokens.reshape(row_count, model_width).astype(f32)
    normed_mixer, back_mixer = jax.vjp(layer_norm, start_resid, gain_mixer)
    normed_low_mixer = normed_mixer.astype(bf16)
    projected = dense(normed_low_mixer, w_mixer_in).reshape(seq_count, block_len, 3 * model_width)
    query_mixer = projected[:, :, :model_width]
    keys_mixer = projected[:, :, model_width : 2 * model_width]
    value_mixer = projected[:, :, 2 * model_width :]
    rim_rows = passed_along(keys_mixer[:, block_len - reach + 1 :], "seq", 1)
    extended = jnp.concatenate([rim_rows, keys_mixer], axis=1)
    inner, shift_back = jax.vjp(shift_mix, extended, taps, value_mixer)
    if by_kernel:
        carried = carried_by_kernel(inner, decay, False, 2)
    else:
        carried = carried_in(encode(inner, decay, False), decay, block_len, False)
    wide = shaped(seq_count, block_len, model_width)
    state_y, gated = per_lane_tile(
        output_kernel,
        (inner, query_mixer, carried, decay, weight, skip[None]),
        (wide, wide),
    )
    gated_low = gated.astype(bf16).reshape(row_count, model_width)
    resid_mixer = start_resid + dense(gated_low, w_mixer_out)
    if by_kernel:
        resid_first, stored_first = feed_forward_blocks(
            resid_mixer, gain_first, w_packed, up1_at, w_down1
        )
    else:
        resid_first, stored_first = feed_forward(resid_mixer, gain_first, w_up1, w_down1)

    normed_attend, back_attend = jax.vjp(layer_norm, resid_first, gain_attend)
    normed_low_attend = normed_attend.astype(bf16)
    proj_low = dense(normed_low_attend, w_attend_in).astype(bf16)
    if dealt:
        length = seq_devices * block_len
        block = min(256, length)

        def deal(array, width):
            array = array.reshape(seq_count, block_len, groups * width)
            parts = jnp.stack(cut_last(array, groups), axis=1)
            parts = parts.reshape(seq_count * groups, block_len, width)
            dealt_parts = lax.all_to_all(parts, "seq", split_axis=0, concat_axis=0, tiled=True)
            return dealt_parts.reshape(length, width)

        def collect(array, width):
            parts = array.reshape(seq_devices, block_len, width)
            back = lax.all_to_all(parts, "seq", split_axis=0, concat_axis=0, tiled=True)
            back = back.reshape(seq_count, groups, block_len, width)
            back = jnp.concatenate([back[:, group] for group in range(groups)], axis=-1)
            return back.reshape(row_count, groups * width)

        qkv = deal(proj_low, padded)
        attended_part, attended_full, stat = attend_whole(qkv, heads, block)
        attended_low = collect(attended_part, out_width)
        w_attend_out = pad_groups(w_attend_out, groups, out_width)
    else:
        attended, attended_back = general_attention(
            proj_low, seq_count, block_len, places, any_live, longest
        )
        attended_low = attended.reshape(row_count, model_width).astype(bf16)
    resid_attend = resid_first + dense(attended_low, w_attend_out)
    if by_kernel:
        final, stored_second = feed_forward_blocks(
            resid_attend, gain_second, w_packed, up2_at, w_down2
        )
    else:
        final, stored_second = feed_forward(resid_attend, gain_second, w_up2, w_down2)
    mixed = (final.reshape(seq_count, block_len, model_width) * valid[..., None]).astype(bf16)

    upstream = (cotangent.astype(f32) * valid[..., None]).reshape(row_count, model_width)
    if by_kernel:
        upstream, second_gain_grad, early = feed_back_blocks(
            stored_second, w_packed, up2_at, w_down2, upstream, packed=(share, fold)
        )
    else:
        upstream, second_gain_grad, second_up_grad, second_down_grad = feed_back(
            stored_second, w_up2, w_down2, upstream
        )
        early = [second_up_grad, fold_all(second_down_grad, share, model_width)]
        early = jnp.concatenate(early, axis=1)
    into_attended, attend_output_grad = dense_back(
        attended_low, w_attend_out, upstream.astype(bf16)
    )
    if dealt:
        attend_output_grad = attend_output_grad.reshape(groups, out_width, model_width)
        attend_output_grad = attend_output_grad[:, :group_width].reshape(model_width, model_width)
    dout_low = into_attended.astype(bf16)
    if dealt:
        dout = deal(dout_low, out_width)
        qkv_grad = attend_whole_back(qkv, dout, attended_full, stat, heads, block)
        qkv_grad, early = lax.optimization_barrier((qkv_grad, early))
        proj_grad = collect(qkv_grad, padded)
    else:
        parts = attended_back(dout_low.reshape(seq_count, block_len, HEADS, HEAD_DIM))
        proj_grad = jnp.concatenate(
            [p.reshape(row_count, model_width) for p in parts], axis=1
        ).astype(bf16)
    early = lax.psum_scatter(early, everyone, scatter_dimension=0, tiled=True)
    second_up_out, second_down_out = cut(early, [second_up.shape[1], fold * model_width])
    into_normed, attend_inputs_grad = dense_back(normed_low_attend, w_attend_in, proj_grad)
    into_resid, attend_gain_grad = back_attend(into_normed)
    upstream = upstream + into_resid
    if by_kernel:
        upstream, first_gain_grad, first_up_grad, first_down_grad = feed_back_blocks(
            stored_first, w_packed, up1_at, w_down1, upstream
        )
    else:
        upstream, first_gain_grad, first_up_grad, first_down_grad = feed_back(
            stored_first, w_up1, w_down1, upstream
        )
    into_gated, mixer_output_grad = dense_back(gated_low, w_mixer_out, upstream.astype(bf16))
    into_gated = into_gated.reshape(seq_count, block_len, model_width)
    query_mixer_grad = into_gated * state_y
    state_grad = into_gated * query_mixer
    if by_kernel:
        later = carried_by_kernel(state_grad, decay, True, 3)
    else:
        later = carried_in(encode(state_grad, decay, True), decay, block_len, True)
    table = shaped(states, model_width)
    inner_grad, weight_grad, power_grad, skip_grad = per_lane_tile(
        back_kernel,
        (inner, state_grad, carried, later, decay, weight, skip[None]),
        (wide, table, table, shaped(1, model_width)),
        scratch=[pltpu.VMEM((block_len, seq_count, states, lanes), f32)],
    )
    extended_grad, taps_grad, value_mixer_grad = shift_back(inner_grad)
    spill = passed_along(extended_grad[:, : reach - 1], "seq", -1)
    keys_mixer_grad = extended_grad[:, reach - 1 :] + jnp.pad(
        spill, ((0, 0), (block_len - reach + 1, 0), (0, 0))
    )
    proj_grad_mixer = (
        jnp.concatenate([query_mixer_grad, keys_mixer_grad, value_mixer_grad], axis=2)
        .astype(bf16)
        .reshape(row_count, 3 * model_width)
    )
    into_normed_mixer, mixer_inputs_grad = dense_back(normed_low_mixer, w_mixer_in, proj_grad_mixer)
    into_start, mixer_gain_grad = back_mixer(into_normed_mixer)
    tokens_gradient = (upstream + into_start).reshape(seq_count, block_len, model_width).astype(bf16)

    small_rows = jnp.concatenate(
        [-jnp.exp(-decay) * power_grad, weight_grad * table_out, weight_grad * table_in, taps_grad.T]
        + [
            g[None]
            for g in (mixer_gain_grad, first_gain_grad, attend_gain_grad, second_gain_grad, skip_grad[0])
        ],
        axis=0,
    )
    small_grad = jnp.pad(small_rows, ((0, small_width - small_count), (0, 0))).T.astype(bf16)
    def unfolded(folded):
        return folded.reshape(share, fold, model_width).transpose(1, 0, 2).reshape(share * fold, model_width)

    gains_at = 3 * states + reach
    table_edges = [0, states, 2 * states, 3 * states, gains_at, small_width]

    def tables_of(block):
        return [block[:, a:b] for a, b in zip(table_edges, table_edges[1:])]

    last = [attend_inputs_grad, first_up_grad, mixer_output_grad, mixer_inputs_grad, small_grad]
    if by_kernel:
        last += [first_down_grad, attend_output_grad]
        orders = ("yxz", "xyz", "xzy", "yxz", "xyz", "yzx")
        plan = chunked([g.shape[1] for g in last], (6, 6, 2, 6, 2, 4, 2), orders)
        part = attend_cols // 3 // groups

        def finish(index, block, results):
            if index == 0:
                for group in range(groups):
                    for kind in range(3):
                        start = (kind * groups + group) * part
                        source = group * padded + kind * part
                        results[0][:, start : start + part] = block[:, source : source + part]
            elif index == 4:
                for place, table in enumerate(tables_of(block)):
                    results[5 + place][...] = table
            else:
                results[{1: 1, 2: 2, 3: 3, 5: 4, 6: 10}[index]][...] = block[...]

        widths = [attend_cols] + [g.shape[1] for g in last[1:4]]
        results = [shaped(share, w) for w in widths] + [shaped(share * fold, model_width)]
        results += [shaped(share, b - a) for a, b in zip(table_edges, table_edges[1:])]
        results.append(shaped(share, model_width))
        attend_inputs_out, first_up_out, mixer_output_out, mixer_inputs_out, first_down_out, *tables = (
            scatter_blocks(last, plan, finish, results, gap=4)
        )
        *tables, attend_output_out = tables
    else:
        last += [fold_all(first_down_grad, share, model_width), attend_output_grad]
        *last, folded, attend_output_out = scattered(last)
        first_down_out = unfolded(folded).astype(f32)
        grouped, first_up_out, mixer_output_out, mixer_inputs_out, small_out = (
            g.astype(f32) for g in last
        )
        attend_inputs_out = ungroup_columns(grouped, groups, padded, attend_cols)
        tables = tables_of(small_out)
    decay_out, in_out, out_out, taps_out, vectors = tables

    return (
        mixed,
        tokens_gradient,
        vectors[:, 0],
        mixer_inputs_out,
        taps_out,
        decay_out,
        in_out,
        out_out,
        vectors[:, 4],
        mixer_output_out,
        vectors[:, 1],
        first_up_out,
        first_down_out,
        vectors[:, 2],
        attend_inputs_out,
        attend_output_out.astype(f32),
        vectors[:, 3],
        second_up_out.astype(f32),
        unfolded(second_down_out).astype(f32),
    )


def solution(mesh):
    return jax.shard_map(
        body,
        mesh=mesh,
        in_specs=(
            P("batch", "seq", None),
            P("batch", "seq", None),
            P("batch"),
            P(("seq", "batch")),
            P(("seq", "batch"), None),
            P(("seq", "batch"), None),
            P(("seq", "batch"), None),
            P(("seq", "batch"), None),
            P(("seq", "batch"), None),
            P(("seq", "batch")),
            P(("seq", "batch"), None),
            P(("seq", "batch")),
            P(("seq", "batch"), None),
            P(("seq", "batch"), None),
            P(("seq", "batch")),
            P(("seq", "batch"), None),
            P(("seq", "batch"), None),
            P(("seq", "batch")),
            P(("seq", "batch"), None),
            P(("seq", "batch"), None),
        ),
        out_specs=(
            P("batch", "seq", None),
            P("batch", "seq", None),
            P(("seq", "batch")),
            P(("seq", "batch"), None),
            P(("seq", "batch"), None),
            P(("seq", "batch"), None),
            P(("seq", "batch"), None),
            P(("seq", "batch"), None),
            P(("seq", "batch")),
            P(("seq", "batch"), None),
            P(("seq", "batch")),
            P(("seq", "batch"), None),
            P(("seq", "batch"), None),
            P(("seq", "batch")),
            P(("seq", "batch"), None),
            P(("seq", "batch"), None),
            P(("seq", "batch")),
            P(("seq", "batch"), None),
            P(("seq", "batch"), None),
        ),
        check_vma=False,
    )
```

```python
import functools

import jax
import jax.numpy as jnp
from jax import lax
from jax.experimental import pallas as pl
from jax.experimental.pallas import tpu as pltpu
from jax.sharding import PartitionSpec as P

HEADS = 12
HEAD_DIM = 64

eps = 1e-05
masked_score = -1e30
lanes = 128
sublanes = 8
everyone = ("seq", "batch")
f32 = jnp.float32
bf16 = jnp.bfloat16


def rows_of(ref, seq, block):
    return ref[seq, pl.ds(pl.multiple_of(block * sublanes, sublanes), sublanes), :]


def spread(rows, index, count):
    return jnp.broadcast_to(rows[index : index + 1], (count, lanes))


def encode_kernel(reverse, input_ref, decay_ref, end_ref):
    seq_count, step_count, _ = input_ref.shape
    state_count = decay_ref.shape[0]
    blocks = step_count // sublanes
    power = jnp.exp(-decay_ref[...])

    def one_block(step, states):
        block = blocks - 1 - step if reverse else step
        rows = [rows_of(input_ref, seq, block) for seq in range(seq_count)]
        order = range(sublanes - 1, -1, -1) if reverse else range(sublanes)
        states = list(states)
        for index in order:
            for seq in range(seq_count):
                states[seq] = states[seq] * power + spread(rows[seq], index, state_count)
        return tuple(states)

    start = tuple(jnp.zeros((state_count, lanes), f32) for _ in range(seq_count))
    ends = lax.fori_loop(0, blocks, one_block, start)
    for seq in range(seq_count):
        end_ref[seq] = ends[seq]


def output_kernel(input_ref, query_ref, carried_ref, decay_ref, weight_ref, skip_ref, out_ref, gated_ref):
    seq_count, step_count, _ = input_ref.shape
    state_count = decay_ref.shape[0]
    power = jnp.exp(-decay_ref[...])
    weight = weight_ref[...]
    skip = skip_ref[...]

    def one_block(block, states):
        states = list(states)
        rows = [rows_of(input_ref, seq, block) for seq in range(seq_count)]
        found = [[] for _ in range(seq_count)]
        for index in range(sublanes):
            for seq in range(seq_count):
                states[seq] = states[seq] * power + spread(rows[seq], index, state_count)
                found[seq].append(jnp.sum(states[seq] * weight, axis=0, keepdims=True))
        place = pl.ds(pl.multiple_of(block * sublanes, sublanes), sublanes)
        for seq in range(seq_count):
            result = jnp.concatenate(found[seq], axis=0) + skip * rows[seq]
            out_ref[seq, place, :] = result
            gated_ref[seq, place, :] = result * rows_of(query_ref, seq, block)
        return tuple(states)

    start = tuple(carried_ref[seq].astype(f32) for seq in range(seq_count))
    lax.fori_loop(0, step_count // sublanes, one_block, start)


def back_kernel(
    input_ref,
    grad_ref,
    carried_ref,
    later_ref,
    decay_ref,
    weight_ref,
    skip_ref,
    input_grad_ref,
    weight_grad_ref,
    power_grad_ref,
    skip_grad_ref,
    held,
):
    seq_count, step_count, _ = input_ref.shape
    state_count = decay_ref.shape[0]
    blocks = step_count // sublanes
    power = jnp.exp(-decay_ref[...])
    weight = weight_ref[...]
    skip = skip_ref[...]
    seqs = range(seq_count)

    def forward_block(block, state):
        states, total, skip_total = list(state[0]), state[1], state[2]
        rows = [rows_of(input_ref, seq, block) for seq in seqs]
        grads = [rows_of(grad_ref, seq, block) for seq in seqs]
        for index in range(sublanes):
            for seq in seqs:
                held[block * sublanes + index, seq] = states[seq]
                states[seq] = states[seq] * power + spread(rows[seq], index, state_count)
                total = total + states[seq] * spread(grads[seq], index, state_count)
        for seq in seqs:
            skip_total = skip_total + rows[seq] * grads[seq]
        return (tuple(states), total, skip_total)

    zeros = jnp.zeros((state_count, lanes), f32)
    _, total, skip_total = lax.fori_loop(
        0,
        blocks,
        forward_block,
        (
            tuple(carried_ref[seq].astype(f32) for seq in seqs),
            zeros,
            jnp.zeros((sublanes, lanes), f32),
        ),
    )
    weight_grad_ref[...] = total
    skip_grad_ref[...] = jnp.sum(skip_total, axis=0, keepdims=True)

    def back_block(step, state):
        states, total = list(state[0]), state[1]
        block = blocks - 1 - step
        grads = [rows_of(grad_ref, seq, block) for seq in seqs]
        found = [[None] * sublanes for _ in seqs]
        for index in range(sublanes - 1, -1, -1):
            for seq in seqs:
                states[seq] = states[seq] * power + spread(grads[seq], index, state_count)
                found[seq][index] = jnp.sum(states[seq] * weight, axis=0, keepdims=True)
                total = total + states[seq] * held[block * sublanes + index, seq]
        place = pl.ds(pl.multiple_of(block * sublanes, sublanes), sublanes)
        for seq in seqs:
            input_grad_ref[seq, place, :] = jnp.concatenate(found[seq], axis=0) + skip * grads[seq]
        return (tuple(states), total)

    _, total = lax.fori_loop(
        0, blocks, back_block, (tuple(later_ref[seq].astype(f32) for seq in seqs), zeros)
    )
    power_grad_ref[...] = total * weight


def per_lane_tile(kernel, args, outs, scratch=(), flops=0):
    def spec(shape):
        lead = len(shape) - 1
        return pl.BlockSpec(tuple(shape[:-1]) + (lanes,), lambda tile: (0,) * lead + (tile,))

    bytes_moved = sum(a.size * a.dtype.itemsize for a in args)
    return pl.pallas_call(
        kernel,
        grid=(args[0].shape[-1] // lanes,),
        in_specs=[spec(a.shape) for a in args],
        out_specs=[spec(o.shape) for o in outs],
        out_shape=list(outs),
        scratch_shapes=list(scratch),
        cost_estimate=pl.CostEstimate(flops=flops, bytes_accessed=bytes_moved, transcendentals=0),
        compiler_params=pltpu.CompilerParams(vmem_limit_bytes=48 * 1024 * 1024),
    )(*args)


def shaped(*dims, dtype=f32):
    return jax.ShapeDtypeStruct(dims, dtype)


def encode(value, decay, reverse):
    seq_count, _, width = value.shape
    (ends,) = per_lane_tile(
        functools.partial(encode_kernel, reverse),
        (value, decay),
        (shaped(seq_count, decay.shape[0], width),),
    )
    return ends


def passed_along(block, axis, distance):
    devices = range(lax.axis_size(axis))
    route = [(i - distance, i) for i in devices if i - distance in devices]
    return lax.ppermute(block, axis, route)


def carried_in(ends, decay, block_len, reverse):
    seq_count, state_count, width = ends.shape
    count = lax.axis_size("seq")
    part = state_count // count

    def exchanged(parts):
        return lax.all_to_all(parts.astype(bf16), "seq", split_axis=0, concat_axis=0, tiled=True)

    parts = ends.reshape(seq_count, count, part, width).transpose(1, 0, 2, 3)
    arrived = exchanged(parts.reshape(count, seq_count * part, width)).astype(f32)
    rates = lax.dynamic_slice_in_dim(decay, lax.axis_index("seq") * part, part, 0)
    power = jnp.tile(jnp.exp(-rates * block_len), (seq_count, 1))
    state, joined = jnp.zeros_like(arrived[0]), [None] * count
    for block in reversed(range(count)) if reverse else range(count):
        joined[block] = state
        state = power * state + arrived[block]
    back = exchanged(jnp.stack(joined))
    back = back.reshape(count, seq_count, part, width).transpose(1, 0, 2, 3)
    return back.reshape(seq_count, state_count, width)


MESH = pl.DeviceIdType.MESH
box = (4, 2, 2, 2)


def here():
    seq, batch = lax.axis_index("seq"), lax.axis_index("batch")
    return lax.div(seq, 2), lax.rem(seq, 2), lax.div(batch, 2), lax.rem(batch, 2)


def device(z, x, y, core):
    return (2 * z + x, 2 * y + core)


def line_peer(z, step):
    return lax.rem(z + step, box[0])


def greet():
    z, x, y, core = here()
    barrier = pltpu.get_barrier_semaphore()
    peers = [device(line_peer(z, step), x, y, core) for step in range(1, box[0])]
    peers += [device(z, 1 - x, y, core), device(z, x, 1 - y, core), device(z, x, y, 1 - core)]
    for peer in peers:
        pl.semaphore_signal(barrier, inc=1, device_id=peer, device_id_type=MESH)
    pl.semaphore_wait(barrier, len(peers))


def staggered(count, stages, gap):
    for turn in range(count + gap * (stages - 1)):
        for stage in reversed(range(stages)):
            chunk = turn - gap * stage
            if 0 <= chunk < count:
                yield stage, chunk


def gather_kernel(plan, gap, *refs):
    count = 1 + max(item[0] for item in plan)
    ins, outs = refs[:count], refs[count : 2 * count]
    send, receive, local = refs[2 * count :]
    z, x, y, core = here()
    greet()
    started = {}

    def push(chunk, slot, source, target, peer):
        copy = pltpu.make_async_remote_copy(
            src_ref=source,
            dst_ref=target,
            send_sem=send.at[chunk, slot],
            recv_sem=receive.at[chunk, slot],
            device_id=peer,
            device_id_type=MESH,
        )
        copy.start()
        started[chunk, slot] = copy

    own = []
    for chunk, (index, first, width, _) in enumerate(plan):
        columns = pl.ds(first, width)
        source = ins[index].at[:, columns]
        target = outs[index].at[z, x, y, core, :, columns]
        for step in range(1, box[0]):
            push(chunk, step - 1, source, target, device(line_peer(z, step), x, y, core))
        keep = pltpu.make_async_copy(source, target, local.at[chunk])
        keep.start()
        own.append(keep)

    for stage, chunk in staggered(len(plan), 3, gap):
        index, first, width, order = plan[chunk]
        x_first = order[1] == "x"
        columns = pl.ds(first, width)
        out = outs[index]
        if stage == 0:
            for step in range(1, box[0]):
                started[chunk, step - 1].wait_recv()
            own[chunk].wait()
            part = out.at[:, x, y, core, :, columns]
            peer = device(z, 1 - x, y, core) if x_first else device(z, x, 1 - y, core)
            push(chunk, 3, part, part, peer)
        elif stage == 1:
            started[chunk, 3].wait_recv()
            if x_first:
                part, peer = out.at[:, :, y, core, :, columns], device(z, x, 1 - y, core)
            else:
                part, peer = out.at[:, x, :, core, :, columns], device(z, 1 - x, y, core)
            push(chunk, 4, part, part, peer)
        else:
            started[chunk, 4].wait_recv()
            part = out.at[:, :, :, core, :, columns]
            push(chunk, 5, part, part, device(z, x, y, 1 - core))
    for chunk in range(len(plan)):
        started[chunk, 5].wait_recv()
        for slot in range(6):
            started[chunk, slot].wait_send()


def gather_blocks(blocks, plan, gap=2, collective=0):
    outs = [jax.ShapeDtypeStruct(box + b.shape, b.dtype) for b in blocks]
    sent = sum(b.size * b.dtype.itemsize for b in blocks)
    whole = pl.pallas_call(
        functools.partial(gather_kernel, plan, gap),
        out_shape=outs,
        in_specs=[pl.BlockSpec(memory_space=pltpu.VMEM)] * len(blocks),
        out_specs=[pl.BlockSpec(memory_space=pl.ANY)] * len(blocks),
        scratch_shapes=[
            pltpu.SemaphoreType.DMA((len(plan), 6)),
            pltpu.SemaphoreType.DMA((len(plan), 6)),
            pltpu.SemaphoreType.DMA((len(plan),)),
        ],
        cost_estimate=pl.CostEstimate(flops=0, bytes_accessed=64 * sent, transcendentals=0),
        compiler_params=pltpu.CompilerParams(collective_id=collective, has_side_effects=True),
    )(*blocks)
    return [w.reshape((32 * w.shape[4], w.shape[5])) for w in whole]


def add_into(total, other):
    return (total.astype(f32) + other.astype(f32)).astype(bf16)


def scatter_kernel(plan, gap, finish, counts, *refs):
    count, out_count = counts
    ins, results = refs[:count], refs[count : count + out_count]
    outs, buffers = refs[count + out_count : 2 * count + out_count], refs[2 * count + out_count : -3]
    send, receive, local = refs[-3:]
    z, x, y, core = here()
    greet()
    started = {}

    def push(chunk, slot, source, target, peer):
        copy = pltpu.make_async_remote_copy(
            src_ref=source,
            dst_ref=target,
            send_sem=send.at[chunk, slot],
            recv_sem=receive.at[chunk, slot],
            device_id=peer,
            device_id_type=MESH,
        )
        copy.start()
        started[chunk, slot] = copy

    loads = []
    for chunk, (index, first, width, _) in enumerate(plan):
        columns = pl.ds(first, width)
        held, from_core = buffers[5 * chunk : 5 * chunk + 2]
        grad = ins[index]
        push(chunk, 0, grad.at[:, :, :, 1 - core, :, columns], from_core, device(z, x, y, 1 - core))
        load = pltpu.make_async_copy(grad.at[:, :, :, core, :, columns], held, local.at[chunk])
        load.start()
        loads.append(load)

    for stage, chunk in staggered(len(plan), 4, gap):
        index, first, width, order = plan[chunk]
        x_first, line_last = order[0] == "y", order[-1] == "z"
        held, from_core, from_one, from_two, from_line = buffers[5 * chunk : 5 * chunk + 5]
        to_x, to_y = device(z, 1 - x, y, core), device(z, x, 1 - y, core)
        if stage == 0:
            started[chunk, 0].wait_recv()
            loads[chunk].wait()

            @pl.loop(0, 4 * box[0])
            def _(turn):
                at = (lax.div(turn, 4), lax.rem(lax.div(turn, 2), 2), lax.rem(turn, 2))
                held[at] = add_into(held[at], from_core[at])

            if x_first:
                push(chunk, 1, held.at[:, :, 1 - y], from_one, to_y)
            else:
                push(chunk, 1, held.at[:, 1 - x], from_one, to_x)
        elif stage == 1:
            started[chunk, 1].wait_recv()

            @pl.loop(0, 2 * box[0])
            def _(turn):
                row, i = lax.div(turn, 2), lax.rem(turn, 2)
                at = (row, i, y) if x_first else (row, x, i)
                held[at] = add_into(held[at], from_one[row, i])

            if not line_last:
                for step in range(1, box[0]):
                    peer = line_peer(z, step)
                    rest = held.at[peer, :, y] if x_first else held.at[peer, x]
                    push(chunk, 2 + step, rest, from_line.at[step - 1], device(peer, x, y, core))
            elif x_first:
                push(chunk, 2, held.at[:, 1 - x, y], from_two, to_x)
            else:
                push(chunk, 2, held.at[:, x, 1 - y], from_two, to_y)
        elif stage == 2 and not line_last:
            for step in range(1, box[0]):
                started[chunk, 2 + step].wait_recv()
            for i in range(2):
                at = (z, i, y) if x_first else (z, x, i)
                total = held[at].astype(f32)
                for step in range(1, box[0]):
                    total = total + from_line[step - 1, i].astype(f32)
                held[at] = total.astype(bf16)
            if x_first:
                push(chunk, 2, held.at[z, 1 - x, y], from_two, to_x)
            else:
                push(chunk, 2, held.at[z, x, 1 - y], from_two, to_y)
        elif stage == 2:
            started[chunk, 2].wait_recv()

            @pl.loop(0, box[0])
            def _(row):
                held[row, x, y] = add_into(held[row, x, y], from_two[row])

            for step in range(1, box[0]):
                peer = line_peer(z, step)
                push(chunk, 2 + step, held.at[peer, x, y], from_line.at[step - 1], device(peer, x, y, core))
        else:
            total = held[z, x, y].astype(f32)
            if line_last:
                for step in range(1, box[0]):
                    started[chunk, 2 + step].wait_recv()
                    total = total + from_line[step - 1].astype(f32)
            else:
                started[chunk, 2].wait_recv()
                total = total + from_two[...].astype(f32)
            outs[index][:, pl.ds(first, width)] = total
            if not any(item[0] == index for item in plan[chunk + 1 :]):
                finish(index, outs[index], results)
    for chunk in range(len(plan)):
        for slot in range(6):
            started[chunk, slot].wait_send()


def scatter_blocks(grads, plan, finish, results, gap=2, collective=1):
    views = [g.reshape(box + (g.shape[0] // 32, g.shape[1])) for g in grads]
    scratch = [pltpu.VMEM(v.shape[4:], f32) for v in views]
    for index, _, width, order in plan:
        tile = (views[index].shape[4], width)
        ends_of = ((4,), (3,)) if order[-1] == "z" else ((), (3, 2))
        for lead in ((4, 2, 2), (4, 2, 2), (4, 2)) + ends_of:
            scratch.append(pltpu.VMEM(lead + tile, bf16))
    sent = sum(v.size * v.dtype.itemsize for v in views)
    return pl.pallas_call(
        functools.partial(scatter_kernel, plan, gap, finish, (len(views), len(results))),
        out_shape=list(results),
        in_specs=[pl.BlockSpec(memory_space=pl.ANY)] * len(views),
        out_specs=[pl.BlockSpec(memory_space=pltpu.VMEM)] * len(results),
        scratch_shapes=scratch
        + [
            pltpu.SemaphoreType.DMA((len(plan), 6)),
            pltpu.SemaphoreType.DMA((len(plan), 6)),
            pltpu.SemaphoreType.DMA((len(plan),)),
        ],
        cost_estimate=pl.CostEstimate(flops=0, bytes_accessed=4 * sent, transcendentals=0),
        compiler_params=pltpu.CompilerParams(
            collective_id=collective, has_side_effects=True, vmem_limit_bytes=60 * 1024 * 1024
        ),
    )(*views)


def chunked(widths, pieces, orders):
    plan = []
    for index, (width, number) in enumerate(zip(widths, pieces)):
        tiles = width // lanes
        edges = [tiles * i // number for i in range(number + 1)]
        for i in range(number):
            plan.append((index, edges[i] * lanes, (edges[i + 1] - edges[i]) * lanes, orders[len(plan) % len(orders)]))
    return plan


def carry_kernel(
    reverse, input_ref, decay_ref, carried_ref, ends, outgoing, arrived, joined, final, send, receive
):
    seq_count, step_count, width = input_ref.shape
    count = lax.axis_size("seq")
    part = decay_ref.shape[0] // count
    me, batch = lax.axis_index("seq"), lax.axis_index("batch")
    others = range(1, count)
    barrier = pltpu.get_barrier_semaphore()
    for step in others:
        peer = (lax.rem(me + step, count), batch)
        pl.semaphore_signal(barrier, inc=1, device_id=peer, device_id_type=MESH)

    @pl.loop(0, width // lanes)
    def _(tile):
        columns = pl.ds(pl.multiple_of(tile * lanes, lanes), lanes)
        encode_kernel(reverse, input_ref.at[:, :, columns], decay_ref.at[:, columns], ends)
        for group in range(count):
            rows = slice(group * part, (group + 1) * part)
            mine = jnp.concatenate([ends[seq, rows] for seq in range(seq_count)], axis=0)
            outgoing[group, :, columns] = mine.astype(bf16)

    pl.semaphore_wait(barrier, count - 1)

    def exchange(phase, source, target):
        copies = []
        for step in others:
            peer = lax.rem(me + step, count)
            copy = pltpu.make_async_remote_copy(
                src_ref=source.at[peer],
                dst_ref=target.at[me],
                send_sem=send.at[phase, step - 1],
                recv_sem=receive.at[phase, step - 1],
                device_id=(peer, batch),
                device_id_type=MESH,
            )
            copy.start()
            copies.append(copy)
        target[me] = source[me]
        for copy in copies:
            copy.wait()

    exchange(0, outgoing, arrived)
    rates = decay_ref[pl.ds(pl.multiple_of(me * part, part), part), :]
    power = jnp.exp(-rates * step_count)
    power = jnp.concatenate([power] * seq_count, axis=0)
    state = jnp.zeros(power.shape, f32)
    for block in reversed(range(count)) if reverse else range(count):
        joined[block] = state.astype(bf16)
        state = power * state + arrived[block].astype(f32)
    exchange(1, joined, final)
    for group in range(count):
        rows = slice(group * part, (group + 1) * part)
        found = final[group].astype(f32)
        for seq in range(seq_count):
            carried_ref[seq, rows] = found[seq * part : (seq + 1) * part]


def carried_by_kernel(value, decay, reverse, collective):
    seq_count, _, width = value.shape
    state_count = decay.shape[0]
    count = lax.axis_size("seq")
    parts = pltpu.VMEM((count, seq_count * state_count // count, width), bf16)
    return pl.pallas_call(
        functools.partial(carry_kernel, reverse),
        out_shape=shaped(seq_count, state_count, width),
        in_specs=[pl.BlockSpec(memory_space=pltpu.VMEM)] * 2,
        out_specs=pl.BlockSpec(memory_space=pltpu.VMEM),
        scratch_shapes=[pltpu.VMEM((seq_count, state_count, lanes), f32)]
        + [parts] * 4
        + [pltpu.SemaphoreType.DMA((2, count - 1)), pltpu.SemaphoreType.DMA((2, count - 1))],
        cost_estimate=pl.CostEstimate(flops=0, bytes_accessed=32 * value.size, transcendentals=0),
        compiler_params=pltpu.CompilerParams(collective_id=collective, has_side_effects=True),
    )(value, decay)


hidden_block = 384
gelu_scale = 0.7978845608
gelu_cubic = 0.044715


def feed_kernel(resid_ref, gain_ref, up_ref, down_ref, out_ref, normed_ref, hidden_ref, active_ref):
    @pl.when(pl.program_id(0) == 0)
    def _():
        resid = resid_ref[...]
        normed_ref[...] = layer_norm(resid, gain_ref[...]).astype(bf16)
        out_ref[...] = resid

    hidden = jnp.dot(normed_ref[...], up_ref[...], preferred_element_type=f32)
    hidden_ref[...] = hidden
    bend = jnp.tanh(gelu_scale * (hidden + gelu_cubic * hidden * hidden * hidden))
    active = (0.5 * hidden * (1.0 + bend)).astype(bf16)
    active_ref[...] = active
    out_ref[...] += jnp.dot(active, down_ref[...], preferred_element_type=f32)


def feed_forward_blocks(resid, gain, up_packed, up_at, down):
    rows, width = resid.shape
    inner = down.shape[0]
    first = up_at // hidden_block
    whole = pl.BlockSpec((rows, width), lambda j: (0, 0))
    part = pl.BlockSpec((rows, hidden_block), lambda j: (0, j))
    out, normed, hidden, active = pl.pallas_call(
        feed_kernel,
        grid=(inner // hidden_block,),
        in_specs=[
            whole,
            pl.BlockSpec((1, width), lambda j: (0, 0)),
            pl.BlockSpec((width, hidden_block), lambda j: (0, first + j)),
            pl.BlockSpec((hidden_block, width), lambda j: (j, 0)),
        ],
        out_specs=[whole, whole, part, part],
        out_shape=[
            shaped(rows, width),
            shaped(rows, width, dtype=bf16),
            shaped(rows, inner),
            shaped(rows, inner, dtype=bf16),
        ],
        cost_estimate=pl.CostEstimate(
            flops=4 * rows * width * inner, bytes_accessed=10 * width * inner, transcendentals=rows * inner
        ),
        compiler_params=pltpu.CompilerParams(vmem_limit_bytes=60 * 1024 * 1024),
    )(resid, gain[None], up_packed, down)
    return out, (resid, gain, normed, hidden, active)


def feed_back_kernel(
    packed,
    upstream_ref,
    resid_ref,
    gain_ref,
    normed_ref,
    hidden_ref,
    active_ref,
    up_ref,
    down_ref,
    out_ref,
    gain_grad_ref,
    *rest,
):
    step = pl.program_id(0)
    last = pl.num_programs(0) - 1
    across = (((1,), (1,)), ((), ()))
    along = (((0,), (0,)), ((), ()))
    upstream_low = upstream_ref[...].astype(bf16)
    into_active = lax.dot_general(upstream_low, down_ref[...], across, preferred_element_type=f32)
    hidden = hidden_ref[...]
    square = hidden * hidden
    bend = jnp.tanh(gelu_scale * hidden * (1.0 + gelu_cubic * square))
    slope = 0.5 * (1.0 + bend) + 0.5 * hidden * (1.0 - bend * bend) * (
        gelu_scale * (1.0 + 3.0 * gelu_cubic * square)
    )
    into_hidden = (into_active * slope).astype(bf16)
    part = lax.dot_general(into_hidden, up_ref[...], across, preferred_element_type=f32)

    @pl.when(step == 0)
    def _():
        out_ref[...] = part

    @pl.when(step > 0)
    def _():
        out_ref[...] += part

    up_grad = lax.dot_general(normed_ref[...], into_hidden, along, preferred_element_type=f32)
    down_grad = lax.dot_general(active_ref[...], upstream_low, along, preferred_element_type=f32)
    if packed:
        grads_ref, up_held, down_held, sems = rest
        share, fold = packed
        width = up_grad.shape[0]
        inner = hidden_block * grads_ref.shape[1] // (2 * hidden_block)
        tall = hidden_block // fold
        slot = lax.rem(step, 2)

        def copies(at, slot):
            columns = pl.ds(pl.multiple_of(at * hidden_block, hidden_block), hidden_block)
            rows = pl.ds(pl.multiple_of(at * tall, tall), tall)
            return (
                pltpu.make_async_copy(up_held.at[slot], grads_ref.at[:, columns], sems.at[0, slot]),
                pltpu.make_async_copy(down_held.at[slot], grads_ref.at[rows, inner:], sems.at[1, slot]),
            )

        @pl.when(step >= 2)
        def _():
            for copy in copies(step - 2, slot):
                copy.wait()

        up_held[slot] = up_grad.astype(bf16)
        for place in range(fold):
            starts = range(place * share, hidden_block, fold * share)
            piece = jnp.concatenate([down_grad[a : a + share] for a in starts], axis=0)
            down_held[slot, :, place * width : (place + 1) * width] = piece.astype(bf16)
        for copy in copies(step, slot):
            copy.start()

        @pl.when(step == last)
        def _():
            for copy in copies(step - 1, 1 - slot) + copies(step, slot):
                copy.wait()
    else:
        up_grad_ref, down_grad_ref = rest
        up_grad_ref[...] = up_grad.astype(bf16)
        down_grad_ref[...] = down_grad.astype(bf16)

    @pl.when(step == last)
    def _():
        into_normed = out_ref[...]
        resid = resid_ref[...]
        centred = resid - jnp.mean(resid, axis=-1, keepdims=True)
        inverse = lax.rsqrt(jnp.mean(centred * centred, axis=-1, keepdims=True) + eps)
        unit = centred * inverse
        gain_grad_ref[...] = jnp.sum(into_normed * unit, axis=0, keepdims=True)
        scaled = into_normed * gain_ref[...]
        along_unit = jnp.mean(scaled * unit, axis=-1, keepdims=True)
        into_resid = inverse * (scaled - jnp.mean(scaled, axis=-1, keepdims=True) - unit * along_unit)
        out_ref[...] = upstream_ref[...] + into_resid


def feed_back_blocks(stored, up_packed, up_at, down, upstream, packed=()):
    resid, gain, normed, hidden, active = stored
    rows, width = resid.shape
    inner = down.shape[0]
    first = up_at // hidden_block
    whole = pl.BlockSpec((rows, width), lambda j: (0, 0))
    part = pl.BlockSpec((rows, hidden_block), lambda j: (0, j))
    line = pl.BlockSpec((1, width), lambda j: (0, 0))
    up_spec = pl.BlockSpec((width, hidden_block), lambda j: (0, j))
    down_spec = pl.BlockSpec((hidden_block, width), lambda j: (j, 0))
    scratch = []
    if packed:
        grad_specs = [pl.BlockSpec(memory_space=pl.ANY)]
        grad_shapes = [shaped(width, 2 * inner, dtype=bf16)]
        scratch = [
            pltpu.VMEM((2, width, hidden_block), bf16),
            pltpu.VMEM((2, hidden_block // packed[1], inner), bf16),
            pltpu.SemaphoreType.DMA((2, 2)),
        ]
    else:
        grad_specs = [up_spec, down_spec]
        grad_shapes = [shaped(width, inner, dtype=bf16), shaped(inner, width, dtype=bf16)]
    out, gain_grad, *grads = pl.pallas_call(
        functools.partial(feed_back_kernel, packed),
        grid=(inner // hidden_block,),
        in_specs=[
            whole,
            whole,
            line,
            whole,
            part,
            part,
            pl.BlockSpec((width, hidden_block), lambda j: (0, first + j)),
            down_spec,
        ],
        out_specs=[whole, line] + grad_specs,
        out_shape=[shaped(rows, width), shaped(1, width)] + grad_shapes,
        scratch_shapes=scratch,
        cost_estimate=pl.CostEstimate(
            flops=8 * rows * width * inner, bytes_accessed=16 * width * inner, transcendentals=rows * inner
        ),
        compiler_params=pltpu.CompilerParams(vmem_limit_bytes=60 * 1024 * 1024),
    )(upstream, resid, gain[None], normed, hidden, active, up_packed, down)
    return (out, gain_grad[0], *grads)


def split_heads(ref, scratch, heads, parts):
    @pl.loop(0, ref.shape[0] // lanes)
    def _(turn):
        rows = pl.ds(pl.multiple_of(turn * lanes, lanes), lanes)
        for part in range(parts * heads):
            scratch[part, rows, :] = ref[rows, part * HEAD_DIM : (part + 1) * HEAD_DIM]


def score_block(query, keys, first, scale):
    scores = (
        lax.dot_general(query, keys, (((1,), (1,)), ((), ())), preferred_element_type=f32) * scale
    )
    rows = lax.broadcasted_iota(jnp.int32, scores.shape, 0) + first
    columns = lax.broadcasted_iota(jnp.int32, scores.shape, 1)
    return jnp.where(columns <= rows, scores, masked_score)


def over_blocks(one_block, heads, length, block):
    span = min(2 * block, length)

    @pl.loop(0, heads)
    def _(head):
        for start in range(0, length, span):

            @pl.loop(0, span // block)
            def _(half):
                one_block(head, pl.multiple_of(start + half * block, block), start + span)


def attend_kernel(heads, block, scale, qkv_ref, low_ref, full_ref, stat_ref, parts, outs):
    length = qkv_ref.shape[0]
    split_heads(qkv_ref, parts, heads, 3)

    def one_block(head, first, extent):
        here_rows = pl.ds(first, block)
        query = parts[head, here_rows, :]
        scores = score_block(query, parts[heads + head, :extent, :], first, scale)
        top = jnp.max(scores, axis=1, keepdims=True)
        soft = jnp.exp(scores - top)
        whole = jnp.sum(soft, axis=1, keepdims=True)
        soft = soft * (1.0 / whole)
        outs[head, here_rows, :] = jnp.dot(
            soft.astype(bf16), parts[2 * heads + head, :extent, :], preferred_element_type=f32
        )
        stat_ref[head, here_rows, :] = jnp.broadcast_to(top + jnp.log(whole), (block, lanes))

    over_blocks(one_block, heads, length, block)

    @pl.loop(0, length // lanes)
    def _(turn):
        rows = pl.ds(pl.multiple_of(turn * lanes, lanes), lanes)
        if low_ref.shape[1] > heads * HEAD_DIM:
            rest = low_ref.shape[1] - heads * HEAD_DIM
            low_ref[rows, heads * HEAD_DIM :] = jnp.zeros((lanes, rest), bf16)
        for head in range(heads):
            place = slice(head * HEAD_DIM, (head + 1) * HEAD_DIM)
            found = outs[head, rows, :]
            full_ref[rows, place] = found
            low_ref[rows, place] = found.astype(bf16)


def attend_back_kernel(
    heads, block, scale, qkv_ref, dout_ref, full_ref, stat_ref, grad_ref, parts, douts, fulls, grads
):
    length = qkv_ref.shape[0]
    split_heads(qkv_ref, parts, heads, 3)
    split_heads(dout_ref, douts, heads, 1)
    split_heads(full_ref, fulls, heads, 1)

    @pl.loop(0, 3 * heads)
    def _(part):
        grads[part] = jnp.zeros(grads.shape[1:], f32)

    def one_block(head, first, extent):
        here_rows = pl.ds(first, block)
        query = parts[head, here_rows, :]
        keys = parts[heads + head, :extent, :]
        value = parts[2 * heads + head, :extent, :]
        dout = douts[head, here_rows, :]
        delta = jnp.sum(dout.astype(f32) * fulls[head, here_rows, :], axis=1, keepdims=True)
        scores = score_block(query, keys, first, scale)
        soft = jnp.exp(scores - stat_ref[head, here_rows, :1])
        across = (((1,), (1,)), ((), ()))
        along = (((0,), (0,)), ((), ()))
        dprob = lax.dot_general(dout, value, across, preferred_element_type=f32)
        dscore = (soft * (dprob - delta) * scale).astype(bf16)
        grads[head, here_rows, :] = jnp.dot(dscore, keys, preferred_element_type=f32)
        grads[heads + head, :extent, :] += lax.dot_general(
            dscore, query, along, preferred_element_type=f32
        )
        grads[2 * heads + head, :extent, :] += lax.dot_general(
            soft.astype(bf16), dout, along, preferred_element_type=f32
        )

    over_blocks(one_block, heads, length, block)

    @pl.loop(0, length // lanes)
    def _(turn):
        rows = pl.ds(pl.multiple_of(turn * lanes, lanes), lanes)
        rest = grad_ref.shape[1] - 3 * heads * HEAD_DIM
        if rest:
            grad_ref[rows, 3 * heads * HEAD_DIM :] = jnp.zeros((lanes, rest), bf16)
        for part in range(3 * heads):
            grad_ref[rows, part * HEAD_DIM : (part + 1) * HEAD_DIM] = grads[part, rows, :].astype(bf16)


def attend_params():
    return pltpu.CompilerParams(vmem_limit_bytes=56 * 1024 * 1024)


def attend_whole(qkv, heads, block):
    length = qkv.shape[0]
    width = heads * HEAD_DIM
    return pl.pallas_call(
        functools.partial(attend_kernel, heads, block, HEAD_DIM ** (-0.5)),
        out_shape=[
            shaped(length, -(-width // lanes) * lanes, dtype=bf16),
            shaped(length, width),
            shaped(heads, length, lanes),
        ],
        scratch_shapes=[
            pltpu.VMEM((3 * heads, length, HEAD_DIM), bf16),
            pltpu.VMEM((heads, length, HEAD_DIM), f32),
        ],
        compiler_params=attend_params(),
    )(qkv)


def attend_whole_back(qkv, dout, full, stat, heads, block):
    length = qkv.shape[0]
    return pl.pallas_call(
        functools.partial(attend_back_kernel, heads, block, HEAD_DIM ** (-0.5)),
        out_shape=shaped(*qkv.shape, dtype=bf16),
        scratch_shapes=[
            pltpu.VMEM((3 * heads, length, HEAD_DIM), bf16),
            pltpu.VMEM((heads, length, HEAD_DIM), bf16),
            pltpu.VMEM((heads, length, HEAD_DIM), f32),
            pltpu.VMEM((3 * heads, length, HEAD_DIM), f32),
        ],
        compiler_params=attend_params(),
    )(qkv, dout, full, stat)


def split_blocks(array, block_len):
    shaped_blocks = array.reshape(
        (array.shape[0], array.shape[1] // block_len, block_len) + array.shape[2:]
    )
    return jnp.moveaxis(shaped_blocks, 1, 0)


def general_attention(proj_low, seq_count, block_len, places, any_live, longest):
    model_width = HEADS * HEAD_DIM
    scale = HEAD_DIM ** (-0.5)
    offsets = jnp.arange(block_len, dtype=jnp.int32)
    head_shape = (seq_count, block_len, HEADS, HEAD_DIM)
    query_low = proj_low[:, :model_width].reshape(head_shape)
    keys_low = proj_low[:, model_width : 2 * model_width].reshape(head_shape)
    value_low = proj_low[:, 2 * model_width :].reshape(head_shape)

    def block_scores(queries, keys_block, query_places, key_places):
        scores = (
            jnp.einsum("sqhe,skhe->sqhk", queries, keys_block, preferred_element_type=jnp.float32)
            * scale
        )
        causal_mask = key_places[None, :] <= query_places[:, None]
        return jnp.where(causal_mask[None, :, None, :], scores, masked_score)

    def key_needed(key_first):
        return (key_first <= places[-1]) & ((key_first == places[0]) | any_live)

    stat_shape = (seq_count, block_len, HEADS)
    start_state = (
        jnp.full(stat_shape, masked_score, jnp.float32),
        jnp.zeros(stat_shape, jnp.float32),
        jnp.zeros(head_shape, jnp.float32),
    )
    shard_piece = (
        lax.all_gather(keys_low, "seq", axis=1, tiled=True),
        lax.all_gather(value_low, "seq", axis=1, tiled=True),
    )
    keys_blocks = split_blocks(shard_piece[0], block_len)
    value_blocks = split_blocks(shard_piece[1], block_len)
    firsts = jnp.arange(keys_blocks.shape[0], dtype=jnp.int32) * block_len

    def attend_one_step(state_now, operand):
        keys_block, value_block, key_first = operand

        def attend_work(state_in_block):
            running_max, running_sum, running_out = state_in_block
            scores = block_scores(query_low, keys_block, places, key_first + offsets)
            new_max = jnp.maximum(running_max, jnp.max(scores, axis=-1))
            fade = jnp.exp(running_max - new_max)
            shifted = jnp.exp(scores - new_max[..., None])
            new_sum = running_sum * fade + jnp.sum(shifted, axis=-1)
            new_out = running_out * fade[..., None] + jnp.einsum(
                "sqhk,skhe->sqhe",
                shifted.astype(jnp.bfloat16),
                value_block,
                preferred_element_type=jnp.float32,
            )
            return (new_max, new_sum, new_out)

        return (
            lax.cond(
                key_needed(key_first), attend_work, lambda state_in_block: state_in_block, state_now
            ),
            None,
        )

    result, _ = lax.scan(attend_one_step, start_state, (keys_blocks, value_blocks, firsts))
    running_max, running_sum, running_out = result
    attended = running_out / running_sum[..., None]
    logsum = running_max + jnp.log(running_sum)
    def backward(dout_low):
        delta = jnp.sum(dout_low.astype(jnp.float32) * attended, axis=-1)
        shard_piece = (
            lax.all_gather(keys_low, "seq", axis=1, tiled=True),
            lax.all_gather(value_low, "seq", axis=1, tiled=True),
        )
        keys_blocks = split_blocks(shard_piece[0], block_len)
        value_blocks = split_blocks(shard_piece[1], block_len)
        firsts = jnp.arange(keys_blocks.shape[0], dtype=jnp.int32) * block_len

        def query_one_step(query_grad, operand):
            keys_block, value_block, key_first = operand

            def query_work(grad_now):
                scores = block_scores(query_low, keys_block, places, key_first + offsets)
                soft = jnp.exp(scores - logsum[..., None])
                dprob = jnp.einsum(
                    "sqhe,skhe->sqhk", dout_low, value_block, preferred_element_type=jnp.float32
                )
                dscore = (soft * (dprob - delta[..., None])).astype(jnp.bfloat16)
                return (
                    grad_now
                    + jnp.einsum(
                        "sqhk,skhe->sqhe", dscore, keys_block, preferred_element_type=jnp.float32
                    )
                    * scale
                )

            return (
                lax.cond(key_needed(key_first), query_work, lambda grad_now: grad_now, query_grad),
                None,
            )

        result, _ = lax.scan(
            query_one_step, jnp.zeros(head_shape, jnp.float32), (keys_blocks, value_blocks, firsts)
        )
        query_grad = result
        sent = (query_low.astype(jnp.float32), dout_low.astype(jnp.float32), logsum, delta)
        shard_piece = (
            lax.all_gather(sent[0].astype(jnp.bfloat16), "seq", axis=1, tiled=True).astype(jnp.float32),
            lax.all_gather(sent[1].astype(jnp.bfloat16), "seq", axis=1, tiled=True).astype(jnp.float32),
            lax.all_gather(sent[2].astype(jnp.bfloat16), "seq", axis=1, tiled=True).astype(jnp.float32),
            lax.all_gather(sent[3].astype(jnp.bfloat16), "seq", axis=1, tiled=True).astype(jnp.float32),
        )
        query_blocks = split_blocks(shard_piece[0], block_len)
        dout_blocks = split_blocks(shard_piece[1], block_len)
        logsum_blocks = split_blocks(shard_piece[2], block_len)
        delta_blocks = split_blocks(shard_piece[3], block_len)
        firsts = jnp.arange(query_blocks.shape[0], dtype=jnp.int32) * block_len

        def key_one_step(grads_now, operand):
            query_block, dout_block, logsum_block, delta_block, query_first = operand

            def key_work(grads_in):
                keys_grad, value_grad = grads_in
                query_cast = query_block.astype(jnp.bfloat16)
                dout_cast = dout_block.astype(jnp.bfloat16)
                scores = block_scores(query_cast, keys_low, query_first + offsets, places)
                soft = jnp.exp(scores - logsum_block[..., None])
                value_grad = value_grad + jnp.einsum(
                    "sqhk,sqhe->skhe",
                    soft.astype(jnp.bfloat16),
                    dout_cast,
                    preferred_element_type=jnp.float32,
                )
                dprob = jnp.einsum(
                    "sqhe,skhe->sqhk", dout_cast, value_low, preferred_element_type=jnp.float32
                )
                dscore = (soft * (dprob - delta_block[..., None])).astype(jnp.bfloat16)
                keys_grad = (
                    keys_grad
                    + jnp.einsum(
                        "sqhk,sqhe->skhe", dscore, query_cast, preferred_element_type=jnp.float32
                    )
                    * scale
                )
                return (keys_grad, value_grad)

            needed = (query_first + block_len - 1 >= places[0]) & (
                (query_first == places[0]) | (query_first < longest)
            )
            return (lax.cond(needed, key_work, lambda grads_in: grads_in, grads_now), None)

        result, _ = lax.scan(
            key_one_step,
            (jnp.zeros(head_shape, jnp.float32), jnp.zeros(head_shape, jnp.float32)),
            (query_blocks, dout_blocks, logsum_blocks, delta_blocks, firsts),
        )
        keys_grad, value_grad = result
        return (query_grad, keys_grad, value_grad)

    return attended, backward


def layer_norm(value, gain):
    centred = value - jnp.mean(value, axis=-1, keepdims=True)
    spread_of = jnp.mean(centred * centred, axis=-1, keepdims=True)
    return centred * lax.rsqrt(spread_of + eps) * gain


def gelu_tanh(value):
    return jax.nn.gelu(value, approximate=True)


def dense(left, weight):
    return jnp.dot(left, weight, preferred_element_type=f32)


def dense_back(left, weight, upstream):
    into_left = lax.dot_general(
        upstream, weight, (((1,), (1,)), ((), ())), preferred_element_type=f32
    )
    into_weight = lax.dot_general(
        left, upstream, (((0,), (0,)), ((), ())), preferred_element_type=f32
    ).astype(bf16)
    return (into_left, into_weight)


def shift_mix(extended, taps, value_part):
    step_count = value_part.shape[1]
    reach = taps.shape[1]
    shifted = extended[:, reach - 1 : reach - 1 + step_count] * taps[:, 0]
    for tap_index in range(1, reach):
        shifted = (
            shifted
            + extended[:, reach - 1 - tap_index : reach - 1 - tap_index + step_count]
            * taps[:, tap_index]
        )
    return shifted * value_part


def feed_forward(resid, gain, up_weight, down_weight):
    normed, norm_back = jax.vjp(layer_norm, resid, gain)
    normed_low = normed.astype(bf16)
    hidden = dense(normed_low, up_weight)
    active, active_back = jax.vjp(gelu_tanh, hidden)
    active_low = active.astype(bf16)
    return (
        resid + dense(active_low, down_weight),
        (norm_back, normed_low, active_back, active_low),
    )


def feed_back(stored, up_weight, down_weight, upstream):
    norm_back, normed_low, active_back, active_low = stored
    into_active, down_grad = dense_back(active_low, down_weight, upstream.astype(bf16))
    (into_hidden,) = active_back(into_active)
    into_normed, up_grad = dense_back(normed_low, up_weight, into_hidden.astype(bf16))
    into_resid, gain_grad = norm_back(into_normed)
    return (upstream + into_resid, gain_grad, up_grad, down_grad)


def fold_rows(weight, share):
    rows, width = weight.shape
    fold = rows // share
    return weight.reshape(fold, share, width).transpose(1, 0, 2).reshape(share, fold * width)


def unfold_rows(folded, fold, share):
    rows, width = folded.shape
    width //= fold
    parts = folded.reshape(rows // share, share, fold, width).transpose(0, 2, 1, 3)
    return parts.reshape(rows * fold, width)


def fold_all(weight, share, rows):
    tall, width = weight.shape
    fold = tall // rows
    parts = weight.reshape(rows // share, fold, share, width).transpose(0, 2, 1, 3)
    return parts.reshape(rows, fold * width)


def group_columns(weight, groups, padded):
    rows, columns = weight.shape
    part = columns // 3 // groups
    grouped = weight.reshape(rows, 3, groups, part).transpose(0, 2, 1, 3).reshape(rows, groups, 3 * part)
    return jnp.pad(grouped, ((0, 0), (0, 0), (0, padded - 3 * part))).reshape(rows, groups * padded)


def pad_groups(weight, groups, padded):
    rows, columns = weight.shape
    part = rows // groups
    grouped = weight.reshape(groups, part, columns)
    return jnp.pad(grouped, ((0, 0), (0, padded - part), (0, 0))).reshape(groups * padded, columns)


def ungroup_columns(grouped, groups, padded, columns):
    rows = grouped.shape[0]
    part = columns // 3 // groups
    parts = grouped.reshape(rows, groups, padded)[:, :, : 3 * part].reshape(rows, groups, 3, part)
    return parts.transpose(0, 2, 1, 3).reshape(rows, columns)


def cut(array, widths):
    pieces, start = [], 0
    for width in widths:
        pieces.append(array[:, start : start + width])
        start += width
    return pieces


def cut_last(array, count):
    width = array.shape[-1] // count
    return [array[..., i * width : (i + 1) * width] for i in range(count)]


def gathered(parts):
    whole = lax.all_gather(jnp.concatenate(parts, axis=1), everyone, axis=0, tiled=True)
    return cut(whole, [p.shape[1] for p in parts])


def scattered(parts):
    mine = lax.psum_scatter(
        jnp.concatenate(parts, axis=1), everyone, scatter_dimension=0, tiled=True
    )
    return cut(mine, [p.shape[1] for p in parts])


def body(
    tokens,
    cotangent,
    lengths,
    mixer_gain,
    mixer_inputs,
    shift_taps,
    decay_rate,
    state_in,
    state_out,
    state_skip,
    mixer_output,
    first_gain,
    first_up,
    first_down,
    attend_gain,
    attend_inputs,
    attend_output,
    second_gain,
    second_up,
    second_down,
):
    seq_count, block_len, model_width = tokens.shape
    row_count = seq_count * block_len
    seq_devices = lax.axis_size("seq")
    share = mixer_inputs.shape[0]
    states, reach = decay_rate.shape[1], shift_taps.shape[1]
    fold = first_down.shape[0] // share
    deals = seq_count * HEADS
    dealt = deals % seq_devices == 0 and HEADS % (deals // seq_devices) == 0
    heads = deals // seq_devices if dealt else HEADS
    groups = HEADS // heads
    group_width = heads * HEAD_DIM
    padded = -(-3 * group_width // lanes) * lanes if dealt else 3 * group_width
    out_width = -(-group_width // lanes) * lanes if dealt else group_width

    columns = [decay_rate, state_in, state_out, shift_taps]
    columns += [g[:, None] for g in (mixer_gain, first_gain, attend_gain, second_gain, state_skip)]
    small = jnp.concatenate(columns, axis=1)
    small_count = small.shape[1]
    small_width = -(-small_count // lanes) * lanes
    small = jnp.pad(small, ((0, 0), (0, small_width - small_count)))
    attend_cols = attend_inputs.shape[1]
    grouped = group_columns(attend_inputs, groups, padded)
    by_kernel = seq_devices == 8 and lax.axis_size("batch") == 4
    packed = [mixer_output, attend_output, first_up, second_up, grouped]
    up1_at = 2 * model_width
    up2_at = up1_at + first_up.shape[1]
    if by_kernel:
        joint = jnp.concatenate([mixer_inputs, small], axis=1)
        w_packed = lax.all_gather(jnp.concatenate(packed, axis=1), everyone, axis=0, tiled=True)
        w_mixer_out, w_attend_out, _, _, w_attend_in = cut(w_packed, [p.shape[1] for p in packed])
        widths = (joint.shape[1], model_width)
        w_joint, w_down1 = gather_blocks((joint, first_down), chunked(widths, (4, 6), ("zxy", "zyx")), gap=3)
        w_mixer_in, w_small = cut(w_joint, [mixer_inputs.shape[1], small_width])
        second_down, w_small = lax.optimization_barrier((second_down, w_small))
        w_down2 = lax.all_gather(second_down, everyone, axis=0, tiled=True)
    else:
        w_mixer_in, w_small = gathered([mixer_inputs, small])
        packed += [fold_rows(first_down, share), fold_rows(second_down, share)]
        w_mixer_out, w_attend_out, w_up1, w_up2, w_attend_in, w_down1, w_down2 = gathered(packed)
        w_down1 = unfold_rows(w_down1, fold, share)
        w_down2 = unfold_rows(w_down2, fold, share)

    rows = w_small.T.astype(f32)
    decay, table_in, table_out = rows[:states], rows[states : 2 * states], rows[2 * states : 3 * states]
    taps_rows = rows[3 * states : 3 * states + reach]
    gain_mixer, gain_first, gain_attend, gain_second, skip = (
        rows[3 * states + reach + i] for i in range(5)
    )
    taps = taps_rows.T
    weight = table_in * table_out

    rank_seq = lax.axis_index("seq")
    offsets = jnp.arange(block_len, dtype=jnp.int32)
    places = rank_seq * block_len + offsets
    valid = (places[None, :] < lengths[:, None]).astype(f32)
    longest = jnp.max(lengths)
    any_live = places[0] < longest

    start_resid = tokens.reshape(row_count, model_width).astype(f32)
    normed_mixer, back_mixer = jax.vjp(layer_norm, start_resid, gain_mixer)
    normed_low_mixer = normed_mixer.astype(bf16)
    projected = dense(normed_low_mixer, w_mixer_in).reshape(seq_count, block_len, 3 * model_width)
    query_mixer = projected[:, :, :model_width]
    keys_mixer = projected[:, :, model_width : 2 * model_width]
    value_mixer = projected[:, :, 2 * model_width :]
    rim_rows = passed_along(keys_mixer[:, block_len - reach + 1 :], "seq", 1)
    extended = jnp.concatenate([rim_rows, keys_mixer], axis=1)
    inner, shift_back = jax.vjp(shift_mix, extended, taps, value_mixer)
    if by_kernel:
        carried = carried_by_kernel(inner, decay, False, 2)
    else:
        carried = carried_in(encode(inner, decay, False), decay, block_len, False)
    wide = shaped(seq_count, block_len, model_width)
    state_y, gated = per_lane_tile(
        output_kernel,
        (inner, query_mixer, carried, decay, weight, skip[None]),
        (wide, wide),
    )
    gated_low = gated.astype(bf16).reshape(row_count, model_width)
    resid_mixer = start_resid + dense(gated_low, w_mixer_out)
    if by_kernel:
        resid_first, stored_first = feed_forward_blocks(
            resid_mixer, gain_first, w_packed, up1_at, w_down1
        )
    else:
        resid_first, stored_first = feed_forward(resid_mixer, gain_first, w_up1, w_down1)

    normed_attend, back_attend = jax.vjp(layer_norm, resid_first, gain_attend)
    normed_low_attend = normed_attend.astype(bf16)
    proj_low = dense(normed_low_attend, w_attend_in).astype(bf16)
    if dealt:
        length = seq_devices * block_len
        block = min(128, length)

        def deal(array, width):
            array = array.reshape(seq_count, block_len, groups * width)
            parts = jnp.stack(cut_last(array, groups), axis=1)
            parts = parts.reshape(seq_count * groups, block_len, width)
            dealt_parts = lax.all_to_all(parts, "seq", split_axis=0, concat_axis=0, tiled=True)
            return dealt_parts.reshape(length, width)

        def collect(array, width):
            parts = array.reshape(seq_devices, block_len, width)
            back = lax.all_to_all(parts, "seq", split_axis=0, concat_axis=0, tiled=True)
            back = back.reshape(seq_count, groups, block_len, width)
            back = jnp.concatenate([back[:, group] for group in range(groups)], axis=-1)
            return back.reshape(row_count, groups * width)

        qkv = deal(proj_low, padded)
        attended_part, attended_full, stat = attend_whole(qkv, heads, block)
        attended_low = collect(attended_part, out_width)
        w_attend_out = pad_groups(w_attend_out, groups, out_width)
    else:
        attended, attended_back = general_attention(
            proj_low, seq_count, block_len, places, any_live, longest
        )
        attended_low = attended.reshape(row_count, model_width).astype(bf16)
    resid_attend = resid_first + dense(attended_low, w_attend_out)
    if by_kernel:
        final, stored_second = feed_forward_blocks(
            resid_attend, gain_second, w_packed, up2_at, w_down2
        )
    else:
        final, stored_second = feed_forward(resid_attend, gain_second, w_up2, w_down2)
    mixed = (final.reshape(seq_count, block_len, model_width) * valid[..., None]).astype(bf16)

    upstream = (cotangent.astype(f32) * valid[..., None]).reshape(row_count, model_width)
    if by_kernel:
        upstream, second_gain_grad, early = feed_back_blocks(
            stored_second, w_packed, up2_at, w_down2, upstream, packed=(share, fold)
        )
    else:
        upstream, second_gain_grad, second_up_grad, second_down_grad = feed_back(
            stored_second, w_up2, w_down2, upstream
        )
        early = [second_up_grad, fold_all(second_down_grad, share, model_width)]
        early = jnp.concatenate(early, axis=1)
    into_attended, attend_output_grad = dense_back(
        attended_low, w_attend_out, upstream.astype(bf16)
    )
    if dealt:
        attend_output_grad = attend_output_grad.reshape(groups, out_width, model_width)
        attend_output_grad = attend_output_grad[:, :group_width].reshape(model_width, model_width)
    dout_low = into_attended.astype(bf16)
    if dealt:
        dout = deal(dout_low, out_width)
        qkv_grad = attend_whole_back(qkv, dout, attended_full, stat, heads, block)
        qkv_grad, early = lax.optimization_barrier((qkv_grad, early))
        proj_grad = collect(qkv_grad, padded)
    else:
        parts = attended_back(dout_low.reshape(seq_count, block_len, HEADS, HEAD_DIM))
        proj_grad = jnp.concatenate(
            [p.reshape(row_count, model_width) for p in parts], axis=1
        ).astype(bf16)
    early = lax.psum_scatter(early, everyone, scatter_dimension=0, tiled=True)
    second_up_out, second_down_out = cut(early, [second_up.shape[1], fold * model_width])
    into_normed, attend_inputs_grad = dense_back(normed_low_attend, w_attend_in, proj_grad)
    into_resid, attend_gain_grad = back_attend(into_normed)
    upstream = upstream + into_resid
    if by_kernel:
        upstream, first_gain_grad, first_up_grad, first_down_grad = feed_back_blocks(
            stored_first, w_packed, up1_at, w_down1, upstream
        )
    else:
        upstream, first_gain_grad, first_up_grad, first_down_grad = feed_back(
            stored_first, w_up1, w_down1, upstream
        )
    into_gated, mixer_output_grad = dense_back(gated_low, w_mixer_out, upstream.astype(bf16))
    into_gated = into_gated.reshape(seq_count, block_len, model_width)
    query_mixer_grad = into_gated * state_y
    state_grad = into_gated * query_mixer
    if by_kernel:
        later = carried_by_kernel(state_grad, decay, True, 3)
    else:
        later = carried_in(encode(state_grad, decay, True), decay, block_len, True)
    table = shaped(states, model_width)
    inner_grad, weight_grad, power_grad, skip_grad = per_lane_tile(
        back_kernel,
        (inner, state_grad, carried, later, decay, weight, skip[None]),
        (wide, table, table, shaped(1, model_width)),
        scratch=[pltpu.VMEM((block_len, seq_count, states, lanes), f32)],
    )
    extended_grad, taps_grad, value_mixer_grad = shift_back(inner_grad)
    spill = passed_along(extended_grad[:, : reach - 1], "seq", -1)
    keys_mixer_grad = extended_grad[:, reach - 1 :] + jnp.pad(
        spill, ((0, 0), (block_len - reach + 1, 0), (0, 0))
    )
    proj_grad_mixer = (
        jnp.concatenate([query_mixer_grad, keys_mixer_grad, value_mixer_grad], axis=2)
        .astype(bf16)
        .reshape(row_count, 3 * model_width)
    )
    into_normed_mixer, mixer_inputs_grad = dense_back(normed_low_mixer, w_mixer_in, proj_grad_mixer)
    into_start, mixer_gain_grad = back_mixer(into_normed_mixer)
    tokens_gradient = (upstream + into_start).reshape(seq_count, block_len, model_width).astype(bf16)

    small_rows = jnp.concatenate(
        [-jnp.exp(-decay) * power_grad, weight_grad * table_out, weight_grad * table_in, taps_grad.T]
        + [
            g[None]
            for g in (mixer_gain_grad, first_gain_grad, attend_gain_grad, second_gain_grad, skip_grad[0])
        ],
        axis=0,
    )
    small_grad = jnp.pad(small_rows, ((0, small_width - small_count), (0, 0))).T.astype(bf16)
    def unfolded(folded):
        return folded.reshape(share, fold, model_width).transpose(1, 0, 2).reshape(share * fold, model_width)

    gains_at = 3 * states + reach
    table_edges = [0, states, 2 * states, 3 * states, gains_at, small_width]

    def tables_of(block):
        return [block[:, a:b] for a, b in zip(table_edges, table_edges[1:])]

    last = [attend_inputs_grad, first_up_grad, mixer_output_grad, mixer_inputs_grad, small_grad]
    if by_kernel:
        last += [first_down_grad, attend_output_grad]
        orders = ("yxz", "xyz", "xzy", "yxz", "xyz", "yzx")
        plan = chunked([g.shape[1] for g in last], (4, 4, 2, 4, 2, 4, 2), orders)
        part = attend_cols // 3 // groups

        def finish(index, block, results):
            if index == 0:
                for group in range(groups):
                    for kind in range(3):
                        start = (kind * groups + group) * part
                        source = group * padded + kind * part
                        results[0][:, start : start + part] = block[:, source : source + part]
            elif index == 4:
                for place, table in enumerate(tables_of(block)):
                    results[5 + place][...] = table
            else:
                results[{1: 1, 2: 2, 3: 3, 5: 4, 6: 10}[index]][...] = block[...]

        widths = [attend_cols] + [g.shape[1] for g in last[1:4]]
        results = [shaped(share, w) for w in widths] + [shaped(share * fold, model_width)]
        results += [shaped(share, b - a) for a, b in zip(table_edges, table_edges[1:])]
        results.append(shaped(share, model_width))
        attend_inputs_out, first_up_out, mixer_output_out, mixer_inputs_out, first_down_out, *tables = (
            scatter_blocks(last, plan, finish, results, gap=4)
        )
        *tables, attend_output_out = tables
    else:
        last += [fold_all(first_down_grad, share, model_width), attend_output_grad]
        *last, folded, attend_output_out = scattered(last)
        first_down_out = unfolded(folded).astype(f32)
        grouped, first_up_out, mixer_output_out, mixer_inputs_out, small_out = (
            g.astype(f32) for g in last
        )
        attend_inputs_out = ungroup_columns(grouped, groups, padded, attend_cols)
        tables = tables_of(small_out)
    decay_out, in_out, out_out, taps_out, vectors = tables

    return (
        mixed,
        tokens_gradient,
        vectors[:, 0],
        mixer_inputs_out,
        taps_out,
        decay_out,
        in_out,
        out_out,
        vectors[:, 4],
        mixer_output_out,
        vectors[:, 1],
        first_up_out,
        first_down_out,
        vectors[:, 2],
        attend_inputs_out,
        attend_output_out.astype(f32),
        vectors[:, 3],
        second_up_out.astype(f32),
        unfolded(second_down_out).astype(f32),
    )


def solution(mesh):
    return jax.shard_map(
        body,
        mesh=mesh,
        in_specs=(
            P("batch", "seq", None),
            P("batch", "seq", None),
            P("batch"),
            P(("seq", "batch")),
            P(("seq", "batch"), None),
            P(("seq", "batch"), None),
            P(("seq", "batch"), None),
            P(("seq", "batch"), None),
            P(("seq", "batch"), None),
            P(("seq", "batch")),
            P(("seq", "batch"), None),
            P(("seq", "batch")),
            P(("seq", "batch"), None),
            P(("seq", "batch"), None),
            P(("seq", "batch")),
            P(("seq", "batch"), None),
            P(("seq", "batch"), None),
            P(("seq", "batch")),
            P(("seq", "batch"), None),
            P(("seq", "batch"), None),
        ),
        out_specs=(
            P("batch", "seq", None),
            P("batch", "seq", None),
            P(("seq", "batch")),
            P(("seq", "batch"), None),
            P(("seq", "batch"), None),
            P(("seq", "batch"), None),
            P(("seq", "batch"), None),
            P(("seq", "batch"), None),
            P(("seq", "batch")),
            P(("seq", "batch"), None),
            P(("seq", "batch")),
            P(("seq", "batch"), None),
            P(("seq", "batch"), None),
            P(("seq", "batch")),
            P(("seq", "batch"), None),
            P(("seq", "batch"), None),
            P(("seq", "batch")),
            P(("seq", "batch"), None),
            P(("seq", "batch"), None),
        ),
        check_vma=False,
    )
```

```python
import functools

import jax
import jax.numpy as jnp
from jax import lax
from jax.experimental import pallas as pl
from jax.experimental.pallas import tpu as pltpu
from jax.sharding import PartitionSpec as P

HEADS = 12
HEAD_DIM = 64

eps = 1e-05
masked_score = -1e30
lanes = 128
sublanes = 8
everyone = ("seq", "batch")
f32 = jnp.float32
bf16 = jnp.bfloat16


def rows_of(ref, seq, block):
    return ref[seq, pl.ds(pl.multiple_of(block * sublanes, sublanes), sublanes), :]


def spread(rows, index, count):
    return jnp.broadcast_to(rows[index : index + 1], (count, lanes))


def encode_kernel(reverse, input_ref, decay_ref, end_ref):
    seq_count, step_count, _ = input_ref.shape
    state_count = decay_ref.shape[0]
    blocks = step_count // sublanes
    power = jnp.exp(-decay_ref[...])

    def one_block(step, states):
        block = blocks - 1 - step if reverse else step
        rows = [rows_of(input_ref, seq, block) for seq in range(seq_count)]
        order = range(sublanes - 1, -1, -1) if reverse else range(sublanes)
        states = list(states)
        for index in order:
            for seq in range(seq_count):
                states[seq] = states[seq] * power + spread(rows[seq], index, state_count)
        return tuple(states)

    start = tuple(jnp.zeros((state_count, lanes), f32) for _ in range(seq_count))
    ends = lax.fori_loop(0, blocks, one_block, start)
    for seq in range(seq_count):
        end_ref[seq] = ends[seq]


def output_kernel(input_ref, query_ref, carried_ref, decay_ref, weight_ref, skip_ref, out_ref, gated_ref):
    seq_count, step_count, _ = input_ref.shape
    state_count = decay_ref.shape[0]
    power = jnp.exp(-decay_ref[...])
    weight = weight_ref[...]
    skip = skip_ref[...]

    def one_block(block, states):
        states = list(states)
        rows = [rows_of(input_ref, seq, block) for seq in range(seq_count)]
        found = [[] for _ in range(seq_count)]
        for index in range(sublanes):
            for seq in range(seq_count):
                states[seq] = states[seq] * power + spread(rows[seq], index, state_count)
                found[seq].append(jnp.sum(states[seq] * weight, axis=0, keepdims=True))
        place = pl.ds(pl.multiple_of(block * sublanes, sublanes), sublanes)
        for seq in range(seq_count):
            result = jnp.concatenate(found[seq], axis=0) + skip * rows[seq]
            out_ref[seq, place, :] = result
            gated_ref[seq, place, :] = result * rows_of(query_ref, seq, block)
        return tuple(states)

    start = tuple(carried_ref[seq].astype(f32) for seq in range(seq_count))
    lax.fori_loop(0, step_count // sublanes, one_block, start)


def back_kernel(
    input_ref,
    grad_ref,
    carried_ref,
    later_ref,
    decay_ref,
    weight_ref,
    skip_ref,
    input_grad_ref,
    weight_grad_ref,
    power_grad_ref,
    skip_grad_ref,
    held,
):
    seq_count, step_count, _ = input_ref.shape
    state_count = decay_ref.shape[0]
    blocks = step_count // sublanes
    power = jnp.exp(-decay_ref[...])
    weight = weight_ref[...]
    skip = skip_ref[...]
    seqs = range(seq_count)

    def forward_block(block, state):
        states, total, skip_total = list(state[0]), state[1], state[2]
        rows = [rows_of(input_ref, seq, block) for seq in seqs]
        grads = [rows_of(grad_ref, seq, block) for seq in seqs]
        for index in range(sublanes):
            for seq in seqs:
                held[block * sublanes + index, seq] = states[seq]
                states[seq] = states[seq] * power + spread(rows[seq], index, state_count)
                total = total + states[seq] * spread(grads[seq], index, state_count)
        for seq in seqs:
            skip_total = skip_total + rows[seq] * grads[seq]
        return (tuple(states), total, skip_total)

    zeros = jnp.zeros((state_count, lanes), f32)
    _, total, skip_total = lax.fori_loop(
        0,
        blocks,
        forward_block,
        (
            tuple(carried_ref[seq].astype(f32) for seq in seqs),
            zeros,
            jnp.zeros((sublanes, lanes), f32),
        ),
    )
    weight_grad_ref[...] = total
    skip_grad_ref[...] = jnp.sum(skip_total, axis=0, keepdims=True)

    def back_block(step, state):
        states, total = list(state[0]), state[1]
        block = blocks - 1 - step
        grads = [rows_of(grad_ref, seq, block) for seq in seqs]
        found = [[None] * sublanes for _ in seqs]
        for index in range(sublanes - 1, -1, -1):
            for seq in seqs:
                states[seq] = states[seq] * power + spread(grads[seq], index, state_count)
                found[seq][index] = jnp.sum(states[seq] * weight, axis=0, keepdims=True)
                total = total + states[seq] * held[block * sublanes + index, seq]
        place = pl.ds(pl.multiple_of(block * sublanes, sublanes), sublanes)
        for seq in seqs:
            input_grad_ref[seq, place, :] = jnp.concatenate(found[seq], axis=0) + skip * grads[seq]
        return (tuple(states), total)

    _, total = lax.fori_loop(
        0, blocks, back_block, (tuple(later_ref[seq].astype(f32) for seq in seqs), zeros)
    )
    power_grad_ref[...] = total * weight


def per_lane_tile(kernel, args, outs, scratch=(), flops=0):
    def spec(shape):
        lead = len(shape) - 1
        return pl.BlockSpec(tuple(shape[:-1]) + (lanes,), lambda tile: (0,) * lead + (tile,))

    bytes_moved = sum(a.size * a.dtype.itemsize for a in args)
    return pl.pallas_call(
        kernel,
        grid=(args[0].shape[-1] // lanes,),
        in_specs=[spec(a.shape) for a in args],
        out_specs=[spec(o.shape) for o in outs],
        out_shape=list(outs),
        scratch_shapes=list(scratch),
        cost_estimate=pl.CostEstimate(flops=flops, bytes_accessed=bytes_moved, transcendentals=0),
        compiler_params=pltpu.CompilerParams(vmem_limit_bytes=48 * 1024 * 1024),
    )(*args)


def shaped(*dims, dtype=f32):
    return jax.ShapeDtypeStruct(dims, dtype)


def encode(value, decay, reverse):
    seq_count, _, width = value.shape
    (ends,) = per_lane_tile(
        functools.partial(encode_kernel, reverse),
        (value, decay),
        (shaped(seq_count, decay.shape[0], width),),
    )
    return ends


def passed_along(block, axis, distance):
    devices = range(lax.axis_size(axis))
    route = [(i - distance, i) for i in devices if i - distance in devices]
    return lax.ppermute(block, axis, route)


def carried_in(ends, decay, block_len, reverse):
    seq_count, state_count, width = ends.shape
    count = lax.axis_size("seq")
    part = state_count // count

    def exchanged(parts):
        return lax.all_to_all(parts.astype(bf16), "seq", split_axis=0, concat_axis=0, tiled=True)

    parts = ends.reshape(seq_count, count, part, width).transpose(1, 0, 2, 3)
    arrived = exchanged(parts.reshape(count, seq_count * part, width)).astype(f32)
    rates = lax.dynamic_slice_in_dim(decay, lax.axis_index("seq") * part, part, 0)
    power = jnp.tile(jnp.exp(-rates * block_len), (seq_count, 1))
    state, joined = jnp.zeros_like(arrived[0]), [None] * count
    for block in reversed(range(count)) if reverse else range(count):
        joined[block] = state
        state = power * state + arrived[block]
    back = exchanged(jnp.stack(joined))
    back = back.reshape(count, seq_count, part, width).transpose(1, 0, 2, 3)
    return back.reshape(seq_count, state_count, width)


MESH = pl.DeviceIdType.MESH
box = (4, 2, 2, 2)


def here():
    seq, batch = lax.axis_index("seq"), lax.axis_index("batch")
    return lax.div(seq, 2), lax.rem(seq, 2), lax.div(batch, 2), lax.rem(batch, 2)


def device(z, x, y, core):
    return (2 * z + x, 2 * y + core)


def line_peer(z, step):
    return lax.rem(z + step, box[0])


def greet():
    z, x, y, core = here()
    barrier = pltpu.get_barrier_semaphore()
    peers = [device(line_peer(z, step), x, y, core) for step in range(1, box[0])]
    peers += [device(z, 1 - x, y, core), device(z, x, 1 - y, core), device(z, x, y, 1 - core)]
    for peer in peers:
        pl.semaphore_signal(barrier, inc=1, device_id=peer, device_id_type=MESH)
    pl.semaphore_wait(barrier, len(peers))


def staggered(count, stages, gap):
    for turn in range(count + gap * (stages - 1)):
        for stage in reversed(range(stages)):
            chunk = turn - gap * stage
            if 0 <= chunk < count:
                yield stage, chunk


def gather_kernel(plan, gap, *refs):
    count = 1 + max(item[0] for item in plan)
    ins, outs = refs[:count], refs[count : 2 * count]
    send, receive, local = refs[2 * count :]
    z, x, y, core = here()
    greet()
    started = {}

    def push(chunk, slot, source, target, peer):
        copy = pltpu.make_async_remote_copy(
            src_ref=source,
            dst_ref=target,
            send_sem=send.at[chunk, slot],
            recv_sem=receive.at[chunk, slot],
            device_id=peer,
            device_id_type=MESH,
        )
        copy.start()
        started[chunk, slot] = copy

    own = []
    for chunk, (index, first, width, _) in enumerate(plan):
        columns = pl.ds(first, width)
        source = ins[index].at[:, columns]
        target = outs[index].at[z, x, y, core, :, columns]
        for step in range(1, box[0]):
            push(chunk, step - 1, source, target, device(line_peer(z, step), x, y, core))
        keep = pltpu.make_async_copy(source, target, local.at[chunk])
        keep.start()
        own.append(keep)

    for stage, chunk in staggered(len(plan), 3, gap):
        index, first, width, order = plan[chunk]
        x_first = order[1] == "x"
        columns = pl.ds(first, width)
        out = outs[index]
        if stage == 0:
            for step in range(1, box[0]):
                started[chunk, step - 1].wait_recv()
            own[chunk].wait()
            part = out.at[:, x, y, core, :, columns]
            peer = device(z, 1 - x, y, core) if x_first else device(z, x, 1 - y, core)
            push(chunk, 3, part, part, peer)
        elif stage == 1:
            started[chunk, 3].wait_recv()
            if x_first:
                part, peer = out.at[:, :, y, core, :, columns], device(z, x, 1 - y, core)
            else:
                part, peer = out.at[:, x, :, core, :, columns], device(z, 1 - x, y, core)
            push(chunk, 4, part, part, peer)
        else:
            started[chunk, 4].wait_recv()
            part = out.at[:, :, :, core, :, columns]
            push(chunk, 5, part, part, device(z, x, y, 1 - core))
    for chunk in range(len(plan)):
        started[chunk, 5].wait_recv()
        for slot in range(6):
            started[chunk, slot].wait_send()


def gather_blocks(blocks, plan, gap=2, collective=0):
    outs = [jax.ShapeDtypeStruct(box + b.shape, b.dtype) for b in blocks]
    sent = sum(b.size * b.dtype.itemsize for b in blocks)
    whole = pl.pallas_call(
        functools.partial(gather_kernel, plan, gap),
        out_shape=outs,
        in_specs=[pl.BlockSpec(memory_space=pltpu.VMEM)] * len(blocks),
        out_specs=[pl.BlockSpec(memory_space=pl.ANY)] * len(blocks),
        scratch_shapes=[
            pltpu.SemaphoreType.DMA((len(plan), 6)),
            pltpu.SemaphoreType.DMA((len(plan), 6)),
            pltpu.SemaphoreType.DMA((len(plan),)),
        ],
        cost_estimate=pl.CostEstimate(flops=0, bytes_accessed=64 * sent, transcendentals=0),
        compiler_params=pltpu.CompilerParams(collective_id=collective, has_side_effects=True),
    )(*blocks)
    return [w.reshape((32 * w.shape[4], w.shape[5])) for w in whole]


def add_into(total, other):
    return (total.astype(f32) + other.astype(f32)).astype(bf16)


def scatter_kernel(plan, gap, finish, counts, *refs):
    count, out_count = counts
    ins, results = refs[:count], refs[count : count + out_count]
    outs, buffers = refs[count + out_count : 2 * count + out_count], refs[2 * count + out_count : -3]
    send, receive, local = refs[-3:]
    z, x, y, core = here()
    greet()
    started = {}

    def push(chunk, slot, source, target, peer):
        copy = pltpu.make_async_remote_copy(
            src_ref=source,
            dst_ref=target,
            send_sem=send.at[chunk, slot],
            recv_sem=receive.at[chunk, slot],
            device_id=peer,
            device_id_type=MESH,
        )
        copy.start()
        started[chunk, slot] = copy

    loads = []
    for chunk, (index, first, width, _) in enumerate(plan):
        columns = pl.ds(first, width)
        held, from_core = buffers[5 * chunk : 5 * chunk + 2]
        grad = ins[index]
        push(chunk, 0, grad.at[:, :, :, 1 - core, :, columns], from_core, device(z, x, y, 1 - core))
        load = pltpu.make_async_copy(grad.at[:, :, :, core, :, columns], held, local.at[chunk])
        load.start()
        loads.append(load)

    for stage, chunk in staggered(len(plan), 4, gap):
        index, first, width, order = plan[chunk]
        x_first, line_last = order[0] == "y", order[-1] == "z"
        held, from_core, from_one, from_two, from_line = buffers[5 * chunk : 5 * chunk + 5]
        to_x, to_y = device(z, 1 - x, y, core), device(z, x, 1 - y, core)
        if stage == 0:
            started[chunk, 0].wait_recv()
            loads[chunk].wait()

            @pl.loop(0, 4 * box[0])
            def _(turn):
                at = (lax.div(turn, 4), lax.rem(lax.div(turn, 2), 2), lax.rem(turn, 2))
                held[at] = add_into(held[at], from_core[at])

            if x_first:
                push(chunk, 1, held.at[:, :, 1 - y], from_one, to_y)
            else:
                push(chunk, 1, held.at[:, 1 - x], from_one, to_x)
        elif stage == 1:
            started[chunk, 1].wait_recv()

            @pl.loop(0, 2 * box[0])
            def _(turn):
                row, i = lax.div(turn, 2), lax.rem(turn, 2)
                at = (row, i, y) if x_first else (row, x, i)
                held[at] = add_into(held[at], from_one[row, i])

            if not line_last:
                for step in range(1, box[0]):
                    peer = line_peer(z, step)
                    rest = held.at[peer, :, y] if x_first else held.at[peer, x]
                    push(chunk, 2 + step, rest, from_line.at[step - 1], device(peer, x, y, core))
            elif x_first:
                push(chunk, 2, held.at[:, 1 - x, y], from_two, to_x)
            else:
                push(chunk, 2, held.at[:, x, 1 - y], from_two, to_y)
        elif stage == 2 and not line_last:
            for step in range(1, box[0]):
                started[chunk, 2 + step].wait_recv()
            for i in range(2):
                at = (z, i, y) if x_first else (z, x, i)
                total = held[at].astype(f32)
                for step in range(1, box[0]):
                    total = total + from_line[step - 1, i].astype(f32)
                held[at] = total.astype(bf16)
            if x_first:
                push(chunk, 2, held.at[z, 1 - x, y], from_two, to_x)
            else:
                push(chunk, 2, held.at[z, x, 1 - y], from_two, to_y)
        elif stage == 2:
            started[chunk, 2].wait_recv()

            @pl.loop(0, box[0])
            def _(row):
                held[row, x, y] = add_into(held[row, x, y], from_two[row])

            for step in range(1, box[0]):
                peer = line_peer(z, step)
                push(chunk, 2 + step, held.at[peer, x, y], from_line.at[step - 1], device(peer, x, y, core))
        else:
            total = held[z, x, y].astype(f32)
            if line_last:
                for step in range(1, box[0]):
                    started[chunk, 2 + step].wait_recv()
                    total = total + from_line[step - 1].astype(f32)
            else:
                started[chunk, 2].wait_recv()
                total = total + from_two[...].astype(f32)
            outs[index][:, pl.ds(first, width)] = total
            if not any(item[0] == index for item in plan[chunk + 1 :]):
                finish(index, outs[index], results)
    for chunk in range(len(plan)):
        for slot in range(6):
            started[chunk, slot].wait_send()


def scatter_blocks(grads, plan, finish, results, gap=2, collective=1):
    views = [g.reshape(box + (g.shape[0] // 32, g.shape[1])) for g in grads]
    scratch = [pltpu.VMEM(v.shape[4:], f32) for v in views]
    for index, _, width, order in plan:
        tile = (views[index].shape[4], width)
        ends_of = ((4,), (3,)) if order[-1] == "z" else ((), (3, 2))
        for lead in ((4, 2, 2), (4, 2, 2), (4, 2)) + ends_of:
            scratch.append(pltpu.VMEM(lead + tile, bf16))
    sent = sum(v.size * v.dtype.itemsize for v in views)
    return pl.pallas_call(
        functools.partial(scatter_kernel, plan, gap, finish, (len(views), len(results))),
        out_shape=list(results),
        in_specs=[pl.BlockSpec(memory_space=pl.ANY)] * len(views),
        out_specs=[pl.BlockSpec(memory_space=pltpu.VMEM)] * len(results),
        scratch_shapes=scratch
        + [
            pltpu.SemaphoreType.DMA((len(plan), 6)),
            pltpu.SemaphoreType.DMA((len(plan), 6)),
            pltpu.SemaphoreType.DMA((len(plan),)),
        ],
        cost_estimate=pl.CostEstimate(flops=0, bytes_accessed=4 * sent, transcendentals=0),
        compiler_params=pltpu.CompilerParams(
            collective_id=collective, has_side_effects=True, vmem_limit_bytes=60 * 1024 * 1024
        ),
    )(*views)


def chunked(widths, pieces, orders):
    plan = []
    for index, (width, number) in enumerate(zip(widths, pieces)):
        tiles = width // lanes
        edges = [tiles * i // number for i in range(number + 1)]
        for i in range(number):
            plan.append((index, edges[i] * lanes, (edges[i + 1] - edges[i]) * lanes, orders[len(plan) % len(orders)]))
    return plan


def carry_kernel(
    reverse, input_ref, decay_ref, carried_ref, ends, outgoing, arrived, joined, final, send, receive
):
    seq_count, step_count, width = input_ref.shape
    count = lax.axis_size("seq")
    part = decay_ref.shape[0] // count
    me, batch = lax.axis_index("seq"), lax.axis_index("batch")
    others = range(1, count)
    barrier = pltpu.get_barrier_semaphore()
    for step in others:
        peer = (lax.rem(me + step, count), batch)
        pl.semaphore_signal(barrier, inc=1, device_id=peer, device_id_type=MESH)

    @pl.loop(0, width // lanes)
    def _(tile):
        columns = pl.ds(pl.multiple_of(tile * lanes, lanes), lanes)
        encode_kernel(reverse, input_ref.at[:, :, columns], decay_ref.at[:, columns], ends)
        for group in range(count):
            rows = slice(group * part, (group + 1) * part)
            mine = jnp.concatenate([ends[seq, rows] for seq in range(seq_count)], axis=0)
            outgoing[group, :, columns] = mine.astype(bf16)

    pl.semaphore_wait(barrier, count - 1)

    def exchange(phase, source, target):
        copies = []
        for step in others:
            peer = lax.rem(me + step, count)
            copy = pltpu.make_async_remote_copy(
                src_ref=source.at[peer],
                dst_ref=target.at[me],
                send_sem=send.at[phase, step - 1],
                recv_sem=receive.at[phase, step - 1],
                device_id=(peer, batch),
                device_id_type=MESH,
            )
            copy.start()
            copies.append(copy)
        target[me] = source[me]
        for copy in copies:
            copy.wait()

    exchange(0, outgoing, arrived)
    rates = decay_ref[pl.ds(pl.multiple_of(me * part, part), part), :]
    power = jnp.exp(-rates * step_count)
    power = jnp.concatenate([power] * seq_count, axis=0)
    state = jnp.zeros(power.shape, f32)
    for block in reversed(range(count)) if reverse else range(count):
        joined[block] = state.astype(bf16)
        state = power * state + arrived[block].astype(f32)
    exchange(1, joined, final)
    for group in range(count):
        rows = slice(group * part, (group + 1) * part)
        found = final[group].astype(f32)
        for seq in range(seq_count):
            carried_ref[seq, rows] = found[seq * part : (seq + 1) * part]


def carried_by_kernel(value, decay, reverse, collective):
    seq_count, _, width = value.shape
    state_count = decay.shape[0]
    count = lax.axis_size("seq")
    parts = pltpu.VMEM((count, seq_count * state_count // count, width), bf16)
    return pl.pallas_call(
        functools.partial(carry_kernel, reverse),
        out_shape=shaped(seq_count, state_count, width),
        in_specs=[pl.BlockSpec(memory_space=pltpu.VMEM)] * 2,
        out_specs=pl.BlockSpec(memory_space=pltpu.VMEM),
        scratch_shapes=[pltpu.VMEM((seq_count, state_count, lanes), f32)]
        + [parts] * 4
        + [pltpu.SemaphoreType.DMA((2, count - 1)), pltpu.SemaphoreType.DMA((2, count - 1))],
        cost_estimate=pl.CostEstimate(flops=0, bytes_accessed=32 * value.size, transcendentals=0),
        compiler_params=pltpu.CompilerParams(collective_id=collective, has_side_effects=True),
    )(value, decay)


hidden_block = 768
gelu_scale = 0.7978845608
gelu_cubic = 0.044715


def feed_kernel(resid_ref, gain_ref, up_ref, down_ref, out_ref, normed_ref, hidden_ref, active_ref):
    @pl.when(pl.program_id(0) == 0)
    def _():
        resid = resid_ref[...]
        normed_ref[...] = layer_norm(resid, gain_ref[...]).astype(bf16)
        out_ref[...] = resid

    hidden = jnp.dot(normed_ref[...], up_ref[...], preferred_element_type=f32)
    hidden_ref[...] = hidden.astype(bf16)
    bend = jnp.tanh(gelu_scale * (hidden + gelu_cubic * hidden * hidden * hidden))
    active = (0.5 * hidden * (1.0 + bend)).astype(bf16)
    active_ref[...] = active
    out_ref[...] += jnp.dot(active, down_ref[...], preferred_element_type=f32)


def feed_forward_blocks(resid, gain, up_packed, up_at, down):
    rows, width = resid.shape
    inner = down.shape[0]
    first = up_at // hidden_block
    whole = pl.BlockSpec((rows, width), lambda j: (0, 0))
    part = pl.BlockSpec((rows, hidden_block), lambda j: (0, j))
    out, normed, hidden, active = pl.pallas_call(
        feed_kernel,
        grid=(inner // hidden_block,),
        in_specs=[
            whole,
            pl.BlockSpec((1, width), lambda j: (0, 0)),
            pl.BlockSpec((width, hidden_block), lambda j: (0, first + j)),
            pl.BlockSpec((hidden_block, width), lambda j: (j, 0)),
        ],
        out_specs=[whole, whole, part, part],
        out_shape=[
            shaped(rows, width),
            shaped(rows, width, dtype=bf16),
            shaped(rows, inner, dtype=bf16),
            shaped(rows, inner, dtype=bf16),
        ],
        cost_estimate=pl.CostEstimate(
            flops=4 * rows * width * inner, bytes_accessed=10 * width * inner, transcendentals=rows * inner
        ),
        compiler_params=pltpu.CompilerParams(vmem_limit_bytes=40 * 1024 * 1024),
    )(resid, gain[None], up_packed, down)
    return out, (resid, gain, normed, hidden, active)


def feed_back_kernel(
    packed,
    upstream_ref,
    resid_ref,
    gain_ref,
    normed_ref,
    hidden_ref,
    active_ref,
    up_ref,
    down_ref,
    out_ref,
    gain_grad_ref,
    *rest,
):
    step = pl.program_id(0)
    last = pl.num_programs(0) - 1
    across = (((1,), (1,)), ((), ()))
    along = (((0,), (0,)), ((), ()))
    upstream_low = upstream_ref[...].astype(bf16)
    into_active = lax.dot_general(upstream_low, down_ref[...], across, preferred_element_type=f32)
    hidden = hidden_ref[...].astype(f32)
    square = hidden * hidden
    bend = jnp.tanh(gelu_scale * hidden * (1.0 + gelu_cubic * square))
    slope = 0.5 * (1.0 + bend) + 0.5 * hidden * (1.0 - bend * bend) * (
        gelu_scale * (1.0 + 3.0 * gelu_cubic * square)
    )
    into_hidden = (into_active * slope).astype(bf16)
    part = lax.dot_general(into_hidden, up_ref[...], across, preferred_element_type=f32)

    @pl.when(step == 0)
    def _():
        out_ref[...] = part

    @pl.when(step > 0)
    def _():
        out_ref[...] += part

    up_grad = lax.dot_general(normed_ref[...], into_hidden, along, preferred_element_type=f32)
    down_grad = lax.dot_general(active_ref[...], upstream_low, along, preferred_element_type=f32)
    if packed:
        grads_ref, up_held, down_held, sems = rest
        share, fold = packed
        width = up_grad.shape[0]
        inner = hidden_block * grads_ref.shape[1] // (2 * hidden_block)
        tall = hidden_block // fold
        slot = lax.rem(step, 2)

        def copies(at, slot):
            columns = pl.ds(pl.multiple_of(at * hidden_block, hidden_block), hidden_block)
            rows = pl.ds(pl.multiple_of(at * tall, tall), tall)
            return (
                pltpu.make_async_copy(up_held.at[slot], grads_ref.at[:, columns], sems.at[0, slot]),
                pltpu.make_async_copy(down_held.at[slot], grads_ref.at[rows, inner:], sems.at[1, slot]),
            )

        @pl.when(step >= 2)
        def _():
            for copy in copies(step - 2, slot):
                copy.wait()

        up_held[slot] = up_grad.astype(bf16)
        for place in range(fold):
            starts = range(place * share, hidden_block, fold * share)
            piece = jnp.concatenate([down_grad[a : a + share] for a in starts], axis=0)
            down_held[slot, :, place * width : (place + 1) * width] = piece.astype(bf16)
        for copy in copies(step, slot):
            copy.start()

        @pl.when(step == last)
        def _():
            for copy in copies(step - 1, 1 - slot) + copies(step, slot):
                copy.wait()
    else:
        up_grad_ref, down_grad_ref = rest
        up_grad_ref[...] = up_grad.astype(bf16)
        down_grad_ref[...] = down_grad.astype(bf16)

    @pl.when(step == last)
    def _():
        into_normed = out_ref[...]
        resid = resid_ref[...]
        centred = resid - jnp.mean(resid, axis=-1, keepdims=True)
        inverse = lax.rsqrt(jnp.mean(centred * centred, axis=-1, keepdims=True) + eps)
        unit = centred * inverse
        gain_grad_ref[...] = jnp.sum(into_normed * unit, axis=0, keepdims=True)
        scaled = into_normed * gain_ref[...]
        along_unit = jnp.mean(scaled * unit, axis=-1, keepdims=True)
        into_resid = inverse * (scaled - jnp.mean(scaled, axis=-1, keepdims=True) - unit * along_unit)
        out_ref[...] = upstream_ref[...] + into_resid


def feed_back_blocks(stored, up_packed, up_at, down, upstream, packed=()):
    resid, gain, normed, hidden, active = stored
    rows, width = resid.shape
    inner = down.shape[0]
    first = up_at // hidden_block
    whole = pl.BlockSpec((rows, width), lambda j: (0, 0))
    part = pl.BlockSpec((rows, hidden_block), lambda j: (0, j))
    line = pl.BlockSpec((1, width), lambda j: (0, 0))
    up_spec = pl.BlockSpec((width, hidden_block), lambda j: (0, j))
    down_spec = pl.BlockSpec((hidden_block, width), lambda j: (j, 0))
    scratch = []
    if packed:
        grad_specs = [pl.BlockSpec(memory_space=pl.ANY)]
        grad_shapes = [shaped(width, 2 * inner, dtype=bf16)]
        scratch = [
            pltpu.VMEM((2, width, hidden_block), bf16),
            pltpu.VMEM((2, hidden_block // packed[1], inner), bf16),
            pltpu.SemaphoreType.DMA((2, 2)),
        ]
    else:
        grad_specs = [up_spec, down_spec]
        grad_shapes = [shaped(width, inner, dtype=bf16), shaped(inner, width, dtype=bf16)]
    out, gain_grad, *grads = pl.pallas_call(
        functools.partial(feed_back_kernel, packed),
        grid=(inner // hidden_block,),
        in_specs=[
            whole,
            whole,
            line,
            whole,
            part,
            part,
            pl.BlockSpec((width, hidden_block), lambda j: (0, first + j)),
            down_spec,
        ],
        out_specs=[whole, line] + grad_specs,
        out_shape=[shaped(rows, width), shaped(1, width)] + grad_shapes,
        scratch_shapes=scratch,
        cost_estimate=pl.CostEstimate(
            flops=8 * rows * width * inner, bytes_accessed=16 * width * inner, transcendentals=rows * inner
        ),
        compiler_params=pltpu.CompilerParams(vmem_limit_bytes=48 * 1024 * 1024),
    )(upstream, resid, gain[None], normed, hidden, active, up_packed, down)
    return (out, gain_grad[0], *grads)


def split_heads(ref, scratch, heads, parts, first=0):
    for part in range(parts):
        for head in range(heads):
            start = (part * heads + head) * HEAD_DIM + first
            scratch[part * heads + head] = ref[:, start : start + HEAD_DIM]


def score_block(query, keys, first, scale):
    scores = (
        lax.dot_general(query, keys, (((1,), (1,)), ((), ())), preferred_element_type=f32) * scale
    )
    rows = lax.broadcasted_iota(jnp.int32, scores.shape, 0) + first
    columns = lax.broadcasted_iota(jnp.int32, scores.shape, 1)
    return jnp.where(columns <= rows, scores, masked_score)


def attend_kernel(heads, block, scale, qkv_ref, low_ref, full_ref, stat_ref, parts, outs):
    length = qkv_ref.shape[0]
    split_heads(qkv_ref, parts, heads, 3)

    @pl.loop(0, heads)
    def _(head):
        for first in range(0, length, block):
            extent = first + block
            query = parts[head, first:extent, :]
            scores = score_block(query, parts[heads + head, :extent, :], first, scale)
            top = jnp.max(scores, axis=1, keepdims=True)
            soft = jnp.exp(scores - top)
            whole = jnp.sum(soft, axis=1, keepdims=True)
            soft = soft * (1.0 / whole)
            outs[head, first:extent, :] = jnp.dot(
                soft.astype(bf16), parts[2 * heads + head, :extent, :], preferred_element_type=f32
            )
            stat_ref[head, first:extent, :] = jnp.broadcast_to(top + jnp.log(whole), (block, lanes))

    if low_ref.shape[1] > heads * HEAD_DIM:
        low_ref[:, heads * HEAD_DIM :] = jnp.zeros((length, low_ref.shape[1] - heads * HEAD_DIM), bf16)
    for head in range(heads):
        place = slice(head * HEAD_DIM, (head + 1) * HEAD_DIM)
        full_ref[:, place] = outs[head]
        low_ref[:, place] = outs[head].astype(bf16)


def attend_back_kernel(
    heads, block, scale, qkv_ref, dout_ref, full_ref, stat_ref, grad_ref, parts, douts, fulls, grads
):
    length = qkv_ref.shape[0]
    split_heads(qkv_ref, parts, heads, 3)
    split_heads(dout_ref, douts, heads, 1)
    split_heads(full_ref, fulls, heads, 1)
    grads[...] = jnp.zeros_like(grads)

    @pl.loop(0, heads)
    def _(head):
        for first in range(0, length, block):
            extent = first + block
            query = parts[head, first:extent, :]
            keys = parts[heads + head, :extent, :]
            value = parts[2 * heads + head, :extent, :]
            dout = douts[head, first:extent, :]
            delta = jnp.sum(dout.astype(f32) * fulls[head, first:extent, :], axis=1, keepdims=True)
            scores = score_block(query, keys, first, scale)
            soft = jnp.exp(scores - stat_ref[head, first:extent, :1])
            across = (((1,), (1,)), ((), ()))
            along = (((0,), (0,)), ((), ()))
            dprob = lax.dot_general(dout, value, across, preferred_element_type=f32)
            dscore = (soft * (dprob - delta) * scale).astype(bf16)
            grads[head, first:extent, :] = jnp.dot(dscore, keys, preferred_element_type=f32)
            grads[heads + head, :extent, :] += lax.dot_general(
                dscore, query, along, preferred_element_type=f32
            )
            grads[2 * heads + head, :extent, :] += lax.dot_general(
                soft.astype(bf16), dout, along, preferred_element_type=f32
            )

    grad_ref[...] = jnp.zeros_like(grad_ref)
    for part in range(3 * heads):
        grad_ref[:, part * HEAD_DIM : (part + 1) * HEAD_DIM] = grads[part].astype(bf16)


def attend_params():
    return pltpu.CompilerParams(vmem_limit_bytes=56 * 1024 * 1024)


def attend_whole(qkv, heads, block):
    length = qkv.shape[0]
    width = heads * HEAD_DIM
    return pl.pallas_call(
        functools.partial(attend_kernel, heads, block, HEAD_DIM ** (-0.5)),
        out_shape=[
            shaped(length, -(-width // lanes) * lanes, dtype=bf16),
            shaped(length, width),
            shaped(heads, length, lanes),
        ],
        scratch_shapes=[
            pltpu.VMEM((3 * heads, length, HEAD_DIM), bf16),
            pltpu.VMEM((heads, length, HEAD_DIM), f32),
        ],
        compiler_params=attend_params(),
    )(qkv)


def attend_whole_back(qkv, dout, full, stat, heads, block):
    length = qkv.shape[0]
    return pl.pallas_call(
        functools.partial(attend_back_kernel, heads, block, HEAD_DIM ** (-0.5)),
        out_shape=shaped(*qkv.shape, dtype=bf16),
        scratch_shapes=[
            pltpu.VMEM((3 * heads, length, HEAD_DIM), bf16),
            pltpu.VMEM((heads, length, HEAD_DIM), bf16),
            pltpu.VMEM((heads, length, HEAD_DIM), f32),
            pltpu.VMEM((3 * heads, length, HEAD_DIM), f32),
        ],
        compiler_params=attend_params(),
    )(qkv, dout, full, stat)


def split_blocks(array, block_len):
    shaped_blocks = array.reshape(
        (array.shape[0], array.shape[1] // block_len, block_len) + array.shape[2:]
    )
    return jnp.moveaxis(shaped_blocks, 1, 0)


def general_attention(proj_low, seq_count, block_len, places, any_live, longest):
    model_width = HEADS * HEAD_DIM
    scale = HEAD_DIM ** (-0.5)
    offsets = jnp.arange(block_len, dtype=jnp.int32)
    head_shape = (seq_count, block_len, HEADS, HEAD_DIM)
    query_low = proj_low[:, :model_width].reshape(head_shape)
    keys_low = proj_low[:, model_width : 2 * model_width].reshape(head_shape)
    value_low = proj_low[:, 2 * model_width :].reshape(head_shape)

    def block_scores(queries, keys_block, query_places, key_places):
        scores = (
            jnp.einsum("sqhe,skhe->sqhk", queries, keys_block, preferred_element_type=jnp.float32)
            * scale
        )
        causal_mask = key_places[None, :] <= query_places[:, None]
        return jnp.where(causal_mask[None, :, None, :], scores, masked_score)

    def key_needed(key_first):
        return (key_first <= places[-1]) & ((key_first == places[0]) | any_live)

    stat_shape = (seq_count, block_len, HEADS)
    start_state = (
        jnp.full(stat_shape, masked_score, jnp.float32),
        jnp.zeros(stat_shape, jnp.float32),
        jnp.zeros(head_shape, jnp.float32),
    )
    shard_piece = (
        lax.all_gather(keys_low, "seq", axis=1, tiled=True),
        lax.all_gather(value_low, "seq", axis=1, tiled=True),
    )
    keys_blocks = split_blocks(shard_piece[0], block_len)
    value_blocks = split_blocks(shard_piece[1], block_len)
    firsts = jnp.arange(keys_blocks.shape[0], dtype=jnp.int32) * block_len

    def attend_one_step(state_now, operand):
        keys_block, value_block, key_first = operand

        def attend_work(state_in_block):
            running_max, running_sum, running_out = state_in_block
            scores = block_scores(query_low, keys_block, places, key_first + offsets)
            new_max = jnp.maximum(running_max, jnp.max(scores, axis=-1))
            fade = jnp.exp(running_max - new_max)
            shifted = jnp.exp(scores - new_max[..., None])
            new_sum = running_sum * fade + jnp.sum(shifted, axis=-1)
            new_out = running_out * fade[..., None] + jnp.einsum(
                "sqhk,skhe->sqhe",
                shifted.astype(jnp.bfloat16),
                value_block,
                preferred_element_type=jnp.float32,
            )
            return (new_max, new_sum, new_out)

        return (
            lax.cond(
                key_needed(key_first), attend_work, lambda state_in_block: state_in_block, state_now
            ),
            None,
        )

    result, _ = lax.scan(attend_one_step, start_state, (keys_blocks, value_blocks, firsts))
    running_max, running_sum, running_out = result
    attended = running_out / running_sum[..., None]
    logsum = running_max + jnp.log(running_sum)
    def backward(dout_low):
        delta = jnp.sum(dout_low.astype(jnp.float32) * attended, axis=-1)
        shard_piece = (
            lax.all_gather(keys_low, "seq", axis=1, tiled=True),
            lax.all_gather(value_low, "seq", axis=1, tiled=True),
        )
        keys_blocks = split_blocks(shard_piece[0], block_len)
        value_blocks = split_blocks(shard_piece[1], block_len)
        firsts = jnp.arange(keys_blocks.shape[0], dtype=jnp.int32) * block_len

        def query_one_step(query_grad, operand):
            keys_block, value_block, key_first = operand

            def query_work(grad_now):
                scores = block_scores(query_low, keys_block, places, key_first + offsets)
                soft = jnp.exp(scores - logsum[..., None])
                dprob = jnp.einsum(
                    "sqhe,skhe->sqhk", dout_low, value_block, preferred_element_type=jnp.float32
                )
                dscore = (soft * (dprob - delta[..., None])).astype(jnp.bfloat16)
                return (
                    grad_now
                    + jnp.einsum(
                        "sqhk,skhe->sqhe", dscore, keys_block, preferred_element_type=jnp.float32
                    )
                    * scale
                )

            return (
                lax.cond(key_needed(key_first), query_work, lambda grad_now: grad_now, query_grad),
                None,
            )

        result, _ = lax.scan(
            query_one_step, jnp.zeros(head_shape, jnp.float32), (keys_blocks, value_blocks, firsts)
        )
        query_grad = result
        sent = (query_low.astype(jnp.float32), dout_low.astype(jnp.float32), logsum, delta)
        shard_piece = (
            lax.all_gather(sent[0].astype(jnp.bfloat16), "seq", axis=1, tiled=True).astype(jnp.float32),
            lax.all_gather(sent[1].astype(jnp.bfloat16), "seq", axis=1, tiled=True).astype(jnp.float32),
            lax.all_gather(sent[2].astype(jnp.bfloat16), "seq", axis=1, tiled=True).astype(jnp.float32),
            lax.all_gather(sent[3].astype(jnp.bfloat16), "seq", axis=1, tiled=True).astype(jnp.float32),
        )
        query_blocks = split_blocks(shard_piece[0], block_len)
        dout_blocks = split_blocks(shard_piece[1], block_len)
        logsum_blocks = split_blocks(shard_piece[2], block_len)
        delta_blocks = split_blocks(shard_piece[3], block_len)
        firsts = jnp.arange(query_blocks.shape[0], dtype=jnp.int32) * block_len

        def key_one_step(grads_now, operand):
            query_block, dout_block, logsum_block, delta_block, query_first = operand

            def key_work(grads_in):
                keys_grad, value_grad = grads_in
                query_cast = query_block.astype(jnp.bfloat16)
                dout_cast = dout_block.astype(jnp.bfloat16)
                scores = block_scores(query_cast, keys_low, query_first + offsets, places)
                soft = jnp.exp(scores - logsum_block[..., None])
                value_grad = value_grad + jnp.einsum(
                    "sqhk,sqhe->skhe",
                    soft.astype(jnp.bfloat16),
                    dout_cast,
                    preferred_element_type=jnp.float32,
                )
                dprob = jnp.einsum(
                    "sqhe,skhe->sqhk", dout_cast, value_low, preferred_element_type=jnp.float32
                )
                dscore = (soft * (dprob - delta_block[..., None])).astype(jnp.bfloat16)
                keys_grad = (
                    keys_grad
                    + jnp.einsum(
                        "sqhk,sqhe->skhe", dscore, query_cast, preferred_element_type=jnp.float32
                    )
                    * scale
                )
                return (keys_grad, value_grad)

            needed = (query_first + block_len - 1 >= places[0]) & (
                (query_first == places[0]) | (query_first < longest)
            )
            return (lax.cond(needed, key_work, lambda grads_in: grads_in, grads_now), None)

        result, _ = lax.scan(
            key_one_step,
            (jnp.zeros(head_shape, jnp.float32), jnp.zeros(head_shape, jnp.float32)),
            (query_blocks, dout_blocks, logsum_blocks, delta_blocks, firsts),
        )
        keys_grad, value_grad = result
        return (query_grad, keys_grad, value_grad)

    return attended, backward


def layer_norm(value, gain):
    centred = value - jnp.mean(value, axis=-1, keepdims=True)
    spread_of = jnp.mean(centred * centred, axis=-1, keepdims=True)
    return centred * lax.rsqrt(spread_of + eps) * gain


def gelu_tanh(value):
    return jax.nn.gelu(value, approximate=True)


def dense(left, weight):
    return jnp.dot(left, weight, preferred_element_type=f32)


def dense_back(left, weight, upstream):
    into_left = lax.dot_general(
        upstream, weight, (((1,), (1,)), ((), ())), preferred_element_type=f32
    )
    into_weight = lax.dot_general(
        left, upstream, (((0,), (0,)), ((), ())), preferred_element_type=f32
    ).astype(bf16)
    return (into_left, into_weight)


def shift_mix(extended, taps, value_part):
    step_count = value_part.shape[1]
    reach = taps.shape[1]
    shifted = extended[:, reach - 1 : reach - 1 + step_count] * taps[:, 0]
    for tap_index in range(1, reach):
        shifted = (
            shifted
            + extended[:, reach - 1 - tap_index : reach - 1 - tap_index + step_count]
            * taps[:, tap_index]
        )
    return shifted * value_part


def feed_forward(resid, gain, up_weight, down_weight):
    normed, norm_back = jax.vjp(layer_norm, resid, gain)
    normed_low = normed.astype(bf16)
    hidden = dense(normed_low, up_weight)
    active, active_back = jax.vjp(gelu_tanh, hidden)
    active_low = active.astype(bf16)
    return (
        resid + dense(active_low, down_weight),
        (norm_back, normed_low, active_back, active_low),
    )


def feed_back(stored, up_weight, down_weight, upstream):
    norm_back, normed_low, active_back, active_low = stored
    into_active, down_grad = dense_back(active_low, down_weight, upstream.astype(bf16))
    (into_hidden,) = active_back(into_active)
    into_normed, up_grad = dense_back(normed_low, up_weight, into_hidden.astype(bf16))
    into_resid, gain_grad = norm_back(into_normed)
    return (upstream + into_resid, gain_grad, up_grad, down_grad)


def fold_rows(weight, share):
    rows, width = weight.shape
    fold = rows // share
    return weight.reshape(fold, share, width).transpose(1, 0, 2).reshape(share, fold * width)


def unfold_rows(folded, fold, share):
    rows, width = folded.shape
    width //= fold
    parts = folded.reshape(rows // share, share, fold, width).transpose(0, 2, 1, 3)
    return parts.reshape(rows * fold, width)


def fold_all(weight, share, rows):
    tall, width = weight.shape
    fold = tall // rows
    parts = weight.reshape(rows // share, fold, share, width).transpose(0, 2, 1, 3)
    return parts.reshape(rows, fold * width)


def group_columns(weight, groups, padded):
    rows, columns = weight.shape
    part = columns // 3 // groups
    grouped = weight.reshape(rows, 3, groups, part).transpose(0, 2, 1, 3).reshape(rows, groups, 3 * part)
    return jnp.pad(grouped, ((0, 0), (0, 0), (0, padded - 3 * part))).reshape(rows, groups * padded)


def pad_groups(weight, groups, padded):
    rows, columns = weight.shape
    part = rows // groups
    grouped = weight.reshape(groups, part, columns)
    return jnp.pad(grouped, ((0, 0), (0, padded - part), (0, 0))).reshape(groups * padded, columns)


def ungroup_columns(grouped, groups, padded, columns):
    rows = grouped.shape[0]
    part = columns // 3 // groups
    parts = grouped.reshape(rows, groups, padded)[:, :, : 3 * part].reshape(rows, groups, 3, part)
    return parts.transpose(0, 2, 1, 3).reshape(rows, columns)


def cut(array, widths):
    pieces, start = [], 0
    for width in widths:
        pieces.append(array[:, start : start + width])
        start += width
    return pieces


def cut_last(array, count):
    width = array.shape[-1] // count
    return [array[..., i * width : (i + 1) * width] for i in range(count)]


def gathered(parts):
    whole = lax.all_gather(jnp.concatenate(parts, axis=1), everyone, axis=0, tiled=True)
    return cut(whole, [p.shape[1] for p in parts])


def scattered(parts):
    mine = lax.psum_scatter(
        jnp.concatenate(parts, axis=1), everyone, scatter_dimension=0, tiled=True
    )
    return cut(mine, [p.shape[1] for p in parts])


def body(
    tokens,
    cotangent,
    lengths,
    mixer_gain,
    mixer_inputs,
    shift_taps,
    decay_rate,
    state_in,
    state_out,
    state_skip,
    mixer_output,
    first_gain,
    first_up,
    first_down,
    attend_gain,
    attend_inputs,
    attend_output,
    second_gain,
    second_up,
    second_down,
):
    seq_count, block_len, model_width = tokens.shape
    row_count = seq_count * block_len
    seq_devices = lax.axis_size("seq")
    share = mixer_inputs.shape[0]
    states, reach = decay_rate.shape[1], shift_taps.shape[1]
    fold = first_down.shape[0] // share
    deals = seq_count * HEADS
    dealt = deals % seq_devices == 0 and HEADS % (deals // seq_devices) == 0
    heads = deals // seq_devices if dealt else HEADS
    groups = HEADS // heads
    group_width = heads * HEAD_DIM
    padded = -(-3 * group_width // lanes) * lanes if dealt else 3 * group_width
    out_width = -(-group_width // lanes) * lanes if dealt else group_width

    columns = [decay_rate, state_in, state_out, shift_taps]
    columns += [g[:, None] for g in (mixer_gain, first_gain, attend_gain, second_gain, state_skip)]
    small = jnp.concatenate(columns, axis=1)
    small_count = small.shape[1]
    small_width = -(-small_count // lanes) * lanes
    small = jnp.pad(small, ((0, 0), (0, small_width - small_count)))
    attend_cols = attend_inputs.shape[1]
    grouped = group_columns(attend_inputs, groups, padded)
    by_kernel = seq_devices == 8 and lax.axis_size("batch") == 4
    packed = [mixer_output, attend_output, first_up, second_up, grouped]
    up1_at = 2 * model_width
    up2_at = up1_at + first_up.shape[1]
    if by_kernel:
        joint = jnp.concatenate([mixer_inputs, small], axis=1)
        w_packed = lax.all_gather(jnp.concatenate(packed, axis=1), everyone, axis=0, tiled=True)
        w_mixer_out, w_attend_out, _, _, w_attend_in = cut(w_packed, [p.shape[1] for p in packed])
        widths = (joint.shape[1], model_width)
        w_joint, w_down1 = gather_blocks((joint, first_down), chunked(widths, (4, 6), ("zxy", "zyx")), gap=3)
        w_mixer_in, w_small = cut(w_joint, [mixer_inputs.shape[1], small_width])
        second_down, w_small = lax.optimization_barrier((second_down, w_small))
        w_down2 = lax.all_gather(second_down, everyone, axis=0, tiled=True)
    else:
        w_mixer_in, w_small = gathered([mixer_inputs, small])
        packed += [fold_rows(first_down, share), fold_rows(second_down, share)]
        w_mixer_out, w_attend_out, w_up1, w_up2, w_attend_in, w_down1, w_down2 = gathered(packed)
        w_down1 = unfold_rows(w_down1, fold, share)
        w_down2 = unfold_rows(w_down2, fold, share)

    rows = w_small.T.astype(f32)
    decay, table_in, table_out = rows[:states], rows[states : 2 * states], rows[2 * states : 3 * states]
    taps_rows = rows[3 * states : 3 * states + reach]
    gain_mixer, gain_first, gain_attend, gain_second, skip = (
        rows[3 * states + reach + i] for i in range(5)
    )
    taps = taps_rows.T
    weight = table_in * table_out

    rank_seq = lax.axis_index("seq")
    offsets = jnp.arange(block_len, dtype=jnp.int32)
    places = rank_seq * block_len + offsets
    valid = (places[None, :] < lengths[:, None]).astype(f32)
    longest = jnp.max(lengths)
    any_live = places[0] < longest

    start_resid = tokens.reshape(row_count, model_width).astype(f32)
    normed_mixer, back_mixer = jax.vjp(layer_norm, start_resid, gain_mixer)
    normed_low_mixer = normed_mixer.astype(bf16)
    projected = dense(normed_low_mixer, w_mixer_in).reshape(seq_count, block_len, 3 * model_width)
    query_mixer = projected[:, :, :model_width]
    keys_mixer = projected[:, :, model_width : 2 * model_width]
    value_mixer = projected[:, :, 2 * model_width :]
    rim_rows = passed_along(keys_mixer[:, block_len - reach + 1 :], "seq", 1)
    extended = jnp.concatenate([rim_rows, keys_mixer], axis=1)
    inner, shift_back = jax.vjp(shift_mix, extended, taps, value_mixer)
    if by_kernel:
        carried = carried_by_kernel(inner, decay, False, 2)
    else:
        carried = carried_in(encode(inner, decay, False), decay, block_len, False)
    wide = shaped(seq_count, block_len, model_width)
    state_y, gated = per_lane_tile(
        output_kernel,
        (inner, query_mixer, carried, decay, weight, skip[None]),
        (wide, wide),
    )
    gated_low = gated.astype(bf16).reshape(row_count, model_width)
    resid_mixer = start_resid + dense(gated_low, w_mixer_out)
    if by_kernel:
        resid_first, stored_first = feed_forward_blocks(
            resid_mixer, gain_first, w_packed, up1_at, w_down1
        )
    else:
        resid_first, stored_first = feed_forward(resid_mixer, gain_first, w_up1, w_down1)

    normed_attend, back_attend = jax.vjp(layer_norm, resid_first, gain_attend)
    normed_low_attend = normed_attend.astype(bf16)
    proj_low = dense(normed_low_attend, w_attend_in).astype(bf16)
    if dealt:
        length = seq_devices * block_len
        block = min(256, length)

        def deal(array, width):
            array = array.reshape(seq_count, block_len, groups * width)
            parts = jnp.stack(cut_last(array, groups), axis=1)
            parts = parts.reshape(seq_count * groups, block_len, width)
            dealt_parts = lax.all_to_all(parts, "seq", split_axis=0, concat_axis=0, tiled=True)
            return dealt_parts.reshape(length, width)

        def collect(array, width):
            parts = array.reshape(seq_devices, block_len, width)
            back = lax.all_to_all(parts, "seq", split_axis=0, concat_axis=0, tiled=True)
            back = back.reshape(seq_count, groups, block_len, width)
            back = jnp.concatenate([back[:, group] for group in range(groups)], axis=-1)
            return back.reshape(row_count, groups * width)

        qkv = deal(proj_low, padded)
        attended_part, attended_full, stat = attend_whole(qkv, heads, block)
        attended_low = collect(attended_part, out_width)
        w_attend_out = pad_groups(w_attend_out, groups, out_width)
    else:
        attended, attended_back = general_attention(
            proj_low, seq_count, block_len, places, any_live, longest
        )
        attended_low = attended.reshape(row_count, model_width).astype(bf16)
    resid_attend = resid_first + dense(attended_low, w_attend_out)
    if by_kernel:
        final, stored_second = feed_forward_blocks(
            resid_attend, gain_second, w_packed, up2_at, w_down2
        )
    else:
        final, stored_second = feed_forward(resid_attend, gain_second, w_up2, w_down2)
    mixed = (final.reshape(seq_count, block_len, model_width) * valid[..., None]).astype(bf16)

    upstream = (cotangent.astype(f32) * valid[..., None]).reshape(row_count, model_width)
    if by_kernel:
        upstream, second_gain_grad, early = feed_back_blocks(
            stored_second, w_packed, up2_at, w_down2, upstream, packed=(share, fold)
        )
    else:
        upstream, second_gain_grad, second_up_grad, second_down_grad = feed_back(
            stored_second, w_up2, w_down2, upstream
        )
        early = [second_up_grad, fold_all(second_down_grad, share, model_width)]
        early = jnp.concatenate(early, axis=1)
    into_attended, attend_output_grad = dense_back(
        attended_low, w_attend_out, upstream.astype(bf16)
    )
    if dealt:
        attend_output_grad = attend_output_grad.reshape(groups, out_width, model_width)
        attend_output_grad = attend_output_grad[:, :group_width].reshape(model_width, model_width)
    dout_low = into_attended.astype(bf16)
    if dealt:
        dout = deal(dout_low, out_width)
        qkv_grad = attend_whole_back(qkv, dout, attended_full, stat, heads, block)
        qkv_grad, early = lax.optimization_barrier((qkv_grad, early))
        proj_grad = collect(qkv_grad, padded)
    else:
        parts = attended_back(dout_low.reshape(seq_count, block_len, HEADS, HEAD_DIM))
        proj_grad = jnp.concatenate(
            [p.reshape(row_count, model_width) for p in parts], axis=1
        ).astype(bf16)
    early = lax.psum_scatter(early, everyone, scatter_dimension=0, tiled=True)
    second_up_out, second_down_out = cut(early, [second_up.shape[1], fold * model_width])
    into_normed, attend_inputs_grad = dense_back(normed_low_attend, w_attend_in, proj_grad)
    into_resid, attend_gain_grad = back_attend(into_normed)
    upstream = upstream + into_resid
    if by_kernel:
        upstream, first_gain_grad, first_up_grad, first_down_grad = feed_back_blocks(
            stored_first, w_packed, up1_at, w_down1, upstream
        )
    else:
        upstream, first_gain_grad, first_up_grad, first_down_grad = feed_back(
            stored_first, w_up1, w_down1, upstream
        )
    into_gated, mixer_output_grad = dense_back(gated_low, w_mixer_out, upstream.astype(bf16))
    into_gated = into_gated.reshape(seq_count, block_len, model_width)
    query_mixer_grad = into_gated * state_y
    state_grad = into_gated * query_mixer
    if by_kernel:
        later = carried_by_kernel(state_grad, decay, True, 3)
    else:
        later = carried_in(encode(state_grad, decay, True), decay, block_len, True)
    table = shaped(states, model_width)
    inner_grad, weight_grad, power_grad, skip_grad = per_lane_tile(
        back_kernel,
        (inner, state_grad, carried, later, decay, weight, skip[None]),
        (wide, table, table, shaped(1, model_width)),
        scratch=[pltpu.VMEM((block_len, seq_count, states, lanes), f32)],
    )
    extended_grad, taps_grad, value_mixer_grad = shift_back(inner_grad)
    spill = passed_along(extended_grad[:, : reach - 1], "seq", -1)
    keys_mixer_grad = extended_grad[:, reach - 1 :] + jnp.pad(
        spill, ((0, 0), (block_len - reach + 1, 0), (0, 0))
    )
    proj_grad_mixer = (
        jnp.concatenate([query_mixer_grad, keys_mixer_grad, value_mixer_grad], axis=2)
        .astype(bf16)
        .reshape(row_count, 3 * model_width)
    )
    into_normed_mixer, mixer_inputs_grad = dense_back(normed_low_mixer, w_mixer_in, proj_grad_mixer)
    into_start, mixer_gain_grad = back_mixer(into_normed_mixer)
    tokens_gradient = (upstream + into_start).reshape(seq_count, block_len, model_width).astype(bf16)

    small_rows = jnp.concatenate(
        [-jnp.exp(-decay) * power_grad, weight_grad * table_out, weight_grad * table_in, taps_grad.T]
        + [
            g[None]
            for g in (mixer_gain_grad, first_gain_grad, attend_gain_grad, second_gain_grad, skip_grad[0])
        ],
        axis=0,
    )
    small_grad = jnp.pad(small_rows, ((0, small_width - small_count), (0, 0))).T.astype(bf16)
    def unfolded(folded):
        return folded.reshape(share, fold, model_width).transpose(1, 0, 2).reshape(share * fold, model_width)

    gains_at = 3 * states + reach
    table_edges = [0, states, 2 * states, 3 * states, gains_at, small_width]

    def tables_of(block):
        return [block[:, a:b] for a, b in zip(table_edges, table_edges[1:])]

    last = [attend_inputs_grad, first_up_grad, mixer_output_grad, mixer_inputs_grad, small_grad]
    if by_kernel:
        last += [first_down_grad, attend_output_grad]
        orders = ("yxz", "xyz", "xzy", "yxz", "xyz", "yzx")
        plan = chunked([g.shape[1] for g in last], (4, 4, 2, 4, 2, 4, 2), orders)
        part = attend_cols // 3 // groups

        def finish(index, block, results):
            if index == 0:
                for group in range(groups):
                    for kind in range(3):
                        start = (kind * groups + group) * part
                        source = group * padded + kind * part
                        results[0][:, start : start + part] = block[:, source : source + part]
            elif index == 4:
                for place, table in enumerate(tables_of(block)):
                    results[5 + place][...] = table
            else:
                results[{1: 1, 2: 2, 3: 3, 5: 4, 6: 10}[index]][...] = block[...]

        widths = [attend_cols] + [g.shape[1] for g in last[1:4]]
        results = [shaped(share, w) for w in widths] + [shaped(share * fold, model_width)]
        results += [shaped(share, b - a) for a, b in zip(table_edges, table_edges[1:])]
        results.append(shaped(share, model_width))
        attend_inputs_out, first_up_out, mixer_output_out, mixer_inputs_out, first_down_out, *tables = (
            scatter_blocks(last, plan, finish, results, gap=4)
        )
        *tables, attend_output_out = tables
    else:
        last += [fold_all(first_down_grad, share, model_width), attend_output_grad]
        *last, folded, attend_output_out = scattered(last)
        first_down_out = unfolded(folded).astype(f32)
        grouped, first_up_out, mixer_output_out, mixer_inputs_out, small_out = (
            g.astype(f32) for g in last
        )
        attend_inputs_out = ungroup_columns(grouped, groups, padded, attend_cols)
        tables = tables_of(small_out)
    decay_out, in_out, out_out, taps_out, vectors = tables

    return (
        mixed,
        tokens_gradient,
        vectors[:, 0],
        mixer_inputs_out,
        taps_out,
        decay_out,
        in_out,
        out_out,
        vectors[:, 4],
        mixer_output_out,
        vectors[:, 1],
        first_up_out,
        first_down_out,
        vectors[:, 2],
        attend_inputs_out,
        attend_output_out.astype(f32),
        vectors[:, 3],
        second_up_out.astype(f32),
        unfolded(second_down_out).astype(f32),
    )


def solution(mesh):
    return jax.shard_map(
        body,
        mesh=mesh,
        in_specs=(
            P("batch", "seq", None),
            P("batch", "seq", None),
            P("batch"),
            P(("seq", "batch")),
            P(("seq", "batch"), None),
            P(("seq", "batch"), None),
            P(("seq", "batch"), None),
            P(("seq", "batch"), None),
            P(("seq", "batch"), None),
            P(("seq", "batch")),
            P(("seq", "batch"), None),
            P(("seq", "batch")),
            P(("seq", "batch"), None),
            P(("seq", "batch"), None),
            P(("seq", "batch")),
            P(("seq", "batch"), None),
            P(("seq", "batch"), None),
            P(("seq", "batch")),
            P(("seq", "batch"), None),
            P(("seq", "batch"), None),
        ),
        out_specs=(
            P("batch", "seq", None),
            P("batch", "seq", None),
            P(("seq", "batch")),
            P(("seq", "batch"), None),
            P(("seq", "batch"), None),
            P(("seq", "batch"), None),
            P(("seq", "batch"), None),
            P(("seq", "batch"), None),
            P(("seq", "batch")),
            P(("seq", "batch"), None),
            P(("seq", "batch")),
            P(("seq", "batch"), None),
            P(("seq", "batch"), None),
            P(("seq", "batch")),
            P(("seq", "batch"), None),
            P(("seq", "batch"), None),
            P(("seq", "batch")),
            P(("seq", "batch"), None),
            P(("seq", "batch"), None),
        ),
        check_vma=False,
    )
```

```python
import functools

import jax
import jax.numpy as jnp
from jax import lax
from jax.experimental import pallas as pl
from jax.experimental.pallas import tpu as pltpu
from jax.sharding import PartitionSpec as P

HEADS = 12
HEAD_DIM = 64

eps = 1e-05
masked_score = -1e30
lanes = 128
sublanes = 8
everyone = ("seq", "batch")
f32 = jnp.float32
bf16 = jnp.bfloat16


def rows_of(ref, seq, block):
    return ref[seq, pl.ds(pl.multiple_of(block * sublanes, sublanes), sublanes), :]


def spread(rows, index, count):
    return jnp.broadcast_to(rows[index : index + 1], (count, lanes))


def encode_kernel(reverse, input_ref, decay_ref, end_ref):
    seq_count, step_count, _ = input_ref.shape
    state_count = decay_ref.shape[0]
    blocks = step_count // sublanes
    power = jnp.exp(-decay_ref[...])

    def one_block(step, states):
        block = blocks - 1 - step if reverse else step
        rows = [rows_of(input_ref, seq, block) for seq in range(seq_count)]
        order = range(sublanes - 1, -1, -1) if reverse else range(sublanes)
        states = list(states)
        for index in order:
            for seq in range(seq_count):
                states[seq] = states[seq] * power + spread(rows[seq], index, state_count)
        return tuple(states)

    start = tuple(jnp.zeros((state_count, lanes), f32) for _ in range(seq_count))
    ends = lax.fori_loop(0, blocks, one_block, start)
    for seq in range(seq_count):
        end_ref[seq] = ends[seq]


def output_kernel(input_ref, query_ref, carried_ref, decay_ref, weight_ref, skip_ref, out_ref, gated_ref):
    seq_count, step_count, _ = input_ref.shape
    state_count = decay_ref.shape[0]
    power = jnp.exp(-decay_ref[...])
    weight = weight_ref[...]
    skip = skip_ref[...]

    def one_block(block, states):
        states = list(states)
        rows = [rows_of(input_ref, seq, block) for seq in range(seq_count)]
        found = [[] for _ in range(seq_count)]
        for index in range(sublanes):
            for seq in range(seq_count):
                states[seq] = states[seq] * power + spread(rows[seq], index, state_count)
                found[seq].append(jnp.sum(states[seq] * weight, axis=0, keepdims=True))
        place = pl.ds(pl.multiple_of(block * sublanes, sublanes), sublanes)
        for seq in range(seq_count):
            result = jnp.concatenate(found[seq], axis=0) + skip * rows[seq]
            out_ref[seq, place, :] = result
            gated_ref[seq, place, :] = result * rows_of(query_ref, seq, block)
        return tuple(states)

    start = tuple(carried_ref[seq].astype(f32) for seq in range(seq_count))
    lax.fori_loop(0, step_count // sublanes, one_block, start)


def back_kernel(
    input_ref,
    grad_ref,
    carried_ref,
    later_ref,
    decay_ref,
    weight_ref,
    skip_ref,
    input_grad_ref,
    weight_grad_ref,
    power_grad_ref,
    skip_grad_ref,
    held,
):
    seq_count, step_count, _ = input_ref.shape
    state_count = decay_ref.shape[0]
    blocks = step_count // sublanes
    power = jnp.exp(-decay_ref[...])
    weight = weight_ref[...]
    skip = skip_ref[...]
    seqs = range(seq_count)

    def forward_block(block, state):
        states, total, skip_total = list(state[0]), state[1], state[2]
        rows = [rows_of(input_ref, seq, block) for seq in seqs]
        grads = [rows_of(grad_ref, seq, block) for seq in seqs]
        for index in range(sublanes):
            for seq in seqs:
                held[block * sublanes + index, seq] = states[seq]
                states[seq] = states[seq] * power + spread(rows[seq], index, state_count)
                total = total + states[seq] * spread(grads[seq], index, state_count)
        for seq in seqs:
            skip_total = skip_total + rows[seq] * grads[seq]
        return (tuple(states), total, skip_total)

    zeros = jnp.zeros((state_count, lanes), f32)
    _, total, skip_total = lax.fori_loop(
        0,
        blocks,
        forward_block,
        (
            tuple(carried_ref[seq].astype(f32) for seq in seqs),
            zeros,
            jnp.zeros((sublanes, lanes), f32),
        ),
    )
    weight_grad_ref[...] = total
    skip_grad_ref[...] = jnp.sum(skip_total, axis=0, keepdims=True)

    def back_block(step, state):
        states, total = list(state[0]), state[1]
        block = blocks - 1 - step
        grads = [rows_of(grad_ref, seq, block) for seq in seqs]
        found = [[None] * sublanes for _ in seqs]
        for index in range(sublanes - 1, -1, -1):
            for seq in seqs:
                states[seq] = states[seq] * power + spread(grads[seq], index, state_count)
                found[seq][index] = jnp.sum(states[seq] * weight, axis=0, keepdims=True)
                total = total + states[seq] * held[block * sublanes + index, seq]
        place = pl.ds(pl.multiple_of(block * sublanes, sublanes), sublanes)
        for seq in seqs:
            input_grad_ref[seq, place, :] = jnp.concatenate(found[seq], axis=0) + skip * grads[seq]
        return (tuple(states), total)

    _, total = lax.fori_loop(
        0, blocks, back_block, (tuple(later_ref[seq].astype(f32) for seq in seqs), zeros)
    )
    power_grad_ref[...] = total * weight


def per_lane_tile(kernel, args, outs, scratch=(), flops=0):
    def spec(shape):
        lead = len(shape) - 1
        return pl.BlockSpec(tuple(shape[:-1]) + (lanes,), lambda tile: (0,) * lead + (tile,))

    bytes_moved = sum(a.size * a.dtype.itemsize for a in args)
    return pl.pallas_call(
        kernel,
        grid=(args[0].shape[-1] // lanes,),
        in_specs=[spec(a.shape) for a in args],
        out_specs=[spec(o.shape) for o in outs],
        out_shape=list(outs),
        scratch_shapes=list(scratch),
        cost_estimate=pl.CostEstimate(flops=flops, bytes_accessed=bytes_moved, transcendentals=0),
        compiler_params=pltpu.CompilerParams(vmem_limit_bytes=48 * 1024 * 1024),
    )(*args)


def shaped(*dims, dtype=f32):
    return jax.ShapeDtypeStruct(dims, dtype)


def encode(value, decay, reverse):
    seq_count, _, width = value.shape
    (ends,) = per_lane_tile(
        functools.partial(encode_kernel, reverse),
        (value, decay),
        (shaped(seq_count, decay.shape[0], width),),
    )
    return ends


def passed_along(block, axis, distance):
    devices = range(lax.axis_size(axis))
    route = [(i - distance, i) for i in devices if i - distance in devices]
    return lax.ppermute(block, axis, route)


def carried_in(ends, decay, block_len, reverse):
    seq_count, state_count, width = ends.shape
    count = lax.axis_size("seq")
    part = state_count // count

    def exchanged(parts):
        return lax.all_to_all(parts.astype(bf16), "seq", split_axis=0, concat_axis=0, tiled=True)

    parts = ends.reshape(seq_count, count, part, width).transpose(1, 0, 2, 3)
    arrived = exchanged(parts.reshape(count, seq_count * part, width)).astype(f32)
    rates = lax.dynamic_slice_in_dim(decay, lax.axis_index("seq") * part, part, 0)
    power = jnp.tile(jnp.exp(-rates * block_len), (seq_count, 1))
    state, joined = jnp.zeros_like(arrived[0]), [None] * count
    for block in reversed(range(count)) if reverse else range(count):
        joined[block] = state
        state = power * state + arrived[block]
    back = exchanged(jnp.stack(joined))
    back = back.reshape(count, seq_count, part, width).transpose(1, 0, 2, 3)
    return back.reshape(seq_count, state_count, width)


MESH = pl.DeviceIdType.MESH
box = (4, 2, 2, 2)


def here():
    seq, batch = lax.axis_index("seq"), lax.axis_index("batch")
    return lax.div(seq, 2), lax.rem(seq, 2), lax.div(batch, 2), lax.rem(batch, 2)


def device(z, x, y, core):
    return (2 * z + x, 2 * y + core)


def line_peer(z, step):
    return lax.rem(z + step, box[0])


def greet(diagonal=False):
    z, x, y, core = here()
    barrier = pltpu.get_barrier_semaphore()
    peers = [device(line_peer(z, step), x, y, core) for step in range(1, box[0])]
    peers += [device(z, 1 - x, y, core), device(z, x, 1 - y, core), device(z, x, y, 1 - core)]
    if diagonal:
        peers += [device(line_peer(z, step), 1 - x, y, core) for step in range(1, box[0])]
    for peer in peers:
        pl.semaphore_signal(barrier, inc=1, device_id=peer, device_id_type=MESH)
    pl.semaphore_wait(barrier, len(peers))


def staggered(count, stages, gap):
    for turn in range(count + gap * (stages - 1)):
        for stage in reversed(range(stages)):
            chunk = turn - gap * stage
            if 0 <= chunk < count:
                yield stage, chunk


def gather_kernel(plan, gap, *refs):
    count = 1 + max(item[0] for item in plan)
    ins, outs = refs[:count], refs[count : 2 * count]
    send, receive, local = refs[2 * count :]
    z, x, y, core = here()
    greet()
    started = {}

    def push(chunk, slot, source, target, peer):
        copy = pltpu.make_async_remote_copy(
            src_ref=source,
            dst_ref=target,
            send_sem=send.at[chunk, slot],
            recv_sem=receive.at[chunk, slot],
            device_id=peer,
            device_id_type=MESH,
        )
        copy.start()
        started[chunk, slot] = copy

    own = []
    for chunk, (index, first, width, _) in enumerate(plan):
        columns = pl.ds(first, width)
        source = ins[index].at[:, columns]
        target = outs[index].at[z, x, y, core, :, columns]
        for step in range(1, box[0]):
            push(chunk, step - 1, source, target, device(line_peer(z, step), x, y, core))
        keep = pltpu.make_async_copy(source, target, local.at[chunk])
        keep.start()
        own.append(keep)

    for stage, chunk in staggered(len(plan), 3, gap):
        index, first, width, order = plan[chunk]
        x_first = order[1] == "x"
        columns = pl.ds(first, width)
        out = outs[index]
        if stage == 0:
            for step in range(1, box[0]):
                started[chunk, step - 1].wait_recv()
            own[chunk].wait()
            part = out.at[:, x, y, core, :, columns]
            peer = device(z, 1 - x, y, core) if x_first else device(z, x, 1 - y, core)
            push(chunk, 3, part, part, peer)
        elif stage == 1:
            started[chunk, 3].wait_recv()
            if x_first:
                part, peer = out.at[:, :, y, core, :, columns], device(z, x, 1 - y, core)
            else:
                part, peer = out.at[:, x, :, core, :, columns], device(z, 1 - x, y, core)
            push(chunk, 4, part, part, peer)
        else:
            started[chunk, 4].wait_recv()
            part = out.at[:, :, :, core, :, columns]
            push(chunk, 5, part, part, device(z, x, y, 1 - core))
    for chunk in range(len(plan)):
        started[chunk, 5].wait_recv()
        for slot in range(6):
            started[chunk, slot].wait_send()


def gather_blocks(blocks, plan, gap=2, collective=0):
    outs = [jax.ShapeDtypeStruct(box + b.shape, b.dtype) for b in blocks]
    sent = sum(b.size * b.dtype.itemsize for b in blocks)
    whole = pl.pallas_call(
        functools.partial(gather_kernel, plan, gap),
        out_shape=outs,
        in_specs=[pl.BlockSpec(memory_space=pltpu.VMEM)] * len(blocks),
        out_specs=[pl.BlockSpec(memory_space=pl.ANY)] * len(blocks),
        scratch_shapes=[
            pltpu.SemaphoreType.DMA((len(plan), 6)),
            pltpu.SemaphoreType.DMA((len(plan), 6)),
            pltpu.SemaphoreType.DMA((len(plan),)),
        ],
        cost_estimate=pl.CostEstimate(flops=0, bytes_accessed=64 * sent, transcendentals=0),
        compiler_params=pltpu.CompilerParams(collective_id=collective, has_side_effects=True),
    )(*blocks)
    return [w.reshape((32 * w.shape[4], w.shape[5])) for w in whole]


def add_into(total, other):
    return (total.astype(f32) + other.astype(f32)).astype(bf16)


def scatter_kernel(plan, gap, finish, beside, counts, *refs):
    count, out_count, work_ins, work_outs, work_scratch = counts
    refs, taken = list(refs), []
    for number in (count, work_ins, out_count, work_outs, count, work_scratch):
        taken.append(refs[:number])
        refs = refs[number:]
    ins, work_in_refs, results, work_out_refs, outs, work_refs = taken
    buffers, (send, receive, local) = refs[:-3], refs[-3:]
    z, x, y, core = here()
    greet(diagonal=beside is not None)
    work = list(beside(*work_in_refs, *work_out_refs, *work_refs)) if beside else []
    started = {}

    def push(chunk, slot, source, target, peer):
        copy = pltpu.make_async_remote_copy(
            src_ref=source,
            dst_ref=target,
            send_sem=send.at[chunk, slot],
            recv_sem=receive.at[chunk, slot],
            device_id=peer,
            device_id_type=MESH,
        )
        copy.start()
        started[chunk, slot] = copy

    loads = []
    for chunk, (index, first, width, _) in enumerate(plan):
        columns = pl.ds(first, width)
        held, from_core = buffers[5 * chunk : 5 * chunk + 2]
        grad = ins[index]
        push(chunk, 0, grad.at[:, :, :, 1 - core, :, columns], from_core, device(z, x, y, 1 - core))
        load = pltpu.make_async_copy(grad.at[:, :, :, core, :, columns], held, local.at[chunk])
        load.start()
        loads.append(load)

    steps, pieces = list(staggered(len(plan), 4, gap)), len(work)
    for turn, (stage, chunk) in enumerate(steps):
        while work and turn * pieces >= (pieces - len(work)) * len(steps) * 3 // 4:
            work.pop(0)()
        index, first, width, order = plan[chunk]
        x_first, line_last = order[0] == "y", order[-1] == "z"
        held, from_core, from_one, from_two, from_line = buffers[5 * chunk : 5 * chunk + 5]
        to_x, to_y = device(z, 1 - x, y, core), device(z, x, 1 - y, core)
        if stage == 0:
            started[chunk, 0].wait_recv()
            loads[chunk].wait()

            @pl.loop(0, 4 * box[0])
            def _(turn):
                at = (lax.div(turn, 4), lax.rem(lax.div(turn, 2), 2), lax.rem(turn, 2))
                held[at] = add_into(held[at], from_core[at])

            if x_first:
                push(chunk, 1, held.at[:, :, 1 - y], from_one, to_y)
            else:
                push(chunk, 1, held.at[:, 1 - x], from_one, to_x)
        elif stage == 1:
            started[chunk, 1].wait_recv()

            @pl.loop(0, 2 * box[0])
            def _(turn):
                row, i = lax.div(turn, 2), lax.rem(turn, 2)
                at = (row, i, y) if x_first else (row, x, i)
                held[at] = add_into(held[at], from_one[row, i])

            if not line_last:
                for step in range(1, box[0]):
                    peer = line_peer(z, step)
                    rest = held.at[peer, :, y] if x_first else held.at[peer, x]
                    push(chunk, 2 + step, rest, from_line.at[step - 1], device(peer, x, y, core))
            elif x_first:
                push(chunk, 2, held.at[:, 1 - x, y], from_two, to_x)
            else:
                push(chunk, 2, held.at[:, x, 1 - y], from_two, to_y)
        elif stage == 2 and not line_last:
            for step in range(1, box[0]):
                started[chunk, 2 + step].wait_recv()
            for i in range(2):
                at = (z, i, y) if x_first else (z, x, i)
                total = held[at].astype(f32)
                for step in range(1, box[0]):
                    total = total + from_line[step - 1, i].astype(f32)
                held[at] = total.astype(bf16)
            if x_first:
                push(chunk, 2, held.at[z, 1 - x, y], from_two, to_x)
            else:
                push(chunk, 2, held.at[z, x, 1 - y], from_two, to_y)
        elif stage == 2:
            started[chunk, 2].wait_recv()

            @pl.loop(0, box[0])
            def _(row):
                held[row, x, y] = add_into(held[row, x, y], from_two[row])

            for step in range(1, box[0]):
                peer = line_peer(z, step)
                push(chunk, 2 + step, held.at[peer, x, y], from_line.at[step - 1], device(peer, x, y, core))
        else:
            total = held[z, x, y].astype(f32)
            if line_last:
                for step in range(1, box[0]):
                    started[chunk, 2 + step].wait_recv()
                    total = total + from_line[step - 1].astype(f32)
            else:
                started[chunk, 2].wait_recv()
                total = total + from_two[...].astype(f32)
            outs[index][:, pl.ds(first, width)] = total
            if not any(item[0] == index for item in plan[chunk + 1 :]):
                finish(index, outs[index], results)
    for chunk in range(len(plan)):
        for slot in range(6):
            started[chunk, slot].wait_send()


def scatter_blocks(grads, plan, finish, results, gap=2, collective=1, work=None):
    views = [g.reshape(box + (g.shape[0] // 32, g.shape[1])) for g in grads]
    beside, work_ins, work_outs, work_scratch = work or (None, [], [], [])
    scratch = [pltpu.VMEM(v.shape[4:], f32) for v in views] + list(work_scratch)
    for index, _, width, order in plan:
        tile = (views[index].shape[4], width)
        ends_of = ((4,), (3,)) if order[-1] == "z" else ((), (3, 2))
        for lead in ((4, 2, 2), (4, 2, 2), (4, 2)) + ends_of:
            scratch.append(pltpu.VMEM(lead + tile, bf16))
    counts = (len(views), len(results), len(work_ins), len(work_outs), len(work_scratch))
    sent = sum(v.size * v.dtype.itemsize for v in views)
    local = pl.BlockSpec(memory_space=pltpu.VMEM)
    return pl.pallas_call(
        functools.partial(scatter_kernel, plan, gap, finish, beside, counts),
        out_shape=list(results) + list(work_outs),
        in_specs=[pl.BlockSpec(memory_space=pl.ANY)] * len(views) + [local] * len(work_ins),
        out_specs=[local] * (len(results) + len(work_outs)),
        scratch_shapes=scratch
        + [
            pltpu.SemaphoreType.DMA((len(plan), 6)),
            pltpu.SemaphoreType.DMA((len(plan), 6)),
            pltpu.SemaphoreType.DMA((len(plan),)),
        ],
        cost_estimate=pl.CostEstimate(flops=0, bytes_accessed=4 * sent, transcendentals=0),
        compiler_params=pltpu.CompilerParams(
            collective_id=collective, has_side_effects=True, vmem_limit_bytes=60 * 1024 * 1024
        ),
    )(*views, *work_ins)


def chunked(widths, pieces, orders):
    plan = []
    for index, (width, number) in enumerate(zip(widths, pieces)):
        tiles = width // lanes
        edges = [tiles * i // number for i in range(number + 1)]
        for i in range(number):
            plan.append((index, edges[i] * lanes, (edges[i + 1] - edges[i]) * lanes, orders[len(plan) % len(orders)]))
    return plan


def carry_pieces(
    reverse, input_ref, decay_ref, carried_ref, ends, outgoing, arrived, joined, final, send, receive
):
    seq_count, step_count, width = input_ref.shape
    count = lax.axis_size("seq")
    part = decay_ref.shape[0] // count
    me, batch = lax.axis_index("seq"), lax.axis_index("batch")

    def encode_all():
        @pl.loop(0, width // lanes)
        def _(tile):
            columns = pl.ds(pl.multiple_of(tile * lanes, lanes), lanes)
            encode_kernel(reverse, input_ref.at[:, :, columns], decay_ref.at[:, columns], ends)
            for group in range(count):
                rows = slice(group * part, (group + 1) * part)
                mine = jnp.concatenate([ends[seq, rows] for seq in range(seq_count)], axis=0)
                outgoing[group, :, columns] = mine.astype(bf16)

    def started(phase, source, target):
        copies = []
        for step in range(1, count):
            peer = lax.rem(me + step, count)
            copy = pltpu.make_async_remote_copy(
                src_ref=source.at[peer],
                dst_ref=target.at[me],
                send_sem=send.at[phase, step - 1],
                recv_sem=receive.at[phase, step - 1],
                device_id=(peer, batch),
                device_id_type=MESH,
            )
            copy.start()
            copies.append(copy)
        target[me] = source[me]
        return copies

    flying = []

    def first():
        encode_all()
        flying.append(started(0, outgoing, arrived))

    def second():
        for copy in flying.pop():
            copy.wait()
        rates = decay_ref[pl.ds(pl.multiple_of(me * part, part), part), :]
        power = jnp.exp(-rates * step_count)
        power = jnp.concatenate([power] * seq_count, axis=0)
        state = jnp.zeros(power.shape, f32)
        for block in reversed(range(count)) if reverse else range(count):
            joined[block] = state.astype(bf16)
            state = power * state + arrived[block].astype(f32)
        flying.append(started(1, joined, final))

    def third():
        for copy in flying.pop():
            copy.wait()
        for group in range(count):
            rows = slice(group * part, (group + 1) * part)
            found = final[group].astype(f32)
            for seq in range(seq_count):
                carried_ref[seq, rows] = found[seq * part : (seq + 1) * part]

    return first, second, third


def carry_kernel(reverse, *refs):
    count = lax.axis_size("seq")
    me, batch = lax.axis_index("seq"), lax.axis_index("batch")
    barrier = pltpu.get_barrier_semaphore()
    for step in range(1, count):
        peer = (lax.rem(me + step, count), batch)
        pl.semaphore_signal(barrier, inc=1, device_id=peer, device_id_type=MESH)
    pl.semaphore_wait(barrier, count - 1)
    for piece in carry_pieces(reverse, *refs):
        piece()


def state_back_work(
    input_ref,
    grad_ref,
    carried_ref,
    decay_ref,
    weight_ref,
    skip_ref,
    input_grad_ref,
    weight_grad_ref,
    power_grad_ref,
    skip_grad_ref,
    later_ref,
    ends,
    outgoing,
    arrived,
    joined,
    final,
    held,
    send,
    receive,
):
    carry = carry_pieces(True, grad_ref, decay_ref, later_ref, ends, outgoing, arrived, joined, final, send, receive)

    def tile_piece(tile):
        cut_at = slice(tile * lanes, (tile + 1) * lanes)
        wide = (input_ref, grad_ref, carried_ref, later_ref)
        flat = (decay_ref, weight_ref, skip_ref)
        results = (weight_grad_ref, power_grad_ref, skip_grad_ref)
        back_kernel(
            *(r.at[:, :, cut_at] for r in wide),
            *(r.at[:, cut_at] for r in flat),
            input_grad_ref.at[:, :, cut_at],
            *(r.at[:, cut_at] for r in results),
            held,
        )

    tiles = [functools.partial(tile_piece, tile) for tile in range(input_ref.shape[2] // lanes)]
    return list(carry) + tiles


def carried_by_kernel(value, decay, reverse, collective):
    seq_count, _, width = value.shape
    state_count = decay.shape[0]
    count = lax.axis_size("seq")
    parts = pltpu.VMEM((count, seq_count * state_count // count, width), bf16)
    return pl.pallas_call(
        functools.partial(carry_kernel, reverse),
        out_shape=shaped(seq_count, state_count, width),
        in_specs=[pl.BlockSpec(memory_space=pltpu.VMEM)] * 2,
        out_specs=pl.BlockSpec(memory_space=pltpu.VMEM),
        scratch_shapes=[pltpu.VMEM((seq_count, state_count, lanes), f32)]
        + [parts] * 4
        + [pltpu.SemaphoreType.DMA((2, count - 1)), pltpu.SemaphoreType.DMA((2, count - 1))],
        cost_estimate=pl.CostEstimate(flops=0, bytes_accessed=32 * value.size, transcendentals=0),
        compiler_params=pltpu.CompilerParams(collective_id=collective, has_side_effects=True),
    )(value, decay)


hidden_block = 768
gelu_scale = 0.7978845608
gelu_cubic = 0.044715


def feed_kernel(resid_ref, gain_ref, up_ref, down_ref, out_ref, normed_ref, hidden_ref, active_ref):
    @pl.when(pl.program_id(0) == 0)
    def _():
        resid = resid_ref[...]
        normed_ref[...] = layer_norm(resid, gain_ref[...]).astype(bf16)
        out_ref[...] = resid

    hidden = jnp.dot(normed_ref[...], up_ref[...], preferred_element_type=f32)
    hidden_ref[...] = hidden.astype(bf16)
    bend = jnp.tanh(gelu_scale * (hidden + gelu_cubic * hidden * hidden * hidden))
    active = (0.5 * hidden * (1.0 + bend)).astype(bf16)
    active_ref[...] = active
    out_ref[...] += jnp.dot(active, down_ref[...], preferred_element_type=f32)


def feed_forward_blocks(resid, gain, up_packed, up_at, down):
    rows, width = resid.shape
    inner = down.shape[0]
    first = up_at // hidden_block
    whole = pl.BlockSpec((rows, width), lambda j: (0, 0))
    part = pl.BlockSpec((rows, hidden_block), lambda j: (0, j))
    out, normed, hidden, active = pl.pallas_call(
        feed_kernel,
        grid=(inner // hidden_block,),
        in_specs=[
            whole,
            pl.BlockSpec((1, width), lambda j: (0, 0)),
            pl.BlockSpec((width, hidden_block), lambda j: (0, first + j)),
            pl.BlockSpec((hidden_block, width), lambda j: (j, 0)),
        ],
        out_specs=[whole, whole, part, part],
        out_shape=[
            shaped(rows, width),
            shaped(rows, width, dtype=bf16),
            shaped(rows, inner, dtype=bf16),
            shaped(rows, inner, dtype=bf16),
        ],
        cost_estimate=pl.CostEstimate(
            flops=4 * rows * width * inner, bytes_accessed=10 * width * inner, transcendentals=rows * inner
        ),
        compiler_params=pltpu.CompilerParams(vmem_limit_bytes=40 * 1024 * 1024),
    )(resid, gain[None], up_packed, down)
    return out, (resid, gain, normed, hidden, active)


def feed_back_kernel(
    packed,
    upstream_ref,
    resid_ref,
    gain_ref,
    normed_ref,
    hidden_ref,
    active_ref,
    up_ref,
    down_ref,
    out_ref,
    gain_grad_ref,
    *rest,
):
    step = pl.program_id(0)
    last = pl.num_programs(0) - 1
    across = (((1,), (1,)), ((), ()))
    along = (((0,), (0,)), ((), ()))
    upstream_low = upstream_ref[...].astype(bf16)
    into_active = lax.dot_general(upstream_low, down_ref[...], across, preferred_element_type=f32)
    hidden = hidden_ref[...].astype(f32)
    square = hidden * hidden
    bend = jnp.tanh(gelu_scale * hidden * (1.0 + gelu_cubic * square))
    slope = 0.5 * (1.0 + bend) + 0.5 * hidden * (1.0 - bend * bend) * (
        gelu_scale * (1.0 + 3.0 * gelu_cubic * square)
    )
    into_hidden = (into_active * slope).astype(bf16)
    part = lax.dot_general(into_hidden, up_ref[...], across, preferred_element_type=f32)

    @pl.when(step == 0)
    def _():
        out_ref[...] = part

    @pl.when(step > 0)
    def _():
        out_ref[...] += part

    up_grad = lax.dot_general(normed_ref[...], into_hidden, along, preferred_element_type=f32)
    down_grad = lax.dot_general(active_ref[...], upstream_low, along, preferred_element_type=f32)
    if packed:
        grads_ref, up_held, down_held, sems = rest
        share, fold = packed
        width = up_grad.shape[0]
        inner = hidden_block * grads_ref.shape[1] // (2 * hidden_block)
        tall = hidden_block // fold
        slot = lax.rem(step, 2)

        def copies(at, slot):
            columns = pl.ds(pl.multiple_of(at * hidden_block, hidden_block), hidden_block)
            rows = pl.ds(pl.multiple_of(at * tall, tall), tall)
            return (
                pltpu.make_async_copy(up_held.at[slot], grads_ref.at[:, columns], sems.at[0, slot]),
                pltpu.make_async_copy(down_held.at[slot], grads_ref.at[rows, inner:], sems.at[1, slot]),
            )

        @pl.when(step >= 2)
        def _():
            for copy in copies(step - 2, slot):
                copy.wait()

        up_held[slot] = up_grad.astype(bf16)
        for place in range(fold):
            starts = range(place * share, hidden_block, fold * share)
            piece = jnp.concatenate([down_grad[a : a + share] for a in starts], axis=0)
            down_held[slot, :, place * width : (place + 1) * width] = piece.astype(bf16)
        for copy in copies(step, slot):
            copy.start()

        @pl.when(step == last)
        def _():
            for copy in copies(step - 1, 1 - slot) + copies(step, slot):
                copy.wait()
    else:
        up_grad_ref, down_grad_ref = rest
        up_grad_ref[...] = up_grad.astype(bf16)
        down_grad_ref[...] = down_grad.astype(bf16)

    @pl.when(step == last)
    def _():
        into_normed = out_ref[...]
        resid = resid_ref[...]
        centred = resid - jnp.mean(resid, axis=-1, keepdims=True)
        inverse = lax.rsqrt(jnp.mean(centred * centred, axis=-1, keepdims=True) + eps)
        unit = centred * inverse
        gain_grad_ref[...] = jnp.sum(into_normed * unit, axis=0, keepdims=True)
        scaled = into_normed * gain_ref[...]
        along_unit = jnp.mean(scaled * unit, axis=-1, keepdims=True)
        into_resid = inverse * (scaled - jnp.mean(scaled, axis=-1, keepdims=True) - unit * along_unit)
        out_ref[...] = upstream_ref[...] + into_resid


def feed_back_blocks(stored, up_packed, up_at, down, upstream, packed=()):
    resid, gain, normed, hidden, active = stored
    rows, width = resid.shape
    inner = down.shape[0]
    first = up_at // hidden_block
    whole = pl.BlockSpec((rows, width), lambda j: (0, 0))
    part = pl.BlockSpec((rows, hidden_block), lambda j: (0, j))
    line = pl.BlockSpec((1, width), lambda j: (0, 0))
    up_spec = pl.BlockSpec((width, hidden_block), lambda j: (0, j))
    down_spec = pl.BlockSpec((hidden_block, width), lambda j: (j, 0))
    scratch = []
    if packed:
        grad_specs = [pl.BlockSpec(memory_space=pl.ANY)]
        grad_shapes = [shaped(width, 2 * inner, dtype=bf16)]
        scratch = [
            pltpu.VMEM((2, width, hidden_block), bf16),
            pltpu.VMEM((2, hidden_block // packed[1], inner), bf16),
            pltpu.SemaphoreType.DMA((2, 2)),
        ]
    else:
        grad_specs = [up_spec, down_spec]
        grad_shapes = [shaped(width, inner, dtype=bf16), shaped(inner, width, dtype=bf16)]
    out, gain_grad, *grads = pl.pallas_call(
        functools.partial(feed_back_kernel, packed),
        grid=(inner // hidden_block,),
        in_specs=[
            whole,
            whole,
            line,
            whole,
            part,
            part,
            pl.BlockSpec((width, hidden_block), lambda j: (0, first + j)),
            down_spec,
        ],
        out_specs=[whole, line] + grad_specs,
        out_shape=[shaped(rows, width), shaped(1, width)] + grad_shapes,
        scratch_shapes=scratch,
        cost_estimate=pl.CostEstimate(
            flops=8 * rows * width * inner, bytes_accessed=16 * width * inner, transcendentals=rows * inner
        ),
        compiler_params=pltpu.CompilerParams(vmem_limit_bytes=48 * 1024 * 1024),
    )(upstream, resid, gain[None], normed, hidden, active, up_packed, down)
    return (out, gain_grad[0], *grads)


def split_heads(ref, scratch, heads, parts, first=0):
    for part in range(parts):
        for head in range(heads):
            start = (part * heads + head) * HEAD_DIM + first
            scratch[part * heads + head] = ref[:, start : start + HEAD_DIM]


def score_block(query, keys, first, scale):
    scores = (
        lax.dot_general(query, keys, (((1,), (1,)), ((), ())), preferred_element_type=f32) * scale
    )
    rows = lax.broadcasted_iota(jnp.int32, scores.shape, 0) + first
    columns = lax.broadcasted_iota(jnp.int32, scores.shape, 1)
    return jnp.where(columns <= rows, scores, masked_score)


def attend_kernel(heads, block, scale, qkv_ref, low_ref, full_ref, stat_ref, parts, outs):
    length = qkv_ref.shape[0]
    split_heads(qkv_ref, parts, heads, 3)

    @pl.loop(0, heads)
    def _(head):
        for first in range(0, length, block):
            extent = first + block
            query = parts[head, first:extent, :]
            scores = score_block(query, parts[heads + head, :extent, :], first, scale)
            top = jnp.max(scores, axis=1, keepdims=True)
            soft = jnp.exp(scores - top)
            whole = jnp.sum(soft, axis=1, keepdims=True)
            soft = soft * (1.0 / whole)
            outs[head, first:extent, :] = jnp.dot(
                soft.astype(bf16), parts[2 * heads + head, :extent, :], preferred_element_type=f32
            )
            stat_ref[head, first:extent, :] = jnp.broadcast_to(top + jnp.log(whole), (block, lanes))

    if low_ref.shape[1] > heads * HEAD_DIM:
        low_ref[:, heads * HEAD_DIM :] = jnp.zeros((length, low_ref.shape[1] - heads * HEAD_DIM), bf16)
    for head in range(heads):
        place = slice(head * HEAD_DIM, (head + 1) * HEAD_DIM)
        full_ref[:, place] = outs[head]
        low_ref[:, place] = outs[head].astype(bf16)


def attend_back_kernel(
    heads, block, scale, qkv_ref, dout_ref, full_ref, stat_ref, grad_ref, parts, douts, fulls, grads
):
    length = qkv_ref.shape[0]
    split_heads(qkv_ref, parts, heads, 3)
    split_heads(dout_ref, douts, heads, 1)
    split_heads(full_ref, fulls, heads, 1)
    grads[...] = jnp.zeros_like(grads)

    @pl.loop(0, heads)
    def _(head):
        for first in range(0, length, block):
            extent = first + block
            query = parts[head, first:extent, :]
            keys = parts[heads + head, :extent, :]
            value = parts[2 * heads + head, :extent, :]
            dout = douts[head, first:extent, :]
            delta = jnp.sum(dout.astype(f32) * fulls[head, first:extent, :], axis=1, keepdims=True)
            scores = score_block(query, keys, first, scale)
            soft = jnp.exp(scores - stat_ref[head, first:extent, :1])
            across = (((1,), (1,)), ((), ()))
            along = (((0,), (0,)), ((), ()))
            dprob = lax.dot_general(dout, value, across, preferred_element_type=f32)
            dscore = (soft * (dprob - delta) * scale).astype(bf16)
            grads[head, first:extent, :] = jnp.dot(dscore, keys, preferred_element_type=f32)
            grads[heads + head, :extent, :] += lax.dot_general(
                dscore, query, along, preferred_element_type=f32
            )
            grads[2 * heads + head, :extent, :] += lax.dot_general(
                soft.astype(bf16), dout, along, preferred_element_type=f32
            )

    grad_ref[...] = jnp.zeros_like(grad_ref)
    for part in range(3 * heads):
        grad_ref[:, part * HEAD_DIM : (part + 1) * HEAD_DIM] = grads[part].astype(bf16)


def attend_params():
    return pltpu.CompilerParams(vmem_limit_bytes=56 * 1024 * 1024)


def attend_whole(qkv, heads, block):
    length = qkv.shape[0]
    width = heads * HEAD_DIM
    return pl.pallas_call(
        functools.partial(attend_kernel, heads, block, HEAD_DIM ** (-0.5)),
        out_shape=[
            shaped(length, -(-width // lanes) * lanes, dtype=bf16),
            shaped(length, width),
            shaped(heads, length, lanes),
        ],
        scratch_shapes=[
            pltpu.VMEM((3 * heads, length, HEAD_DIM), bf16),
            pltpu.VMEM((heads, length, HEAD_DIM), f32),
        ],
        compiler_params=attend_params(),
    )(qkv)


def attend_whole_back(qkv, dout, full, stat, heads, block):
    length = qkv.shape[0]
    return pl.pallas_call(
        functools.partial(attend_back_kernel, heads, block, HEAD_DIM ** (-0.5)),
        out_shape=shaped(*qkv.shape, dtype=bf16),
        scratch_shapes=[
            pltpu.VMEM((3 * heads, length, HEAD_DIM), bf16),
            pltpu.VMEM((heads, length, HEAD_DIM), bf16),
            pltpu.VMEM((heads, length, HEAD_DIM), f32),
            pltpu.VMEM((3 * heads, length, HEAD_DIM), f32),
        ],
        compiler_params=attend_params(),
    )(qkv, dout, full, stat)


def split_blocks(array, block_len):
    shaped_blocks = array.reshape(
        (array.shape[0], array.shape[1] // block_len, block_len) + array.shape[2:]
    )
    return jnp.moveaxis(shaped_blocks, 1, 0)


def general_attention(proj_low, seq_count, block_len, places, any_live, longest):
    model_width = HEADS * HEAD_DIM
    scale = HEAD_DIM ** (-0.5)
    offsets = jnp.arange(block_len, dtype=jnp.int32)
    head_shape = (seq_count, block_len, HEADS, HEAD_DIM)
    query_low = proj_low[:, :model_width].reshape(head_shape)
    keys_low = proj_low[:, model_width : 2 * model_width].reshape(head_shape)
    value_low = proj_low[:, 2 * model_width :].reshape(head_shape)

    def block_scores(queries, keys_block, query_places, key_places):
        scores = (
            jnp.einsum("sqhe,skhe->sqhk", queries, keys_block, preferred_element_type=jnp.float32)
            * scale
        )
        causal_mask = key_places[None, :] <= query_places[:, None]
        return jnp.where(causal_mask[None, :, None, :], scores, masked_score)

    def key_needed(key_first):
        return (key_first <= places[-1]) & ((key_first == places[0]) | any_live)

    stat_shape = (seq_count, block_len, HEADS)
    start_state = (
        jnp.full(stat_shape, masked_score, jnp.float32),
        jnp.zeros(stat_shape, jnp.float32),
        jnp.zeros(head_shape, jnp.float32),
    )
    shard_piece = (
        lax.all_gather(keys_low, "seq", axis=1, tiled=True),
        lax.all_gather(value_low, "seq", axis=1, tiled=True),
    )
    keys_blocks = split_blocks(shard_piece[0], block_len)
    value_blocks = split_blocks(shard_piece[1], block_len)
    firsts = jnp.arange(keys_blocks.shape[0], dtype=jnp.int32) * block_len

    def attend_one_step(state_now, operand):
        keys_block, value_block, key_first = operand

        def attend_work(state_in_block):
            running_max, running_sum, running_out = state_in_block
            scores = block_scores(query_low, keys_block, places, key_first + offsets)
            new_max = jnp.maximum(running_max, jnp.max(scores, axis=-1))
            fade = jnp.exp(running_max - new_max)
            shifted = jnp.exp(scores - new_max[..., None])
            new_sum = running_sum * fade + jnp.sum(shifted, axis=-1)
            new_out = running_out * fade[..., None] + jnp.einsum(
                "sqhk,skhe->sqhe",
                shifted.astype(jnp.bfloat16),
                value_block,
                preferred_element_type=jnp.float32,
            )
            return (new_max, new_sum, new_out)

        return (
            lax.cond(
                key_needed(key_first), attend_work, lambda state_in_block: state_in_block, state_now
            ),
            None,
        )

    result, _ = lax.scan(attend_one_step, start_state, (keys_blocks, value_blocks, firsts))
    running_max, running_sum, running_out = result
    attended = running_out / running_sum[..., None]
    logsum = running_max + jnp.log(running_sum)
    def backward(dout_low):
        delta = jnp.sum(dout_low.astype(jnp.float32) * attended, axis=-1)
        shard_piece = (
            lax.all_gather(keys_low, "seq", axis=1, tiled=True),
            lax.all_gather(value_low, "seq", axis=1, tiled=True),
        )
        keys_blocks = split_blocks(shard_piece[0], block_len)
        value_blocks = split_blocks(shard_piece[1], block_len)
        firsts = jnp.arange(keys_blocks.shape[0], dtype=jnp.int32) * block_len

        def query_one_step(query_grad, operand):
            keys_block, value_block, key_first = operand

            def query_work(grad_now):
                scores = block_scores(query_low, keys_block, places, key_first + offsets)
                soft = jnp.exp(scores - logsum[..., None])
                dprob = jnp.einsum(
                    "sqhe,skhe->sqhk", dout_low, value_block, preferred_element_type=jnp.float32
                )
                dscore = (soft * (dprob - delta[..., None])).astype(jnp.bfloat16)
                return (
                    grad_now
                    + jnp.einsum(
                        "sqhk,skhe->sqhe", dscore, keys_block, preferred_element_type=jnp.float32
                    )
                    * scale
                )

            return (
                lax.cond(key_needed(key_first), query_work, lambda grad_now: grad_now, query_grad),
                None,
            )

        result, _ = lax.scan(
            query_one_step, jnp.zeros(head_shape, jnp.float32), (keys_blocks, value_blocks, firsts)
        )
        query_grad = result
        sent = (query_low.astype(jnp.float32), dout_low.astype(jnp.float32), logsum, delta)
        shard_piece = (
            lax.all_gather(sent[0].astype(jnp.bfloat16), "seq", axis=1, tiled=True).astype(jnp.float32),
            lax.all_gather(sent[1].astype(jnp.bfloat16), "seq", axis=1, tiled=True).astype(jnp.float32),
            lax.all_gather(sent[2].astype(jnp.bfloat16), "seq", axis=1, tiled=True).astype(jnp.float32),
            lax.all_gather(sent[3].astype(jnp.bfloat16), "seq", axis=1, tiled=True).astype(jnp.float32),
        )
        query_blocks = split_blocks(shard_piece[0], block_len)
        dout_blocks = split_blocks(shard_piece[1], block_len)
        logsum_blocks = split_blocks(shard_piece[2], block_len)
        delta_blocks = split_blocks(shard_piece[3], block_len)
        firsts = jnp.arange(query_blocks.shape[0], dtype=jnp.int32) * block_len

        def key_one_step(grads_now, operand):
            query_block, dout_block, logsum_block, delta_block, query_first = operand

            def key_work(grads_in):
                keys_grad, value_grad = grads_in
                query_cast = query_block.astype(jnp.bfloat16)
                dout_cast = dout_block.astype(jnp.bfloat16)
                scores = block_scores(query_cast, keys_low, query_first + offsets, places)
                soft = jnp.exp(scores - logsum_block[..., None])
                value_grad = value_grad + jnp.einsum(
                    "sqhk,sqhe->skhe",
                    soft.astype(jnp.bfloat16),
                    dout_cast,
                    preferred_element_type=jnp.float32,
                )
                dprob = jnp.einsum(
                    "sqhe,skhe->sqhk", dout_cast, value_low, preferred_element_type=jnp.float32
                )
                dscore = (soft * (dprob - delta_block[..., None])).astype(jnp.bfloat16)
                keys_grad = (
                    keys_grad
                    + jnp.einsum(
                        "sqhk,sqhe->skhe", dscore, query_cast, preferred_element_type=jnp.float32
                    )
                    * scale
                )
                return (keys_grad, value_grad)

            needed = (query_first + block_len - 1 >= places[0]) & (
                (query_first == places[0]) | (query_first < longest)
            )
            return (lax.cond(needed, key_work, lambda grads_in: grads_in, grads_now), None)

        result, _ = lax.scan(
            key_one_step,
            (jnp.zeros(head_shape, jnp.float32), jnp.zeros(head_shape, jnp.float32)),
            (query_blocks, dout_blocks, logsum_blocks, delta_blocks, firsts),
        )
        keys_grad, value_grad = result
        return (query_grad, keys_grad, value_grad)

    return attended, backward


def layer_norm(value, gain):
    centred = value - jnp.mean(value, axis=-1, keepdims=True)
    spread_of = jnp.mean(centred * centred, axis=-1, keepdims=True)
    return centred * lax.rsqrt(spread_of + eps) * gain


def gelu_tanh(value):
    return jax.nn.gelu(value, approximate=True)


def dense(left, weight):
    return jnp.dot(left, weight, preferred_element_type=f32)


def dense_back(left, weight, upstream):
    into_left = lax.dot_general(
        upstream, weight, (((1,), (1,)), ((), ())), preferred_element_type=f32
    )
    into_weight = lax.dot_general(
        left, upstream, (((0,), (0,)), ((), ())), preferred_element_type=f32
    ).astype(bf16)
    return (into_left, into_weight)


def shift_mix(extended, taps, value_part):
    step_count = value_part.shape[1]
    reach = taps.shape[1]
    shifted = extended[:, reach - 1 : reach - 1 + step_count] * taps[:, 0]
    for tap_index in range(1, reach):
        shifted = (
            shifted
            + extended[:, reach - 1 - tap_index : reach - 1 - tap_index + step_count]
            * taps[:, tap_index]
        )
    return shifted * value_part


def feed_forward(resid, gain, up_weight, down_weight):
    normed, norm_back = jax.vjp(layer_norm, resid, gain)
    normed_low = normed.astype(bf16)
    hidden = dense(normed_low, up_weight)
    active, active_back = jax.vjp(gelu_tanh, hidden)
    active_low = active.astype(bf16)
    return (
        resid + dense(active_low, down_weight),
        (norm_back, normed_low, active_back, active_low),
    )


def feed_back(stored, up_weight, down_weight, upstream):
    norm_back, normed_low, active_back, active_low = stored
    into_active, down_grad = dense_back(active_low, down_weight, upstream.astype(bf16))
    (into_hidden,) = active_back(into_active)
    into_normed, up_grad = dense_back(normed_low, up_weight, into_hidden.astype(bf16))
    into_resid, gain_grad = norm_back(into_normed)
    return (upstream + into_resid, gain_grad, up_grad, down_grad)


def fold_rows(weight, share):
    rows, width = weight.shape
    fold = rows // share
    return weight.reshape(fold, share, width).transpose(1, 0, 2).reshape(share, fold * width)


def unfold_rows(folded, fold, share):
    rows, width = folded.shape
    width //= fold
    parts = folded.reshape(rows // share, share, fold, width).transpose(0, 2, 1, 3)
    return parts.reshape(rows * fold, width)


def fold_all(weight, share, rows):
    tall, width = weight.shape
    fold = tall // rows
    parts = weight.reshape(rows // share, fold, share, width).transpose(0, 2, 1, 3)
    return parts.reshape(rows, fold * width)


def group_columns(weight, groups, padded):
    rows, columns = weight.shape
    part = columns // 3 // groups
    grouped = weight.reshape(rows, 3, groups, part).transpose(0, 2, 1, 3).reshape(rows, groups, 3 * part)
    return jnp.pad(grouped, ((0, 0), (0, 0), (0, padded - 3 * part))).reshape(rows, groups * padded)


def pad_groups(weight, groups, padded):
    rows, columns = weight.shape
    part = rows // groups
    grouped = weight.reshape(groups, part, columns)
    return jnp.pad(grouped, ((0, 0), (0, padded - part), (0, 0))).reshape(groups * padded, columns)


def ungroup_columns(grouped, groups, padded, columns):
    rows = grouped.shape[0]
    part = columns // 3 // groups
    parts = grouped.reshape(rows, groups, padded)[:, :, : 3 * part].reshape(rows, groups, 3, part)
    return parts.transpose(0, 2, 1, 3).reshape(rows, columns)


def cut(array, widths):
    pieces, start = [], 0
    for width in widths:
        pieces.append(array[:, start : start + width])
        start += width
    return pieces


def cut_last(array, count):
    width = array.shape[-1] // count
    return [array[..., i * width : (i + 1) * width] for i in range(count)]


def gathered(parts):
    whole = lax.all_gather(jnp.concatenate(parts, axis=1), everyone, axis=0, tiled=True)
    return cut(whole, [p.shape[1] for p in parts])


def scattered(parts):
    mine = lax.psum_scatter(
        jnp.concatenate(parts, axis=1), everyone, scatter_dimension=0, tiled=True
    )
    return cut(mine, [p.shape[1] for p in parts])


def body(
    tokens,
    cotangent,
    lengths,
    mixer_gain,
    mixer_inputs,
    shift_taps,
    decay_rate,
    state_in,
    state_out,
    state_skip,
    mixer_output,
    first_gain,
    first_up,
    first_down,
    attend_gain,
    attend_inputs,
    attend_output,
    second_gain,
    second_up,
    second_down,
):
    seq_count, block_len, model_width = tokens.shape
    row_count = seq_count * block_len
    seq_devices = lax.axis_size("seq")
    share = mixer_inputs.shape[0]
    states, reach = decay_rate.shape[1], shift_taps.shape[1]
    fold = first_down.shape[0] // share
    deals = seq_count * HEADS
    dealt = deals % seq_devices == 0 and HEADS % (deals // seq_devices) == 0
    heads = deals // seq_devices if dealt else HEADS
    groups = HEADS // heads
    group_width = heads * HEAD_DIM
    padded = -(-3 * group_width // lanes) * lanes if dealt else 3 * group_width
    out_width = -(-group_width // lanes) * lanes if dealt else group_width

    columns = [decay_rate, state_in, state_out, shift_taps]
    columns += [g[:, None] for g in (mixer_gain, first_gain, attend_gain, second_gain, state_skip)]
    small = jnp.concatenate(columns, axis=1)
    small_count = small.shape[1]
    small_width = -(-small_count // lanes) * lanes
    small = jnp.pad(small, ((0, 0), (0, small_width - small_count)))
    attend_cols = attend_inputs.shape[1]
    grouped = group_columns(attend_inputs, groups, padded)
    by_kernel = seq_devices == 8 and lax.axis_size("batch") == 4
    packed = [mixer_output, attend_output, first_up, second_up, grouped]
    up1_at = 2 * model_width
    up2_at = up1_at + first_up.shape[1]
    if by_kernel:
        joint = jnp.concatenate([mixer_inputs, small], axis=1)
        w_packed = lax.all_gather(jnp.concatenate(packed, axis=1), everyone, axis=0, tiled=True)
        w_mixer_out, w_attend_out, _, _, w_attend_in = cut(w_packed, [p.shape[1] for p in packed])
        widths = (joint.shape[1], model_width)
        w_joint, w_down1 = gather_blocks((joint, first_down), chunked(widths, (4, 6), ("zxy", "zyx")), gap=3)
        w_mixer_in, w_small = cut(w_joint, [mixer_inputs.shape[1], small_width])
        second_down, w_small = lax.optimization_barrier((second_down, w_small))
        w_down2 = lax.all_gather(second_down, everyone, axis=0, tiled=True)
    else:
        w_mixer_in, w_small = gathered([mixer_inputs, small])
        packed += [fold_rows(first_down, share), fold_rows(second_down, share)]
        w_mixer_out, w_attend_out, w_up1, w_up2, w_attend_in, w_down1, w_down2 = gathered(packed)
        w_down1 = unfold_rows(w_down1, fold, share)
        w_down2 = unfold_rows(w_down2, fold, share)

    rows = w_small.T.astype(f32)
    decay, table_in, table_out = rows[:states], rows[states : 2 * states], rows[2 * states : 3 * states]
    taps_rows = rows[3 * states : 3 * states + reach]
    gain_mixer, gain_first, gain_attend, gain_second, skip = (
        rows[3 * states + reach + i] for i in range(5)
    )
    taps = taps_rows.T
    weight = table_in * table_out

    rank_seq = lax.axis_index("seq")
    offsets = jnp.arange(block_len, dtype=jnp.int32)
    places = rank_seq * block_len + offsets
    valid = (places[None, :] < lengths[:, None]).astype(f32)
    longest = jnp.max(lengths)
    any_live = places[0] < longest

    start_resid = tokens.reshape(row_count, model_width).astype(f32)
    normed_mixer, back_mixer = jax.vjp(layer_norm, start_resid, gain_mixer)
    normed_low_mixer = normed_mixer.astype(bf16)
    projected = dense(normed_low_mixer, w_mixer_in).reshape(seq_count, block_len, 3 * model_width)
    query_mixer = projected[:, :, :model_width]
    keys_mixer = projected[:, :, model_width : 2 * model_width]
    value_mixer = projected[:, :, 2 * model_width :]
    rim_rows = passed_along(keys_mixer[:, block_len - reach + 1 :], "seq", 1)
    extended = jnp.concatenate([rim_rows, keys_mixer], axis=1)
    inner, shift_back = jax.vjp(shift_mix, extended, taps, value_mixer)
    if by_kernel:
        carried = carried_by_kernel(inner, decay, False, 2)
    else:
        carried = carried_in(encode(inner, decay, False), decay, block_len, False)
    wide = shaped(seq_count, block_len, model_width)
    state_y, gated = per_lane_tile(
        output_kernel,
        (inner, query_mixer, carried, decay, weight, skip[None]),
        (wide, wide),
    )
    gated_low = gated.astype(bf16).reshape(row_count, model_width)
    resid_mixer = start_resid + dense(gated_low, w_mixer_out)
    if by_kernel:
        resid_first, stored_first = feed_forward_blocks(
            resid_mixer, gain_first, w_packed, up1_at, w_down1
        )
    else:
        resid_first, stored_first = feed_forward(resid_mixer, gain_first, w_up1, w_down1)

    normed_attend, back_attend = jax.vjp(layer_norm, resid_first, gain_attend)
    normed_low_attend = normed_attend.astype(bf16)
    proj_low = dense(normed_low_attend, w_attend_in).astype(bf16)
    if dealt:
        length = seq_devices * block_len
        block = min(256, length)

        def deal(array, width):
            array = array.reshape(seq_count, block_len, groups * width)
            parts = jnp.stack(cut_last(array, groups), axis=1)
            parts = parts.reshape(seq_count * groups, block_len, width)
            dealt_parts = lax.all_to_all(parts, "seq", split_axis=0, concat_axis=0, tiled=True)
            return dealt_parts.reshape(length, width)

        def collect(array, width):
            parts = array.reshape(seq_devices, block_len, width)
            back = lax.all_to_all(parts, "seq", split_axis=0, concat_axis=0, tiled=True)
            back = back.reshape(seq_count, groups, block_len, width)
            back = jnp.concatenate([back[:, group] for group in range(groups)], axis=-1)
            return back.reshape(row_count, groups * width)

        qkv = deal(proj_low, padded)
        attended_part, attended_full, stat = attend_whole(qkv, heads, block)
        attended_low = collect(attended_part, out_width)
        w_attend_out = pad_groups(w_attend_out, groups, out_width)
    else:
        attended, attended_back = general_attention(
            proj_low, seq_count, block_len, places, any_live, longest
        )
        attended_low = attended.reshape(row_count, model_width).astype(bf16)
    resid_attend = resid_first + dense(attended_low, w_attend_out)
    if by_kernel:
        final, stored_second = feed_forward_blocks(
            resid_attend, gain_second, w_packed, up2_at, w_down2
        )
    else:
        final, stored_second = feed_forward(resid_attend, gain_second, w_up2, w_down2)
    mixed = (final.reshape(seq_count, block_len, model_width) * valid[..., None]).astype(bf16)

    upstream = (cotangent.astype(f32) * valid[..., None]).reshape(row_count, model_width)
    if by_kernel:
        upstream, second_gain_grad, early = feed_back_blocks(
            stored_second, w_packed, up2_at, w_down2, upstream, packed=(share, fold)
        )
    else:
        upstream, second_gain_grad, second_up_grad, second_down_grad = feed_back(
            stored_second, w_up2, w_down2, upstream
        )
        early = [second_up_grad, fold_all(second_down_grad, share, model_width)]
        early = jnp.concatenate(early, axis=1)
    into_attended, attend_output_grad = dense_back(
        attended_low, w_attend_out, upstream.astype(bf16)
    )
    if dealt:
        attend_output_grad = attend_output_grad.reshape(groups, out_width, model_width)
        attend_output_grad = attend_output_grad[:, :group_width].reshape(model_width, model_width)
    dout_low = into_attended.astype(bf16)
    if dealt:
        dout = deal(dout_low, out_width)
        qkv_grad = attend_whole_back(qkv, dout, attended_full, stat, heads, block)
        qkv_grad, early = lax.optimization_barrier((qkv_grad, early))
        proj_grad = collect(qkv_grad, padded)
    else:
        parts = attended_back(dout_low.reshape(seq_count, block_len, HEADS, HEAD_DIM))
        proj_grad = jnp.concatenate(
            [p.reshape(row_count, model_width) for p in parts], axis=1
        ).astype(bf16)
    early = lax.psum_scatter(early, everyone, scatter_dimension=0, tiled=True)
    second_up_out, second_down_out = cut(early, [second_up.shape[1], fold * model_width])
    into_normed, attend_inputs_grad = dense_back(normed_low_attend, w_attend_in, proj_grad)
    into_resid, attend_gain_grad = back_attend(into_normed)
    upstream = upstream + into_resid
    if by_kernel:
        upstream, first_gain_grad, first_up_grad, first_down_grad = feed_back_blocks(
            stored_first, w_packed, up1_at, w_down1, upstream
        )
    else:
        upstream, first_gain_grad, first_up_grad, first_down_grad = feed_back(
            stored_first, w_up1, w_down1, upstream
        )
    into_gated, mixer_output_grad = dense_back(gated_low, w_mixer_out, upstream.astype(bf16))
    into_gated = into_gated.reshape(seq_count, block_len, model_width)
    query_mixer_grad = into_gated * state_y
    state_grad = into_gated * query_mixer
    table = shaped(states, model_width)
    gains_at = 3 * states + reach
    table_edges = [0, states, 2 * states, 3 * states, gains_at, small_width]

    def tables_of(block):
        return [block[:, a:b] for a, b in zip(table_edges, table_edges[1:])]

    orders = ("yxz", "xyz", "xzy", "yxz", "xyz", "yzx")
    if by_kernel:
        main = [attend_inputs_grad, first_up_grad, mixer_output_grad, first_down_grad, attend_output_grad]
        plan = chunked([g.shape[1] for g in main], (4, 4, 2, 4, 2), orders)
        part = attend_cols // 3 // groups

        def finish(index, block, results):
            if index > 0:
                results[index][...] = block[...]
                return
            for group in range(groups):
                for kind in range(3):
                    start = (kind * groups + group) * part
                    source = group * padded + kind * part
                    results[0][:, start : start + part] = block[:, source : source + part]

        results = [shaped(share, w) for w in (attend_cols, first_up.shape[1], model_width)]
        results += [shaped(share * fold, model_width), shaped(share, model_width)]
        parts = pltpu.VMEM((seq_devices, seq_count * states // seq_devices, model_width), bf16)
        exchange_sems = pltpu.SemaphoreType.DMA((2, seq_devices - 1))
        work = (
            state_back_work,
            (inner, state_grad, carried, decay, weight, skip[None]),
            (wide, table, table, shaped(1, model_width)),
            (
                pltpu.VMEM((seq_count, states, model_width), f32),
                pltpu.VMEM((seq_count, states, lanes), f32),
                parts,
                parts,
                parts,
                parts,
                pltpu.VMEM((block_len, seq_count, states, lanes), f32),
                exchange_sems,
                exchange_sems,
            ),
        )
        scattered_main = scatter_blocks(main, plan, finish, results, gap=4, work=work)
        attend_inputs_out, first_up_out, mixer_output_out, first_down_out, attend_output_out = scattered_main[:5]
        inner_grad, weight_grad, power_grad, skip_grad = scattered_main[5:]
    else:
        later = carried_in(encode(state_grad, decay, True), decay, block_len, True)
        inner_grad, weight_grad, power_grad, skip_grad = per_lane_tile(
            back_kernel,
            (inner, state_grad, carried, later, decay, weight, skip[None]),
            (wide, table, table, shaped(1, model_width)),
            scratch=[pltpu.VMEM((block_len, seq_count, states, lanes), f32)],
        )
    extended_grad, taps_grad, value_mixer_grad = shift_back(inner_grad)
    spill = passed_along(extended_grad[:, : reach - 1], "seq", -1)
    keys_mixer_grad = extended_grad[:, reach - 1 :] + jnp.pad(
        spill, ((0, 0), (block_len - reach + 1, 0), (0, 0))
    )
    proj_grad_mixer = (
        jnp.concatenate([query_mixer_grad, keys_mixer_grad, value_mixer_grad], axis=2)
        .astype(bf16)
        .reshape(row_count, 3 * model_width)
    )
    into_normed_mixer, mixer_inputs_grad = dense_back(normed_low_mixer, w_mixer_in, proj_grad_mixer)
    into_start, mixer_gain_grad = back_mixer(into_normed_mixer)
    tokens_gradient = (upstream + into_start).reshape(seq_count, block_len, model_width).astype(bf16)

    small_rows = jnp.concatenate(
        [-jnp.exp(-decay) * power_grad, weight_grad * table_out, weight_grad * table_in, taps_grad.T]
        + [
            g[None]
            for g in (mixer_gain_grad, first_gain_grad, attend_gain_grad, second_gain_grad, skip_grad[0])
        ],
        axis=0,
    )
    small_grad = jnp.pad(small_rows, ((0, small_width - small_count), (0, 0))).T.astype(bf16)
    def unfolded(folded):
        return folded.reshape(share, fold, model_width).transpose(1, 0, 2).reshape(share * fold, model_width)

    if by_kernel:
        plan = chunked((mixer_inputs_grad.shape[1], small_width), (4, 2), orders)

        def finish_small(index, block, results):
            for result, piece in zip(results[1:] if index else results[:1], tables_of(block) if index else [block]):
                result[...] = piece[...]

        results = [shaped(share, mixer_inputs_grad.shape[1])]
        results += [shaped(share, b - a) for a, b in zip(table_edges, table_edges[1:])]
        mixer_inputs_out, *tables = scatter_blocks(
            [mixer_inputs_grad, small_grad], plan, finish_small, results, gap=2, collective=4
        )
    else:
        last = [attend_inputs_grad, first_up_grad, mixer_output_grad, mixer_inputs_grad, small_grad]
        last += [fold_all(first_down_grad, share, model_width), attend_output_grad]
        *last, folded, attend_output_out = scattered(last)
        first_down_out = unfolded(folded).astype(f32)
        grouped, first_up_out, mixer_output_out, mixer_inputs_out, small_out = (
            g.astype(f32) for g in last
        )
        attend_inputs_out = ungroup_columns(grouped, groups, padded, attend_cols)
        tables = tables_of(small_out)
    decay_out, in_out, out_out, taps_out, vectors = tables

    return (
        mixed,
        tokens_gradient,
        vectors[:, 0],
        mixer_inputs_out,
        taps_out,
        decay_out,
        in_out,
        out_out,
        vectors[:, 4],
        mixer_output_out,
        vectors[:, 1],
        first_up_out,
        first_down_out,
        vectors[:, 2],
        attend_inputs_out,
        attend_output_out.astype(f32),
        vectors[:, 3],
        second_up_out.astype(f32),
        unfolded(second_down_out).astype(f32),
    )


def solution(mesh):
    return jax.shard_map(
        body,
        mesh=mesh,
        in_specs=(
            P("batch", "seq", None),
            P("batch", "seq", None),
            P("batch"),
            P(("seq", "batch")),
            P(("seq", "batch"), None),
            P(("seq", "batch"), None),
            P(("seq", "batch"), None),
            P(("seq", "batch"), None),
            P(("seq", "batch"), None),
            P(("seq", "batch")),
            P(("seq", "batch"), None),
            P(("seq", "batch")),
            P(("seq", "batch"), None),
            P(("seq", "batch"), None),
            P(("seq", "batch")),
            P(("seq", "batch"), None),
            P(("seq", "batch"), None),
            P(("seq", "batch")),
            P(("seq", "batch"), None),
            P(("seq", "batch"), None),
        ),
        out_specs=(
            P("batch", "seq", None),
            P("batch", "seq", None),
            P(("seq", "batch")),
            P(("seq", "batch"), None),
            P(("seq", "batch"), None),
            P(("seq", "batch"), None),
            P(("seq", "batch"), None),
            P(("seq", "batch"), None),
            P(("seq", "batch")),
            P(("seq", "batch"), None),
            P(("seq", "batch")),
            P(("seq", "batch"), None),
            P(("seq", "batch"), None),
            P(("seq", "batch")),
            P(("seq", "batch"), None),
            P(("seq", "batch"), None),
            P(("seq", "batch")),
            P(("seq", "batch"), None),
            P(("seq", "batch"), None),
        ),
        check_vma=False,
    )
```

```python
import functools

import jax
import jax.numpy as jnp
from jax import lax
from jax.experimental import pallas as pl
from jax.experimental.pallas import tpu as pltpu
from jax.sharding import PartitionSpec as P

HEADS = 12
HEAD_DIM = 64

eps = 1e-05
masked_score = -1e30
lanes = 128
sublanes = 8
everyone = ("seq", "batch")
f32 = jnp.float32
bf16 = jnp.bfloat16


def rows_of(ref, seq, block):
    return ref[seq, pl.ds(pl.multiple_of(block * sublanes, sublanes), sublanes), :]


def spread(rows, index, count):
    return jnp.broadcast_to(rows[index : index + 1], (count, lanes))


def encode_kernel(reverse, input_ref, decay_ref, end_ref):
    seq_count, step_count, _ = input_ref.shape
    state_count = decay_ref.shape[0]
    blocks = step_count // sublanes
    power = jnp.exp(-decay_ref[...])

    def one_block(step, states):
        block = blocks - 1 - step if reverse else step
        rows = [rows_of(input_ref, seq, block) for seq in range(seq_count)]
        order = range(sublanes - 1, -1, -1) if reverse else range(sublanes)
        states = list(states)
        for index in order:
            for seq in range(seq_count):
                states[seq] = states[seq] * power + spread(rows[seq], index, state_count)
        return tuple(states)

    start = tuple(jnp.zeros((state_count, lanes), f32) for _ in range(seq_count))
    ends = lax.fori_loop(0, blocks, one_block, start)
    for seq in range(seq_count):
        end_ref[seq] = ends[seq]


def output_kernel(input_ref, query_ref, carried_ref, decay_ref, weight_ref, skip_ref, out_ref, gated_ref):
    seq_count, step_count, _ = input_ref.shape
    state_count = decay_ref.shape[0]
    power = jnp.exp(-decay_ref[...])
    weight = weight_ref[...]
    skip = skip_ref[...]

    def one_block(block, states):
        states = list(states)
        rows = [rows_of(input_ref, seq, block) for seq in range(seq_count)]
        found = [[] for _ in range(seq_count)]
        for index in range(sublanes):
            for seq in range(seq_count):
                states[seq] = states[seq] * power + spread(rows[seq], index, state_count)
                found[seq].append(jnp.sum(states[seq] * weight, axis=0, keepdims=True))
        place = pl.ds(pl.multiple_of(block * sublanes, sublanes), sublanes)
        for seq in range(seq_count):
            result = jnp.concatenate(found[seq], axis=0) + skip * rows[seq]
            out_ref[seq, place, :] = result
            gated_ref[seq, place, :] = result * rows_of(query_ref, seq, block)
        return tuple(states)

    start = tuple(carried_ref[seq].astype(f32) for seq in range(seq_count))
    lax.fori_loop(0, step_count // sublanes, one_block, start)


def back_kernel(
    input_ref,
    grad_ref,
    carried_ref,
    later_ref,
    decay_ref,
    weight_ref,
    skip_ref,
    input_grad_ref,
    weight_grad_ref,
    power_grad_ref,
    skip_grad_ref,
    held,
):
    seq_count, step_count, _ = input_ref.shape
    state_count = decay_ref.shape[0]
    blocks = step_count // sublanes
    power = jnp.exp(-decay_ref[...])
    weight = weight_ref[...]
    skip = skip_ref[...]
    seqs = range(seq_count)

    def forward_block(block, state):
        states, total, skip_total = list(state[0]), state[1], state[2]
        rows = [rows_of(input_ref, seq, block) for seq in seqs]
        grads = [rows_of(grad_ref, seq, block) for seq in seqs]
        for index in range(sublanes):
            for seq in seqs:
                held[block * sublanes + index, seq] = states[seq]
                states[seq] = states[seq] * power + spread(rows[seq], index, state_count)
                total = total + states[seq] * spread(grads[seq], index, state_count)
        for seq in seqs:
            skip_total = skip_total + rows[seq] * grads[seq]
        return (tuple(states), total, skip_total)

    zeros = jnp.zeros((state_count, lanes), f32)
    _, total, skip_total = lax.fori_loop(
        0,
        blocks,
        forward_block,
        (
            tuple(carried_ref[seq].astype(f32) for seq in seqs),
            zeros,
            jnp.zeros((sublanes, lanes), f32),
        ),
    )
    weight_grad_ref[...] = total
    skip_grad_ref[...] = jnp.sum(skip_total, axis=0, keepdims=True)

    def back_block(step, state):
        states, total = list(state[0]), state[1]
        block = blocks - 1 - step
        grads = [rows_of(grad_ref, seq, block) for seq in seqs]
        found = [[None] * sublanes for _ in seqs]
        for index in range(sublanes - 1, -1, -1):
            for seq in seqs:
                states[seq] = states[seq] * power + spread(grads[seq], index, state_count)
                found[seq][index] = jnp.sum(states[seq] * weight, axis=0, keepdims=True)
                total = total + states[seq] * held[block * sublanes + index, seq]
        place = pl.ds(pl.multiple_of(block * sublanes, sublanes), sublanes)
        for seq in seqs:
            input_grad_ref[seq, place, :] = jnp.concatenate(found[seq], axis=0) + skip * grads[seq]
        return (tuple(states), total)

    _, total = lax.fori_loop(
        0, blocks, back_block, (tuple(later_ref[seq].astype(f32) for seq in seqs), zeros)
    )
    power_grad_ref[...] = total * weight


def per_lane_tile(kernel, args, outs, scratch=(), flops=0):
    def spec(shape):
        lead = len(shape) - 1
        return pl.BlockSpec(tuple(shape[:-1]) + (lanes,), lambda tile: (0,) * lead + (tile,))

    bytes_moved = sum(a.size * a.dtype.itemsize for a in args)
    return pl.pallas_call(
        kernel,
        grid=(args[0].shape[-1] // lanes,),
        in_specs=[spec(a.shape) for a in args],
        out_specs=[spec(o.shape) for o in outs],
        out_shape=list(outs),
        scratch_shapes=list(scratch),
        cost_estimate=pl.CostEstimate(flops=flops, bytes_accessed=bytes_moved, transcendentals=0),
        compiler_params=pltpu.CompilerParams(vmem_limit_bytes=48 * 1024 * 1024),
    )(*args)


def shaped(*dims, dtype=f32):
    return jax.ShapeDtypeStruct(dims, dtype)


def encode(value, decay, reverse):
    seq_count, _, width = value.shape
    (ends,) = per_lane_tile(
        functools.partial(encode_kernel, reverse),
        (value, decay),
        (shaped(seq_count, decay.shape[0], width),),
    )
    return ends


def passed_along(block, axis, distance):
    devices = range(lax.axis_size(axis))
    route = [(i - distance, i) for i in devices if i - distance in devices]
    return lax.ppermute(block, axis, route)


def carried_in(ends, decay, block_len, reverse):
    seq_count, state_count, width = ends.shape
    count = lax.axis_size("seq")
    part = state_count // count

    def exchanged(parts):
        return lax.all_to_all(parts.astype(bf16), "seq", split_axis=0, concat_axis=0, tiled=True)

    parts = ends.reshape(seq_count, count, part, width).transpose(1, 0, 2, 3)
    arrived = exchanged(parts.reshape(count, seq_count * part, width)).astype(f32)
    rates = lax.dynamic_slice_in_dim(decay, lax.axis_index("seq") * part, part, 0)
    power = jnp.tile(jnp.exp(-rates * block_len), (seq_count, 1))
    state, joined = jnp.zeros_like(arrived[0]), [None] * count
    for block in reversed(range(count)) if reverse else range(count):
        joined[block] = state
        state = power * state + arrived[block]
    back = exchanged(jnp.stack(joined))
    back = back.reshape(count, seq_count, part, width).transpose(1, 0, 2, 3)
    return back.reshape(seq_count, state_count, width)


MESH = pl.DeviceIdType.MESH
box = (4, 2, 2, 2)


def here():
    seq, batch = lax.axis_index("seq"), lax.axis_index("batch")
    return lax.div(seq, 2), lax.rem(seq, 2), lax.div(batch, 2), lax.rem(batch, 2)


def device(z, x, y, core):
    return (2 * z + x, 2 * y + core)


def line_peer(z, step):
    return lax.rem(z + step, box[0])


def greet(diagonal=False):
    z, x, y, core = here()
    barrier = pltpu.get_barrier_semaphore()
    peers = [device(line_peer(z, step), x, y, core) for step in range(1, box[0])]
    peers += [device(z, 1 - x, y, core), device(z, x, 1 - y, core), device(z, x, y, 1 - core)]
    if diagonal:
        peers += [device(line_peer(z, step), 1 - x, y, core) for step in range(1, box[0])]
    for peer in peers:
        pl.semaphore_signal(barrier, inc=1, device_id=peer, device_id_type=MESH)
    pl.semaphore_wait(barrier, len(peers))


def staggered(count, stages, gap):
    for turn in range(count + gap * (stages - 1)):
        for stage in reversed(range(stages)):
            chunk = turn - gap * stage
            if 0 <= chunk < count:
                yield stage, chunk


def gather_kernel(plan, gap, *refs):
    count = 1 + max(item[0] for item in plan)
    ins, outs = refs[:count], refs[count : 2 * count]
    send, receive, local = refs[2 * count :]
    z, x, y, core = here()
    greet()
    started = {}

    def push(chunk, slot, source, target, peer):
        copy = pltpu.make_async_remote_copy(
            src_ref=source,
            dst_ref=target,
            send_sem=send.at[chunk, slot],
            recv_sem=receive.at[chunk, slot],
            device_id=peer,
            device_id_type=MESH,
        )
        copy.start()
        started[chunk, slot] = copy

    own = []
    for chunk, (index, first, width, _) in enumerate(plan):
        columns = pl.ds(first, width)
        source = ins[index].at[:, columns]
        target = outs[index].at[z, x, y, core, :, columns]
        for step in range(1, box[0]):
            push(chunk, step - 1, source, target, device(line_peer(z, step), x, y, core))
        keep = pltpu.make_async_copy(source, target, local.at[chunk])
        keep.start()
        own.append(keep)

    for stage, chunk in staggered(len(plan), 3, gap):
        index, first, width, order = plan[chunk]
        x_first = order[1] == "x"
        columns = pl.ds(first, width)
        out = outs[index]
        if stage == 0:
            for step in range(1, box[0]):
                started[chunk, step - 1].wait_recv()
            own[chunk].wait()
            part = out.at[:, x, y, core, :, columns]
            peer = device(z, 1 - x, y, core) if x_first else device(z, x, 1 - y, core)
            push(chunk, 3, part, part, peer)
        elif stage == 1:
            started[chunk, 3].wait_recv()
            if x_first:
                part, peer = out.at[:, :, y, core, :, columns], device(z, x, 1 - y, core)
            else:
                part, peer = out.at[:, x, :, core, :, columns], device(z, 1 - x, y, core)
            push(chunk, 4, part, part, peer)
        else:
            started[chunk, 4].wait_recv()
            part = out.at[:, :, :, core, :, columns]
            push(chunk, 5, part, part, device(z, x, y, 1 - core))
    for chunk in range(len(plan)):
        started[chunk, 5].wait_recv()
        for slot in range(6):
            started[chunk, slot].wait_send()


def gather_blocks(blocks, plan, gap=2, collective=0):
    outs = [jax.ShapeDtypeStruct(box + b.shape, b.dtype) for b in blocks]
    sent = sum(b.size * b.dtype.itemsize for b in blocks)
    whole = pl.pallas_call(
        functools.partial(gather_kernel, plan, gap),
        out_shape=outs,
        in_specs=[pl.BlockSpec(memory_space=pltpu.VMEM)] * len(blocks),
        out_specs=[pl.BlockSpec(memory_space=pl.ANY)] * len(blocks),
        scratch_shapes=[
            pltpu.SemaphoreType.DMA((len(plan), 6)),
            pltpu.SemaphoreType.DMA((len(plan), 6)),
            pltpu.SemaphoreType.DMA((len(plan),)),
        ],
        cost_estimate=pl.CostEstimate(flops=0, bytes_accessed=64 * sent, transcendentals=0),
        compiler_params=pltpu.CompilerParams(collective_id=collective, has_side_effects=True),
    )(*blocks)
    return [w.reshape((32 * w.shape[4], w.shape[5])) for w in whole]


def add_into(total, other):
    return (total.astype(f32) + other.astype(f32)).astype(bf16)


def scatter_kernel(plan, gap, finish, beside, counts, *refs):
    count, out_count, work_ins, work_outs, work_scratch = counts
    refs, taken = list(refs), []
    for number in (count, work_ins, out_count, work_outs, count, work_scratch):
        taken.append(refs[:number])
        refs = refs[number:]
    ins, work_in_refs, results, work_out_refs, outs, work_refs = taken
    buffers, (send, receive, local) = refs[:-3], refs[-3:]
    z, x, y, core = here()
    greet(diagonal=beside is not None)
    work = list(beside(*work_in_refs, *work_out_refs, *work_refs)) if beside else []
    started = {}

    def push(chunk, slot, source, target, peer):
        copy = pltpu.make_async_remote_copy(
            src_ref=source,
            dst_ref=target,
            send_sem=send.at[chunk, slot],
            recv_sem=receive.at[chunk, slot],
            device_id=peer,
            device_id_type=MESH,
        )
        copy.start()
        started[chunk, slot] = copy

    loads = []
    for chunk, (index, first, width, _) in enumerate(plan):
        columns = pl.ds(first, width)
        held, from_core = buffers[5 * chunk : 5 * chunk + 2]
        grad = ins[index]
        push(chunk, 0, grad.at[:, :, :, 1 - core, :, columns], from_core, device(z, x, y, 1 - core))
        load = pltpu.make_async_copy(grad.at[:, :, :, core, :, columns], held, local.at[chunk])
        load.start()
        loads.append(load)

    steps, pieces = list(staggered(len(plan), 4, gap)), len(work)
    for turn, (stage, chunk) in enumerate(steps):
        while work and turn >= work_starts[pieces - len(work)] * len(steps) // 100:
            work.pop(0)()
        index, first, width, order = plan[chunk]
        x_first, line_last = order[0] == "y", order[-1] == "z"
        held, from_core, from_one, from_two, from_line = buffers[5 * chunk : 5 * chunk + 5]
        to_x, to_y = device(z, 1 - x, y, core), device(z, x, 1 - y, core)
        if stage == 0:
            started[chunk, 0].wait_recv()
            loads[chunk].wait()

            @pl.loop(0, 4 * box[0])
            def _(turn):
                at = (lax.div(turn, 4), lax.rem(lax.div(turn, 2), 2), lax.rem(turn, 2))
                held[at] = add_into(held[at], from_core[at])

            if x_first:
                push(chunk, 1, held.at[:, :, 1 - y], from_one, to_y)
            else:
                push(chunk, 1, held.at[:, 1 - x], from_one, to_x)
        elif stage == 1:
            started[chunk, 1].wait_recv()

            @pl.loop(0, 2 * box[0])
            def _(turn):
                row, i = lax.div(turn, 2), lax.rem(turn, 2)
                at = (row, i, y) if x_first else (row, x, i)
                held[at] = add_into(held[at], from_one[row, i])

            if not line_last:
                for step in range(1, box[0]):
                    peer = line_peer(z, step)
                    rest = held.at[peer, :, y] if x_first else held.at[peer, x]
                    push(chunk, 2 + step, rest, from_line.at[step - 1], device(peer, x, y, core))
            elif x_first:
                push(chunk, 2, held.at[:, 1 - x, y], from_two, to_x)
            else:
                push(chunk, 2, held.at[:, x, 1 - y], from_two, to_y)
        elif stage == 2 and not line_last:
            for step in range(1, box[0]):
                started[chunk, 2 + step].wait_recv()
            for i in range(2):
                at = (z, i, y) if x_first else (z, x, i)
                total = held[at].astype(f32)
                for step in range(1, box[0]):
                    total = total + from_line[step - 1, i].astype(f32)
                held[at] = total.astype(bf16)
            if x_first:
                push(chunk, 2, held.at[z, 1 - x, y], from_two, to_x)
            else:
                push(chunk, 2, held.at[z, x, 1 - y], from_two, to_y)
        elif stage == 2:
            started[chunk, 2].wait_recv()

            @pl.loop(0, box[0])
            def _(row):
                held[row, x, y] = add_into(held[row, x, y], from_two[row])

            for step in range(1, box[0]):
                peer = line_peer(z, step)
                push(chunk, 2 + step, held.at[peer, x, y], from_line.at[step - 1], device(peer, x, y, core))
        else:
            total = held[z, x, y].astype(f32)
            if line_last:
                for step in range(1, box[0]):
                    started[chunk, 2 + step].wait_recv()
                    total = total + from_line[step - 1].astype(f32)
            else:
                started[chunk, 2].wait_recv()
                total = total + from_two[...].astype(f32)
            outs[index][:, pl.ds(first, width)] = total
            if not any(item[0] == index for item in plan[chunk + 1 :]):
                finish(index, outs[index], results)
    for chunk in range(len(plan)):
        for slot in range(6):
            started[chunk, slot].wait_send()


def scatter_blocks(grads, plan, finish, results, gap=2, collective=1, work=None):
    views = [g.reshape(box + (g.shape[0] // 32, g.shape[1])) for g in grads]
    beside, work_ins, work_outs, work_scratch = work or (None, [], [], [])
    scratch = [pltpu.VMEM(v.shape[4:], f32) for v in views] + list(work_scratch)
    for index, _, width, order in plan:
        tile = (views[index].shape[4], width)
        ends_of = ((4,), (3,)) if order[-1] == "z" else ((), (3, 2))
        for lead in ((4, 2, 2), (4, 2, 2), (4, 2)) + ends_of:
            scratch.append(pltpu.VMEM(lead + tile, bf16))
    counts = (len(views), len(results), len(work_ins), len(work_outs), len(work_scratch))
    sent = sum(v.size * v.dtype.itemsize for v in views)
    local = pl.BlockSpec(memory_space=pltpu.VMEM)
    return pl.pallas_call(
        functools.partial(scatter_kernel, plan, gap, finish, beside, counts),
        out_shape=list(results) + list(work_outs),
        in_specs=[pl.BlockSpec(memory_space=pl.ANY)] * len(views) + [local] * len(work_ins),
        out_specs=[local] * (len(results) + len(work_outs)),
        scratch_shapes=scratch
        + [
            pltpu.SemaphoreType.DMA((len(plan), 6)),
            pltpu.SemaphoreType.DMA((len(plan), 6)),
            pltpu.SemaphoreType.DMA((len(plan),)),
        ],
        cost_estimate=pl.CostEstimate(flops=0, bytes_accessed=4 * sent, transcendentals=0),
        compiler_params=pltpu.CompilerParams(
            collective_id=collective, has_side_effects=True, vmem_limit_bytes=60 * 1024 * 1024
        ),
    )(*views, *work_ins)


def chunked(widths, pieces, orders):
    plan = []
    for index, (width, number) in enumerate(zip(widths, pieces)):
        tiles = width // lanes
        edges = [tiles * i // number for i in range(number + 1)]
        for i in range(number):
            plan.append((index, edges[i] * lanes, (edges[i + 1] - edges[i]) * lanes, orders[len(plan) % len(orders)]))
    return plan


def carry_pieces(
    reverse, input_ref, decay_ref, carried_ref, ends, outgoing, arrived, joined, final, send, receive
):
    seq_count, step_count, width = input_ref.shape
    count = lax.axis_size("seq")
    part = decay_ref.shape[0] // count
    me, batch = lax.axis_index("seq"), lax.axis_index("batch")

    def encode_all():
        @pl.loop(0, width // lanes)
        def _(tile):
            columns = pl.ds(pl.multiple_of(tile * lanes, lanes), lanes)
            encode_kernel(reverse, input_ref.at[:, :, columns], decay_ref.at[:, columns], ends)
            for group in range(count):
                rows = slice(group * part, (group + 1) * part)
                mine = jnp.concatenate([ends[seq, rows] for seq in range(seq_count)], axis=0)
                outgoing[group, :, columns] = mine.astype(bf16)

    def started(phase, source, target):
        copies = []
        for step in range(1, count):
            peer = lax.rem(me + step, count)
            copy = pltpu.make_async_remote_copy(
                src_ref=source.at[peer],
                dst_ref=target.at[me],
                send_sem=send.at[phase, step - 1],
                recv_sem=receive.at[phase, step - 1],
                device_id=(peer, batch),
                device_id_type=MESH,
            )
            copy.start()
            copies.append(copy)
        target[me] = source[me]
        return copies

    flying = []

    def first():
        encode_all()
        flying.append(started(0, outgoing, arrived))

    def second():
        for copy in flying.pop():
            copy.wait()
        rates = decay_ref[pl.ds(pl.multiple_of(me * part, part), part), :]
        power = jnp.exp(-rates * step_count)
        power = jnp.concatenate([power] * seq_count, axis=0)
        state = jnp.zeros(power.shape, f32)
        for block in reversed(range(count)) if reverse else range(count):
            joined[block] = state.astype(bf16)
            state = power * state + arrived[block].astype(f32)
        flying.append(started(1, joined, final))

    def third():
        for copy in flying.pop():
            copy.wait()
        for group in range(count):
            rows = slice(group * part, (group + 1) * part)
            found = final[group].astype(f32)
            for seq in range(seq_count):
                carried_ref[seq, rows] = found[seq * part : (seq + 1) * part]

    return first, second, third


def carry_kernel(reverse, *refs):
    count = lax.axis_size("seq")
    me, batch = lax.axis_index("seq"), lax.axis_index("batch")
    barrier = pltpu.get_barrier_semaphore()
    for step in range(1, count):
        peer = (lax.rem(me + step, count), batch)
        pl.semaphore_signal(barrier, inc=1, device_id=peer, device_id_type=MESH)
    pl.semaphore_wait(barrier, count - 1)
    for piece in carry_pieces(reverse, *refs):
        piece()


work_starts = (0, 22, 40, 45, 51, 57, 63, 69, 75)


def state_back_work(
    input_ref,
    grad_ref,
    carried_ref,
    decay_ref,
    weight_ref,
    skip_ref,
    input_grad_ref,
    weight_grad_ref,
    power_grad_ref,
    skip_grad_ref,
    later_ref,
    ends,
    outgoing,
    arrived,
    joined,
    final,
    held,
    send,
    receive,
):
    carry = carry_pieces(True, grad_ref, decay_ref, later_ref, ends, outgoing, arrived, joined, final, send, receive)

    def tile_piece(tile):
        cut_at = slice(tile * lanes, (tile + 1) * lanes)
        wide = (input_ref, grad_ref, carried_ref, later_ref)
        flat = (decay_ref, weight_ref, skip_ref)
        results = (weight_grad_ref, power_grad_ref, skip_grad_ref)
        back_kernel(
            *(r.at[:, :, cut_at] for r in wide),
            *(r.at[:, cut_at] for r in flat),
            input_grad_ref.at[:, :, cut_at],
            *(r.at[:, cut_at] for r in results),
            held,
        )

    tiles = [functools.partial(tile_piece, tile) for tile in range(input_ref.shape[2] // lanes)]
    return list(carry) + tiles


def carried_by_kernel(value, decay, reverse, collective):
    seq_count, _, width = value.shape
    state_count = decay.shape[0]
    count = lax.axis_size("seq")
    parts = pltpu.VMEM((count, seq_count * state_count // count, width), bf16)
    return pl.pallas_call(
        functools.partial(carry_kernel, reverse),
        out_shape=shaped(seq_count, state_count, width),
        in_specs=[pl.BlockSpec(memory_space=pltpu.VMEM)] * 2,
        out_specs=pl.BlockSpec(memory_space=pltpu.VMEM),
        scratch_shapes=[pltpu.VMEM((seq_count, state_count, lanes), f32)]
        + [parts] * 4
        + [pltpu.SemaphoreType.DMA((2, count - 1)), pltpu.SemaphoreType.DMA((2, count - 1))],
        cost_estimate=pl.CostEstimate(flops=0, bytes_accessed=32 * value.size, transcendentals=0),
        compiler_params=pltpu.CompilerParams(collective_id=collective, has_side_effects=True),
    )(value, decay)


hidden_block = 768
gelu_scale = 0.7978845608
gelu_cubic = 0.044715


def feed_kernel(resid_ref, gain_ref, up_ref, down_ref, out_ref, normed_ref, hidden_ref, active_ref):
    @pl.when(pl.program_id(0) == 0)
    def _():
        resid = resid_ref[...]
        normed_ref[...] = layer_norm(resid, gain_ref[...]).astype(bf16)
        out_ref[...] = resid

    hidden = jnp.dot(normed_ref[...], up_ref[...], preferred_element_type=f32)
    hidden_ref[...] = hidden.astype(bf16)
    bend = jnp.tanh(gelu_scale * (hidden + gelu_cubic * hidden * hidden * hidden))
    active = (0.5 * hidden * (1.0 + bend)).astype(bf16)
    active_ref[...] = active
    out_ref[...] += jnp.dot(active, down_ref[...], preferred_element_type=f32)


def feed_forward_blocks(resid, gain, up_packed, up_at, down):
    rows, width = resid.shape
    inner = down.shape[0]
    first = up_at // hidden_block
    whole = pl.BlockSpec((rows, width), lambda j: (0, 0))
    part = pl.BlockSpec((rows, hidden_block), lambda j: (0, j))
    out, normed, hidden, active = pl.pallas_call(
        feed_kernel,
        grid=(inner // hidden_block,),
        in_specs=[
            whole,
            pl.BlockSpec((1, width), lambda j: (0, 0)),
            pl.BlockSpec((width, hidden_block), lambda j: (0, first + j)),
            pl.BlockSpec((hidden_block, width), lambda j: (j, 0)),
        ],
        out_specs=[whole, whole, part, part],
        out_shape=[
            shaped(rows, width),
            shaped(rows, width, dtype=bf16),
            shaped(rows, inner, dtype=bf16),
            shaped(rows, inner, dtype=bf16),
        ],
        cost_estimate=pl.CostEstimate(
            flops=4 * rows * width * inner, bytes_accessed=10 * width * inner, transcendentals=rows * inner
        ),
        compiler_params=pltpu.CompilerParams(vmem_limit_bytes=40 * 1024 * 1024),
    )(resid, gain[None], up_packed, down)
    return out, (resid, gain, normed, hidden, active)


def feed_back_kernel(
    packed,
    upstream_ref,
    resid_ref,
    gain_ref,
    normed_ref,
    hidden_ref,
    active_ref,
    up_ref,
    down_ref,
    out_ref,
    gain_grad_ref,
    *rest,
):
    step = pl.program_id(0)
    last = pl.num_programs(0) - 1
    across = (((1,), (1,)), ((), ()))
    along = (((0,), (0,)), ((), ()))
    upstream_low = upstream_ref[...].astype(bf16)
    into_active = lax.dot_general(upstream_low, down_ref[...], across, preferred_element_type=f32)
    hidden = hidden_ref[...].astype(f32)
    square = hidden * hidden
    bend = jnp.tanh(gelu_scale * hidden * (1.0 + gelu_cubic * square))
    slope = 0.5 * (1.0 + bend) + 0.5 * hidden * (1.0 - bend * bend) * (
        gelu_scale * (1.0 + 3.0 * gelu_cubic * square)
    )
    into_hidden = (into_active * slope).astype(bf16)
    part = lax.dot_general(into_hidden, up_ref[...], across, preferred_element_type=f32)

    @pl.when(step == 0)
    def _():
        out_ref[...] = part

    @pl.when(step > 0)
    def _():
        out_ref[...] += part

    up_grad = lax.dot_general(normed_ref[...], into_hidden, along, preferred_element_type=f32)
    down_grad = lax.dot_general(active_ref[...], upstream_low, along, preferred_element_type=f32)
    if packed:
        grads_ref, up_held, down_held, sems = rest
        share, fold = packed
        width = up_grad.shape[0]
        inner = hidden_block * grads_ref.shape[1] // (2 * hidden_block)
        tall = hidden_block // fold
        slot = lax.rem(step, 2)

        def copies(at, slot):
            columns = pl.ds(pl.multiple_of(at * hidden_block, hidden_block), hidden_block)
            rows = pl.ds(pl.multiple_of(at * tall, tall), tall)
            return (
                pltpu.make_async_copy(up_held.at[slot], grads_ref.at[:, columns], sems.at[0, slot]),
                pltpu.make_async_copy(down_held.at[slot], grads_ref.at[rows, inner:], sems.at[1, slot]),
            )

        @pl.when(step >= 2)
        def _():
            for copy in copies(step - 2, slot):
                copy.wait()

        up_held[slot] = up_grad.astype(bf16)
        for place in range(fold):
            starts = range(place * share, hidden_block, fold * share)
            piece = jnp.concatenate([down_grad[a : a + share] for a in starts], axis=0)
            down_held[slot, :, place * width : (place + 1) * width] = piece.astype(bf16)
        for copy in copies(step, slot):
            copy.start()

        @pl.when(step == last)
        def _():
            for copy in copies(step - 1, 1 - slot) + copies(step, slot):
                copy.wait()
    else:
        up_grad_ref, down_grad_ref = rest
        up_grad_ref[...] = up_grad.astype(bf16)
        down_grad_ref[...] = down_grad.astype(bf16)

    @pl.when(step == last)
    def _():
        into_normed = out_ref[...]
        resid = resid_ref[...]
        centred = resid - jnp.mean(resid, axis=-1, keepdims=True)
        inverse = lax.rsqrt(jnp.mean(centred * centred, axis=-1, keepdims=True) + eps)
        unit = centred * inverse
        gain_grad_ref[...] = jnp.sum(into_normed * unit, axis=0, keepdims=True)
        scaled = into_normed * gain_ref[...]
        along_unit = jnp.mean(scaled * unit, axis=-1, keepdims=True)
        into_resid = inverse * (scaled - jnp.mean(scaled, axis=-1, keepdims=True) - unit * along_unit)
        out_ref[...] = upstream_ref[...] + into_resid


def feed_back_blocks(stored, up_packed, up_at, down, upstream, packed=()):
    resid, gain, normed, hidden, active = stored
    rows, width = resid.shape
    inner = down.shape[0]
    first = up_at // hidden_block
    whole = pl.BlockSpec((rows, width), lambda j: (0, 0))
    part = pl.BlockSpec((rows, hidden_block), lambda j: (0, j))
    line = pl.BlockSpec((1, width), lambda j: (0, 0))
    up_spec = pl.BlockSpec((width, hidden_block), lambda j: (0, j))
    down_spec = pl.BlockSpec((hidden_block, width), lambda j: (j, 0))
    scratch = []
    if packed:
        grad_specs = [pl.BlockSpec(memory_space=pl.ANY)]
        grad_shapes = [shaped(width, 2 * inner, dtype=bf16)]
        scratch = [
            pltpu.VMEM((2, width, hidden_block), bf16),
            pltpu.VMEM((2, hidden_block // packed[1], inner), bf16),
            pltpu.SemaphoreType.DMA((2, 2)),
        ]
    else:
        grad_specs = [up_spec, down_spec]
        grad_shapes = [shaped(width, inner, dtype=bf16), shaped(inner, width, dtype=bf16)]
    out, gain_grad, *grads = pl.pallas_call(
        functools.partial(feed_back_kernel, packed),
        grid=(inner // hidden_block,),
        in_specs=[
            whole,
            whole,
            line,
            whole,
            part,
            part,
            pl.BlockSpec((width, hidden_block), lambda j: (0, first + j)),
            down_spec,
        ],
        out_specs=[whole, line] + grad_specs,
        out_shape=[shaped(rows, width), shaped(1, width)] + grad_shapes,
        scratch_shapes=scratch,
        cost_estimate=pl.CostEstimate(
            flops=8 * rows * width * inner, bytes_accessed=16 * width * inner, transcendentals=rows * inner
        ),
        compiler_params=pltpu.CompilerParams(vmem_limit_bytes=48 * 1024 * 1024),
    )(upstream, resid, gain[None], normed, hidden, active, up_packed, down)
    return (out, gain_grad[0], *grads)


def split_heads(ref, scratch, heads, parts, first=0):
    for part in range(parts):
        for head in range(heads):
            start = (part * heads + head) * HEAD_DIM + first
            scratch[part * heads + head] = ref[:, start : start + HEAD_DIM]


def score_block(query, keys, first, scale):
    scores = (
        lax.dot_general(query, keys, (((1,), (1,)), ((), ())), preferred_element_type=f32) * scale
    )
    rows = lax.broadcasted_iota(jnp.int32, scores.shape, 0) + first
    columns = lax.broadcasted_iota(jnp.int32, scores.shape, 1)
    return jnp.where(columns <= rows, scores, masked_score)


def attend_kernel(heads, block, scale, qkv_ref, low_ref, full_ref, stat_ref, parts, outs):
    length = qkv_ref.shape[0]
    split_heads(qkv_ref, parts, heads, 3)

    @pl.loop(0, heads)
    def _(head):
        for first in range(0, length, block):
            extent = first + block
            query = parts[head, first:extent, :]
            scores = score_block(query, parts[heads + head, :extent, :], first, scale)
            top = jnp.max(scores, axis=1, keepdims=True)
            soft = jnp.exp(scores - top)
            whole = jnp.sum(soft, axis=1, keepdims=True)
            soft = soft * (1.0 / whole)
            outs[head, first:extent, :] = jnp.dot(
                soft.astype(bf16), parts[2 * heads + head, :extent, :], preferred_element_type=f32
            )
            stat_ref[head, first:extent, :] = jnp.broadcast_to(top + jnp.log(whole), (block, lanes))

    if low_ref.shape[1] > heads * HEAD_DIM:
        low_ref[:, heads * HEAD_DIM :] = jnp.zeros((length, low_ref.shape[1] - heads * HEAD_DIM), bf16)
    for head in range(heads):
        place = slice(head * HEAD_DIM, (head + 1) * HEAD_DIM)
        full_ref[:, place] = outs[head]
        low_ref[:, place] = outs[head].astype(bf16)


def attend_back_kernel(
    heads, block, scale, qkv_ref, dout_ref, full_ref, stat_ref, grad_ref, parts, douts, fulls, grads
):
    length = qkv_ref.shape[0]
    split_heads(qkv_ref, parts, heads, 3)
    split_heads(dout_ref, douts, heads, 1)
    split_heads(full_ref, fulls, heads, 1)
    grads[...] = jnp.zeros_like(grads)

    @pl.loop(0, heads)
    def _(head):
        for first in range(0, length, block):
            extent = first + block
            query = parts[head, first:extent, :]
            keys = parts[heads + head, :extent, :]
            value = parts[2 * heads + head, :extent, :]
            dout = douts[head, first:extent, :]
            delta = jnp.sum(dout.astype(f32) * fulls[head, first:extent, :], axis=1, keepdims=True)
            scores = score_block(query, keys, first, scale)
            soft = jnp.exp(scores - stat_ref[head, first:extent, :1])
            across = (((1,), (1,)), ((), ()))
            along = (((0,), (0,)), ((), ()))
            dprob = lax.dot_general(dout, value, across, preferred_element_type=f32)
            dscore = (soft * (dprob - delta) * scale).astype(bf16)
            grads[head, first:extent, :] = jnp.dot(dscore, keys, preferred_element_type=f32)
            grads[heads + head, :extent, :] += lax.dot_general(
                dscore, query, along, preferred_element_type=f32
            )
            grads[2 * heads + head, :extent, :] += lax.dot_general(
                soft.astype(bf16), dout, along, preferred_element_type=f32
            )

    grad_ref[...] = jnp.zeros_like(grad_ref)
    for part in range(3 * heads):
        grad_ref[:, part * HEAD_DIM : (part + 1) * HEAD_DIM] = grads[part].astype(bf16)


def attend_params():
    return pltpu.CompilerParams(vmem_limit_bytes=56 * 1024 * 1024)


def attend_whole(qkv, heads, block):
    length = qkv.shape[0]
    width = heads * HEAD_DIM
    return pl.pallas_call(
        functools.partial(attend_kernel, heads, block, HEAD_DIM ** (-0.5)),
        out_shape=[
            shaped(length, -(-width // lanes) * lanes, dtype=bf16),
            shaped(length, width),
            shaped(heads, length, lanes),
        ],
        scratch_shapes=[
            pltpu.VMEM((3 * heads, length, HEAD_DIM), bf16),
            pltpu.VMEM((heads, length, HEAD_DIM), f32),
        ],
        compiler_params=attend_params(),
    )(qkv)


def attend_whole_back(qkv, dout, full, stat, heads, block):
    length = qkv.shape[0]
    return pl.pallas_call(
        functools.partial(attend_back_kernel, heads, block, HEAD_DIM ** (-0.5)),
        out_shape=shaped(*qkv.shape, dtype=bf16),
        scratch_shapes=[
            pltpu.VMEM((3 * heads, length, HEAD_DIM), bf16),
            pltpu.VMEM((heads, length, HEAD_DIM), bf16),
            pltpu.VMEM((heads, length, HEAD_DIM), f32),
            pltpu.VMEM((3 * heads, length, HEAD_DIM), f32),
        ],
        compiler_params=attend_params(),
    )(qkv, dout, full, stat)


def split_blocks(array, block_len):
    shaped_blocks = array.reshape(
        (array.shape[0], array.shape[1] // block_len, block_len) + array.shape[2:]
    )
    return jnp.moveaxis(shaped_blocks, 1, 0)


def general_attention(proj_low, seq_count, block_len, places, any_live, longest):
    model_width = HEADS * HEAD_DIM
    scale = HEAD_DIM ** (-0.5)
    offsets = jnp.arange(block_len, dtype=jnp.int32)
    head_shape = (seq_count, block_len, HEADS, HEAD_DIM)
    query_low = proj_low[:, :model_width].reshape(head_shape)
    keys_low = proj_low[:, model_width : 2 * model_width].reshape(head_shape)
    value_low = proj_low[:, 2 * model_width :].reshape(head_shape)

    def block_scores(queries, keys_block, query_places, key_places):
        scores = (
            jnp.einsum("sqhe,skhe->sqhk", queries, keys_block, preferred_element_type=jnp.float32)
            * scale
        )
        causal_mask = key_places[None, :] <= query_places[:, None]
        return jnp.where(causal_mask[None, :, None, :], scores, masked_score)

    def key_needed(key_first):
        return (key_first <= places[-1]) & ((key_first == places[0]) | any_live)

    stat_shape = (seq_count, block_len, HEADS)
    start_state = (
        jnp.full(stat_shape, masked_score, jnp.float32),
        jnp.zeros(stat_shape, jnp.float32),
        jnp.zeros(head_shape, jnp.float32),
    )
    shard_piece = (
        lax.all_gather(keys_low, "seq", axis=1, tiled=True),
        lax.all_gather(value_low, "seq", axis=1, tiled=True),
    )
    keys_blocks = split_blocks(shard_piece[0], block_len)
    value_blocks = split_blocks(shard_piece[1], block_len)
    firsts = jnp.arange(keys_blocks.shape[0], dtype=jnp.int32) * block_len

    def attend_one_step(state_now, operand):
        keys_block, value_block, key_first = operand

        def attend_work(state_in_block):
            running_max, running_sum, running_out = state_in_block
            scores = block_scores(query_low, keys_block, places, key_first + offsets)
            new_max = jnp.maximum(running_max, jnp.max(scores, axis=-1))
            fade = jnp.exp(running_max - new_max)
            shifted = jnp.exp(scores - new_max[..., None])
            new_sum = running_sum * fade + jnp.sum(shifted, axis=-1)
            new_out = running_out * fade[..., None] + jnp.einsum(
                "sqhk,skhe->sqhe",
                shifted.astype(jnp.bfloat16),
                value_block,
                preferred_element_type=jnp.float32,
            )
            return (new_max, new_sum, new_out)

        return (
            lax.cond(
                key_needed(key_first), attend_work, lambda state_in_block: state_in_block, state_now
            ),
            None,
        )

    result, _ = lax.scan(attend_one_step, start_state, (keys_blocks, value_blocks, firsts))
    running_max, running_sum, running_out = result
    attended = running_out / running_sum[..., None]
    logsum = running_max + jnp.log(running_sum)
    def backward(dout_low):
        delta = jnp.sum(dout_low.astype(jnp.float32) * attended, axis=-1)
        shard_piece = (
            lax.all_gather(keys_low, "seq", axis=1, tiled=True),
            lax.all_gather(value_low, "seq", axis=1, tiled=True),
        )
        keys_blocks = split_blocks(shard_piece[0], block_len)
        value_blocks = split_blocks(shard_piece[1], block_len)
        firsts = jnp.arange(keys_blocks.shape[0], dtype=jnp.int32) * block_len

        def query_one_step(query_grad, operand):
            keys_block, value_block, key_first = operand

            def query_work(grad_now):
                scores = block_scores(query_low, keys_block, places, key_first + offsets)
                soft = jnp.exp(scores - logsum[..., None])
                dprob = jnp.einsum(
                    "sqhe,skhe->sqhk", dout_low, value_block, preferred_element_type=jnp.float32
                )
                dscore = (soft * (dprob - delta[..., None])).astype(jnp.bfloat16)
                return (
                    grad_now
                    + jnp.einsum(
                        "sqhk,skhe->sqhe", dscore, keys_block, preferred_element_type=jnp.float32
                    )
                    * scale
                )

            return (
                lax.cond(key_needed(key_first), query_work, lambda grad_now: grad_now, query_grad),
                None,
            )

        result, _ = lax.scan(
            query_one_step, jnp.zeros(head_shape, jnp.float32), (keys_blocks, value_blocks, firsts)
        )
        query_grad = result
        sent = (query_low.astype(jnp.float32), dout_low.astype(jnp.float32), logsum, delta)
        shard_piece = (
            lax.all_gather(sent[0].astype(jnp.bfloat16), "seq", axis=1, tiled=True).astype(jnp.float32),
            lax.all_gather(sent[1].astype(jnp.bfloat16), "seq", axis=1, tiled=True).astype(jnp.float32),
            lax.all_gather(sent[2].astype(jnp.bfloat16), "seq", axis=1, tiled=True).astype(jnp.float32),
            lax.all_gather(sent[3].astype(jnp.bfloat16), "seq", axis=1, tiled=True).astype(jnp.float32),
        )
        query_blocks = split_blocks(shard_piece[0], block_len)
        dout_blocks = split_blocks(shard_piece[1], block_len)
        logsum_blocks = split_blocks(shard_piece[2], block_len)
        delta_blocks = split_blocks(shard_piece[3], block_len)
        firsts = jnp.arange(query_blocks.shape[0], dtype=jnp.int32) * block_len

        def key_one_step(grads_now, operand):
            query_block, dout_block, logsum_block, delta_block, query_first = operand

            def key_work(grads_in):
                keys_grad, value_grad = grads_in
                query_cast = query_block.astype(jnp.bfloat16)
                dout_cast = dout_block.astype(jnp.bfloat16)
                scores = block_scores(query_cast, keys_low, query_first + offsets, places)
                soft = jnp.exp(scores - logsum_block[..., None])
                value_grad = value_grad + jnp.einsum(
                    "sqhk,sqhe->skhe",
                    soft.astype(jnp.bfloat16),
                    dout_cast,
                    preferred_element_type=jnp.float32,
                )
                dprob = jnp.einsum(
                    "sqhe,skhe->sqhk", dout_cast, value_low, preferred_element_type=jnp.float32
                )
                dscore = (soft * (dprob - delta_block[..., None])).astype(jnp.bfloat16)
                keys_grad = (
                    keys_grad
                    + jnp.einsum(
                        "sqhk,sqhe->skhe", dscore, query_cast, preferred_element_type=jnp.float32
                    )
                    * scale
                )
                return (keys_grad, value_grad)

            needed = (query_first + block_len - 1 >= places[0]) & (
                (query_first == places[0]) | (query_first < longest)
            )
            return (lax.cond(needed, key_work, lambda grads_in: grads_in, grads_now), None)

        result, _ = lax.scan(
            key_one_step,
            (jnp.zeros(head_shape, jnp.float32), jnp.zeros(head_shape, jnp.float32)),
            (query_blocks, dout_blocks, logsum_blocks, delta_blocks, firsts),
        )
        keys_grad, value_grad = result
        return (query_grad, keys_grad, value_grad)

    return attended, backward


def layer_norm(value, gain):
    centred = value - jnp.mean(value, axis=-1, keepdims=True)
    spread_of = jnp.mean(centred * centred, axis=-1, keepdims=True)
    return centred * lax.rsqrt(spread_of + eps) * gain


def gelu_tanh(value):
    return jax.nn.gelu(value, approximate=True)


def dense(left, weight):
    return jnp.dot(left, weight, preferred_element_type=f32)


def dense_back(left, weight, upstream):
    into_left = lax.dot_general(
        upstream, weight, (((1,), (1,)), ((), ())), preferred_element_type=f32
    )
    into_weight = lax.dot_general(
        left, upstream, (((0,), (0,)), ((), ())), preferred_element_type=f32
    ).astype(bf16)
    return (into_left, into_weight)


def shift_mix(extended, taps, value_part):
    step_count = value_part.shape[1]
    reach = taps.shape[1]
    shifted = extended[:, reach - 1 : reach - 1 + step_count] * taps[:, 0]
    for tap_index in range(1, reach):
        shifted = (
            shifted
            + extended[:, reach - 1 - tap_index : reach - 1 - tap_index + step_count]
            * taps[:, tap_index]
        )
    return shifted * value_part


def feed_forward(resid, gain, up_weight, down_weight):
    normed, norm_back = jax.vjp(layer_norm, resid, gain)
    normed_low = normed.astype(bf16)
    hidden = dense(normed_low, up_weight)
    active, active_back = jax.vjp(gelu_tanh, hidden)
    active_low = active.astype(bf16)
    return (
        resid + dense(active_low, down_weight),
        (norm_back, normed_low, active_back, active_low),
    )


def feed_back(stored, up_weight, down_weight, upstream):
    norm_back, normed_low, active_back, active_low = stored
    into_active, down_grad = dense_back(active_low, down_weight, upstream.astype(bf16))
    (into_hidden,) = active_back(into_active)
    into_normed, up_grad = dense_back(normed_low, up_weight, into_hidden.astype(bf16))
    into_resid, gain_grad = norm_back(into_normed)
    return (upstream + into_resid, gain_grad, up_grad, down_grad)


def fold_rows(weight, share):
    rows, width = weight.shape
    fold = rows // share
    return weight.reshape(fold, share, width).transpose(1, 0, 2).reshape(share, fold * width)


def unfold_rows(folded, fold, share):
    rows, width = folded.shape
    width //= fold
    parts = folded.reshape(rows // share, share, fold, width).transpose(0, 2, 1, 3)
    return parts.reshape(rows * fold, width)


def fold_all(weight, share, rows):
    tall, width = weight.shape
    fold = tall // rows
    parts = weight.reshape(rows // share, fold, share, width).transpose(0, 2, 1, 3)
    return parts.reshape(rows, fold * width)


def group_columns(weight, groups, padded):
    rows, columns = weight.shape
    part = columns // 3 // groups
    grouped = weight.reshape(rows, 3, groups, part).transpose(0, 2, 1, 3).reshape(rows, groups, 3 * part)
    return jnp.pad(grouped, ((0, 0), (0, 0), (0, padded - 3 * part))).reshape(rows, groups * padded)


def pad_groups(weight, groups, padded):
    rows, columns = weight.shape
    part = rows // groups
    grouped = weight.reshape(groups, part, columns)
    return jnp.pad(grouped, ((0, 0), (0, padded - part), (0, 0))).reshape(groups * padded, columns)


def ungroup_columns(grouped, groups, padded, columns):
    rows = grouped.shape[0]
    part = columns // 3 // groups
    parts = grouped.reshape(rows, groups, padded)[:, :, : 3 * part].reshape(rows, groups, 3, part)
    return parts.transpose(0, 2, 1, 3).reshape(rows, columns)


def cut(array, widths):
    pieces, start = [], 0
    for width in widths:
        pieces.append(array[:, start : start + width])
        start += width
    return pieces


def cut_last(array, count):
    width = array.shape[-1] // count
    return [array[..., i * width : (i + 1) * width] for i in range(count)]


def gathered(parts):
    whole = lax.all_gather(jnp.concatenate(parts, axis=1), everyone, axis=0, tiled=True)
    return cut(whole, [p.shape[1] for p in parts])


def scattered(parts):
    mine = lax.psum_scatter(
        jnp.concatenate(parts, axis=1), everyone, scatter_dimension=0, tiled=True
    )
    return cut(mine, [p.shape[1] for p in parts])


def body(
    tokens,
    cotangent,
    lengths,
    mixer_gain,
    mixer_inputs,
    shift_taps,
    decay_rate,
    state_in,
    state_out,
    state_skip,
    mixer_output,
    first_gain,
    first_up,
    first_down,
    attend_gain,
    attend_inputs,
    attend_output,
    second_gain,
    second_up,
    second_down,
):
    seq_count, block_len, model_width = tokens.shape
    row_count = seq_count * block_len
    seq_devices = lax.axis_size("seq")
    share = mixer_inputs.shape[0]
    states, reach = decay_rate.shape[1], shift_taps.shape[1]
    fold = first_down.shape[0] // share
    deals = seq_count * HEADS
    dealt = deals % seq_devices == 0 and HEADS % (deals // seq_devices) == 0
    heads = deals // seq_devices if dealt else HEADS
    groups = HEADS // heads
    group_width = heads * HEAD_DIM
    padded = -(-3 * group_width // lanes) * lanes if dealt else 3 * group_width
    out_width = -(-group_width // lanes) * lanes if dealt else group_width

    columns = [decay_rate, state_in, state_out, shift_taps]
    columns += [g[:, None] for g in (mixer_gain, first_gain, attend_gain, second_gain, state_skip)]
    small = jnp.concatenate(columns, axis=1)
    small_count = small.shape[1]
    small_width = -(-small_count // lanes) * lanes
    small = jnp.pad(small, ((0, 0), (0, small_width - small_count)))
    attend_cols = attend_inputs.shape[1]
    grouped = group_columns(attend_inputs, groups, padded)
    by_kernel = seq_devices == 8 and lax.axis_size("batch") == 4
    packed = [mixer_output, attend_output, first_up, second_up, grouped]
    up1_at = 2 * model_width
    up2_at = up1_at + first_up.shape[1]
    if by_kernel:
        joint = jnp.concatenate([mixer_inputs, small], axis=1)
        w_packed = lax.all_gather(jnp.concatenate(packed, axis=1), everyone, axis=0, tiled=True)
        w_mixer_out, w_attend_out, _, _, w_attend_in = cut(w_packed, [p.shape[1] for p in packed])
        widths = (joint.shape[1], model_width)
        w_joint, w_down1 = gather_blocks((joint, first_down), chunked(widths, (4, 6), ("zxy", "zyx")), gap=3)
        w_mixer_in, w_small = cut(w_joint, [mixer_inputs.shape[1], small_width])
        second_down, w_small = lax.optimization_barrier((second_down, w_small))
        w_down2 = lax.all_gather(second_down, everyone, axis=0, tiled=True)
    else:
        w_mixer_in, w_small = gathered([mixer_inputs, small])
        packed += [fold_rows(first_down, share), fold_rows(second_down, share)]
        w_mixer_out, w_attend_out, w_up1, w_up2, w_attend_in, w_down1, w_down2 = gathered(packed)
        w_down1 = unfold_rows(w_down1, fold, share)
        w_down2 = unfold_rows(w_down2, fold, share)

    rows = w_small.T.astype(f32)
    decay, table_in, table_out = rows[:states], rows[states : 2 * states], rows[2 * states : 3 * states]
    taps_rows = rows[3 * states : 3 * states + reach]
    gain_mixer, gain_first, gain_attend, gain_second, skip = (
        rows[3 * states + reach + i] for i in range(5)
    )
    taps = taps_rows.T
    weight = table_in * table_out

    rank_seq = lax.axis_index("seq")
    offsets = jnp.arange(block_len, dtype=jnp.int32)
    places = rank_seq * block_len + offsets
    valid = (places[None, :] < lengths[:, None]).astype(f32)
    longest = jnp.max(lengths)
    any_live = places[0] < longest

    start_resid = tokens.reshape(row_count, model_width).astype(f32)
    normed_mixer, back_mixer = jax.vjp(layer_norm, start_resid, gain_mixer)
    normed_low_mixer = normed_mixer.astype(bf16)
    projected = dense(normed_low_mixer, w_mixer_in).reshape(seq_count, block_len, 3 * model_width)
    query_mixer = projected[:, :, :model_width]
    keys_mixer = projected[:, :, model_width : 2 * model_width]
    value_mixer = projected[:, :, 2 * model_width :]
    rim_rows = passed_along(keys_mixer[:, block_len - reach + 1 :], "seq", 1)
    extended = jnp.concatenate([rim_rows, keys_mixer], axis=1)
    inner, shift_back = jax.vjp(shift_mix, extended, taps, value_mixer)
    if by_kernel:
        carried = carried_by_kernel(inner, decay, False, 2)
    else:
        carried = carried_in(encode(inner, decay, False), decay, block_len, False)
    wide = shaped(seq_count, block_len, model_width)
    state_y, gated = per_lane_tile(
        output_kernel,
        (inner, query_mixer, carried, decay, weight, skip[None]),
        (wide, wide),
    )
    gated_low = gated.astype(bf16).reshape(row_count, model_width)
    resid_mixer = start_resid + dense(gated_low, w_mixer_out)
    if by_kernel:
        resid_first, stored_first = feed_forward_blocks(
            resid_mixer, gain_first, w_packed, up1_at, w_down1
        )
    else:
        resid_first, stored_first = feed_forward(resid_mixer, gain_first, w_up1, w_down1)

    normed_attend, back_attend = jax.vjp(layer_norm, resid_first, gain_attend)
    normed_low_attend = normed_attend.astype(bf16)
    proj_low = dense(normed_low_attend, w_attend_in).astype(bf16)
    if dealt:
        length = seq_devices * block_len
        block = min(256, length)

        def deal(array, width):
            array = array.reshape(seq_count, block_len, groups * width)
            parts = jnp.stack(cut_last(array, groups), axis=1)
            parts = parts.reshape(seq_count * groups, block_len, width)
            dealt_parts = lax.all_to_all(parts, "seq", split_axis=0, concat_axis=0, tiled=True)
            return dealt_parts.reshape(length, width)

        def collect(array, width):
            parts = array.reshape(seq_devices, block_len, width)
            back = lax.all_to_all(parts, "seq", split_axis=0, concat_axis=0, tiled=True)
            back = back.reshape(seq_count, groups, block_len, width)
            back = jnp.concatenate([back[:, group] for group in range(groups)], axis=-1)
            return back.reshape(row_count, groups * width)

        qkv = deal(proj_low, padded)
        attended_part, attended_full, stat = attend_whole(qkv, heads, block)
        attended_low = collect(attended_part, out_width)
        w_attend_out = pad_groups(w_attend_out, groups, out_width)
    else:
        attended, attended_back = general_attention(
            proj_low, seq_count, block_len, places, any_live, longest
        )
        attended_low = attended.reshape(row_count, model_width).astype(bf16)
    resid_attend = resid_first + dense(attended_low, w_attend_out)
    if by_kernel:
        final, stored_second = feed_forward_blocks(
            resid_attend, gain_second, w_packed, up2_at, w_down2
        )
    else:
        final, stored_second = feed_forward(resid_attend, gain_second, w_up2, w_down2)
    mixed = (final.reshape(seq_count, block_len, model_width) * valid[..., None]).astype(bf16)

    upstream = (cotangent.astype(f32) * valid[..., None]).reshape(row_count, model_width)
    if by_kernel:
        upstream, second_gain_grad, early = feed_back_blocks(
            stored_second, w_packed, up2_at, w_down2, upstream, packed=(share, fold)
        )
    else:
        upstream, second_gain_grad, second_up_grad, second_down_grad = feed_back(
            stored_second, w_up2, w_down2, upstream
        )
        early = [second_up_grad, fold_all(second_down_grad, share, model_width)]
        early = jnp.concatenate(early, axis=1)
    into_attended, attend_output_grad = dense_back(
        attended_low, w_attend_out, upstream.astype(bf16)
    )
    if dealt:
        attend_output_grad = attend_output_grad.reshape(groups, out_width, model_width)
        attend_output_grad = attend_output_grad[:, :group_width].reshape(model_width, model_width)
    dout_low = into_attended.astype(bf16)
    if dealt:
        dout = deal(dout_low, out_width)
        qkv_grad = attend_whole_back(qkv, dout, attended_full, stat, heads, block)
        qkv_grad, early = lax.optimization_barrier((qkv_grad, early))
        proj_grad = collect(qkv_grad, padded)
    else:
        parts = attended_back(dout_low.reshape(seq_count, block_len, HEADS, HEAD_DIM))
        proj_grad = jnp.concatenate(
            [p.reshape(row_count, model_width) for p in parts], axis=1
        ).astype(bf16)
    early = lax.psum_scatter(early, everyone, scatter_dimension=0, tiled=True)
    second_up_out, second_down_out = cut(early, [second_up.shape[1], fold * model_width])
    into_normed, attend_inputs_grad = dense_back(normed_low_attend, w_attend_in, proj_grad)
    into_resid, attend_gain_grad = back_attend(into_normed)
    upstream = upstream + into_resid
    if by_kernel:
        upstream, first_gain_grad, first_up_grad, first_down_grad = feed_back_blocks(
            stored_first, w_packed, up1_at, w_down1, upstream
        )
    else:
        upstream, first_gain_grad, first_up_grad, first_down_grad = feed_back(
            stored_first, w_up1, w_down1, upstream
        )
    into_gated, mixer_output_grad = dense_back(gated_low, w_mixer_out, upstream.astype(bf16))
    into_gated = into_gated.reshape(seq_count, block_len, model_width)
    query_mixer_grad = into_gated * state_y
    state_grad = into_gated * query_mixer
    table = shaped(states, model_width)
    gains_at = 3 * states + reach
    table_edges = [0, states, 2 * states, 3 * states, gains_at, small_width]

    def tables_of(block):
        return [block[:, a:b] for a, b in zip(table_edges, table_edges[1:])]

    orders = ("yxz", "xyz", "xzy", "yxz", "xyz", "yzx")
    if by_kernel:
        main = [attend_inputs_grad, first_up_grad, mixer_output_grad, first_down_grad, attend_output_grad]
        plan = chunked([g.shape[1] for g in main], (4, 4, 2, 4, 2), orders)
        part = attend_cols // 3 // groups

        def finish(index, block, results):
            if index > 0:
                results[index][...] = block[...]
                return
            for group in range(groups):
                for kind in range(3):
                    start = (kind * groups + group) * part
                    source = group * padded + kind * part
                    results[0][:, start : start + part] = block[:, source : source + part]

        results = [shaped(share, w) for w in (attend_cols, first_up.shape[1], model_width)]
        results += [shaped(share * fold, model_width), shaped(share, model_width)]
        parts = pltpu.VMEM((seq_devices, seq_count * states // seq_devices, model_width), bf16)
        exchange_sems = pltpu.SemaphoreType.DMA((2, seq_devices - 1))
        work = (
            state_back_work,
            (inner, state_grad, carried, decay, weight, skip[None]),
            (wide, table, table, shaped(1, model_width)),
            (
                pltpu.VMEM((seq_count, states, model_width), f32),
                pltpu.VMEM((seq_count, states, lanes), f32),
                parts,
                parts,
                parts,
                parts,
                pltpu.VMEM((block_len, seq_count, states, lanes), f32),
                exchange_sems,
                exchange_sems,
            ),
        )
        scattered_main = scatter_blocks(main, plan, finish, results, gap=4, work=work)
        attend_inputs_out, first_up_out, mixer_output_out, first_down_out, attend_output_out = scattered_main[:5]
        inner_grad, weight_grad, power_grad, skip_grad = scattered_main[5:]
    else:
        later = carried_in(encode(state_grad, decay, True), decay, block_len, True)
        inner_grad, weight_grad, power_grad, skip_grad = per_lane_tile(
            back_kernel,
            (inner, state_grad, carried, later, decay, weight, skip[None]),
            (wide, table, table, shaped(1, model_width)),
            scratch=[pltpu.VMEM((block_len, seq_count, states, lanes), f32)],
        )
    extended_grad, taps_grad, value_mixer_grad = shift_back(inner_grad)
    spill = passed_along(extended_grad[:, : reach - 1], "seq", -1)
    keys_mixer_grad = extended_grad[:, reach - 1 :] + jnp.pad(
        spill, ((0, 0), (block_len - reach + 1, 0), (0, 0))
    )
    proj_grad_mixer = (
        jnp.concatenate([query_mixer_grad, keys_mixer_grad, value_mixer_grad], axis=2)
        .astype(bf16)
        .reshape(row_count, 3 * model_width)
    )
    into_normed_mixer, mixer_inputs_grad = dense_back(normed_low_mixer, w_mixer_in, proj_grad_mixer)
    into_start, mixer_gain_grad = back_mixer(into_normed_mixer)
    tokens_gradient = (upstream + into_start).reshape(seq_count, block_len, model_width).astype(bf16)

    small_rows = jnp.concatenate(
        [-jnp.exp(-decay) * power_grad, weight_grad * table_out, weight_grad * table_in, taps_grad.T]
        + [
            g[None]
            for g in (mixer_gain_grad, first_gain_grad, attend_gain_grad, second_gain_grad, skip_grad[0])
        ],
        axis=0,
    )
    small_grad = jnp.pad(small_rows, ((0, small_width - small_count), (0, 0))).T.astype(bf16)
    def unfolded(folded):
        return folded.reshape(share, fold, model_width).transpose(1, 0, 2).reshape(share * fold, model_width)

    if by_kernel:
        plan = chunked((mixer_inputs_grad.shape[1], small_width), (4, 2), orders)

        def finish_small(index, block, results):
            for result, piece in zip(results[1:] if index else results[:1], tables_of(block) if index else [block]):
                result[...] = piece[...]

        results = [shaped(share, mixer_inputs_grad.shape[1])]
        results += [shaped(share, b - a) for a, b in zip(table_edges, table_edges[1:])]
        mixer_inputs_out, *tables = scatter_blocks(
            [mixer_inputs_grad, small_grad], plan, finish_small, results, gap=2, collective=4
        )
    else:
        last = [attend_inputs_grad, first_up_grad, mixer_output_grad, mixer_inputs_grad, small_grad]
        last += [fold_all(first_down_grad, share, model_width), attend_output_grad]
        *last, folded, attend_output_out = scattered(last)
        first_down_out = unfolded(folded).astype(f32)
        grouped, first_up_out, mixer_output_out, mixer_inputs_out, small_out = (
            g.astype(f32) for g in last
        )
        attend_inputs_out = ungroup_columns(grouped, groups, padded, attend_cols)
        tables = tables_of(small_out)
    decay_out, in_out, out_out, taps_out, vectors = tables

    return (
        mixed,
        tokens_gradient,
        vectors[:, 0],
        mixer_inputs_out,
        taps_out,
        decay_out,
        in_out,
        out_out,
        vectors[:, 4],
        mixer_output_out,
        vectors[:, 1],
        first_up_out,
        first_down_out,
        vectors[:, 2],
        attend_inputs_out,
        attend_output_out.astype(f32),
        vectors[:, 3],
        second_up_out.astype(f32),
        unfolded(second_down_out).astype(f32),
    )


def solution(mesh):
    return jax.shard_map(
        body,
        mesh=mesh,
        in_specs=(
            P("batch", "seq", None),
            P("batch", "seq", None),
            P("batch"),
            P(("seq", "batch")),
            P(("seq", "batch"), None),
            P(("seq", "batch"), None),
            P(("seq", "batch"), None),
            P(("seq", "batch"), None),
            P(("seq", "batch"), None),
            P(("seq", "batch")),
            P(("seq", "batch"), None),
            P(("seq", "batch")),
            P(("seq", "batch"), None),
            P(("seq", "batch"), None),
            P(("seq", "batch")),
            P(("seq", "batch"), None),
            P(("seq", "batch"), None),
            P(("seq", "batch")),
            P(("seq", "batch"), None),
            P(("seq", "batch"), None),
        ),
        out_specs=(
            P("batch", "seq", None),
            P("batch", "seq", None),
            P(("seq", "batch")),
            P(("seq", "batch"), None),
            P(("seq", "batch"), None),
            P(("seq", "batch"), None),
            P(("seq", "batch"), None),
            P(("seq", "batch"), None),
            P(("seq", "batch")),
            P(("seq", "batch"), None),
            P(("seq", "batch")),
            P(("seq", "batch"), None),
            P(("seq", "batch"), None),
            P(("seq", "batch")),
            P(("seq", "batch"), None),
            P(("seq", "batch"), None),
            P(("seq", "batch")),
            P(("seq", "batch"), None),
            P(("seq", "batch"), None),
        ),
        check_vma=False,
    )
```
